32 devices in a mesh: expert: 8 (over y, x, core), shard: 4 (over z).
Axes of the slice: x: 2, y: 2, z: 4, core: 2. Of those that a mesh axis runs over, the one named last changes fastest.
Arguments:
- hidden_in: bfloat16 [8192, 2048], P(('expert', 'shard')), may hold values from -6 to 6
- g_attn: bfloat16 [2048], P(('expert', 'shard')), may hold values from 0.5 to 1.5
- w_query: bfloat16 [2048, 4096], P(('expert', 'shard')), may hold values from -0.125 to 0.125
- w_key: bfloat16 [2048, 512], P(('expert', 'shard')), may hold values from -0.125 to 0.125
- w_value: bfloat16 [2048, 512], P(('expert', 'shard')), may hold values from -0.125 to 0.125
- g_query: bfloat16 [128], P(('expert', 'shard')), may hold values from 0.5 to 1.5
- g_key: bfloat16 [128], P(('expert', 'shard')), may hold values from 0.5 to 1.5
- w_out: bfloat16 [4096, 2048], P(('expert', 'shard')), may hold values from -1.5 to 1.5
- g_ffn: bfloat16 [2048], P(('expert', 'shard')), may hold values from 0.5 to 1.5
- w_router: bfloat16 [2048, 32], P(('expert', 'shard')), may hold values from -0.125 to 0.125
- w_gate: bfloat16 [32, 2048, 768], P(('expert', 'shard')), may hold values from -0.125 to 0.125
- w_up: bfloat16 [32, 2048, 768], P(('expert', 'shard')), may hold values from -0.125 to 0.125
- w_down: bfloat16 [32, 768, 2048], P(('expert', 'shard')), may hold values from -0.625 to 0.625
- routes: int32 [8192, 8], P(('expert', 'shard')), may hold values from 0 to 31, all different within a row; in each aligned block of 256 rows (0 to 255, 256 to 511, ...) at most 128 rows name the same one
- cotangent: bfloat16 [8192, 2048], P(('expert', 'shard')), may hold values from -6 to 6
Outputs:
- block_out: bfloat16 [8192, 2048], P(('expert', 'shard'))
- grad_input: bfloat16 [8192, 2048], P(('expert', 'shard'))
- grad_g_attn: float32 [2048], P(('expert', 'shard'))
- grad_w_query: float32 [2048, 4096], P(('expert', 'shard'))
- grad_w_key: float32 [2048, 512], P(('expert', 'shard'))
- grad_w_value: float32 [2048, 512], P(('expert', 'shard'))
- grad_g_query: float32 [128], P(('expert', 'shard'))
- grad_g_key: float32 [128], P(('expert', 'shard'))
- grad_w_out: float32 [4096, 2048], P(('expert', 'shard'))
- grad_g_ffn: float32 [2048], P(('expert', 'shard'))
- grad_router: float32 [2048, 32], P(('expert', 'shard'))
- grad_w_gate: float32 [32, 2048, 768], P(('expert', 'shard'))
- grad_w_up: float32 [32, 2048, 768], P(('expert', 'shard'))
- grad_w_down: float32 [32, 768, 2048], P(('expert', 'shard'))
The draws below stay inside these ranges and needn't reach their ends.
Inputs may be any that keep to these rules, and one draw needn't show every extreme that they name: `routes`: each row names 8 different experts; among the rows of one device no expert is named more than 128 times.
All inputs are finite; a program needn't handle non-finite values.
Results may differ from the reference program's by a relative error of at most 0.025.
Values may be sent and summed in bfloat16 or wider, within the bound.
A program may use at most 448 MiB of HBM per device.

```python
import math
from functools import partial
import jax
import jax.numpy as jnp
import numpy as np
from jax import lax

D = 2048
HQ = 32
HK = 4
HD = 128
FF = 768
TOP = 8
EXPERTS = 32
SEQ = 1024
ROWS = 256
NSEQ = 8
TOKENS = 8192
CAP = 128
N_EXPERT = 8
N_SHARD = 4


def level_of(key, dims, cuts, least, high):
    factor_of = 1.0
    for dim, parts in cuts:
        heights = jax.random.uniform(jax.random.fold_in(jax.random.fold_in(key, 6), dim), (parts,), jnp.float32, least / len(cuts), high / len(cuts))
        factor_of = factor_of * jnp.repeat(jnp.exp(heights), dims[dim] // parts).reshape((-1,) + (1,) * (len(dims) - 1 - dim))
    return factor_of


def deal_out(stream_key, own, number, rows, amount, top, reach, slope):
    order = jax.random.permutation(stream_key, amount)
    heavy_load, common = shares(amount, rows * top, reach, slope, True), shares(amount, rows * top, reach, slope, False)
    places = jnp.arange(amount)

    def named(lengths, rotation):
        used = int((lengths > 0).sum())
        fixed = max(1, used // 4)
        shifted = fixed + (places - fixed + rotation * (used - fixed)) % max(1, amount - fixed)
        return jnp.zeros((amount,), jnp.int32).at[order[jnp.where(places < fixed, places, shifted)]].set(jnp.asarray(lengths, jnp.int32))

    lengths = jnp.where(number % 4 == 0, named(heavy_load, number // 4), named(common, number - number // 4 - 1))
    mixed = jax.random.permutation(jax.random.fold_in(own, 3), amount)
    giver, taker = mixed[0:amount // 2 * 2:2], mixed[1:amount // 2 * 2:2]
    slack = jnp.minimum(lengths[giver] - 1, reach - lengths[taker]) // 2
    slack = jnp.where((giver == order[0]) | (taker == order[0]) | (lengths[taker] == 0), 0, jnp.maximum(slack, 0))
    shifted = jax.random.randint(jax.random.fold_in(own, 4), (amount // 2,), 0, 1 << 20) % (slack + 1)
    lengths = lengths.at[giver].add(-shifted).at[taker].add(shifted)
    labels = jnp.searchsorted(jnp.cumsum(lengths), jnp.arange(rows * top), side="right").astype(jnp.int32)
    table = labels.reshape(top, rows).T
    table = table[jax.random.permutation(jax.random.fold_in(own, 1), rows)]
    rotation = jax.random.randint(jax.random.fold_in(own, 2), (rows, 1), 0, top)
    return jnp.take_along_axis(table, (jnp.arange(top)[None, :] + rotation) % top, axis=1)


def shares(count, total, reach, slope, full):
    loads = [(1 << 20) // math.isqrt(rank ** slope) + 1 for rank in range(1, count + 1)]
    largest = reach if full else min(reach, max(-(-total // count), total * loads[0] // sum(loads)))
    least = 1 if total - largest >= count - 1 else 0
    given, rest = [largest] + [least] * (count - 1), total - largest - least * (count - 1)
    while rest > 0:
        movable = [i for i in range(1, count) if given[i] < largest] or [i for i in range(1, count) if given[i] < reach]
        whole, left = sum([loads[i] for i in movable]), rest
        for i in movable:
            extra = min(reach - given[i], max(1, left * loads[i] // whole), rest)
            given[i] = given[i] + extra
            rest = rest - extra
    return np.array(given)


def noise(own_key, shape, spread, reach, cuts=(), kind=jnp.bfloat16):
    array = spread * jax.random.normal(own_key, shape, jnp.float32)
    if cuts:
        array = array * level_of(own_key, shape, cuts, -0.22, 0.18)
    return jnp.clip(array, -reach, reach).astype(kind)


def setup_inputs(seed: int = 0) -> dict:
    splits = jax.random.split(jax.random.key(seed), 16)
    hidden_in = noise(splits[0], (TOKENS, D), 1.0, 6.0, ((0, 32),))
    g_attn = jnp.clip(1.0 + 0.1 * jax.random.normal(splits[1], (D,), jnp.float32), 0.5, 1.5).astype(jnp.bfloat16)
    w_query = noise(splits[2], (D, HQ * HD), D ** -0.5, 0.125, ((0, 32),))
    w_key = noise(splits[3], (D, HK * HD), D ** -0.5, 0.125, ((0, 32),))
    w_value = noise(splits[4], (D, HK * HD), D ** -0.5, 0.125, ((0, 32),))
    g_query = jnp.clip(1.0 + 0.1 * jax.random.normal(splits[5], (HD,), jnp.float32), 0.5, 1.5).astype(jnp.bfloat16)
    g_key = jnp.clip(1.0 + 0.1 * jax.random.normal(splits[6], (HD,), jnp.float32), 0.5, 1.5).astype(jnp.bfloat16)
    w_out = noise(splits[7], (HQ * HD, D), (HQ * HD // 256) ** -0.5, 1.5, ((0, 32),))
    g_ffn = jnp.clip(1.0 + 0.1 * jax.random.normal(splits[8], (D,), jnp.float32), 0.5, 1.5).astype(jnp.bfloat16)
    w_router = noise(splits[9], (D, EXPERTS), D ** -0.5, 0.125, ((0, 32),))
    w_gate = noise(splits[10], (EXPERTS, D, FF), D ** -0.5, 0.125, ((0, 32),))
    w_up = noise(splits[11], (EXPERTS, D, FF), D ** -0.5, 0.125, ((0, 32),))
    w_down = noise(splits[12], (EXPERTS, FF, D), (FF // 8) ** -0.5, 0.625, ((0, 32),))
    routes_keys = jax.random.split(jax.random.fold_in(splits[13], 1), TOKENS // ROWS)
    routes_turns = jax.random.permutation(jax.random.fold_in(splits[13], 3), TOKENS // ROWS)
    routes = jax.vmap(lambda own, number: deal_out(jax.random.fold_in(splits[13], 2), own, number, ROWS, EXPERTS, TOP, CAP, 1))(routes_keys, routes_turns).reshape((TOKENS, TOP))
    cotangent = noise(splits[14], (TOKENS, D), 1.0, 6.0, ((0, 32),))
    return dict(hidden_in=hidden_in, g_attn=g_attn, w_query=w_query, w_key=w_key, w_value=w_value, g_query=g_query, g_key=g_key, w_out=w_out, g_ffn=g_ffn, w_router=w_router, w_gate=w_gate, w_up=w_up, w_down=w_down, routes=routes, cotangent=cotangent)


epsilon = 1e-06
theta_base = 1000000.0

@jax.custom_vjp
def low(v):
    return lax.optimization_barrier(v.astype(jnp.bfloat16)).astype(jnp.float32)

@jax.custom_vjp
def low_back(v):
    return v

def low_keep(v):
    return (low(v), None)

def low_pass(kept, grad):
    return (grad,)

def back_keep(v):
    return (v, None)

def back_low(kept, grad):
    return (low(grad),)
low.defvjp(low_keep, low_pass)
low_back.defvjp(back_keep, back_low)

def matmul(left, right):
    return jnp.dot(left, right, precision=lax.Precision.HIGHEST, preferred_element_type=jnp.float32)

def norm_rows(values, gain_vec):
    return values * lax.rsqrt(lax.optimization_barrier(jnp.mean(values * values, axis=-1, keepdims=True)) + epsilon) * gain_vec

def rotary(values, positions):
    head_width = values.shape[-1]
    half_width = head_width // 2
    frequency = theta_base ** (-2.0 * jnp.arange(half_width, dtype=jnp.float32) / head_width)
    angles = positions.astype(jnp.float32)[:, None] * frequency[None, :]
    cosine = jnp.concatenate([jnp.cos(angles), jnp.cos(angles)], axis=-1)[:, None, :]
    sine_part = jnp.concatenate([jnp.sin(angles), jnp.sin(angles)], axis=-1)[:, None, :]
    turned = jnp.concatenate([-values[..., half_width:], values[..., :half_width]], axis=-1)
    return values * cosine + turned * sine_part

def head_prep(projected, gain_vec, positions, head_count, factor):
    shaped = projected.reshape(projected.shape[0], head_count, projected.shape[1] // head_count)
    return rotary(norm_rows(shaped, gain_vec), positions) * factor

def slot_tables(routes):
    device_count = N_EXPERT * N_SHARD
    flat_routes = routes.reshape(device_count, ROWS * TOP).astype(jnp.int32)
    hit_table = (flat_routes[:, :, None] == jnp.arange(EXPERTS, dtype=jnp.int32)[None, None, :]).astype(jnp.int32)
    earlier = (jnp.cumsum(hit_table, axis=1) - hit_table).astype(jnp.int32)
    slot_index = lax.optimization_barrier(jnp.sum(earlier * hit_table, axis=-1)).astype(jnp.int32)
    block_ids = jnp.arange(device_count, dtype=jnp.int32)[:, None]
    pair_place = (flat_routes * (device_count * CAP) + block_ids * CAP + slot_index).reshape(-1).astype(jnp.int32)
    pair_total = TOKENS * TOP
    slot_owner = jnp.full((EXPERTS * device_count * CAP,), pair_total, jnp.int32)
    slot_owner = slot_owner.at[pair_place].set(jnp.arange(pair_total, dtype=jnp.int32))
    token_of = jnp.where(slot_owner == pair_total, TOKENS, slot_owner // TOP).astype(jnp.int32)
    return (pair_place, token_of.reshape(EXPERTS, device_count * CAP))

def forward(routes, pair_place, token_of, hidden_in, g_attn, w_query, w_key, w_value, g_query, g_key, w_out, g_ffn, w_router, w_gate, w_up, w_down):
    group_size = HQ // HK
    positions = jnp.tile(jnp.arange(SEQ, dtype=jnp.int32), NSEQ)
    normed = low(norm_rows(hidden_in, g_attn))
    q_proj = low_back(matmul(normed, w_query))
    k_proj = low_back(matmul(normed, w_key))
    v_proj = low_back(matmul(normed, w_value))
    queries = low(head_prep(q_proj, g_query, positions, HQ, HD ** (-0.5)))
    keys = low(head_prep(k_proj, g_key, positions, HK, 1.0))
    values = low(v_proj)
    q_seq = queries.reshape(NSEQ, SEQ, HK, group_size, HD)
    k_seq = keys.reshape(NSEQ, SEQ, HK, HD)
    v_seq = values.reshape(NSEQ, SEQ, HK, HD)
    allowed = jnp.arange(SEQ)[None, :] <= jnp.arange(SEQ)[:, None]

    def attend(pieces):
        query_block, key_block, value_block = pieces
        scores = low_back(jnp.einsum('shgd,thd->hsgt', query_block, key_block, precision=lax.Precision.HIGHEST))
        raised = jnp.where(allowed[None, :, None, :], jnp.exp(scores), 0.0)
        probs_low = low(raised / lax.optimization_barrier(jnp.sum(raised, axis=-1, keepdims=True)))
        return jnp.einsum('hsgt,thd->shgd', probs_low, value_block, precision=lax.Precision.HIGHEST)
    mixed_heads = lax.map(jax.checkpoint(attend), (q_seq, k_seq, v_seq))
    mix = low(low_back(mixed_heads.reshape(TOKENS, HQ * HD)))
    attn_out = low_back(matmul(mix, w_out))
    residual = hidden_in + attn_out
    ffn_in = low(norm_rows(residual, g_ffn))
    logits = low_back(matmul(ffn_in, w_router))
    picked = jnp.take_along_axis(logits, routes, axis=1)
    raised_gate = jnp.exp(picked)
    gate_probs = raised_gate / lax.optimization_barrier(jnp.sum(raised_gate, axis=-1, keepdims=True))
    padded = jnp.concatenate([ffn_in, jnp.zeros((1, D), ffn_in.dtype)], axis=0)

    def expert(pieces):
        taken, gate_w, up_w, down_w = pieces
        expert_rows = low_back(jnp.take(padded, taken, axis=0))
        gate_act = low_back(matmul(expert_rows, gate_w))
        up_act = low_back(matmul(expert_rows, up_w))
        hidden = low(jax.nn.silu(gate_act) * up_act)
        return low_back(low(matmul(hidden, down_w)))
    expert_outs = lax.map(jax.checkpoint(expert), (token_of, w_gate, w_up, w_down))
    per_pair = jnp.take(expert_outs.reshape(-1, D), pair_place, axis=0).reshape(TOKENS, TOP, D)
    return residual + lax.optimization_barrier(jnp.sum(gate_probs[:, :, None] * per_pair, axis=1))

def reference(hidden_in, g_attn, w_query, w_key, w_value, g_query, g_key, w_out, g_ffn, w_router, w_gate, w_up, w_down, routes, cotangent):
    pair_place, token_of = slot_tables(routes)
    floats = tuple((array_in.astype(jnp.float32) for array_in in (hidden_in, g_attn, w_query, w_key, w_value, g_query, g_key, w_out, g_ffn, w_router, w_gate, w_up, w_down)))
    block_out, pull = jax.vjp(partial(forward, routes, pair_place, token_of), *floats)
    grads = pull(cotangent.astype(jnp.float32))
    return (block_out.astype(jnp.bfloat16), grads[0].astype(jnp.bfloat16), grads[1], grads[2], grads[3], grads[4], grads[5], grads[6], grads[7], grads[8], grads[9], grads[10], grads[11], grads[12])
```

```python
import functools

import jax
import jax.numpy as jnp
from jax import lax
from jax.experimental import pallas as pl
from jax.experimental.pallas import tpu as pltpu
from jax.sharding import PartitionSpec as P

MESH = pl.DeviceIdType.MESH
NZ = 4

def placed():
    return lax.axis_size("expert") == 8 and lax.axis_size("shard") == NZ

def place():
    e = lax.axis_index("expert"); s = lax.axis_index("shard")
    return e // 4, lax.rem(e // 2, 2), lax.rem(e, 2), s

def dev(y, x, c, s):
    return (y * 4 + x * 2 + c, s)

def barrier_all(y, x, c, s):
    bar = pltpu.get_barrier_semaphore()
    def sig(d): pl.semaphore_signal(bar, inc=1, device_id=d, device_id_type=MESH)
    sig(dev(1 - y, x, c, s)); sig(dev(y, 1 - x, c, s)); sig(dev(y, x, 1 - c, s))
    @pl.when(s > 0)
    def _(): sig(dev(y, x, c, s - 1))
    @pl.when(s < NZ - 1)
    def _(): sig(dev(y, x, c, s + 1))
    pl.semaphore_wait(bar, 3 + jnp.where(s > 0, 1, 0) + jnp.where(s < NZ - 1, 1, 0))

def ag_kernel(n_arr, *refs):
    ins = refs[:n_arr]; outs = refs[n_arr:2 * n_arr]
    loc_sem, zs, zr, ps, pr, cs, cr = refs[2 * n_arr:]
    y, x, c, s = place()
    barrier_all(y, x, c, s)
    def rc(src, dst, ss, rs, d):
        return pltpu.make_async_remote_copy(src_ref=src, dst_ref=dst, send_sem=ss, recv_sem=rs, device_id=d, device_id_type=MESH)
    X = dev(y, 1 - x, c, s); Y = dev(1 - y, x, c, s); C = dev(y, x, 1 - c, s)
    A = range(n_arr)
    steps = [(0, 0)] + [(d, g) for d in range(1, NZ) for g in (1, -1)]
    def valid(d, g):
        return (s >= d) if g == 1 else (s + d <= NZ - 1)
    def zof(d, g): return s - d * g
    def src_own(a, h, zz, k):
        return ins[a].at[h] if k == 0 else outs[a].at[y, x, c, zz, h]
    def zcopy(a, h, zz, k, g):
        kk = 1 + 2 * (k_dist(k)) + (0 if g == 1 else 1)
        return rc(src_own(a, h, zz, k), outs[a].at[y, x, c, zz, h], zs.at[a, h, kk], zr.at[a, h, kk], dev(y, x, c, s + g))
    def k_dist(k): return steps[k][0]
    def plane(a, h, zz, k, which):
        return rc(src_own(a, h, zz, k), outs[a].at[y, x, c, zz, h], ps.at[a, k, h, which], pr.at[a, k, h, which], X if which == 0 else Y)
    def plane_recv(a, h, zz, k, which):
        d = outs[a].at[y, 1 - x, c, zz, h] if which == 0 else outs[a].at[1 - y, x, c, zz, h]
        return rc(d, d, ps.at[a, k, h, which], pr.at[a, k, h, which], X if which == 0 else Y)
    def diag(a, h, zz, k):
        d = outs[a].at[y, 1 - x, c, zz, h] if h == 0 else outs[a].at[1 - y, x, c, zz, h]
        return rc(d, d, ps.at[a, k, h, 2], pr.at[a, k, h, 2], Y if h == 0 else X)
    def diag_recv(a, h, zz, k):
        d = outs[a].at[1 - y, 1 - x, c, zz, h]
        return rc(d, d, ps.at[a, k, h, 2], pr.at[a, k, h, 2], Y if h == 0 else X)
    def core(a, zz, k, part):
        d = outs[a].at[:, :, c, zz]
        return rc(d, d, cs.at[a, k], cr.at[a, k], C)
    def core_recv(a, zz, k):
        d = outs[a].at[:, :, 1 - c, zz]
        return rc(d, d, cs.at[a, k], cr.at[a, k], C)
    def loc(a):
        return pltpu.make_async_copy(ins[a], outs[a].at[y, x, c, s], loc_sem.at[a])

    def when(k, f):
        d, g = steps[k]
        if k == 0: f()
        else: pl.when(valid(d, g))(f)

    def stage_a(k):
        d, g = steps[k]
        def go():
            zz = zof(d, g)
            for a in A:
                for h in range(2):
                    if k:
                        kk = k
                        dref = outs[a].at[y, x, c, zz, h]
                        rc(dref, dref, zs.at[a, h, kk], zr.at[a, h, kk], X).wait_recv()
                    for gg in ((1, -1) if k == 0 else (g,)):
                        okc = (s < NZ - 1) if gg == 1 else (s > 0)
                        if d + 1 < NZ:
                            @pl.when(okc)
                            def _(): zcopy(a, h, zz, k, gg).start()
                    plane(a, h, zz, k, 0).start()
                    plane(a, h, zz, k, 1).start()
        when(k, go)
    def stage_b(k):
        d, g = steps[k]
        def go():
            zz = zof(d, g)
            for a in A:
                plane_recv(a, 0, zz, k, 0).wait_recv()
                diag(a, 0, zz, k).start()
                plane_recv(a, 1, zz, k, 1).wait_recv()
                diag(a, 1, zz, k).start()
        when(k, go)
    def stage_c(k):
        d, g = steps[k]
        def go():
            zz = zof(d, g)
            for a in A:
                if k == 0: loc(a).wait()
                plane_recv(a, 1, zz, k, 0).wait_recv()
                plane_recv(a, 0, zz, k, 1).wait_recv()
                diag_recv(a, 0, zz, k).wait_recv()
                diag_recv(a, 1, zz, k).wait_recv()
                core(a, zz, k, 0).start()
        when(k, go)
    for a in A: loc(a).start()
    n = len(steps)
    for i in range(n + 2):
        if i < n: stage_a(i)
        if 0 <= i - 1 < n: stage_b(i - 1)
        if 0 <= i - 2 < n: stage_c(i - 2)
    for k in range(n):
        d, g = steps[k]
        def go():
            zz = zof(d, g)
            for a in A:
                core_recv(a, zz, k).wait_recv()
                core(a, zz, k, 0).wait_send()
                for h in range(2):
                    for gg in ((1, -1) if k == 0 else (g,)):
                        okc = (s < NZ - 1) if gg == 1 else (s > 0)
                        if d + 1 < NZ:
                            @pl.when(okc)
                            def _(): zcopy(a, h, zz, k, gg).wait_send()
                    plane(a, h, zz, k, 0).wait_send()
                    plane(a, h, zz, k, 1).wait_send()
                    diag(a, h, zz, k).wait_send()
        when(k, go)

def ag32(arrs, cid):
    ins = [a.reshape(2, a.shape[0] // 2, a.shape[1]) for a in arrs]
    n = len(ins); nk = 7
    outs = pl.pallas_call(
        functools.partial(ag_kernel, n),
        out_shape=[jax.ShapeDtypeStruct((2, 2, 2, NZ) + a.shape, a.dtype) for a in ins],
        in_specs=[pl.BlockSpec(memory_space=pltpu.VMEM)] * n,
        out_specs=[pl.BlockSpec(memory_space=pl.ANY)] * n,
        scratch_shapes=[pltpu.SemaphoreType.DMA((n,)),
            pltpu.SemaphoreType.DMA((n, 2, 9)), pltpu.SemaphoreType.DMA((n, 2, 9)),
            pltpu.SemaphoreType.DMA((n, nk, 2, 3)), pltpu.SemaphoreType.DMA((n, nk, 2, 3)),
            pltpu.SemaphoreType.DMA((n, nk)), pltpu.SemaphoreType.DMA((n, nk))],
        compiler_params=pltpu.CompilerParams(collective_id=cid, has_side_effects=True, vmem_limit_bytes=8 << 20),
        name="gather_all",
    )(*ins)
    return [o.reshape(32, a.shape[0], a.shape[1]) for o, a in zip(outs, arrs)]

ZORDER = (0, 3, 1, 2)

def rs_kernel(n_arr, *refs):
    ins = refs[:n_arr]; outs = refs[n_arr:2 * n_arr]
    sc = refs[2 * n_arr:]
    own_b = sc[:n_arr]; r0_b = sc[n_arr:2 * n_arr]; ra_b = sc[2 * n_arr:3 * n_arr]; rb_b = sc[3 * n_arr:4 * n_arr]; zu_b = sc[4 * n_arr:5 * n_arr]; zd_b = sc[5 * n_arr:6 * n_arr]
    lsem, s0s, s0r, sas, sar, sbs, sbr, zus, zur, zds, zdr = sc[6 * n_arr:]
    y, x, c, s = place()
    barrier_all(y, x, c, s)
    X = dev(y, 1 - x, c, s); Y = dev(1 - y, x, c, s); C = dev(y, x, 1 - c, s)
    UP = dev(y, x, c, s + 1); DN = dev(y, x, c, s - 1)
    def rc(src, dst, ss, rs, d):
        return pltpu.make_async_remote_copy(src_ref=src, dst_ref=dst, send_sem=ss, recv_sem=rs, device_id=d, device_id_type=MESH)
    units = [(a, zz, h) for zz in ZORDER for a in range(n_arr) for h in range(2)]
    def jj(zz, h): return ZORDER.index(zz) * 2 + h
    def load(a, zz, h):
        j = jj(zz, h)
        return pltpu.make_async_copy(ins[a].at[:, :, c, zz, h], own_b[a].at[j], lsem.at[a, j])
    def c0(a, zz, h):
        j = jj(zz, h)
        return rc(ins[a].at[:, :, 1 - c, zz, h], r0_b[a].at[j], s0s.at[a, j], s0r.at[a, j], C)
    def ca(a, zz, h):
        j = jj(zz, h)
        if h == 0: return rc(own_b[a].at[j, :, 1 - x], ra_b[a].at[j], sas.at[a, j], sar.at[a, j], X)
        return rc(own_b[a].at[j, 1 - y], ra_b[a].at[j], sas.at[a, j], sar.at[a, j], Y)
    def cb(a, zz, h):
        j = jj(zz, h)
        if h == 0: return rc(own_b[a].at[j, 1 - y, x], rb_b[a].at[j], sbs.at[a, j], sbr.at[a, j], Y)
        return rc(own_b[a].at[j, y, 1 - x], rb_b[a].at[j], sbs.at[a, j], sbr.at[a, j], X)
    def cu(a, zz, h):
        j = jj(zz, h)
        return rc(own_b[a].at[j, y, x], zu_b[a].at[j], zus.at[a, j], zur.at[a, j], UP)
    def cd(a, zz, h):
        j = jj(zz, h)
        return rc(own_b[a].at[j, y, x], zd_b[a].at[j], zds.at[a, j], zdr.at[a, j], DN)
    def add_into(dst, other):
        rows = dst.shape[0]
        st = 16 if rows % 16 == 0 else rows
        @pl.loop(0, rows // st)
        def _(i):
            r = pl.ds(i * st, st)
            dst[r, :] = (dst[r, :].astype(jnp.float32) + other[r, :].astype(jnp.float32)).astype(dst.dtype)
    def stage0(u):
        a, zz, h = u; j = jj(zz, h)
        load(a, zz, h).wait()
        c0(a, zz, h).wait_recv()
        for yy in range(2):
            for xx in range(2):
                add_into(own_b[a].at[j, yy, xx], r0_b[a].at[j, yy, xx])
        ca(a, zz, h).start()
    def stage1(u):
        a, zz, h = u; j = jj(zz, h)
        ca(a, zz, h).wait_recv()
        for q in range(2):
            if h == 0: add_into(own_b[a].at[j, q, x], ra_b[a].at[j, q])
            else: add_into(own_b[a].at[j, y, q], ra_b[a].at[j, q])
        cb(a, zz, h).start()
    def zflow(u):
        a, zz, h = u; j = jj(zz, h)
        mine = own_b[a].at[j, y, x]
        if zz > 0:
            @pl.when(jnp.logical_and(s > 0, s <= zz))
            def _():
                cu(a, zz, h).wait_recv()
                add_into(mine, zu_b[a].at[j])
            @pl.when(s < zz)
            def _(): cu(a, zz, h).start()
        if zz < NZ - 1:
            @pl.when(jnp.logical_and(s < NZ - 1, s >= zz))
            def _():
                cd(a, zz, h).wait_recv()
                add_into(mine, zd_b[a].at[j])
            @pl.when(s > zz)
            def _(): cd(a, zz, h).start()
        @pl.when(s == zz)
        def _(): outs[a][h] = mine[...].astype(outs[a].dtype)
    def stage2(u):
        a, zz, h = u; j = jj(zz, h)
        cb(a, zz, h).wait_recv()
        add_into(own_b[a].at[j, y, x], rb_b[a].at[j])
    for u in units:
        c0(*u).start(); load(*u).start()
    n = len(units)
    L1, L2, L3 = 2, 4, 5
    for i in range(n + L3):
        if i < n: stage0(units[i])
        if 0 <= i - L1 < n: stage1(units[i - L1])
        if 0 <= i - L2 < n: stage2(units[i - L2])
        if 0 <= i - L3 < n: zflow(units[i - L3])
    for u in units:
        c0(*u).wait_send(); ca(*u).wait_send(); cb(*u).wait_send()
        zz = u[1]
        if zz > 0:
            @pl.when(s < zz)
            def _(): cu(*u).wait_send()
        if zz < NZ - 1:
            @pl.when(s > zz)
            def _(): cd(*u).wait_send()

def rs32(arrs, cid, out_dtype=jnp.float32):
    n = len(arrs)
    ins = [a.reshape(2, 2, 2, NZ, 2, a.shape[1] // 2, a.shape[2]) for a in arrs]
    hs = [i.shape[-2:] for i in ins]
    V = pltpu.VMEM; bt = jnp.bfloat16
    sems = [pltpu.SemaphoreType.DMA((n, 8))] * 11
    outs = pl.pallas_call(
        functools.partial(rs_kernel, n),
        out_shape=[jax.ShapeDtypeStruct((2,) + h, out_dtype) for h in hs],
        in_specs=[pl.BlockSpec(memory_space=pl.ANY)] * n,
        out_specs=[pl.BlockSpec(memory_space=pltpu.VMEM)] * n,
        scratch_shapes=[V((8, 2, 2) + h, bt) for h in hs] + [V((8, 2, 2) + h, bt) for h in hs] + [V((8, 2) + h, bt) for h in hs]
            + [V((8,) + h, bt) for h in hs] + [V((8,) + h, bt) for h in hs] + [V((8,) + h, bt) for h in hs] + sems,
        compiler_params=pltpu.CompilerParams(collective_id=cid, has_side_effects=True, vmem_limit_bytes=64000 * 1024),
        name="scatter_all",
    )(*ins)
    return [o.reshape(a.shape[1], a.shape[2]) for o, a in zip(outs, arrs)]

def line_gather_kernel(x_ref, o_ref, ss, rs):
    y, x, c, s = place()
    bar = pltpu.get_barrier_semaphore()
    for k in range(1, NZ):
        pl.semaphore_signal(bar, inc=1, device_id=dev(y, x, c, lax.rem(s + k, NZ)), device_id_type=MESH)
    pl.semaphore_wait(bar, NZ - 1)
    def cp(k):
        return pltpu.make_async_remote_copy(src_ref=x_ref, dst_ref=o_ref.at[s], send_sem=ss.at[k], recv_sem=rs.at[k],
            device_id=dev(y, x, c, lax.rem(s + k, NZ)), device_id_type=MESH)
    def back(k):
        t = lax.rem(s + NZ - k, NZ)
        return pltpu.make_async_remote_copy(src_ref=x_ref, dst_ref=o_ref.at[t], send_sem=ss.at[k], recv_sem=rs.at[k],
            device_id=dev(y, x, c, t), device_id_type=MESH)
    for k in (2, 1, 3): cp(k).start()
    o_ref[s] = x_ref[...]
    for k in range(1, NZ): back(k).wait_recv()
    for k in range(1, NZ): cp(k).wait_send()

def line_gather(x, cid):
    if not placed():
        return lax.all_gather(x, "shard", axis=0, tiled=True)
    sem = pltpu.SemaphoreType.DMA((NZ,))
    o = pl.pallas_call(line_gather_kernel, out_shape=jax.ShapeDtypeStruct((NZ,) + x.shape, x.dtype),
        in_specs=[pl.BlockSpec(memory_space=pltpu.VMEM)], out_specs=pl.BlockSpec(memory_space=pltpu.VMEM),
        scratch_shapes=[sem, sem], compiler_params=pltpu.CompilerParams(collective_id=cid, has_side_effects=True, vmem_limit_bytes=16 << 20),
        name="line_gather")(x)
    return o.reshape(NZ * x.shape[0], x.shape[1])

def line_scatter_kernel(p_ref, o_ref, buf, ss, rs):
    y, x, c, s = place()
    bar = pltpu.get_barrier_semaphore()
    for k in range(1, NZ):
        pl.semaphore_signal(bar, inc=1, device_id=dev(y, x, c, lax.rem(s + k, NZ)), device_id_type=MESH)
    pl.semaphore_wait(bar, NZ - 1)
    def cp(k):
        t = lax.rem(s + k, NZ)
        return pltpu.make_async_remote_copy(src_ref=p_ref.at[t], dst_ref=buf.at[k], send_sem=ss.at[k], recv_sem=rs.at[k],
            device_id=dev(y, x, c, t), device_id_type=MESH)
    for k in (2, 1, 3): cp(k).start()
    for k in (1, 3, 2): cp(k).wait_recv()
    st = 32
    @pl.loop(0, o_ref.shape[0] // st)
    def _(i):
        r = pl.ds(i * st, st)
        t = p_ref[s, r, :].astype(jnp.float32)
        for k in range(1, NZ): t = t + buf[k, r, :].astype(jnp.float32)
        o_ref[r, :] = t
    for k in range(1, NZ): cp(k).wait_send()

def line_scatter(p, cid):
    if not placed():
        return lax.psum_scatter(p, "shard", scatter_dimension=0, tiled=True).astype(jnp.float32)
    R, C = p.shape[0] // NZ, p.shape[1]
    sem = pltpu.SemaphoreType.DMA((NZ,))
    return pl.pallas_call(line_scatter_kernel, out_shape=jax.ShapeDtypeStruct((R, C), jnp.float32),
        in_specs=[pl.BlockSpec(memory_space=pltpu.VMEM)], out_specs=pl.BlockSpec(memory_space=pltpu.VMEM),
        scratch_shapes=[pltpu.VMEM((NZ, R, C), p.dtype), sem, sem], compiler_params=pltpu.CompilerParams(collective_id=cid, has_side_effects=True, vmem_limit_bytes=16 << 20),
        name="line_scatter")(p.reshape(NZ, R, C))


def dot(a, b, ca, cb):
    return lax.dot_general(a, b, (((ca,), (cb,)), ((), ())), preferred_element_type=jnp.float32)

def expert_kernel(experts, slots, SB, x_ref, cot_ref, wg_hbm, wu_hbm, wd_hbm, out_ref, gr_ref, dwg_hbm, dwu_hbm, dwd_hbm,
                  wg, wu, wd, dwg, dwu, dwd, rows, gp, wsem, osem):
    bf = jnp.bfloat16
    step = pl.program_id(0)
    nsub = x_ref.shape[0] // SB
    D = cot_ref.shape[1]
    WM = x_ref.shape[1] - D
    me = lax.axis_index(("expert", "shard"))
    loads = [pltpu.make_async_copy(h.at[0], v, wsem.at[i]) for i, (h, v) in enumerate(((wg_hbm, wg), (wu_hbm, wu), (wd_hbm, wd)))]
    @pl.when(step == 0)
    def _():
        for l in loads: l.start()
        for a in (dwg, dwu, dwd): a[...] = jnp.zeros_like(a)
    tri = (lax.broadcasted_iota(jnp.int32, (SB, SB), 1) < lax.broadcasted_iota(jnp.int32, (SB, SB), 0)).astype(bf)
    lane = lax.broadcasted_iota(jnp.int32, (SB, WM), 1)
    picks, gates = [], []
    for i in range(nsub):
        r = pl.ds(i * SB, SB)
        meta = x_ref[r, D:]
        cnt = dot(tri, meta, 1, 0)
        metaf = meta.astype(jnp.float32)
        msk = jnp.sum(jnp.where(lane == me, metaf, 0.0), axis=-1, keepdims=True)
        pos = jnp.sum(jnp.where(lane == me, cnt, 0.0), axis=-1, keepdims=True)
        gate = jnp.sum(jnp.where((lane == me + experts) | (lane == me + 2 * experts), metaf, 0.0), axis=-1, keepdims=True)
        want = jnp.where(msk > 0.0, pos, -1.0).astype(jnp.int32)
        pick = (want == lax.broadcasted_iota(jnp.int32, (SB, slots), 1)).astype(bf)
        picks.append(pick); gates.append(gate)
        rows[i * slots:(i + 1) * slots, :] = dot(pick, x_ref[r, :D], 0, 0).astype(bf)
        gcot = (gate * cot_ref[r, :].astype(jnp.float32)).astype(bf)
        gp[i * slots:(i + 1) * slots, :] = dot(pick, gcot, 0, 0).astype(bf)
    @pl.when(step == 0)
    def _():
        for l in loads: l.wait()
    ga = dot(rows[...], wg[...], 1, 0)
    ua = dot(rows[...], wu[...], 1, 0)
    sig = 1.0 / (1.0 + jnp.exp(-ga))
    act = ga * sig
    hid = (act * ua).astype(bf)
    eo = dot(hid, wd[...], 1, 0).astype(bf)
    gg = []
    for i in range(nsub):
        r = pl.ds(i * SB, SB)
        tok = dot(picks[i], eo[i * slots:(i + 1) * slots, :], 1, 0)
        out_ref[r, :] = (gates[i] * tok).astype(bf)
        gg.append(jnp.sum(tok * cot_ref[r, :].astype(jnp.float32), axis=-1, keepdims=True))
    gh = dot(gp[...], wd[...], 1, 1)
    dga = (gh * ua * (sig * (1.0 + ga * (1.0 - sig)))).astype(bf)
    dua = (gh * act).astype(bf)
    dwd[...] += dot(hid, gp[...], 0, 0)
    grow = (dot(dga, wg[...], 1, 1) + dot(dua, wu[...], 1, 1)).astype(bf)
    dwg[...] += dot(rows[...], dga, 0, 0)
    dwu[...] += dot(rows[...], dua, 0, 0)
    for i in range(nsub):
        r = pl.ds(i * SB, SB)
        gr_ref[r, :D] = dot(picks[i], grow[i * slots:(i + 1) * slots, :], 1, 0).astype(bf)
        hi = gg[i].astype(bf).astype(jnp.float32)
        lo = gg[i] - hi
        gr_ref[r, D:] = (jnp.where(lane == me, hi, 0.0) + jnp.where(lane == me + experts, lo, 0.0)).astype(bf)
    @pl.when(step == pl.num_programs(0) - 1)
    def _():
        outs = [pltpu.make_async_copy(v, h.at[0], osem.at[i]) for i, (v, h) in enumerate(((dwg, dwg_hbm), (dwu, dwu_hbm), (dwd, dwd_hbm)))]
        for o in outs: o.start()
        for o in outs: o.wait()

def experts_call(x_all, cot_all, w_gate, w_up, w_down, experts, block, capacity, TB=512, SB=256):
    T, C = x_all.shape; D = cot_all.shape[1]
    F = w_gate.shape[2]
    slots = max(SB // block, 1) * capacity
    total = TB // SB * slots
    any_ = pl.BlockSpec(memory_space=pl.ANY)
    V = pltpu.VMEM; bf = jnp.bfloat16; f32 = jnp.float32
    return pl.pallas_call(
        functools.partial(expert_kernel, experts, slots, SB),
        grid=(T // TB,),
        out_shape=[jax.ShapeDtypeStruct((T, D), bf), jax.ShapeDtypeStruct((T, C), bf), jax.ShapeDtypeStruct(w_gate.shape, f32), jax.ShapeDtypeStruct(w_up.shape, f32), jax.ShapeDtypeStruct(w_down.shape, f32)],
        in_specs=[pl.BlockSpec((TB, C), lambda i: (i, 0)), pl.BlockSpec((TB, D), lambda i: (i, 0)), any_, any_, any_],
        out_specs=[pl.BlockSpec((TB, D), lambda i: (i, 0)), pl.BlockSpec((TB, C), lambda i: (i, 0)), any_, any_, any_],
        scratch_shapes=[V((D, F), bf), V((D, F), bf), V((F, D), bf), V((D, F), f32), V((D, F), f32), V((F, D), f32), V((total, D), bf), V((total, D), bf), pltpu.SemaphoreType.DMA((3,)), pltpu.SemaphoreType.DMA((3,))],
        compiler_params=pltpu.CompilerParams(dimension_semantics=("arbitrary",), vmem_limit_bytes=65000 * 1024),
        cost_estimate=pl.CostEstimate(flops=133_000_000_000, bytes_accessed=160_000_000, transcendentals=0),
        name="experts",
    )(x_all, cot_all, w_gate, w_up, w_down)

HQ = 32
HK = 4
HD = 128
epsilon = 1e-06
theta_base = 1000000.0
BOTH = ("expert", "shard")


def matmul(left, right):
    return jnp.dot(left, right, preferred_element_type=jnp.float32)


def matmul_tn(left, right):
    return lax.dot_general(
        left, right, (((0,), (0,)), ((), ())), preferred_element_type=jnp.float32
    )


def matmul_nt(left, right):
    return lax.dot_general(
        left, right, (((1,), (1,)), ((), ())), preferred_element_type=jnp.float32
    )


def norm_rows(values, gain_vec):
    return (
        values * lax.rsqrt(jnp.mean(values * values, axis=-1, keepdims=True) + epsilon) * gain_vec
    )


def norm_back(values, gain_vec, upstream):
    scaling = lax.rsqrt(jnp.mean(values * values, axis=-1, keepdims=True) + epsilon)
    gain_grad = jnp.sum(upstream * values * scaling, axis=0)
    weighted = upstream * gain_vec
    inner_sum = jnp.mean(weighted * values, axis=-1, keepdims=True)
    return (scaling * weighted - values * (scaling * scaling * scaling) * inner_sum, gain_grad)


def rotary(values, positions):
    head_width = values.shape[-1]
    half_width = head_width // 2
    frequency = theta_base ** (-2.0 * jnp.arange(half_width, dtype=jnp.float32) / head_width)
    angles = positions.astype(jnp.float32)[:, None] * frequency[None, :]
    cosine = jnp.concatenate([jnp.cos(angles), jnp.cos(angles)], axis=-1)[:, None, :]
    sine_part = jnp.concatenate([jnp.sin(angles), jnp.sin(angles)], axis=-1)[:, None, :]
    turned = jnp.concatenate([-values[..., half_width:], values[..., :half_width]], axis=-1)
    return values * cosine + turned * sine_part


def head_prep(projected, gain_vec, positions, head_count, factor):
    shaped = projected.reshape(projected.shape[0], head_count, projected.shape[1] // head_count)
    return rotary(norm_rows(shaped, gain_vec), positions) * factor


def head_forward(query_block, key_block, value_block, allowed):
    scores = jnp.einsum("rgd,sd->rgs", query_block, key_block, preferred_element_type=jnp.float32)
    raised = jnp.where(allowed[:, None, :], jnp.exp(scores), 0.0)
    totals = jnp.sum(raised, axis=-1)
    probs_low = (raised / totals[..., None]).astype(jnp.bfloat16)
    return (
        jnp.einsum("rgs,sd->rgd", probs_low, value_block, preferred_element_type=jnp.float32),
        totals,
    )


def head_backward(query_block, key_block, value_block, totals, upstream, allowed):
    scores = jnp.einsum("rgd,sd->rgs", query_block, key_block, preferred_element_type=jnp.float32)
    raised = jnp.where(allowed[:, None, :], jnp.exp(scores), 0.0)
    probs_f = raised / totals[..., None]
    probs_low = probs_f.astype(jnp.bfloat16)
    grad_probs = jnp.einsum(
        "rgd,sd->rgs", upstream, value_block, preferred_element_type=jnp.float32
    )
    inner_sum = jnp.sum(probs_f * grad_probs, axis=-1, keepdims=True)
    grad_scores = (probs_f * (grad_probs - inner_sum)).astype(jnp.bfloat16)
    grad_query = jnp.einsum(
        "rgs,sd->rgd", grad_scores, key_block, preferred_element_type=jnp.float32
    )
    grad_key = jnp.einsum(
        "rgs,rgd->sd", grad_scores, query_block, preferred_element_type=jnp.float32
    )
    grad_value = jnp.einsum("rgs,rgd->sd", probs_low, upstream, preferred_element_type=jnp.float32)
    return (grad_query, grad_key, grad_value)


def gather_all(arrays, cid):
    if placed():
        return [o.reshape(-1, o.shape[-1]) for o in ag32(arrays, cid)]
    return [lax.all_gather(a, BOTH, axis=0, tiled=True) for a in arrays]


def scatter_all(arrays, cid, out_dtype=jnp.float32):
    if placed():
        return rs32([a.reshape(32, -1, a.shape[-1]) for a in arrays], cid, out_dtype)
    return [lax.psum_scatter(a, BOTH, scatter_dimension=0, tiled=True).astype(out_dtype) for a in arrays]


def per_device(
    hidden_in,
    g_attn,
    w_query,
    w_key,
    w_value,
    g_query,
    g_key,
    w_out,
    g_ffn,
    w_router,
    w_gate,
    w_up,
    w_down,
    routes,
    cotangent,
):
    bf, f32 = jnp.bfloat16, jnp.float32
    tok_rows, model_width = hidden_in.shape
    top_count = routes.shape[1]
    devices = lax.axis_size(BOTH)
    expert_count = devices * w_gate.shape[0]
    capacity = 2 * tok_rows * top_count // expert_count
    shard_count = lax.axis_size("shard")
    shard_pos = lax.axis_index("shard")
    seq_len = tok_rows * shard_count
    group_size = HQ // HK
    factor = HD ** (-0.5)
    q_cols, kv_cols = HQ * HD, HK * HD

    pieces = [w_router.reshape(-1), g_attn, g_ffn, g_query, g_key]
    sizes = [p.shape[0] for p in pieces]
    used = sum(sizes)
    small_rows = -(-used // (32 * 128)) * 32
    small = jnp.concatenate(pieces + [jnp.zeros((small_rows * 128 - used,), bf)]).reshape(small_rows, 128)
    wqkv = jnp.concatenate([w_query, w_key, w_value], axis=1)
    wqkv_full, small_all = gather_all([wqkv, small], 1)
    small_all = small_all.reshape(devices, small_rows * 128)
    starts = [sum(sizes[:i]) for i in range(5)]
    wr_full, attn_gain, ffn_gain, query_gain, key_gain = [small_all[:, o : o + n].reshape(-1) for o, n in zip(starts, sizes)]
    wr_full = wr_full.reshape(model_width, expert_count)
    attn_gain, ffn_gain, query_gain, key_gain = [g.astype(f32) for g in (attn_gain, ffn_gain, query_gain, key_gain)]
    wo_full = lax.all_gather(w_out, BOTH, axis=0, tiled=True)
    cot_all = lax.all_gather(cotangent, BOTH, axis=0, tiled=True)

    positions = shard_pos * tok_rows + jnp.arange(tok_rows, dtype=jnp.int32)
    inputs_f = hidden_in.astype(f32)
    normed_low = norm_rows(inputs_f, attn_gain).astype(bf)
    qkv = matmul(normed_low, wqkv_full)
    q_proj, k_proj, v_proj = qkv[:, :q_cols], qkv[:, q_cols : q_cols + kv_cols], qkv[:, q_cols + kv_cols :]
    k_rot, k_pull = jax.vjp(
        lambda projected, gain_vec: head_prep(projected, gain_vec, positions, HK, 1.0),
        k_proj,
        key_gain,
    )
    q_rot, q_pull = jax.vjp(
        lambda projected, gain_vec: head_prep(projected, gain_vec, positions, HQ, factor),
        q_proj,
        query_gain,
    )
    q_low = q_rot.astype(bf)
    kv_low = jnp.concatenate([k_rot.reshape(tok_rows, kv_cols).astype(bf), v_proj.astype(bf)], axis=1)
    allowed = jnp.arange(seq_len, dtype=jnp.int32)[None, :] <= positions[:, None]
    kv_all = line_gather(kv_low, 2)
    q_heads = q_low.reshape(tok_rows, HK, group_size, HD).transpose(1, 0, 2, 3)
    k_heads = kv_all[:, :kv_cols].reshape(seq_len, HK, HD).transpose(1, 0, 2)
    v_heads = kv_all[:, kv_cols:].reshape(seq_len, HK, HD).transpose(1, 0, 2)

    def attend(pieces):
        return head_forward(pieces[0], pieces[1], pieces[2], allowed)

    head_outs, totals = lax.map(attend, (q_heads, k_heads, v_heads))
    mix_low = head_outs.transpose(1, 0, 2, 3).reshape(tok_rows, q_cols).astype(bf)
    residual = inputs_f + matmul(mix_low, wo_full)
    ffn_low = norm_rows(residual, ffn_gain).astype(bf)

    logits = matmul(ffn_low, wr_full)
    expert_ids = jnp.arange(expert_count, dtype=jnp.int32)
    chosen = jnp.any(routes[:, :, None] == expert_ids[None, None, :], axis=1)
    raised_gate = jnp.where(chosen, jnp.exp(logits), 0.0)
    gates = raised_gate / jnp.sum(raised_gate, axis=-1, keepdims=True)
    gate_high = lax.reduce_precision(gates, 8, 7)
    gate_low = gates - gate_high
    extra = -(-3 * expert_count // 128) * 128
    payload = jnp.concatenate(
        [
            ffn_low,
            chosen.astype(bf),
            gate_high.astype(bf),
            gate_low.astype(bf),
            jnp.zeros((tok_rows, extra - 3 * expert_count), bf),
        ],
        axis=1,
    )
    (payload_all,) = gather_all([payload], 3)
    out_part, grad_part, grad_wgate, grad_wup, grad_wdown = experts_call(
        payload_all, cot_all, w_gate, w_up, w_down, expert_count, tok_rows, capacity
    )
    (grad_sum,) = scatter_all([grad_part], 4)
    (moe_out,) = scatter_all([out_part], 5)
    block_out = (residual + moe_out).astype(bf)
    upstream = cotangent.astype(f32)
    grad_ffn = grad_sum[:, :model_width]
    grad_gates = (
        grad_sum[:, model_width : model_width + expert_count]
        + grad_sum[:, model_width + expert_count : model_width + 2 * expert_count]
    )
    grad_logits = (gates * (grad_gates - jnp.sum(gates * grad_gates, axis=-1, keepdims=True))).astype(bf)
    grad_wrouter = matmul_tn(ffn_low, grad_logits)
    grad_ffn = grad_ffn + matmul_nt(grad_logits, wr_full)
    grad_second, grad_ffn_gain = norm_back(residual, ffn_gain, grad_ffn)
    grad_residual = upstream + grad_second
    grad_attn_low = grad_residual.astype(bf)
    grad_wout = matmul_tn(mix_low, grad_attn_low).astype(bf)
    grad_mix = matmul_nt(grad_attn_low, wo_full).astype(bf)
    grad_heads = grad_mix.reshape(tok_rows, HK, group_size, HD).transpose(1, 0, 2, 3)

    def attend_back(pieces):
        return head_backward(pieces[0], pieces[1], pieces[2], pieces[3], pieces[4], allowed)

    grad_qheads, grad_kheads, grad_vheads = lax.map(
        attend_back, (q_heads, k_heads, v_heads, totals, grad_heads)
    )
    grad_q_rot = grad_qheads.transpose(1, 0, 2, 3).reshape(tok_rows, HQ, HD)
    grad_kv = jnp.concatenate(
        [
            grad_kheads.transpose(1, 0, 2).reshape(seq_len, kv_cols).astype(bf),
            grad_vheads.transpose(1, 0, 2).reshape(seq_len, kv_cols).astype(bf),
        ],
        axis=1,
    )
    grad_kv = line_scatter(grad_kv, 6)
    grad_q_proj, grad_query_gain = q_pull(grad_q_rot)
    grad_k_proj, grad_key_gain = k_pull(grad_kv[:, :kv_cols].reshape(tok_rows, HK, HD))
    grad_qkv_low = jnp.concatenate(
        [grad_q_proj.astype(bf), grad_k_proj.astype(bf), grad_kv[:, kv_cols:].astype(bf)], axis=1
    )
    grad_wqkv = matmul_tn(normed_low, grad_qkv_low).astype(bf)
    grad_normed = matmul_nt(grad_qkv_low, wqkv_full)
    grad_front, grad_attn_gain = norm_back(inputs_f, attn_gain, grad_normed)
    grad_input = (grad_residual + grad_front).astype(bf)

    grads = [grad_wrouter, grad_attn_gain, grad_ffn_gain, grad_query_gain, grad_key_gain]
    packed = jnp.concatenate(
        [g.astype(bf).reshape(devices, -1) for g in grads] + [jnp.zeros((devices, small_rows * 128 - used), bf)], axis=1
    ).reshape(devices * small_rows, 128)
    (out_grad,) = scatter_all([grad_wout], 7)
    qkv_grad, small_grad = scatter_all([grad_wqkv, packed], 8)
    small_grad = small_grad.reshape(-1)
    router_g, attn_g, ffn_g, query_g, key_g = [small_grad[o : o + n] for o, n in zip(starts, sizes)]
    return (
        block_out,
        grad_input,
        attn_g,
        qkv_grad[:, :q_cols],
        qkv_grad[:, q_cols : q_cols + kv_cols],
        qkv_grad[:, q_cols + kv_cols :],
        query_g,
        key_g,
        out_grad,
        ffn_g,
        router_g.reshape(w_router.shape),
        grad_wgate,
        grad_wup,
        grad_wdown,
    )


def solution(mesh):
    row = P(BOTH, None)
    vec = P(BOTH)
    cube = P(BOTH, None, None)
    in_specs = (row, vec, row, row, row, vec, vec, row, vec, row, cube, cube, cube, row, row)
    out_specs = (row, row, vec, row, row, row, vec, vec, row, vec, row, cube, cube, cube)
    return jax.shard_map(
        per_device, mesh=mesh, in_specs=in_specs, out_specs=out_specs, check_vma=False
    )
```

```python
import functools

import jax
import jax.numpy as jnp
from jax import lax
from jax.experimental import pallas as pl
from jax.experimental.pallas import tpu as pltpu
from jax.sharding import PartitionSpec as P

MESH = pl.DeviceIdType.MESH
NZ = 4

def placed():
    return lax.axis_size("expert") == 8 and lax.axis_size("shard") == NZ

def place():
    e = lax.axis_index("expert"); s = lax.axis_index("shard")
    return e // 4, lax.rem(e // 2, 2), lax.rem(e, 2), s

def dev(y, x, c, s):
    return (y * 4 + x * 2 + c, s)

def barrier_all(y, x, c, s):
    bar = pltpu.get_barrier_semaphore()
    def sig(d): pl.semaphore_signal(bar, inc=1, device_id=d, device_id_type=MESH)
    sig(dev(1 - y, x, c, s)); sig(dev(y, 1 - x, c, s)); sig(dev(y, x, 1 - c, s))
    @pl.when(s > 0)
    def _(): sig(dev(y, x, c, s - 1))
    @pl.when(s < NZ - 1)
    def _(): sig(dev(y, x, c, s + 1))
    pl.semaphore_wait(bar, 3 + jnp.where(s > 0, 1, 0) + jnp.where(s < NZ - 1, 1, 0))

def ag_kernel(n_arr, *refs):
    ins = refs[:n_arr]; outs = refs[n_arr:2 * n_arr]
    loc_sem, zs, zr, ps, pr, cs, cr = refs[2 * n_arr:]
    y, x, c, s = place()
    barrier_all(y, x, c, s)
    def rc(src, dst, ss, rs, d):
        return pltpu.make_async_remote_copy(src_ref=src, dst_ref=dst, send_sem=ss, recv_sem=rs, device_id=d, device_id_type=MESH)
    X = dev(y, 1 - x, c, s); Y = dev(1 - y, x, c, s); C = dev(y, x, 1 - c, s)
    A = range(n_arr)
    steps = [(0, 0)] + [(d, g) for d in range(1, NZ) for g in (1, -1)]
    def valid(d, g):
        return (s >= d) if g == 1 else (s + d <= NZ - 1)
    def zof(d, g): return s - d * g
    def src_own(a, h, zz, k):
        return ins[a].at[h] if k == 0 else outs[a].at[y, x, c, zz, h]
    def zcopy(a, h, zz, k, g):
        kk = 1 + 2 * (k_dist(k)) + (0 if g == 1 else 1)
        return rc(src_own(a, h, zz, k), outs[a].at[y, x, c, zz, h], zs.at[a, h, kk], zr.at[a, h, kk], dev(y, x, c, s + g))
    def k_dist(k): return steps[k][0]
    def plane(a, h, zz, k, which):
        return rc(src_own(a, h, zz, k), outs[a].at[y, x, c, zz, h], ps.at[a, k, h, which], pr.at[a, k, h, which], X if which == 0 else Y)
    def plane_recv(a, h, zz, k, which):
        d = outs[a].at[y, 1 - x, c, zz, h] if which == 0 else outs[a].at[1 - y, x, c, zz, h]
        return rc(d, d, ps.at[a, k, h, which], pr.at[a, k, h, which], X if which == 0 else Y)
    def diag(a, h, zz, k):
        d = outs[a].at[y, 1 - x, c, zz, h] if h == 0 else outs[a].at[1 - y, x, c, zz, h]
        return rc(d, d, ps.at[a, k, h, 2], pr.at[a, k, h, 2], Y if h == 0 else X)
    def diag_recv(a, h, zz, k):
        d = outs[a].at[1 - y, 1 - x, c, zz, h]
        return rc(d, d, ps.at[a, k, h, 2], pr.at[a, k, h, 2], Y if h == 0 else X)
    def core(a, zz, k, part):
        d = outs[a].at[:, :, c, zz]
        return rc(d, d, cs.at[a, k], cr.at[a, k], C)
    def core_recv(a, zz, k):
        d = outs[a].at[:, :, 1 - c, zz]
        return rc(d, d, cs.at[a, k], cr.at[a, k], C)
    def loc(a):
        return pltpu.make_async_copy(ins[a], outs[a].at[y, x, c, s], loc_sem.at[a])

    def when(k, f):
        d, g = steps[k]
        if k == 0: f()
        else: pl.when(valid(d, g))(f)

    def stage_a(k):
        d, g = steps[k]
        def go():
            zz = zof(d, g)
            for a in A:
                for h in range(2):
                    if k:
                        kk = k
                        dref = outs[a].at[y, x, c, zz, h]
                        rc(dref, dref, zs.at[a, h, kk], zr.at[a, h, kk], X).wait_recv()
                    for gg in ((1, -1) if k == 0 else (g,)):
                        okc = (s < NZ - 1) if gg == 1 else (s > 0)
                        if d + 1 < NZ:
                            @pl.when(okc)
                            def _(): zcopy(a, h, zz, k, gg).start()
                    plane(a, h, zz, k, 0).start()
                    plane(a, h, zz, k, 1).start()
        when(k, go)
    def stage_b(k):
        d, g = steps[k]
        def go():
            zz = zof(d, g)
            for a in A:
                plane_recv(a, 0, zz, k, 0).wait_recv()
                diag(a, 0, zz, k).start()
                plane_recv(a, 1, zz, k, 1).wait_recv()
                diag(a, 1, zz, k).start()
        when(k, go)
    def stage_c(k):
        d, g = steps[k]
        def go():
            zz = zof(d, g)
            for a in A:
                if k == 0: loc(a).wait()
                plane_recv(a, 1, zz, k, 0).wait_recv()
                plane_recv(a, 0, zz, k, 1).wait_recv()
                diag_recv(a, 0, zz, k).wait_recv()
                diag_recv(a, 1, zz, k).wait_recv()
                core(a, zz, k, 0).start()
        when(k, go)
    for a in A: loc(a).start()
    n = len(steps)
    for i in range(n + 2):
        if i < n: stage_a(i)
        if 0 <= i - 1 < n: stage_b(i - 1)
        if 0 <= i - 2 < n: stage_c(i - 2)
    for k in range(n):
        d, g = steps[k]
        def go():
            zz = zof(d, g)
            for a in A:
                core_recv(a, zz, k).wait_recv()
                core(a, zz, k, 0).wait_send()
                for h in range(2):
                    for gg in ((1, -1) if k == 0 else (g,)):
                        okc = (s < NZ - 1) if gg == 1 else (s > 0)
                        if d + 1 < NZ:
                            @pl.when(okc)
                            def _(): zcopy(a, h, zz, k, gg).wait_send()
                    plane(a, h, zz, k, 0).wait_send()
                    plane(a, h, zz, k, 1).wait_send()
                    diag(a, h, zz, k).wait_send()
        when(k, go)

def ag32(arrs, cid):
    ins = [a.reshape(2, a.shape[0] // 2, a.shape[1]) for a in arrs]
    n = len(ins); nk = 7
    outs = pl.pallas_call(
        functools.partial(ag_kernel, n),
        out_shape=[jax.ShapeDtypeStruct((2, 2, 2, NZ) + a.shape, a.dtype) for a in ins],
        in_specs=[pl.BlockSpec(memory_space=pltpu.VMEM)] * n,
        out_specs=[pl.BlockSpec(memory_space=pl.ANY)] * n,
        scratch_shapes=[pltpu.SemaphoreType.DMA((n,)),
            pltpu.SemaphoreType.DMA((n, 2, 9)), pltpu.SemaphoreType.DMA((n, 2, 9)),
            pltpu.SemaphoreType.DMA((n, nk, 2, 3)), pltpu.SemaphoreType.DMA((n, nk, 2, 3)),
            pltpu.SemaphoreType.DMA((n, nk)), pltpu.SemaphoreType.DMA((n, nk))],
        compiler_params=pltpu.CompilerParams(collective_id=cid, has_side_effects=True, vmem_limit_bytes=64000 * 1024),
        name="gather_all",
    )(*ins)
    return [o.reshape(32, a.shape[0], a.shape[1]) for o, a in zip(outs, arrs)]

ZORDER = (0, 3, 1, 2)
LAGS = (1, 1, 1, 1)

def rs_kernel(n_arr, parts, *refs):
    ins = refs[:n_arr]; outs = refs[n_arr:2 * n_arr]
    sc = refs[2 * n_arr:]
    own_b, r0_b, ra_b, rb_b, zu_b, zd_b = [sc[i * n_arr:(i + 1) * n_arr] for i in range(6)]
    lsem, s0s, s0r, sas, sar, sbs, sbr, zus, zur, zds, zdr = sc[6 * n_arr:]
    y, x, c, s = place()
    barrier_all(y, x, c, s)
    X = dev(y, 1 - x, c, s); Y = dev(1 - y, x, c, s); C = dev(y, x, 1 - c, s)
    UP = dev(y, x, c, s + 1); DN = dev(y, x, c, s - 1)
    def rc(src, dst, ss, rs, d):
        return pltpu.make_async_remote_copy(src_ref=src, dst_ref=dst, send_sem=ss, recv_sem=rs, device_id=d, device_id_type=MESH)
    units = [(a, zz, h) for zz in ZORDER for h in range(parts) for a in range(n_arr)]
    def jj(zz, h): return ZORDER.index(zz) * parts + h
    def load(a, zz, h):
        j = jj(zz, h)
        return pltpu.make_async_copy(ins[a].at[:, :, c, zz, h], own_b[a].at[j], lsem.at[a, j])
    def c0(a, zz, h):
        j = jj(zz, h)
        return rc(ins[a].at[:, :, 1 - c, zz, h], r0_b[a].at[j], s0s.at[a, j], s0r.at[a, j], C)
    def ca(a, zz, h):
        j = jj(zz, h)
        if h % 2 == 0: return rc(own_b[a].at[j, :, 1 - x], ra_b[a].at[j], sas.at[a, j], sar.at[a, j], X)
        return rc(own_b[a].at[j, 1 - y], ra_b[a].at[j], sas.at[a, j], sar.at[a, j], Y)
    def cb(a, zz, h):
        j = jj(zz, h)
        if h % 2 == 0: return rc(own_b[a].at[j, 1 - y, x], rb_b[a].at[j], sbs.at[a, j], sbr.at[a, j], Y)
        return rc(own_b[a].at[j, y, 1 - x], rb_b[a].at[j], sbs.at[a, j], sbr.at[a, j], X)
    def cu(a, zz, h):
        j = jj(zz, h)
        return rc(own_b[a].at[j, y, x], zu_b[a].at[j], zus.at[a, j], zur.at[a, j], UP)
    def cd(a, zz, h):
        j = jj(zz, h)
        return rc(own_b[a].at[j, y, x], zd_b[a].at[j], zds.at[a, j], zdr.at[a, j], DN)
    def add_into(dst, other):
        rows = dst.shape[0]
        st = 16 if rows % 16 == 0 else rows
        @pl.loop(0, rows // st)
        def _(i):
            r = pl.ds(i * st, st)
            dst[r, :] = (dst[r, :].astype(jnp.float32) + other[r, :].astype(jnp.float32)).astype(dst.dtype)
    def stage0(u):
        a, zz, h = u; j = jj(zz, h)
        load(a, zz, h).wait()
        c0(a, zz, h).wait_recv()
        for yy in range(2):
            for xx in range(2):
                add_into(own_b[a].at[j, yy, xx], r0_b[a].at[j, yy, xx])
        ca(a, zz, h).start()
    def stage1(u):
        a, zz, h = u; j = jj(zz, h)
        ca(a, zz, h).wait_recv()
        for q in range(2):
            if h % 2 == 0: add_into(own_b[a].at[j, q, x], ra_b[a].at[j, q])
            else: add_into(own_b[a].at[j, y, q], ra_b[a].at[j, q])
        cb(a, zz, h).start()
    def stage2(u):
        a, zz, h = u; j = jj(zz, h)
        cb(a, zz, h).wait_recv()
        add_into(own_b[a].at[j, y, x], rb_b[a].at[j])
    def hop(u, k):
        a, zz, h = u; j = jj(zz, h)
        if k < zz:
            @pl.when(s == k)
            def _():
                if k > 0:
                    cu(a, zz, h).wait_recv()
                    add_into(own_b[a].at[j, y, x], zu_b[a].at[j])
                cu(a, zz, h).start()
        t = NZ - 1 - k
        if t > zz:
            @pl.when(s == t)
            def _():
                if k > 0:
                    cd(a, zz, h).wait_recv()
                    add_into(own_b[a].at[j, y, x], zd_b[a].at[j])
                cd(a, zz, h).start()
    def last(u):
        a, zz, h = u; j = jj(zz, h)
        @pl.when(s == zz)
        def _():
            if zz > 0: cu(a, zz, h).wait_recv()
            if zz < NZ - 1: cd(a, zz, h).wait_recv()
            t = own_b[a][j, y, x].astype(jnp.float32)
            if zz > 0: t = t + zu_b[a][j].astype(jnp.float32)
            if zz < NZ - 1: t = t + zd_b[a][j].astype(jnp.float32)
            outs[a][h] = t.astype(outs[a].dtype)
    for u in units:
        c0(*u).start(); load(*u).start()
    n = len(units)
    L1 = LAGS[0] * n_arr; L2 = L1 + LAGS[1] * n_arr; L3 = L2 + LAGS[2] * n_arr; dl = LAGS[3] * n_arr
    for i in range(n + L3 + (NZ - 1) * dl):
        if i < n: stage0(units[i])
        if 0 <= i - L1 < n: stage1(units[i - L1])
        if 0 <= i - L2 < n: stage2(units[i - L2])
        for k in range(NZ - 1):
            if 0 <= i - L3 - k * dl < n: hop(units[i - L3 - k * dl], k)
    for u in units: last(u)
    for u in units:
        c0(*u).wait_send(); ca(*u).wait_send(); cb(*u).wait_send()
        zz = u[1]
        if zz > 0:
            @pl.when(s < zz)
            def _(): cu(*u).wait_send()
        if zz < NZ - 1:
            @pl.when(s > zz)
            def _(): cd(*u).wait_send()

def rs32(arrs, cid, out_dtype=jnp.float32, parts=4):
    n = len(arrs)
    if any(a.shape[1] % (parts * 16) for a in arrs): parts = 2
    ins = [a.reshape(2, 2, 2, NZ, parts, a.shape[1] // parts, a.shape[2]) for a in arrs]
    hs = [i.shape[-2:] for i in ins]
    V = pltpu.VMEM; bt = jnp.bfloat16; m = NZ * parts
    sems = [pltpu.SemaphoreType.DMA((n, m))] * 11
    outs = pl.pallas_call(
        functools.partial(rs_kernel, n, parts),
        out_shape=[jax.ShapeDtypeStruct((parts,) + h, out_dtype) for h in hs],
        in_specs=[pl.BlockSpec(memory_space=pl.ANY)] * n,
        out_specs=[pl.BlockSpec(memory_space=pltpu.VMEM)] * n,
        scratch_shapes=[V((m, 2, 2) + h, bt) for h in hs] + [V((m, 2, 2) + h, bt) for h in hs] + [V((m, 2) + h, bt) for h in hs]
            + [V((m,) + h, bt) for h in hs] + [V((m,) + h, bt) for h in hs] + [V((m,) + h, bt) for h in hs] + sems,
        compiler_params=pltpu.CompilerParams(collective_id=cid, has_side_effects=True, vmem_limit_bytes=64000 * 1024),
        name="scatter_all",
    )(*ins)
    return [o.reshape(a.shape[1], a.shape[2]) for o, a in zip(outs, arrs)]

def line_barrier(y, x, c, s):
    bar = pltpu.get_barrier_semaphore()
    @pl.when(s > 0)
    def _(): pl.semaphore_signal(bar, inc=1, device_id=dev(y, x, c, s - 1), device_id_type=MESH)
    @pl.when(s < NZ - 1)
    def _(): pl.semaphore_signal(bar, inc=1, device_id=dev(y, x, c, s + 1), device_id_type=MESH)
    pl.semaphore_wait(bar, jnp.where(s > 0, 1, 0) + jnp.where(s < NZ - 1, 1, 0))

def line_gather_kernel(parts, x_ref, o_ref, ss, rs):
    y, x, c, s = place()
    line_barrier(y, x, c, s)
    def cp(d, g, h):
        src = x_ref.at[h] if d == 0 else o_ref.at[s - d * g, h]
        k = 0 if g == 1 else 1
        return pltpu.make_async_remote_copy(src_ref=src, dst_ref=o_ref.at[s - d * g, h], send_sem=ss.at[k, d, h], recv_sem=rs.at[k, d, h],
            device_id=dev(y, x, c, s + g), device_id_type=MESH)
    def arrived(d, g, h):
        k = 0 if g == 1 else 1
        ref = o_ref.at[s - (d + 1) * g, h]
        return pltpu.make_async_remote_copy(src_ref=ref, dst_ref=ref, send_sem=ss.at[k, d, h], recv_sem=rs.at[k, d, h],
            device_id=dev(y, x, c, s + g), device_id_type=MESH)
    def sends(d, g): return (s >= d) & (s < NZ - 1) if g == 1 else (s + d <= NZ - 1) & (s > 0)
    def gets(d, g): return s >= d + 1 if g == 1 else s + d + 1 <= NZ - 1
    for d in range(NZ):
        for h in range(parts):
            for g in (1, -1):
                if d:
                    @pl.when(gets(d - 1, g))
                    def _(): arrived(d - 1, g, h).wait_recv()
                if d < NZ - 1:
                    @pl.when(sends(d, g))
                    def _(): cp(d, g, h).start()
        if d == 0: o_ref[s] = x_ref[...]
    for d in range(NZ - 1):
        for h in range(parts):
            for g in (1, -1):
                @pl.when(sends(d, g))
                def _(): cp(d, g, h).wait_send()

def line_gather(x, cid, parts=4):
    if not placed():
        return lax.all_gather(x, "shard", axis=0, tiled=True)
    R, C = x.shape
    sem = pltpu.SemaphoreType.DMA((2, NZ, parts))
    o = pl.pallas_call(functools.partial(line_gather_kernel, parts), out_shape=jax.ShapeDtypeStruct((NZ, parts, R // parts, C), x.dtype),
        in_specs=[pl.BlockSpec(memory_space=pltpu.VMEM)], out_specs=pl.BlockSpec(memory_space=pltpu.VMEM),
        scratch_shapes=[sem, sem], compiler_params=pltpu.CompilerParams(collective_id=cid, has_side_effects=True, vmem_limit_bytes=16 << 20),
        name="line_gather")(x.reshape(parts, R // parts, C))
    return o.reshape(NZ * R, C)

def line_scatter_kernel(parts, p_ref, o_ref, acc, zu, zd, ss_u, rs_u, ss_d, rs_d):
    y, x, c, s = place()
    line_barrier(y, x, c, s)
    def rc(src, dst, a, b, d):
        return pltpu.make_async_remote_copy(src_ref=src, dst_ref=dst, send_sem=a, recv_sem=b, device_id=d, device_id_type=MESH)
    def cu(zz, h, k):
        src = p_ref.at[zz, h] if k == 0 else acc.at[zz, h]
        return rc(src, zu.at[zz, h], ss_u.at[zz, h], rs_u.at[zz, h], dev(y, x, c, s + 1))
    def cd(zz, h, k):
        src = p_ref.at[zz, h] if k == 0 else acc.at[zz, h]
        return rc(src, zd.at[zz, h], ss_d.at[zz, h], rs_d.at[zz, h], dev(y, x, c, s - 1))
    st = 32
    def total(dst, refs):
        @pl.loop(0, dst.shape[0] // st)
        def _(i):
            r = pl.ds(i * st, st)
            t = refs[0][r, :].astype(jnp.float32)
            for f in refs[1:]: t = t + f[r, :].astype(jnp.float32)
            dst[r, :] = t.astype(dst.dtype)
    ups = [(zz, h) for zz in (3, 2, 1) for h in range(parts)]
    dns = [(zz, h) for zz in (0, 1, 2) for h in range(parts)]
    n = len(ups)
    for i in range(n + NZ):
        for k in range(NZ - 1):
            if 0 <= i - k < n:
                zz, h = ups[i - k]
                if k < zz:
                    @pl.when(s == k)
                    def _():
                        if k:
                            cu(zz, h, k).wait_recv()
                            total(acc.at[zz, h], [p_ref.at[zz, h], zu.at[zz, h]])
                        cu(zz, h, k).start()
                zz, h = dns[i - k]
                if NZ - 1 - k > zz:
                    @pl.when(s == NZ - 1 - k)
                    def _():
                        if k:
                            cd(zz, h, k).wait_recv()
                            total(acc.at[zz, h], [p_ref.at[zz, h], zd.at[zz, h]])
                        cd(zz, h, k).start()
    for zz in range(NZ):
        @pl.when(s == zz)
        def _():
            for h in range(parts):
                refs = [p_ref.at[zz, h]]
                if zz > 0:
                    cu(zz, h, 1).wait_recv()
                    refs.append(zu.at[zz, h])
                if zz < NZ - 1:
                    cd(zz, h, 1).wait_recv()
                    refs.append(zd.at[zz, h])
                total(o_ref.at[h], refs)
    for zz, h in ups:
        @pl.when(s < zz)
        def _(): cu(zz, h, 1).wait_send()
    for zz, h in dns:
        @pl.when(s > zz)
        def _(): cd(zz, h, 1).wait_send()

def line_scatter(p, cid, parts=4):
    if not placed():
        return lax.psum_scatter(p, "shard", scatter_dimension=0, tiled=True).astype(jnp.float32)
    R, C = p.shape[0] // NZ, p.shape[1]
    sem = pltpu.SemaphoreType.DMA((NZ, parts))
    shape = (NZ, parts, R // parts, C)
    buf = pltpu.VMEM(shape, p.dtype)
    o = pl.pallas_call(functools.partial(line_scatter_kernel, parts), out_shape=jax.ShapeDtypeStruct(shape[1:], jnp.float32),
        in_specs=[pl.BlockSpec(memory_space=pltpu.VMEM)], out_specs=pl.BlockSpec(memory_space=pltpu.VMEM),
        scratch_shapes=[buf, buf, buf, sem, sem, sem, sem], compiler_params=pltpu.CompilerParams(collective_id=cid, has_side_effects=True, vmem_limit_bytes=24 << 20),
        name="line_scatter")(p.reshape(shape))
    return o.reshape(R, C)


def dot(a, b, ca, cb):
    return lax.dot_general(a, b, (((ca,), (cb,)), ((), ())), preferred_element_type=jnp.float32)

def expert_kernel(experts, slots, SB, x_ref, cot_ref, wg_hbm, wu_hbm, wd_hbm, out_ref, gr_ref, dwg_hbm, dwu_hbm, dwd_hbm,
                  wg, wu, wd, dwg, dwu, dwd, rows, gp, wsem, osem):
    bf = jnp.bfloat16
    step = pl.program_id(0)
    nsub = x_ref.shape[0] // SB
    D = cot_ref.shape[1]
    WM = x_ref.shape[1] - D
    me = lax.axis_index(("expert", "shard"))
    loads = [pltpu.make_async_copy(h.at[0], v, wsem.at[i]) for i, (h, v) in enumerate(((wg_hbm, wg), (wu_hbm, wu), (wd_hbm, wd)))]
    @pl.when(step == 0)
    def _():
        for l in loads: l.start()
        for a in (dwg, dwu, dwd): a[...] = jnp.zeros_like(a)
    tri = (lax.broadcasted_iota(jnp.int32, (SB, SB), 1) < lax.broadcasted_iota(jnp.int32, (SB, SB), 0)).astype(bf)
    lane = lax.broadcasted_iota(jnp.int32, (SB, WM), 1)
    picks, gates = [], []
    for i in range(nsub):
        r = pl.ds(i * SB, SB)
        meta = x_ref[r, D:]
        cnt = dot(tri, meta, 1, 0)
        metaf = meta.astype(jnp.float32)
        msk = jnp.sum(jnp.where(lane == me, metaf, 0.0), axis=-1, keepdims=True)
        pos = jnp.sum(jnp.where(lane == me, cnt, 0.0), axis=-1, keepdims=True)
        gate = jnp.sum(jnp.where((lane == me + experts) | (lane == me + 2 * experts), metaf, 0.0), axis=-1, keepdims=True)
        want = jnp.where(msk > 0.0, pos, -1.0).astype(jnp.int32)
        pick = (want == lax.broadcasted_iota(jnp.int32, (SB, slots), 1)).astype(bf)
        picks.append(pick); gates.append(gate)
        rows[i * slots:(i + 1) * slots, :] = dot(pick, x_ref[r, :D], 0, 0).astype(bf)
        gcot = (gate * cot_ref[r, :].astype(jnp.float32)).astype(bf)
        gp[i * slots:(i + 1) * slots, :] = dot(pick, gcot, 0, 0).astype(bf)
    @pl.when(step == 0)
    def _():
        for l in loads: l.wait()
    ga = dot(rows[...], wg[...], 1, 0)
    ua = dot(rows[...], wu[...], 1, 0)
    sig = 1.0 / (1.0 + jnp.exp(-ga))
    act = ga * sig
    hid = (act * ua).astype(bf)
    eo = dot(hid, wd[...], 1, 0).astype(bf)
    gg = []
    for i in range(nsub):
        r = pl.ds(i * SB, SB)
        tok = dot(picks[i], eo[i * slots:(i + 1) * slots, :], 1, 0)
        out_ref[r, :] = (gates[i] * tok).astype(bf)
        gg.append(jnp.sum(tok * cot_ref[r, :].astype(jnp.float32), axis=-1, keepdims=True))
    gh = dot(gp[...], wd[...], 1, 1)
    dga = (gh * ua * (sig * (1.0 + ga * (1.0 - sig)))).astype(bf)
    dua = (gh * act).astype(bf)
    dwd[...] += dot(hid, gp[...], 0, 0)
    grow = (dot(dga, wg[...], 1, 1) + dot(dua, wu[...], 1, 1)).astype(bf)
    dwg[...] += dot(rows[...], dga, 0, 0)
    dwu[...] += dot(rows[...], dua, 0, 0)
    for i in range(nsub):
        r = pl.ds(i * SB, SB)
        gr_ref[r, :D] = dot(picks[i], grow[i * slots:(i + 1) * slots, :], 1, 0).astype(bf)
        hi = gg[i].astype(bf).astype(jnp.float32)
        lo = gg[i] - hi
        gr_ref[r, D:] = (jnp.where(lane == me, hi, 0.0) + jnp.where(lane == me + experts, lo, 0.0)).astype(bf)
    @pl.when(step == pl.num_programs(0) - 1)
    def _():
        outs = [pltpu.make_async_copy(v, h.at[0], osem.at[i]) for i, (v, h) in enumerate(((dwg, dwg_hbm), (dwu, dwu_hbm), (dwd, dwd_hbm)))]
        for o in outs: o.start()
        for o in outs: o.wait()

def experts_call(x_all, cot_all, w_gate, w_up, w_down, experts, block, capacity, TB=512, SB=256):
    T, C = x_all.shape; D = cot_all.shape[1]
    F = w_gate.shape[2]
    slots = max(SB // block, 1) * capacity
    total = TB // SB * slots
    any_ = pl.BlockSpec(memory_space=pl.ANY)
    V = pltpu.VMEM; bf = jnp.bfloat16; f32 = jnp.float32
    return pl.pallas_call(
        functools.partial(expert_kernel, experts, slots, SB),
        grid=(T // TB,),
        out_shape=[jax.ShapeDtypeStruct((T, D), bf), jax.ShapeDtypeStruct((T, C), bf), jax.ShapeDtypeStruct(w_gate.shape, f32), jax.ShapeDtypeStruct(w_up.shape, f32), jax.ShapeDtypeStruct(w_down.shape, f32)],
        in_specs=[pl.BlockSpec((TB, C), lambda i: (i, 0)), pl.BlockSpec((TB, D), lambda i: (i, 0)), any_, any_, any_],
        out_specs=[pl.BlockSpec((TB, D), lambda i: (i, 0)), pl.BlockSpec((TB, C), lambda i: (i, 0)), any_, any_, any_],
        scratch_shapes=[V((D, F), bf), V((D, F), bf), V((F, D), bf), V((D, F), f32), V((D, F), f32), V((F, D), f32), V((total, D), bf), V((total, D), bf), pltpu.SemaphoreType.DMA((3,)), pltpu.SemaphoreType.DMA((3,))],
        compiler_params=pltpu.CompilerParams(dimension_semantics=("arbitrary",), vmem_limit_bytes=65000 * 1024),
        cost_estimate=pl.CostEstimate(flops=133_000_000_000, bytes_accessed=160_000_000, transcendentals=0),
        name="experts",
    )(x_all, cot_all, w_gate, w_up, w_down)

HQ = 32
HK = 4
HD = 128
epsilon = 1e-06
theta_base = 1000000.0
BOTH = ("expert", "shard")


def matmul(left, right):
    return jnp.dot(left, right, preferred_element_type=jnp.float32)


def matmul_tn(left, right):
    return lax.dot_general(
        left, right, (((0,), (0,)), ((), ())), preferred_element_type=jnp.float32
    )


def matmul_nt(left, right):
    return lax.dot_general(
        left, right, (((1,), (1,)), ((), ())), preferred_element_type=jnp.float32
    )


def norm_rows(values, gain_vec):
    return (
        values * lax.rsqrt(jnp.mean(values * values, axis=-1, keepdims=True) + epsilon) * gain_vec
    )


def norm_back(values, gain_vec, upstream):
    scaling = lax.rsqrt(jnp.mean(values * values, axis=-1, keepdims=True) + epsilon)
    gain_grad = jnp.sum(upstream * values * scaling, axis=0)
    weighted = upstream * gain_vec
    inner_sum = jnp.mean(weighted * values, axis=-1, keepdims=True)
    return (scaling * weighted - values * (scaling * scaling * scaling) * inner_sum, gain_grad)


def rotary(values, positions):
    head_width = values.shape[-1]
    half_width = head_width // 2
    frequency = theta_base ** (-2.0 * jnp.arange(half_width, dtype=jnp.float32) / head_width)
    angles = positions.astype(jnp.float32)[:, None] * frequency[None, :]
    cosine = jnp.concatenate([jnp.cos(angles), jnp.cos(angles)], axis=-1)[:, None, :]
    sine_part = jnp.concatenate([jnp.sin(angles), jnp.sin(angles)], axis=-1)[:, None, :]
    turned = jnp.concatenate([-values[..., half_width:], values[..., :half_width]], axis=-1)
    return values * cosine + turned * sine_part


def head_prep(projected, gain_vec, positions, head_count, factor):
    shaped = projected.reshape(projected.shape[0], head_count, projected.shape[1] // head_count)
    return rotary(norm_rows(shaped, gain_vec), positions) * factor


def head_forward(query_block, key_block, value_block, allowed):
    scores = jnp.einsum("rgd,sd->rgs", query_block, key_block, preferred_element_type=jnp.float32)
    raised = jnp.where(allowed[:, None, :], jnp.exp(scores), 0.0)
    totals = jnp.sum(raised, axis=-1)
    probs_low = (raised / totals[..., None]).astype(jnp.bfloat16)
    return (
        jnp.einsum("rgs,sd->rgd", probs_low, value_block, preferred_element_type=jnp.float32),
        totals,
    )


def head_backward(query_block, key_block, value_block, totals, upstream, allowed):
    scores = jnp.einsum("rgd,sd->rgs", query_block, key_block, preferred_element_type=jnp.float32)
    raised = jnp.where(allowed[:, None, :], jnp.exp(scores), 0.0)
    probs_f = raised / totals[..., None]
    probs_low = probs_f.astype(jnp.bfloat16)
    grad_probs = jnp.einsum(
        "rgd,sd->rgs", upstream, value_block, preferred_element_type=jnp.float32
    )
    inner_sum = jnp.sum(probs_f * grad_probs, axis=-1, keepdims=True)
    grad_scores = (probs_f * (grad_probs - inner_sum)).astype(jnp.bfloat16)
    grad_query = jnp.einsum(
        "rgs,sd->rgd", grad_scores, key_block, preferred_element_type=jnp.float32
    )
    grad_key = jnp.einsum(
        "rgs,rgd->sd", grad_scores, query_block, preferred_element_type=jnp.float32
    )
    grad_value = jnp.einsum("rgs,rgd->sd", probs_low, upstream, preferred_element_type=jnp.float32)
    return (grad_query, grad_key, grad_value)


def gather_all(arrays, cid):
    if placed():
        return [o.reshape(-1, o.shape[-1]) for o in ag32(arrays, cid)]
    return [lax.all_gather(a, BOTH, axis=0, tiled=True) for a in arrays]


def scatter_all(arrays, cid, out_dtype=jnp.float32):
    if placed():
        return rs32([a.reshape(32, -1, a.shape[-1]) for a in arrays], cid, out_dtype)
    return [lax.psum_scatter(a, BOTH, scatter_dimension=0, tiled=True).astype(out_dtype) for a in arrays]


def per_device(
    hidden_in,
    g_attn,
    w_query,
    w_key,
    w_value,
    g_query,
    g_key,
    w_out,
    g_ffn,
    w_router,
    w_gate,
    w_up,
    w_down,
    routes,
    cotangent,
):
    bf, f32 = jnp.bfloat16, jnp.float32
    tok_rows, model_width = hidden_in.shape
    top_count = routes.shape[1]
    devices = lax.axis_size(BOTH)
    expert_count = devices * w_gate.shape[0]
    capacity = 2 * tok_rows * top_count // expert_count
    shard_count = lax.axis_size("shard")
    shard_pos = lax.axis_index("shard")
    seq_len = tok_rows * shard_count
    group_size = HQ // HK
    factor = HD ** (-0.5)
    q_cols, kv_cols = HQ * HD, HK * HD

    pieces = [w_router.reshape(-1), g_attn, g_ffn, g_query, g_key]
    sizes = [p.shape[0] for p in pieces]
    used = sum(sizes)
    small_rows = -(-used // (64 * 128)) * 64
    small = jnp.concatenate(pieces + [jnp.zeros((small_rows * 128 - used,), bf)]).reshape(small_rows, 128)
    wqkv = jnp.concatenate([w_query, w_key, w_value], axis=1)
    wqkv_full, small_all = gather_all([wqkv, small], 1)
    small_all = small_all.reshape(devices, small_rows * 128)
    starts = [sum(sizes[:i]) for i in range(5)]
    wr_full, attn_gain, ffn_gain, query_gain, key_gain = [small_all[:, o : o + n].reshape(-1) for o, n in zip(starts, sizes)]
    wr_full = wr_full.reshape(model_width, expert_count)
    attn_gain, ffn_gain, query_gain, key_gain = [g.astype(f32) for g in (attn_gain, ffn_gain, query_gain, key_gain)]
    w_out, wqkv_full = lax.optimization_barrier((w_out, wqkv_full))
    wo_full = lax.all_gather(w_out, BOTH, axis=0, tiled=True)
    cotangent, _ = lax.optimization_barrier((cotangent, wo_full[:8, :128]))
    cot_all = lax.all_gather(cotangent, BOTH, axis=0, tiled=True)

    positions = shard_pos * tok_rows + jnp.arange(tok_rows, dtype=jnp.int32)
    inputs_f = hidden_in.astype(f32)
    normed_low = norm_rows(inputs_f, attn_gain).astype(bf)
    qkv = matmul(normed_low, wqkv_full)
    q_proj, k_proj, v_proj = qkv[:, :q_cols], qkv[:, q_cols : q_cols + kv_cols], qkv[:, q_cols + kv_cols :]
    k_rot, k_pull = jax.vjp(
        lambda projected, gain_vec: head_prep(projected, gain_vec, positions, HK, 1.0),
        k_proj,
        key_gain,
    )
    q_rot, q_pull = jax.vjp(
        lambda projected, gain_vec: head_prep(projected, gain_vec, positions, HQ, factor),
        q_proj,
        query_gain,
    )
    q_low = q_rot.astype(bf)
    kv_low = jnp.concatenate([k_rot.reshape(tok_rows, kv_cols).astype(bf), v_proj.astype(bf)], axis=1)
    allowed = jnp.arange(seq_len, dtype=jnp.int32)[None, :] <= positions[:, None]
    kv_all = line_gather(kv_low, 2)
    q_heads = q_low.reshape(tok_rows, HK, group_size, HD).transpose(1, 0, 2, 3)
    k_heads = kv_all[:, :kv_cols].reshape(seq_len, HK, HD).transpose(1, 0, 2)
    v_heads = kv_all[:, kv_cols:].reshape(seq_len, HK, HD).transpose(1, 0, 2)

    def attend(pieces):
        return head_forward(pieces[0], pieces[1], pieces[2], allowed)

    head_outs, totals = lax.map(attend, (q_heads, k_heads, v_heads))
    mix_low = head_outs.transpose(1, 0, 2, 3).reshape(tok_rows, q_cols).astype(bf)
    residual = inputs_f + matmul(mix_low, wo_full)
    ffn_low = norm_rows(residual, ffn_gain).astype(bf)

    logits = matmul(ffn_low, wr_full)
    expert_ids = jnp.arange(expert_count, dtype=jnp.int32)
    chosen = jnp.any(routes[:, :, None] == expert_ids[None, None, :], axis=1)
    raised_gate = jnp.where(chosen, jnp.exp(logits), 0.0)
    gates = raised_gate / jnp.sum(raised_gate, axis=-1, keepdims=True)
    gate_high = lax.reduce_precision(gates, 8, 7)
    gate_low = gates - gate_high
    extra = -(-3 * expert_count // 128) * 128
    payload = jnp.concatenate(
        [
            ffn_low,
            chosen.astype(bf),
            gate_high.astype(bf),
            gate_low.astype(bf),
            jnp.zeros((tok_rows, extra - 3 * expert_count), bf),
        ],
        axis=1,
    )
    (payload_all,) = gather_all([payload], 3)
    out_part, grad_part, grad_wgate, grad_wup, grad_wdown = experts_call(
        payload_all, cot_all, w_gate, w_up, w_down, expert_count, tok_rows, capacity
    )
    (grad_sum,) = scatter_all([grad_part], 4)
    moe_out = lax.psum_scatter(out_part, "expert", scatter_dimension=0, tiled=True)
    moe_out = lax.psum_scatter(moe_out, "shard", scatter_dimension=0, tiled=True).astype(f32)
    block_out = (residual + moe_out).astype(bf)
    upstream = cotangent.astype(f32)
    grad_ffn = grad_sum[:, :model_width]
    grad_gates = (
        grad_sum[:, model_width : model_width + expert_count]
        + grad_sum[:, model_width + expert_count : model_width + 2 * expert_count]
    )
    grad_logits = (gates * (grad_gates - jnp.sum(gates * grad_gates, axis=-1, keepdims=True))).astype(bf)
    grad_wrouter = matmul_tn(ffn_low, grad_logits)
    grad_ffn = grad_ffn + matmul_nt(grad_logits, wr_full)
    grad_second, grad_ffn_gain = norm_back(residual, ffn_gain, grad_ffn)
    grad_residual = upstream + grad_second
    grad_attn_low = grad_residual.astype(bf)
    grad_wout = matmul_tn(mix_low, grad_attn_low).astype(bf)
    grad_mix = matmul_nt(grad_attn_low, wo_full).astype(bf)
    grad_heads = grad_mix.reshape(tok_rows, HK, group_size, HD).transpose(1, 0, 2, 3)

    def attend_back(pieces):
        return head_backward(pieces[0], pieces[1], pieces[2], pieces[3], pieces[4], allowed)

    grad_qheads, grad_kheads, grad_vheads = lax.map(
        attend_back, (q_heads, k_heads, v_heads, totals, grad_heads)
    )
    grad_q_rot = grad_qheads.transpose(1, 0, 2, 3).reshape(tok_rows, HQ, HD)
    grad_kv = jnp.concatenate(
        [
            grad_kheads.transpose(1, 0, 2).reshape(seq_len, kv_cols).astype(bf),
            grad_vheads.transpose(1, 0, 2).reshape(seq_len, kv_cols).astype(bf),
        ],
        axis=1,
    )
    grad_kv = line_scatter(grad_kv, 6)
    grad_q_proj, grad_query_gain = q_pull(grad_q_rot)
    grad_k_proj, grad_key_gain = k_pull(grad_kv[:, :kv_cols].reshape(tok_rows, HK, HD))
    grad_qkv_low = jnp.concatenate(
        [grad_q_proj.astype(bf), grad_k_proj.astype(bf), grad_kv[:, kv_cols:].astype(bf)], axis=1
    )
    grad_wqkv = matmul_tn(normed_low, grad_qkv_low).astype(bf)
    grad_normed = matmul_nt(grad_qkv_low, wqkv_full)
    grad_front, grad_attn_gain = norm_back(inputs_f, attn_gain, grad_normed)
    grad_input = (grad_residual + grad_front).astype(bf)

    grads = [grad_wrouter, grad_attn_gain, grad_ffn_gain, grad_query_gain, grad_key_gain]
    packed = jnp.concatenate(
        [g.astype(bf).reshape(devices, -1) for g in grads] + [jnp.zeros((devices, small_rows * 128 - used), bf)], axis=1
    ).reshape(devices * small_rows, 128)
    out_grad, qkv_grad, small_grad = scatter_all([grad_wout, grad_wqkv, packed], 8)
    small_grad = small_grad.reshape(-1)
    router_g, attn_g, ffn_g, query_g, key_g = [small_grad[o : o + n] for o, n in zip(starts, sizes)]
    return (
        block_out,
        grad_input,
        attn_g,
        qkv_grad[:, :q_cols],
        qkv_grad[:, q_cols : q_cols + kv_cols],
        qkv_grad[:, q_cols + kv_cols :],
        query_g,
        key_g,
        out_grad,
        ffn_g,
        router_g.reshape(w_router.shape),
        grad_wgate,
        grad_wup,
        grad_wdown,
    )


def solution(mesh):
    row = P(BOTH, None)
    vec = P(BOTH)
    cube = P(BOTH, None, None)
    in_specs = (row, vec, row, row, row, vec, vec, row, vec, row, cube, cube, cube, row, row)
    out_specs = (row, row, vec, row, row, row, vec, vec, row, vec, row, cube, cube, cube)
    return jax.shard_map(
        per_device, mesh=mesh, in_specs=in_specs, out_specs=out_specs, check_vma=False
    )
```

```python
import functools

import jax
import jax.numpy as jnp
from jax import lax
from jax.experimental import pallas as pl
from jax.experimental.pallas import tpu as pltpu
from jax.sharding import PartitionSpec as P

MESH = pl.DeviceIdType.MESH
NZ = 4

def placed():
    return lax.axis_size("expert") == 8 and lax.axis_size("shard") == NZ

def place():
    e = lax.axis_index("expert"); s = lax.axis_index("shard")
    return e // 4, lax.rem(e // 2, 2), lax.rem(e, 2), s

def dev(y, x, c, s):
    return (y * 4 + x * 2 + c, s)

def barrier_all(y, x, c, s):
    bar = pltpu.get_barrier_semaphore()
    def sig(d): pl.semaphore_signal(bar, inc=1, device_id=d, device_id_type=MESH)
    sig(dev(1 - y, x, c, s)); sig(dev(y, 1 - x, c, s)); sig(dev(y, x, 1 - c, s))
    @pl.when(s > 0)
    def _(): sig(dev(y, x, c, s - 1))
    @pl.when(s < NZ - 1)
    def _(): sig(dev(y, x, c, s + 1))
    pl.semaphore_wait(bar, 3 + jnp.where(s > 0, 1, 0) + jnp.where(s < NZ - 1, 1, 0))

def ag_kernel(n_arr, *refs):
    ins = refs[:n_arr]; outs = refs[n_arr:2 * n_arr]
    loc_sem, zs, zr, ps, pr, cs, cr = refs[2 * n_arr:]
    y, x, c, s = place()
    barrier_all(y, x, c, s)
    def rc(src, dst, ss, rs, d):
        return pltpu.make_async_remote_copy(src_ref=src, dst_ref=dst, send_sem=ss, recv_sem=rs, device_id=d, device_id_type=MESH)
    X = dev(y, 1 - x, c, s); Y = dev(1 - y, x, c, s); C = dev(y, x, 1 - c, s)
    A = range(n_arr)
    steps = [(0, 0)] + [(d, g) for d in range(1, NZ) for g in (1, -1)]
    def valid(d, g):
        return (s >= d) if g == 1 else (s + d <= NZ - 1)
    def zof(d, g): return s - d * g
    def src_own(a, h, zz, k):
        return ins[a].at[h] if k == 0 else outs[a].at[y, x, c, zz, h]
    def zcopy(a, h, zz, k, g):
        kk = 1 + 2 * (k_dist(k)) + (0 if g == 1 else 1)
        return rc(src_own(a, h, zz, k), outs[a].at[y, x, c, zz, h], zs.at[a, h, kk], zr.at[a, h, kk], dev(y, x, c, s + g))
    def k_dist(k): return steps[k][0]
    def plane(a, h, zz, k, which):
        return rc(src_own(a, h, zz, k), outs[a].at[y, x, c, zz, h], ps.at[a, k, h, which], pr.at[a, k, h, which], X if which == 0 else Y)
    def plane_recv(a, h, zz, k, which):
        d = outs[a].at[y, 1 - x, c, zz, h] if which == 0 else outs[a].at[1 - y, x, c, zz, h]
        return rc(d, d, ps.at[a, k, h, which], pr.at[a, k, h, which], X if which == 0 else Y)
    def diag(a, h, zz, k):
        d = outs[a].at[y, 1 - x, c, zz, h] if h == 0 else outs[a].at[1 - y, x, c, zz, h]
        return rc(d, d, ps.at[a, k, h, 2], pr.at[a, k, h, 2], Y if h == 0 else X)
    def diag_recv(a, h, zz, k):
        d = outs[a].at[1 - y, 1 - x, c, zz, h]
        return rc(d, d, ps.at[a, k, h, 2], pr.at[a, k, h, 2], Y if h == 0 else X)
    def core(a, zz, k, part):
        d = outs[a].at[:, :, c, zz]
        return rc(d, d, cs.at[a, k], cr.at[a, k], C)
    def core_recv(a, zz, k):
        d = outs[a].at[:, :, 1 - c, zz]
        return rc(d, d, cs.at[a, k], cr.at[a, k], C)
    def loc(a):
        return pltpu.make_async_copy(ins[a], outs[a].at[y, x, c, s], loc_sem.at[a])

    def when(k, f):
        d, g = steps[k]
        if k == 0: f()
        else: pl.when(valid(d, g))(f)

    def stage_a(k):
        d, g = steps[k]
        def go():
            zz = zof(d, g)
            for a in A:
                for h in range(2):
                    if k:
                        kk = k
                        dref = outs[a].at[y, x, c, zz, h]
                        rc(dref, dref, zs.at[a, h, kk], zr.at[a, h, kk], X).wait_recv()
                    for gg in ((1, -1) if k == 0 else (g,)):
                        okc = (s < NZ - 1) if gg == 1 else (s > 0)
                        if d + 1 < NZ:
                            @pl.when(okc)
                            def _(): zcopy(a, h, zz, k, gg).start()
                    plane(a, h, zz, k, 0).start()
                    plane(a, h, zz, k, 1).start()
        when(k, go)
    def stage_b(k):
        d, g = steps[k]
        def go():
            zz = zof(d, g)
            for a in A:
                plane_recv(a, 0, zz, k, 0).wait_recv()
                diag(a, 0, zz, k).start()
                plane_recv(a, 1, zz, k, 1).wait_recv()
                diag(a, 1, zz, k).start()
        when(k, go)
    def stage_c(k):
        d, g = steps[k]
        def go():
            zz = zof(d, g)
            for a in A:
                if k == 0: loc(a).wait()
                plane_recv(a, 1, zz, k, 0).wait_recv()
                plane_recv(a, 0, zz, k, 1).wait_recv()
                diag_recv(a, 0, zz, k).wait_recv()
                diag_recv(a, 1, zz, k).wait_recv()
                core(a, zz, k, 0).start()
        when(k, go)
    for a in A: loc(a).start()
    n = len(steps)
    for i in range(n + 2):
        if i < n: stage_a(i)
        if 0 <= i - 1 < n: stage_b(i - 1)
        if 0 <= i - 2 < n: stage_c(i - 2)
    for k in range(n):
        d, g = steps[k]
        def go():
            zz = zof(d, g)
            for a in A:
                core_recv(a, zz, k).wait_recv()
                core(a, zz, k, 0).wait_send()
                for h in range(2):
                    for gg in ((1, -1) if k == 0 else (g,)):
                        okc = (s < NZ - 1) if gg == 1 else (s > 0)
                        if d + 1 < NZ:
                            @pl.when(okc)
                            def _(): zcopy(a, h, zz, k, gg).wait_send()
                    plane(a, h, zz, k, 0).wait_send()
                    plane(a, h, zz, k, 1).wait_send()
                    diag(a, h, zz, k).wait_send()
        when(k, go)

def ag32(arrs, cid):
    ins = [a.reshape(2, a.shape[0] // 2, a.shape[1]) for a in arrs]
    n = len(ins); nk = 7
    outs = pl.pallas_call(
        functools.partial(ag_kernel, n),
        out_shape=[jax.ShapeDtypeStruct((2, 2, 2, NZ) + a.shape, a.dtype) for a in ins],
        in_specs=[pl.BlockSpec(memory_space=pltpu.VMEM)] * n,
        out_specs=[pl.BlockSpec(memory_space=pl.ANY)] * n,
        scratch_shapes=[pltpu.SemaphoreType.DMA((n,)),
            pltpu.SemaphoreType.DMA((n, 2, 9)), pltpu.SemaphoreType.DMA((n, 2, 9)),
            pltpu.SemaphoreType.DMA((n, nk, 2, 3)), pltpu.SemaphoreType.DMA((n, nk, 2, 3)),
            pltpu.SemaphoreType.DMA((n, nk)), pltpu.SemaphoreType.DMA((n, nk))],
        compiler_params=pltpu.CompilerParams(collective_id=cid, has_side_effects=True, vmem_limit_bytes=64000 * 1024),
        name="gather_all",
    )(*ins)
    return [o.reshape(32, a.shape[0], a.shape[1]) for o, a in zip(outs, arrs)]

ZORDER = (0, 3, 1, 2)
LAGS = (1, 1, 1, 1)

def rs_kernel(n_arr, parts, *refs):
    ins = refs[:n_arr]; outs = refs[n_arr:2 * n_arr]
    sc = refs[2 * n_arr:]
    own_b, r0_b, ra_b, rb_b, zu_b, zd_b = [sc[i * n_arr:(i + 1) * n_arr] for i in range(6)]
    lsem, s0s, s0r, sas, sar, sbs, sbr, zus, zur, zds, zdr = sc[6 * n_arr:]
    y, x, c, s = place()
    barrier_all(y, x, c, s)
    X = dev(y, 1 - x, c, s); Y = dev(1 - y, x, c, s); C = dev(y, x, 1 - c, s)
    UP = dev(y, x, c, s + 1); DN = dev(y, x, c, s - 1)
    def rc(src, dst, ss, rs, d):
        return pltpu.make_async_remote_copy(src_ref=src, dst_ref=dst, send_sem=ss, recv_sem=rs, device_id=d, device_id_type=MESH)
    units = [(a, zz, h) for zz in ZORDER for h in range(parts) for a in range(n_arr)]
    def jj(zz, h): return ZORDER.index(zz) * parts + h
    def load(a, zz, h):
        j = jj(zz, h)
        return pltpu.make_async_copy(ins[a].at[:, :, c, zz, h], own_b[a].at[j], lsem.at[a, j])
    def c0(a, zz, h):
        j = jj(zz, h)
        return rc(ins[a].at[:, :, 1 - c, zz, h], r0_b[a].at[j], s0s.at[a, j], s0r.at[a, j], C)
    def ca(a, zz, h):
        j = jj(zz, h)
        if h % 2 == 0: return rc(own_b[a].at[j, :, 1 - x], ra_b[a].at[j], sas.at[a, j], sar.at[a, j], X)
        return rc(own_b[a].at[j, 1 - y], ra_b[a].at[j], sas.at[a, j], sar.at[a, j], Y)
    def cb(a, zz, h):
        j = jj(zz, h)
        if h % 2 == 0: return rc(own_b[a].at[j, 1 - y, x], rb_b[a].at[j], sbs.at[a, j], sbr.at[a, j], Y)
        return rc(own_b[a].at[j, y, 1 - x], rb_b[a].at[j], sbs.at[a, j], sbr.at[a, j], X)
    def cu(a, zz, h):
        j = jj(zz, h)
        return rc(own_b[a].at[j, y, x], zu_b[a].at[j], zus.at[a, j], zur.at[a, j], UP)
    def cd(a, zz, h):
        j = jj(zz, h)
        return rc(own_b[a].at[j, y, x], zd_b[a].at[j], zds.at[a, j], zdr.at[a, j], DN)
    def add_into(dst, other):
        rows = dst.shape[0]
        st = 16 if rows % 16 == 0 else rows
        @pl.loop(0, rows // st)
        def _(i):
            r = pl.ds(i * st, st)
            dst[r, :] = (dst[r, :].astype(jnp.float32) + other[r, :].astype(jnp.float32)).astype(dst.dtype)
    def stage0(u):
        a, zz, h = u; j = jj(zz, h)
        load(a, zz, h).wait()
        c0(a, zz, h).wait_recv()
        for yy in range(2):
            for xx in range(2):
                add_into(own_b[a].at[j, yy, xx], r0_b[a].at[j, yy, xx])
        ca(a, zz, h).start()
    def stage1(u):
        a, zz, h = u; j = jj(zz, h)
        ca(a, zz, h).wait_recv()
        for q in range(2):
            if h % 2 == 0: add_into(own_b[a].at[j, q, x], ra_b[a].at[j, q])
            else: add_into(own_b[a].at[j, y, q], ra_b[a].at[j, q])
        cb(a, zz, h).start()
    def stage2(u):
        a, zz, h = u; j = jj(zz, h)
        cb(a, zz, h).wait_recv()
        add_into(own_b[a].at[j, y, x], rb_b[a].at[j])
    def hop(u, k):
        a, zz, h = u; j = jj(zz, h)
        if k < zz:
            @pl.when(s == k)
            def _():
                if k > 0:
                    cu(a, zz, h).wait_recv()
                    add_into(own_b[a].at[j, y, x], zu_b[a].at[j])
                cu(a, zz, h).start()
        t = NZ - 1 - k
        if t > zz:
            @pl.when(s == t)
            def _():
                if k > 0:
                    cd(a, zz, h).wait_recv()
                    add_into(own_b[a].at[j, y, x], zd_b[a].at[j])
                cd(a, zz, h).start()
    def last(u):
        a, zz, h = u; j = jj(zz, h)
        @pl.when(s == zz)
        def _():
            if zz > 0: cu(a, zz, h).wait_recv()
            if zz < NZ - 1: cd(a, zz, h).wait_recv()
            t = own_b[a][j, y, x].astype(jnp.float32)
            if zz > 0: t = t + zu_b[a][j].astype(jnp.float32)
            if zz < NZ - 1: t = t + zd_b[a][j].astype(jnp.float32)
            outs[a][h] = t.astype(outs[a].dtype)
    for u in units:
        c0(*u).start(); load(*u).start()
    n = len(units)
    L1 = LAGS[0] * n_arr; L2 = L1 + LAGS[1] * n_arr; L3 = L2 + LAGS[2] * n_arr; dl = LAGS[3] * n_arr
    for i in range(n + L3 + (NZ - 1) * dl):
        if i < n: stage0(units[i])
        if 0 <= i - L1 < n: stage1(units[i - L1])
        if 0 <= i - L2 < n: stage2(units[i - L2])
        for k in range(NZ - 1):
            if 0 <= i - L3 - k * dl < n: hop(units[i - L3 - k * dl], k)
    for u in units: last(u)
    for u in units:
        c0(*u).wait_send(); ca(*u).wait_send(); cb(*u).wait_send()
        zz = u[1]
        if zz > 0:
            @pl.when(s < zz)
            def _(): cu(*u).wait_send()
        if zz < NZ - 1:
            @pl.when(s > zz)
            def _(): cd(*u).wait_send()

def rs32(arrs, cid, out_dtype=jnp.float32, parts=4):
    n = len(arrs)
    if any(a.shape[1] % (parts * 16) for a in arrs): parts = 2
    ins = [a.reshape(2, 2, 2, NZ, parts, a.shape[1] // parts, a.shape[2]) for a in arrs]
    hs = [i.shape[-2:] for i in ins]
    V = pltpu.VMEM; bt = jnp.bfloat16; m = NZ * parts
    sems = [pltpu.SemaphoreType.DMA((n, m))] * 11
    outs = pl.pallas_call(
        functools.partial(rs_kernel, n, parts),
        out_shape=[jax.ShapeDtypeStruct((parts,) + h, out_dtype) for h in hs],
        in_specs=[pl.BlockSpec(memory_space=pl.ANY)] * n,
        out_specs=[pl.BlockSpec(memory_space=pltpu.VMEM)] * n,
        scratch_shapes=[V((m, 2, 2) + h, bt) for h in hs] + [V((m, 2, 2) + h, bt) for h in hs] + [V((m, 2) + h, bt) for h in hs]
            + [V((m,) + h, bt) for h in hs] + [V((m,) + h, bt) for h in hs] + [V((m,) + h, bt) for h in hs] + sems,
        compiler_params=pltpu.CompilerParams(collective_id=cid, has_side_effects=True, vmem_limit_bytes=64000 * 1024),
        name="scatter_all",
    )(*ins)
    return [o.reshape(a.shape[1], a.shape[2]) for o, a in zip(outs, arrs)]

def line_barrier(y, x, c, s):
    bar = pltpu.get_barrier_semaphore()
    @pl.when(s > 0)
    def _(): pl.semaphore_signal(bar, inc=1, device_id=dev(y, x, c, s - 1), device_id_type=MESH)
    @pl.when(s < NZ - 1)
    def _(): pl.semaphore_signal(bar, inc=1, device_id=dev(y, x, c, s + 1), device_id_type=MESH)
    pl.semaphore_wait(bar, jnp.where(s > 0, 1, 0) + jnp.where(s < NZ - 1, 1, 0))

def line_gather_kernel(parts, x_ref, o_ref, ss, rs):
    y, x, c, s = place()
    line_barrier(y, x, c, s)
    def cp(d, g, h):
        src = x_ref.at[h] if d == 0 else o_ref.at[s - d * g, h]
        k = 0 if g == 1 else 1
        return pltpu.make_async_remote_copy(src_ref=src, dst_ref=o_ref.at[s - d * g, h], send_sem=ss.at[k, d, h], recv_sem=rs.at[k, d, h],
            device_id=dev(y, x, c, s + g), device_id_type=MESH)
    def arrived(d, g, h):
        k = 0 if g == 1 else 1
        ref = o_ref.at[s - (d + 1) * g, h]
        return pltpu.make_async_remote_copy(src_ref=ref, dst_ref=ref, send_sem=ss.at[k, d, h], recv_sem=rs.at[k, d, h],
            device_id=dev(y, x, c, s + g), device_id_type=MESH)
    def sends(d, g): return (s >= d) & (s < NZ - 1) if g == 1 else (s + d <= NZ - 1) & (s > 0)
    def gets(d, g): return s >= d + 1 if g == 1 else s + d + 1 <= NZ - 1
    for d in range(NZ):
        for h in range(parts):
            for g in (1, -1):
                if d:
                    @pl.when(gets(d - 1, g))
                    def _(): arrived(d - 1, g, h).wait_recv()
                if d < NZ - 1:
                    @pl.when(sends(d, g))
                    def _(): cp(d, g, h).start()
        if d == 0: o_ref[s] = x_ref[...]
    for d in range(NZ - 1):
        for h in range(parts):
            for g in (1, -1):
                @pl.when(sends(d, g))
                def _(): cp(d, g, h).wait_send()

def line_gather(x, cid, parts=4):
    if not placed():
        return lax.all_gather(x, "shard", axis=0, tiled=True)
    R, C = x.shape
    sem = pltpu.SemaphoreType.DMA((2, NZ, parts))
    o = pl.pallas_call(functools.partial(line_gather_kernel, parts), out_shape=jax.ShapeDtypeStruct((NZ, parts, R // parts, C), x.dtype),
        in_specs=[pl.BlockSpec(memory_space=pltpu.VMEM)], out_specs=pl.BlockSpec(memory_space=pltpu.VMEM),
        scratch_shapes=[sem, sem], compiler_params=pltpu.CompilerParams(collective_id=cid, has_side_effects=True, vmem_limit_bytes=16 << 20),
        name="line_gather")(x.reshape(parts, R // parts, C))
    return o.reshape(NZ * R, C)

def line_scatter_kernel(parts, p_ref, o_ref, acc, zu, zd, ss_u, rs_u, ss_d, rs_d):
    y, x, c, s = place()
    line_barrier(y, x, c, s)
    def rc(src, dst, a, b, d):
        return pltpu.make_async_remote_copy(src_ref=src, dst_ref=dst, send_sem=a, recv_sem=b, device_id=d, device_id_type=MESH)
    def cu(zz, h, k):
        src = p_ref.at[zz, h] if k == 0 else acc.at[zz, h]
        return rc(src, zu.at[zz, h], ss_u.at[zz, h], rs_u.at[zz, h], dev(y, x, c, s + 1))
    def cd(zz, h, k):
        src = p_ref.at[zz, h] if k == 0 else acc.at[zz, h]
        return rc(src, zd.at[zz, h], ss_d.at[zz, h], rs_d.at[zz, h], dev(y, x, c, s - 1))
    st = 32
    def total(dst, refs):
        @pl.loop(0, dst.shape[0] // st)
        def _(i):
            r = pl.ds(i * st, st)
            t = refs[0][r, :].astype(jnp.float32)
            for f in refs[1:]: t = t + f[r, :].astype(jnp.float32)
            dst[r, :] = t.astype(dst.dtype)
    ups = [(zz, h) for zz in (3, 2, 1) for h in range(parts)]
    dns = [(zz, h) for zz in (0, 1, 2) for h in range(parts)]
    n = len(ups)
    for i in range(n + NZ):
        for k in range(NZ - 1):
            if 0 <= i - k < n:
                zz, h = ups[i - k]
                if k < zz:
                    @pl.when(s == k)
                    def _():
                        if k:
                            cu(zz, h, k).wait_recv()
                            total(acc.at[zz, h], [p_ref.at[zz, h], zu.at[zz, h]])
                        cu(zz, h, k).start()
                zz, h = dns[i - k]
                if NZ - 1 - k > zz:
                    @pl.when(s == NZ - 1 - k)
                    def _():
                        if k:
                            cd(zz, h, k).wait_recv()
                            total(acc.at[zz, h], [p_ref.at[zz, h], zd.at[zz, h]])
                        cd(zz, h, k).start()
    for zz in range(NZ):
        @pl.when(s == zz)
        def _():
            for h in range(parts):
                refs = [p_ref.at[zz, h]]
                if zz > 0:
                    cu(zz, h, 1).wait_recv()
                    refs.append(zu.at[zz, h])
                if zz < NZ - 1:
                    cd(zz, h, 1).wait_recv()
                    refs.append(zd.at[zz, h])
                total(o_ref.at[h], refs)
    for zz, h in ups:
        @pl.when(s < zz)
        def _(): cu(zz, h, 1).wait_send()
    for zz, h in dns:
        @pl.when(s > zz)
        def _(): cd(zz, h, 1).wait_send()

def line_scatter(p, cid, parts=4):
    if not placed():
        return lax.psum_scatter(p, "shard", scatter_dimension=0, tiled=True).astype(jnp.float32)
    R, C = p.shape[0] // NZ, p.shape[1]
    sem = pltpu.SemaphoreType.DMA((NZ, parts))
    shape = (NZ, parts, R // parts, C)
    buf = pltpu.VMEM(shape, p.dtype)
    o = pl.pallas_call(functools.partial(line_scatter_kernel, parts), out_shape=jax.ShapeDtypeStruct(shape[1:], jnp.float32),
        in_specs=[pl.BlockSpec(memory_space=pltpu.VMEM)], out_specs=pl.BlockSpec(memory_space=pltpu.VMEM),
        scratch_shapes=[buf, buf, buf, sem, sem, sem, sem], compiler_params=pltpu.CompilerParams(collective_id=cid, has_side_effects=True, vmem_limit_bytes=24 << 20),
        name="line_scatter")(p.reshape(shape))
    return o.reshape(R, C)


def dot(a, b, ca, cb):
    return lax.dot_general(a, b, (((ca,), (cb,)), ((), ())), preferred_element_type=jnp.float32)

def token_picks(meta, experts, slots, me):
    SB, WM = meta.shape
    bf, f32 = jnp.bfloat16, jnp.float32
    tri = (lax.broadcasted_iota(jnp.int32, (SB, SB), 1) < lax.broadcasted_iota(jnp.int32, (SB, SB), 0)).astype(bf)
    lane = lax.broadcasted_iota(jnp.int32, (SB, WM), 1)
    cnt = dot(tri, meta, 1, 0)
    metaf = meta.astype(f32)
    msk = jnp.sum(jnp.where(lane == me, metaf, 0.0), axis=-1, keepdims=True)
    pos = jnp.sum(jnp.where(lane == me, cnt, 0.0), axis=-1, keepdims=True)
    gate = jnp.sum(jnp.where((lane == me + experts) | (lane == me + 2 * experts), metaf, 0.0), axis=-1, keepdims=True)
    want = jnp.where(msk > 0.0, pos, -1.0).astype(jnp.int32)
    pick = (want == lax.broadcasted_iota(jnp.int32, (SB, slots), 1)).astype(bf)
    return pick, gate

def forward_kernel(experts, slots, SB, x_ref, wg_hbm, wu_hbm, wd_hbm, out_ref, rows_ref, ga_ref, ua_ref, wg, wu, wd, wsem):
    bf = jnp.bfloat16
    step = pl.program_id(0)
    nsub = x_ref.shape[0] // SB
    D = out_ref.shape[1]
    me = lax.axis_index(("expert", "shard"))
    loads = [pltpu.make_async_copy(h.at[0], v, wsem.at[i]) for i, (h, v) in enumerate(((wg_hbm, wg), (wu_hbm, wu), (wd_hbm, wd)))]
    @pl.when(step == 0)
    def _():
        for l in loads: l.start()
    picks, gates = [], []
    for i in range(nsub):
        r = pl.ds(i * SB, SB)
        pick, gate = token_picks(x_ref[r, D:], experts, slots, me)
        picks.append(pick); gates.append(gate)
        rows_ref[i * slots:(i + 1) * slots, :] = dot(pick, x_ref[r, :D], 0, 0).astype(bf)
    @pl.when(step == 0)
    def _():
        for l in loads: l.wait()
    ga = dot(rows_ref[...], wg[...], 1, 0)
    ua = dot(rows_ref[...], wu[...], 1, 0)
    ga_ref[...] = ga
    ua_ref[...] = ua
    hid = (ga * (1.0 / (1.0 + jnp.exp(-ga))) * ua).astype(bf)
    eo = dot(hid, wd[...], 1, 0).astype(bf)
    for i in range(nsub):
        r = pl.ds(i * SB, SB)
        tok = dot(picks[i], eo[i * slots:(i + 1) * slots, :], 1, 0)
        out_ref[r, :] = (gates[i] * tok).astype(bf)

def backward_kernel(experts, slots, SB, meta_ref, cot_ref, rows_ref, ga_ref, ua_ref, wg_hbm, wu_hbm, wd_hbm, gr_ref, dwg_hbm, dwu_hbm, dwd_hbm,
                  wg, wu, wd, dwg, dwu, dwd, gp, wsem, osem):
    bf = jnp.bfloat16
    step = pl.program_id(0)
    nsub = cot_ref.shape[0] // SB
    D = cot_ref.shape[1]
    WM = meta_ref.shape[1]
    me = lax.axis_index(("expert", "shard"))
    loads = [pltpu.make_async_copy(h.at[0], v, wsem.at[i]) for i, (h, v) in enumerate(((wg_hbm, wg), (wu_hbm, wu), (wd_hbm, wd)))]
    @pl.when(step == 0)
    def _():
        for l in loads: l.start()
        for a in (dwg, dwu, dwd): a[...] = jnp.zeros_like(a)
    picks = []
    for i in range(nsub):
        r = pl.ds(i * SB, SB)
        pick, gate = token_picks(meta_ref[r, :], experts, slots, me)
        picks.append(pick)
        gcot = (gate * cot_ref[r, :].astype(jnp.float32)).astype(bf)
        gp[i * slots:(i + 1) * slots, :] = dot(pick, gcot, 0, 0).astype(bf)
    @pl.when(step == 0)
    def _():
        for l in loads: l.wait()
    ga = ga_ref[...]
    ua = ua_ref[...]
    sig = 1.0 / (1.0 + jnp.exp(-ga))
    act = ga * sig
    hidf = act * ua
    hid = hidf.astype(bf)
    gh = dot(gp[...], wd[...], 1, 1)
    share = jnp.sum(gh * hid.astype(jnp.float32), axis=-1, keepdims=True)
    dga = (gh * ua * (sig * (1.0 + ga * (1.0 - sig)))).astype(bf)
    dua = (gh * act).astype(bf)
    dwd[...] += dot(hid, gp[...], 0, 0)
    grow = (dot(dga, wg[...], 1, 1) + dot(dua, wu[...], 1, 1)).astype(bf)
    dwg[...] += dot(rows_ref[...], dga, 0, 0)
    dwu[...] += dot(rows_ref[...], dua, 0, 0)
    lane = lax.broadcasted_iota(jnp.int32, (share.shape[0], WM), 1)
    high = share.astype(bf).astype(jnp.float32)
    tail = (jnp.where(lane == me, high, 0.0) + jnp.where(lane == me + experts, share - high, 0.0)).astype(bf)
    for i in range(nsub):
        r = pl.ds(i * SB, SB)
        q = slice(i * slots, (i + 1) * slots)
        gr_ref[r, :D] = dot(picks[i], grow[q, :], 1, 0).astype(bf)
        gr_ref[r, D:] = dot(picks[i], tail[q, :], 1, 0).astype(bf)
    @pl.when(step == pl.num_programs(0) - 1)
    def _():
        outs = [pltpu.make_async_copy(v, h.at[0], osem.at[i]) for i, (v, h) in enumerate(((dwg, dwg_hbm), (dwu, dwu_hbm), (dwd, dwd_hbm)))]
        for o in outs: o.start()
        for o in outs: o.wait()

def experts_forward(x_all, w_gate, w_up, w_down, experts, block, capacity, TB=512, SB=256):
    T, C = x_all.shape; D, F = w_gate.shape[1:]
    slots = max(SB // block, 1) * capacity
    total = TB // SB * slots
    S = T // SB * slots
    any_ = pl.BlockSpec(memory_space=pl.ANY)
    V = pltpu.VMEM; bf = jnp.bfloat16; f32 = jnp.float32
    blk = lambda r, c: pl.BlockSpec((r, c), lambda i: (i, 0))
    return pl.pallas_call(
        functools.partial(forward_kernel, experts, slots, SB),
        grid=(T // TB,),
        out_shape=[jax.ShapeDtypeStruct((T, D), bf), jax.ShapeDtypeStruct((S, D), bf), jax.ShapeDtypeStruct((S, F), f32), jax.ShapeDtypeStruct((S, F), f32)],
        in_specs=[blk(TB, C), any_, any_, any_],
        out_specs=[blk(TB, D), blk(total, D), blk(total, F), blk(total, F)],
        scratch_shapes=[V((D, F), bf), V((D, F), bf), V((F, D), bf), pltpu.SemaphoreType.DMA((3,))],
        compiler_params=pltpu.CompilerParams(dimension_semantics=("arbitrary",), vmem_limit_bytes=65000 * 1024),
        cost_estimate=pl.CostEstimate(flops=48_000_000_000, bytes_accessed=130_000_000, transcendentals=0),
        name="experts_forward",
    )(x_all, w_gate, w_up, w_down)

def experts_backward(x_all, cot_all, rows, ga, ua, w_gate, w_up, w_down, experts, block, capacity, TB=512, SB=256):
    T, C = x_all.shape; D, F = w_gate.shape[1:]
    slots = max(SB // block, 1) * capacity
    total = TB // SB * slots
    WM = C - D
    any_ = pl.BlockSpec(memory_space=pl.ANY)
    V = pltpu.VMEM; bf = jnp.bfloat16; f32 = jnp.float32
    blk = lambda r, c: pl.BlockSpec((r, c), lambda i: (i, 0))
    meta = pl.BlockSpec((TB, WM), lambda i: (i, D // WM)) if D % WM == 0 else blk(TB, WM)
    meta_in = x_all if D % WM == 0 else x_all[:, D:]
    return pl.pallas_call(
        functools.partial(backward_kernel, experts, slots, SB),
        grid=(T // TB,),
        out_shape=[jax.ShapeDtypeStruct((T, C), bf), jax.ShapeDtypeStruct(w_gate.shape, f32), jax.ShapeDtypeStruct(w_up.shape, f32), jax.ShapeDtypeStruct(w_down.shape, f32)],
        in_specs=[meta, blk(TB, D), blk(total, D), blk(total, F), blk(total, F), any_, any_, any_],
        out_specs=[blk(TB, C), any_, any_, any_],
        scratch_shapes=[V((D, F), bf), V((D, F), bf), V((F, D), bf), V((D, F), f32), V((D, F), f32), V((F, D), f32), V((total, D), bf), pltpu.SemaphoreType.DMA((3,)), pltpu.SemaphoreType.DMA((3,))],
        compiler_params=pltpu.CompilerParams(dimension_semantics=("arbitrary",), vmem_limit_bytes=65000 * 1024),
        cost_estimate=pl.CostEstimate(flops=85_000_000_000, bytes_accessed=150_000_000, transcendentals=0),
        name="experts_backward",
    )(meta_in, cot_all, rows, ga, ua, w_gate, w_up, w_down)

HQ = 32
HK = 4
HD = 128
epsilon = 1e-06
theta_base = 1000000.0
BOTH = ("expert", "shard")


def matmul(left, right):
    return jnp.dot(left, right, preferred_element_type=jnp.float32)


def matmul_tn(left, right):
    return lax.dot_general(
        left, right, (((0,), (0,)), ((), ())), preferred_element_type=jnp.float32
    )


def matmul_nt(left, right):
    return lax.dot_general(
        left, right, (((1,), (1,)), ((), ())), preferred_element_type=jnp.float32
    )


def norm_rows(values, gain_vec):
    return (
        values * lax.rsqrt(jnp.mean(values * values, axis=-1, keepdims=True) + epsilon) * gain_vec
    )


def norm_back(values, gain_vec, upstream):
    scaling = lax.rsqrt(jnp.mean(values * values, axis=-1, keepdims=True) + epsilon)
    gain_grad = jnp.sum(upstream * values * scaling, axis=0)
    weighted = upstream * gain_vec
    inner_sum = jnp.mean(weighted * values, axis=-1, keepdims=True)
    return (scaling * weighted - values * (scaling * scaling * scaling) * inner_sum, gain_grad)


def rotary(values, positions):
    head_width = values.shape[-1]
    half_width = head_width // 2
    frequency = theta_base ** (-2.0 * jnp.arange(half_width, dtype=jnp.float32) / head_width)
    angles = positions.astype(jnp.float32)[:, None] * frequency[None, :]
    cosine = jnp.concatenate([jnp.cos(angles), jnp.cos(angles)], axis=-1)[:, None, :]
    sine_part = jnp.concatenate([jnp.sin(angles), jnp.sin(angles)], axis=-1)[:, None, :]
    turned = jnp.concatenate([-values[..., half_width:], values[..., :half_width]], axis=-1)
    return values * cosine + turned * sine_part


def head_prep(projected, gain_vec, positions, head_count, factor):
    shaped = projected.reshape(projected.shape[0], head_count, projected.shape[1] // head_count)
    return rotary(norm_rows(shaped, gain_vec), positions) * factor


def head_forward(query_block, key_block, value_block, allowed):
    scores = jnp.einsum("rgd,sd->rgs", query_block, key_block, preferred_element_type=jnp.float32)
    raised = jnp.where(allowed[:, None, :], jnp.exp(scores), 0.0)
    totals = jnp.sum(raised, axis=-1)
    probs_low = (raised / totals[..., None]).astype(jnp.bfloat16)
    return (
        jnp.einsum("rgs,sd->rgd", probs_low, value_block, preferred_element_type=jnp.float32),
        totals,
    )


def head_backward(query_block, key_block, value_block, totals, upstream, allowed):
    scores = jnp.einsum("rgd,sd->rgs", query_block, key_block, preferred_element_type=jnp.float32)
    raised = jnp.where(allowed[:, None, :], jnp.exp(scores), 0.0)
    probs_f = raised / totals[..., None]
    probs_low = probs_f.astype(jnp.bfloat16)
    grad_probs = jnp.einsum(
        "rgd,sd->rgs", upstream, value_block, preferred_element_type=jnp.float32
    )
    inner_sum = jnp.sum(probs_f * grad_probs, axis=-1, keepdims=True)
    grad_scores = (probs_f * (grad_probs - inner_sum)).astype(jnp.bfloat16)
    grad_query = jnp.einsum(
        "rgs,sd->rgd", grad_scores, key_block, preferred_element_type=jnp.float32
    )
    grad_key = jnp.einsum(
        "rgs,rgd->sd", grad_scores, query_block, preferred_element_type=jnp.float32
    )
    grad_value = jnp.einsum("rgs,rgd->sd", probs_low, upstream, preferred_element_type=jnp.float32)
    return (grad_query, grad_key, grad_value)


def gather_all(arrays, cid):
    if placed():
        return [o.reshape(-1, o.shape[-1]) for o in ag32(arrays, cid)]
    return [lax.all_gather(a, BOTH, axis=0, tiled=True) for a in arrays]


def scatter_all(arrays, cid, out_dtype=jnp.float32):
    if placed():
        return rs32([a.reshape(32, -1, a.shape[-1]) for a in arrays], cid, out_dtype)
    return [lax.psum_scatter(a, BOTH, scatter_dimension=0, tiled=True).astype(out_dtype) for a in arrays]


def per_device(
    hidden_in,
    g_attn,
    w_query,
    w_key,
    w_value,
    g_query,
    g_key,
    w_out,
    g_ffn,
    w_router,
    w_gate,
    w_up,
    w_down,
    routes,
    cotangent,
):
    bf, f32 = jnp.bfloat16, jnp.float32
    tok_rows, model_width = hidden_in.shape
    top_count = routes.shape[1]
    devices = lax.axis_size(BOTH)
    expert_count = devices * w_gate.shape[0]
    capacity = 2 * tok_rows * top_count // expert_count
    shard_count = lax.axis_size("shard")
    shard_pos = lax.axis_index("shard")
    seq_len = tok_rows * shard_count
    group_size = HQ // HK
    factor = HD ** (-0.5)
    q_cols, kv_cols = HQ * HD, HK * HD

    pieces = [w_router.reshape(-1), g_attn, g_ffn, g_query, g_key]
    sizes = [p.shape[0] for p in pieces]
    used = sum(sizes)
    small_rows = -(-used // (64 * 128)) * 64
    small = jnp.concatenate(pieces + [jnp.zeros((small_rows * 128 - used,), bf)]).reshape(small_rows, 128)
    wqkv = jnp.concatenate([w_query, w_key, w_value], axis=1)
    wqkv_full, small_all, wo_full = gather_all([wqkv, small, w_out], 1)
    small_all = small_all.reshape(devices, small_rows * 128)
    starts = [sum(sizes[:i]) for i in range(5)]
    wr_full, attn_gain, ffn_gain, query_gain, key_gain = [small_all[:, o : o + n].reshape(-1) for o, n in zip(starts, sizes)]
    wr_full = wr_full.reshape(model_width, expert_count)
    attn_gain, ffn_gain, query_gain, key_gain = [g.astype(f32) for g in (attn_gain, ffn_gain, query_gain, key_gain)]
    cotangent, wo_full = lax.optimization_barrier((cotangent, wo_full))
    cot_all = lax.all_gather(cotangent, BOTH, axis=0, tiled=True)

    positions = shard_pos * tok_rows + jnp.arange(tok_rows, dtype=jnp.int32)
    inputs_f = hidden_in.astype(f32)
    normed_low = norm_rows(inputs_f, attn_gain).astype(bf)
    qkv = matmul(normed_low, wqkv_full)
    q_proj, k_proj, v_proj = qkv[:, :q_cols], qkv[:, q_cols : q_cols + kv_cols], qkv[:, q_cols + kv_cols :]
    k_rot, k_pull = jax.vjp(
        lambda projected, gain_vec: head_prep(projected, gain_vec, positions, HK, 1.0),
        k_proj,
        key_gain,
    )
    q_rot, q_pull = jax.vjp(
        lambda projected, gain_vec: head_prep(projected, gain_vec, positions, HQ, factor),
        q_proj,
        query_gain,
    )
    q_low = q_rot.astype(bf)
    kv_low = jnp.concatenate([k_rot.reshape(tok_rows, kv_cols).astype(bf), v_proj.astype(bf)], axis=1)
    allowed = jnp.arange(seq_len, dtype=jnp.int32)[None, :] <= positions[:, None]
    kv_all = line_gather(kv_low, 2)
    q_heads = q_low.reshape(tok_rows, HK, group_size, HD).transpose(1, 0, 2, 3)
    k_heads = kv_all[:, :kv_cols].reshape(seq_len, HK, HD).transpose(1, 0, 2)
    v_heads = kv_all[:, kv_cols:].reshape(seq_len, HK, HD).transpose(1, 0, 2)

    def attend(pieces):
        return head_forward(pieces[0], pieces[1], pieces[2], allowed)

    head_outs, totals = lax.map(attend, (q_heads, k_heads, v_heads))
    mix_low = head_outs.transpose(1, 0, 2, 3).reshape(tok_rows, q_cols).astype(bf)
    residual = inputs_f + matmul(mix_low, wo_full)
    ffn_low = norm_rows(residual, ffn_gain).astype(bf)

    logits = matmul(ffn_low, wr_full)
    expert_ids = jnp.arange(expert_count, dtype=jnp.int32)
    chosen = jnp.any(routes[:, :, None] == expert_ids[None, None, :], axis=1)
    raised_gate = jnp.where(chosen, jnp.exp(logits), 0.0)
    gates = raised_gate / jnp.sum(raised_gate, axis=-1, keepdims=True)
    gate_high = lax.reduce_precision(gates, 8, 7)
    gate_low = gates - gate_high
    extra = -(-3 * expert_count // 128) * 128
    payload = jnp.concatenate(
        [
            ffn_low,
            chosen.astype(bf),
            gate_high.astype(bf),
            gate_low.astype(bf),
            jnp.zeros((tok_rows, extra - 3 * expert_count), bf),
        ],
        axis=1,
    )
    (payload_all,) = gather_all([payload], 3)
    out_part, rows, gate_act, up_act = experts_forward(
        payload_all, w_gate, w_up, w_down, expert_count, tok_rows, capacity
    )
    moe_out = lax.psum_scatter(out_part, "expert", scatter_dimension=0, tiled=True)
    grad_part, grad_wgate, grad_wup, grad_wdown = experts_backward(
        payload_all, cot_all, rows, gate_act, up_act, w_gate, w_up, w_down, expert_count, tok_rows, capacity
    )
    (grad_sum,) = scatter_all([grad_part], 4)
    upstream = cotangent.astype(f32)
    grad_ffn = grad_sum[:, :model_width]
    grad_shares = (
        grad_sum[:, model_width : model_width + expert_count]
        + grad_sum[:, model_width + expert_count : model_width + 2 * expert_count]
    )
    grad_logits = (grad_shares - gates * jnp.sum(grad_shares, axis=-1, keepdims=True)).astype(bf)
    grad_wrouter = matmul_tn(ffn_low, grad_logits)
    grad_ffn = grad_ffn + matmul_nt(grad_logits, wr_full)
    grad_second, grad_ffn_gain = norm_back(residual, ffn_gain, grad_ffn)
    grad_residual = upstream + grad_second
    grad_attn_low = grad_residual.astype(bf)
    grad_wout = matmul_tn(mix_low, grad_attn_low).astype(bf)
    grad_mix = matmul_nt(grad_attn_low, wo_full).astype(bf)
    grad_mix, grad_wout = lax.optimization_barrier((grad_mix, grad_wout))
    out_grad = lax.psum_scatter(grad_wout, "expert", scatter_dimension=0, tiled=True)
    out_grad = lax.psum_scatter(out_grad, "shard", scatter_dimension=0, tiled=True).astype(f32)
    grad_heads = grad_mix.reshape(tok_rows, HK, group_size, HD).transpose(1, 0, 2, 3)

    def attend_back(pieces):
        return head_backward(pieces[0], pieces[1], pieces[2], pieces[3], pieces[4], allowed)

    grad_qheads, grad_kheads, grad_vheads = lax.map(
        attend_back, (q_heads, k_heads, v_heads, totals, grad_heads)
    )
    grad_q_rot = grad_qheads.transpose(1, 0, 2, 3).reshape(tok_rows, HQ, HD)
    grad_kv = jnp.concatenate(
        [
            grad_kheads.transpose(1, 0, 2).reshape(seq_len, kv_cols).astype(bf),
            grad_vheads.transpose(1, 0, 2).reshape(seq_len, kv_cols).astype(bf),
        ],
        axis=1,
    )
    grad_kv = line_scatter(grad_kv, 6)
    grad_kv, moe_out = lax.optimization_barrier((grad_kv, moe_out))
    moe_out = lax.psum_scatter(moe_out, "shard", scatter_dimension=0, tiled=True).astype(f32)
    block_out = (residual + moe_out).astype(bf)
    grad_q_proj, grad_query_gain = q_pull(grad_q_rot)
    grad_k_proj, grad_key_gain = k_pull(grad_kv[:, :kv_cols].reshape(tok_rows, HK, HD))
    grad_qkv_low = jnp.concatenate(
        [grad_q_proj.astype(bf), grad_k_proj.astype(bf), grad_kv[:, kv_cols:].astype(bf)], axis=1
    )
    grad_wqkv = matmul_tn(normed_low, grad_qkv_low).astype(bf)
    grad_normed = matmul_nt(grad_qkv_low, wqkv_full)
    grad_front, grad_attn_gain = norm_back(inputs_f, attn_gain, grad_normed)
    grad_input = (grad_residual + grad_front).astype(bf)

    grads = [grad_wrouter, grad_attn_gain, grad_ffn_gain, grad_query_gain, grad_key_gain]
    packed = jnp.concatenate(
        [g.astype(bf).reshape(devices, -1) for g in grads] + [jnp.zeros((devices, small_rows * 128 - used), bf)], axis=1
    ).reshape(devices * small_rows, 128)
    qkv_grad, small_grad = scatter_all([grad_wqkv, packed], 8)
    small_grad = small_grad.reshape(-1)
    router_g, attn_g, ffn_g, query_g, key_g = [small_grad[o : o + n] for o, n in zip(starts, sizes)]
    return (
        block_out,
        grad_input,
        attn_g,
        qkv_grad[:, :q_cols],
        qkv_grad[:, q_cols : q_cols + kv_cols],
        qkv_grad[:, q_cols + kv_cols :],
        query_g,
        key_g,
        out_grad,
        ffn_g,
        router_g.reshape(w_router.shape),
        grad_wgate,
        grad_wup,
        grad_wdown,
    )


def solution(mesh):
    row = P(BOTH, None)
    vec = P(BOTH)
    cube = P(BOTH, None, None)
    in_specs = (row, vec, row, row, row, vec, vec, row, vec, row, cube, cube, cube, row, row)
    out_specs = (row, row, vec, row, row, row, vec, vec, row, vec, row, cube, cube, cube)
    return jax.shard_map(
        per_device, mesh=mesh, in_specs=in_specs, out_specs=out_specs, check_vma=False
    )
```

```python
import functools

import jax
import jax.numpy as jnp
from jax import lax
from jax.experimental import pallas as pl
from jax.experimental.pallas import tpu as pltpu
from jax.sharding import PartitionSpec as P

MESH = pl.DeviceIdType.MESH
NZ = 4

def placed():
    return lax.axis_size("expert") == 8 and lax.axis_size("shard") == NZ

def place():
    e = lax.axis_index("expert"); s = lax.axis_index("shard")
    return e // 4, lax.rem(e // 2, 2), lax.rem(e, 2), s

def dev(y, x, c, s):
    return (y * 4 + x * 2 + c, s)

def barrier_all(y, x, c, s):
    bar = pltpu.get_barrier_semaphore()
    def sig(d): pl.semaphore_signal(bar, inc=1, device_id=d, device_id_type=MESH)
    sig(dev(1 - y, x, c, s)); sig(dev(y, 1 - x, c, s)); sig(dev(y, x, 1 - c, s))
    @pl.when(s > 0)
    def _(): sig(dev(y, x, c, s - 1))
    @pl.when(s < NZ - 1)
    def _(): sig(dev(y, x, c, s + 1))
    pl.semaphore_wait(bar, 3 + jnp.where(s > 0, 1, 0) + jnp.where(s < NZ - 1, 1, 0))

def ag_kernel(n_arr, n_line, *refs):
    n_all = n_arr + n_line
    ins = refs[:n_all]; outs = refs[n_all:2 * n_all]
    loc_sem, zs, zr, ps, pr, cs, cr = refs[2 * n_all:]
    y, x, c, s = place()
    barrier_all(y, x, c, s)
    def rc(src, dst, ss, rs, d):
        return pltpu.make_async_remote_copy(src_ref=src, dst_ref=dst, send_sem=ss, recv_sem=rs, device_id=d, device_id_type=MESH)
    X = dev(y, 1 - x, c, s); Y = dev(1 - y, x, c, s); C = dev(y, x, 1 - c, s)
    A = range(n_arr)
    every = range(n_all)
    def home(a, zz):
        return outs[a].at[y, x, c, zz] if a < n_arr else outs[a].at[zz]
    steps = [(0, 0)] + [(d, g) for d in range(1, NZ) for g in (1, -1)]
    def valid(d, g):
        return (s >= d) if g == 1 else (s + d <= NZ - 1)
    def zof(d, g): return s - d * g
    def src_own(a, h, zz, k):
        return ins[a].at[h] if k == 0 else home(a, zz).at[h]
    def zcopy(a, h, zz, k, g):
        kk = 1 + 2 * (k_dist(k)) + (0 if g == 1 else 1)
        return rc(src_own(a, h, zz, k), home(a, zz).at[h], zs.at[a, h, kk], zr.at[a, h, kk], dev(y, x, c, s + g))
    def k_dist(k): return steps[k][0]
    def plane(a, h, zz, k, which):
        return rc(src_own(a, h, zz, k), outs[a].at[y, x, c, zz, h], ps.at[a, k, h, which], pr.at[a, k, h, which], X if which == 0 else Y)
    def plane_recv(a, h, zz, k, which):
        d = outs[a].at[y, 1 - x, c, zz, h] if which == 0 else outs[a].at[1 - y, x, c, zz, h]
        return rc(d, d, ps.at[a, k, h, which], pr.at[a, k, h, which], X if which == 0 else Y)
    def diag(a, h, zz, k):
        d = outs[a].at[y, 1 - x, c, zz, h] if h == 0 else outs[a].at[1 - y, x, c, zz, h]
        return rc(d, d, ps.at[a, k, h, 2], pr.at[a, k, h, 2], Y if h == 0 else X)
    def diag_recv(a, h, zz, k):
        d = outs[a].at[1 - y, 1 - x, c, zz, h]
        return rc(d, d, ps.at[a, k, h, 2], pr.at[a, k, h, 2], Y if h == 0 else X)
    def core(a, zz, k, part):
        d = outs[a].at[:, :, c, zz]
        return rc(d, d, cs.at[a, k], cr.at[a, k], C)
    def core_recv(a, zz, k):
        d = outs[a].at[:, :, 1 - c, zz]
        return rc(d, d, cs.at[a, k], cr.at[a, k], C)
    def loc(a):
        return pltpu.make_async_copy(ins[a], home(a, s), loc_sem.at[a])

    def when(k, f):
        d, g = steps[k]
        if k == 0: f()
        else: pl.when(valid(d, g))(f)

    def stage_a(k):
        d, g = steps[k]
        def go():
            zz = zof(d, g)
            for a in every:
                for h in range(2):
                    if k:
                        kk = k
                        dref = home(a, zz).at[h]
                        rc(dref, dref, zs.at[a, h, kk], zr.at[a, h, kk], X).wait_recv()
                    for gg in ((1, -1) if k == 0 else (g,)):
                        okc = (s < NZ - 1) if gg == 1 else (s > 0)
                        if d + 1 < NZ:
                            @pl.when(okc)
                            def _(): zcopy(a, h, zz, k, gg).start()
                    if a < n_arr:
                        plane(a, h, zz, k, 0).start()
                        plane(a, h, zz, k, 1).start()
        when(k, go)
    def stage_b(k):
        d, g = steps[k]
        def go():
            zz = zof(d, g)
            for a in A:
                plane_recv(a, 0, zz, k, 0).wait_recv()
                diag(a, 0, zz, k).start()
                plane_recv(a, 1, zz, k, 1).wait_recv()
                diag(a, 1, zz, k).start()
        when(k, go)
    def stage_c(k):
        d, g = steps[k]
        def go():
            zz = zof(d, g)
            for a in A:
                if k == 0: loc(a).wait()
                plane_recv(a, 1, zz, k, 0).wait_recv()
                plane_recv(a, 0, zz, k, 1).wait_recv()
                diag_recv(a, 0, zz, k).wait_recv()
                diag_recv(a, 1, zz, k).wait_recv()
                core(a, zz, k, 0).start()
        when(k, go)
    for a in every: loc(a).start()
    n = len(steps)
    for i in range(n + 2):
        if i < n: stage_a(i)
        if 0 <= i - 1 < n: stage_b(i - 1)
        if 0 <= i - 2 < n: stage_c(i - 2)
    for k in range(n):
        d, g = steps[k]
        def go():
            zz = zof(d, g)
            for a in every:
                if a < n_arr:
                    core_recv(a, zz, k).wait_recv()
                    core(a, zz, k, 0).wait_send()
                elif k == 0: loc(a).wait()
                for h in range(2):
                    for gg in ((1, -1) if k == 0 else (g,)):
                        okc = (s < NZ - 1) if gg == 1 else (s > 0)
                        if d + 1 < NZ:
                            @pl.when(okc)
                            def _(): zcopy(a, h, zz, k, gg).wait_send()
                    if a < n_arr:
                        plane(a, h, zz, k, 0).wait_send()
                        plane(a, h, zz, k, 1).wait_send()
                        diag(a, h, zz, k).wait_send()
        when(k, go)

def ag32(arrs, cid, line=()):
    ins = [a.reshape(2, a.shape[0] // 2, a.shape[1]) for a in list(arrs) + list(line)]
    n, m = len(arrs), len(line); nk = 7
    outs = pl.pallas_call(
        functools.partial(ag_kernel, n, m),
        out_shape=[jax.ShapeDtypeStruct(((2, 2, 2, NZ) if i < n else (NZ,)) + a.shape, a.dtype) for i, a in enumerate(ins)],
        in_specs=[pl.BlockSpec(memory_space=pltpu.VMEM)] * (n + m),
        out_specs=[pl.BlockSpec(memory_space=pl.ANY)] * (n + m),
        scratch_shapes=[pltpu.SemaphoreType.DMA((n + m,)),
            pltpu.SemaphoreType.DMA((n + m, 2, 9)), pltpu.SemaphoreType.DMA((n + m, 2, 9)),
            pltpu.SemaphoreType.DMA((n, nk, 2, 3)), pltpu.SemaphoreType.DMA((n, nk, 2, 3)),
            pltpu.SemaphoreType.DMA((n, nk)), pltpu.SemaphoreType.DMA((n, nk))],
        compiler_params=pltpu.CompilerParams(collective_id=cid, has_side_effects=True, vmem_limit_bytes=64000 * 1024),
        name="gather_all",
    )(*ins)
    return [o.reshape(-1, a.shape[1] * 2, a.shape[2]) for o, a in zip(outs, ins)]

ZORDER = (0, 3, 1, 2)
LAGS = (1, 1, 1, 1)

def rs_kernel(n_arr, parts, *refs):
    ins = refs[:n_arr]; outs = refs[n_arr:2 * n_arr]
    sc = refs[2 * n_arr:]
    own_b, r0_b, ra_b, rb_b, zu_b, zd_b = [sc[i * n_arr:(i + 1) * n_arr] for i in range(6)]
    lsem, s0s, s0r, sas, sar, sbs, sbr, zus, zur, zds, zdr = sc[6 * n_arr:]
    y, x, c, s = place()
    barrier_all(y, x, c, s)
    X = dev(y, 1 - x, c, s); Y = dev(1 - y, x, c, s); C = dev(y, x, 1 - c, s)
    UP = dev(y, x, c, s + 1); DN = dev(y, x, c, s - 1)
    def rc(src, dst, ss, rs, d):
        return pltpu.make_async_remote_copy(src_ref=src, dst_ref=dst, send_sem=ss, recv_sem=rs, device_id=d, device_id_type=MESH)
    units = [(a, zz, h) for zz in ZORDER for h in range(parts) for a in range(n_arr)]
    def jj(zz, h): return ZORDER.index(zz) * parts + h
    def load(a, zz, h):
        j = jj(zz, h)
        return pltpu.make_async_copy(ins[a].at[:, :, c, zz, h], own_b[a].at[j], lsem.at[a, j])
    def c0(a, zz, h):
        j = jj(zz, h)
        return rc(ins[a].at[:, :, 1 - c, zz, h], r0_b[a].at[j], s0s.at[a, j], s0r.at[a, j], C)
    def ca(a, zz, h):
        j = jj(zz, h)
        if h % 2 == 0: return rc(own_b[a].at[j, :, 1 - x], ra_b[a].at[j], sas.at[a, j], sar.at[a, j], X)
        return rc(own_b[a].at[j, 1 - y], ra_b[a].at[j], sas.at[a, j], sar.at[a, j], Y)
    def cb(a, zz, h):
        j = jj(zz, h)
        if h % 2 == 0: return rc(own_b[a].at[j, 1 - y, x], rb_b[a].at[j], sbs.at[a, j], sbr.at[a, j], Y)
        return rc(own_b[a].at[j, y, 1 - x], rb_b[a].at[j], sbs.at[a, j], sbr.at[a, j], X)
    def cu(a, zz, h):
        j = jj(zz, h)
        return rc(own_b[a].at[j, y, x], zu_b[a].at[j], zus.at[a, j], zur.at[a, j], UP)
    def cd(a, zz, h):
        j = jj(zz, h)
        return rc(own_b[a].at[j, y, x], zd_b[a].at[j], zds.at[a, j], zdr.at[a, j], DN)
    def add_into(dst, other):
        rows = dst.shape[0]
        st = 16 if rows % 16 == 0 else rows
        @pl.loop(0, rows // st)
        def _(i):
            r = pl.ds(i * st, st)
            dst[r, :] = (dst[r, :].astype(jnp.float32) + other[r, :].astype(jnp.float32)).astype(dst.dtype)
    def stage0(u):
        a, zz, h = u; j = jj(zz, h)
        load(a, zz, h).wait()
        c0(a, zz, h).wait_recv()
        for yy in range(2):
            for xx in range(2):
                add_into(own_b[a].at[j, yy, xx], r0_b[a].at[j, yy, xx])
        ca(a, zz, h).start()
    def stage1(u):
        a, zz, h = u; j = jj(zz, h)
        ca(a, zz, h).wait_recv()
        for q in range(2):
            if h % 2 == 0: add_into(own_b[a].at[j, q, x], ra_b[a].at[j, q])
            else: add_into(own_b[a].at[j, y, q], ra_b[a].at[j, q])
        cb(a, zz, h).start()
    def stage2(u):
        a, zz, h = u; j = jj(zz, h)
        cb(a, zz, h).wait_recv()
        add_into(own_b[a].at[j, y, x], rb_b[a].at[j])
    def hop(u, k):
        a, zz, h = u; j = jj(zz, h)
        if k < zz:
            @pl.when(s == k)
            def _():
                if k > 0:
                    cu(a, zz, h).wait_recv()
                    add_into(own_b[a].at[j, y, x], zu_b[a].at[j])
                cu(a, zz, h).start()
        t = NZ - 1 - k
        if t > zz:
            @pl.when(s == t)
            def _():
                if k > 0:
                    cd(a, zz, h).wait_recv()
                    add_into(own_b[a].at[j, y, x], zd_b[a].at[j])
                cd(a, zz, h).start()
    def last(u):
        a, zz, h = u; j = jj(zz, h)
        @pl.when(s == zz)
        def _():
            if zz > 0: cu(a, zz, h).wait_recv()
            if zz < NZ - 1: cd(a, zz, h).wait_recv()
            t = own_b[a][j, y, x].astype(jnp.float32)
            if zz > 0: t = t + zu_b[a][j].astype(jnp.float32)
            if zz < NZ - 1: t = t + zd_b[a][j].astype(jnp.float32)
            outs[a][h] = t.astype(outs[a].dtype)
    for u in units:
        c0(*u).start(); load(*u).start()
    n = len(units)
    L1 = LAGS[0] * n_arr; L2 = L1 + LAGS[1] * n_arr; L3 = L2 + LAGS[2] * n_arr; dl = LAGS[3] * n_arr
    for i in range(n + L3 + (NZ - 1) * dl):
        if i < n: stage0(units[i])
        if 0 <= i - L1 < n: stage1(units[i - L1])
        if 0 <= i - L2 < n: stage2(units[i - L2])
        for k in range(NZ - 1):
            if 0 <= i - L3 - k * dl < n: hop(units[i - L3 - k * dl], k)
    for u in units: last(u)
    for u in units:
        c0(*u).wait_send(); ca(*u).wait_send(); cb(*u).wait_send()
        zz = u[1]
        if zz > 0:
            @pl.when(s < zz)
            def _(): cu(*u).wait_send()
        if zz < NZ - 1:
            @pl.when(s > zz)
            def _(): cd(*u).wait_send()

def rs32(arrs, cid, out_dtype=jnp.float32, parts=4):
    n = len(arrs)
    if any(a.shape[1] % (parts * 16) for a in arrs): parts = 2
    ins = [a.reshape(2, 2, 2, NZ, parts, a.shape[1] // parts, a.shape[2]) for a in arrs]
    hs = [i.shape[-2:] for i in ins]
    V = pltpu.VMEM; bt = jnp.bfloat16; m = NZ * parts
    sems = [pltpu.SemaphoreType.DMA((n, m))] * 11
    outs = pl.pallas_call(
        functools.partial(rs_kernel, n, parts),
        out_shape=[jax.ShapeDtypeStruct((parts,) + h, out_dtype) for h in hs],
        in_specs=[pl.BlockSpec(memory_space=pl.ANY)] * n,
        out_specs=[pl.BlockSpec(memory_space=pltpu.VMEM)] * n,
        scratch_shapes=[V((m, 2, 2) + h, bt) for h in hs] + [V((m, 2, 2) + h, bt) for h in hs] + [V((m, 2) + h, bt) for h in hs]
            + [V((m,) + h, bt) for h in hs] + [V((m,) + h, bt) for h in hs] + [V((m,) + h, bt) for h in hs] + sems,
        compiler_params=pltpu.CompilerParams(collective_id=cid, has_side_effects=True, vmem_limit_bytes=64000 * 1024),
        name="scatter_all",
    )(*ins)
    return [o.reshape(a.shape[1], a.shape[2]) for o, a in zip(outs, arrs)]

def line_barrier(y, x, c, s):
    bar = pltpu.get_barrier_semaphore()
    @pl.when(s > 0)
    def _(): pl.semaphore_signal(bar, inc=1, device_id=dev(y, x, c, s - 1), device_id_type=MESH)
    @pl.when(s < NZ - 1)
    def _(): pl.semaphore_signal(bar, inc=1, device_id=dev(y, x, c, s + 1), device_id_type=MESH)
    pl.semaphore_wait(bar, jnp.where(s > 0, 1, 0) + jnp.where(s < NZ - 1, 1, 0))

def line_gather_kernel(parts, x_ref, o_ref, ss, rs):
    y, x, c, s = place()
    line_barrier(y, x, c, s)
    def cp(d, g, h):
        src = x_ref.at[h] if d == 0 else o_ref.at[s - d * g, h]
        k = 0 if g == 1 else 1
        return pltpu.make_async_remote_copy(src_ref=src, dst_ref=o_ref.at[s - d * g, h], send_sem=ss.at[k, d, h], recv_sem=rs.at[k, d, h],
            device_id=dev(y, x, c, s + g), device_id_type=MESH)
    def arrived(d, g, h):
        k = 0 if g == 1 else 1
        ref = o_ref.at[s - (d + 1) * g, h]
        return pltpu.make_async_remote_copy(src_ref=ref, dst_ref=ref, send_sem=ss.at[k, d, h], recv_sem=rs.at[k, d, h],
            device_id=dev(y, x, c, s + g), device_id_type=MESH)
    def sends(d, g): return (s >= d) & (s < NZ - 1) if g == 1 else (s + d <= NZ - 1) & (s > 0)
    def gets(d, g): return s >= d + 1 if g == 1 else s + d + 1 <= NZ - 1
    for d in range(NZ):
        for h in range(parts):
            for g in (1, -1):
                if d:
                    @pl.when(gets(d - 1, g))
                    def _(): arrived(d - 1, g, h).wait_recv()
                if d < NZ - 1:
                    @pl.when(sends(d, g))
                    def _(): cp(d, g, h).start()
        if d == 0: o_ref[s] = x_ref[...]
    for d in range(NZ - 1):
        for h in range(parts):
            for g in (1, -1):
                @pl.when(sends(d, g))
                def _(): cp(d, g, h).wait_send()

def line_gather(x, cid, parts=4):
    if not placed():
        return lax.all_gather(x, "shard", axis=0, tiled=True)
    R, C = x.shape
    sem = pltpu.SemaphoreType.DMA((2, NZ, parts))
    o = pl.pallas_call(functools.partial(line_gather_kernel, parts), out_shape=jax.ShapeDtypeStruct((NZ, parts, R // parts, C), x.dtype),
        in_specs=[pl.BlockSpec(memory_space=pltpu.VMEM)], out_specs=pl.BlockSpec(memory_space=pltpu.VMEM),
        scratch_shapes=[sem, sem], compiler_params=pltpu.CompilerParams(collective_id=cid, has_side_effects=True, vmem_limit_bytes=16 << 20),
        name="line_gather")(x.reshape(parts, R // parts, C))
    return o.reshape(NZ * R, C)

def line_scatter_kernel(parts, p_ref, o_ref, acc, zu, zd, ss_u, rs_u, ss_d, rs_d):
    y, x, c, s = place()
    line_barrier(y, x, c, s)
    def rc(src, dst, a, b, d):
        return pltpu.make_async_remote_copy(src_ref=src, dst_ref=dst, send_sem=a, recv_sem=b, device_id=d, device_id_type=MESH)
    def cu(zz, h, k):
        src = p_ref.at[zz, h] if k == 0 else acc.at[zz, h]
        return rc(src, zu.at[zz, h], ss_u.at[zz, h], rs_u.at[zz, h], dev(y, x, c, s + 1))
    def cd(zz, h, k):
        src = p_ref.at[zz, h] if k == 0 else acc.at[zz, h]
        return rc(src, zd.at[zz, h], ss_d.at[zz, h], rs_d.at[zz, h], dev(y, x, c, s - 1))
    st = 32
    def total(dst, refs):
        @pl.loop(0, dst.shape[0] // st)
        def _(i):
            r = pl.ds(i * st, st)
            t = refs[0][r, :].astype(jnp.float32)
            for f in refs[1:]: t = t + f[r, :].astype(jnp.float32)
            dst[r, :] = t.astype(dst.dtype)
    ups = [(zz, h) for zz in (3, 2, 1) for h in range(parts)]
    dns = [(zz, h) for zz in (0, 1, 2) for h in range(parts)]
    n = len(ups)
    for i in range(n + NZ):
        for k in range(NZ - 1):
            if 0 <= i - k < n:
                zz, h = ups[i - k]
                if k < zz:
                    @pl.when(s == k)
                    def _():
                        if k:
                            cu(zz, h, k).wait_recv()
                            total(acc.at[zz, h], [p_ref.at[zz, h], zu.at[zz, h]])
                        cu(zz, h, k).start()
                zz, h = dns[i - k]
                if NZ - 1 - k > zz:
                    @pl.when(s == NZ - 1 - k)
                    def _():
                        if k:
                            cd(zz, h, k).wait_recv()
                            total(acc.at[zz, h], [p_ref.at[zz, h], zd.at[zz, h]])
                        cd(zz, h, k).start()
    for zz in range(NZ):
        @pl.when(s == zz)
        def _():
            for h in range(parts):
                refs = [p_ref.at[zz, h]]
                if zz > 0:
                    cu(zz, h, 1).wait_recv()
                    refs.append(zu.at[zz, h])
                if zz < NZ - 1:
                    cd(zz, h, 1).wait_recv()
                    refs.append(zd.at[zz, h])
                total(o_ref.at[h], refs)
    for zz, h in ups:
        @pl.when(s < zz)
        def _(): cu(zz, h, 1).wait_send()
    for zz, h in dns:
        @pl.when(s > zz)
        def _(): cd(zz, h, 1).wait_send()

def line_scatter(p, cid, parts=4):
    if not placed():
        return lax.psum_scatter(p, "shard", scatter_dimension=0, tiled=True).astype(jnp.float32)
    R, C = p.shape[0] // NZ, p.shape[1]
    sem = pltpu.SemaphoreType.DMA((NZ, parts))
    shape = (NZ, parts, R // parts, C)
    buf = pltpu.VMEM(shape, p.dtype)
    o = pl.pallas_call(functools.partial(line_scatter_kernel, parts), out_shape=jax.ShapeDtypeStruct(shape[1:], jnp.float32),
        in_specs=[pl.BlockSpec(memory_space=pltpu.VMEM)], out_specs=pl.BlockSpec(memory_space=pltpu.VMEM),
        scratch_shapes=[buf, buf, buf, sem, sem, sem, sem], compiler_params=pltpu.CompilerParams(collective_id=cid, has_side_effects=True, vmem_limit_bytes=24 << 20),
        name="line_scatter")(p.reshape(shape))
    return o.reshape(R, C)


def dot(a, b, ca, cb):
    return lax.dot_general(a, b, (((ca,), (cb,)), ((), ())), preferred_element_type=jnp.float32)

def token_picks(meta, experts, slots, me):
    SB, WM = meta.shape
    bf, f32 = jnp.bfloat16, jnp.float32
    tri = (lax.broadcasted_iota(jnp.int32, (SB, SB), 1) < lax.broadcasted_iota(jnp.int32, (SB, SB), 0)).astype(bf)
    lane = lax.broadcasted_iota(jnp.int32, (SB, WM), 1)
    cnt = dot(tri, meta, 1, 0)
    metaf = meta.astype(f32)
    msk = jnp.sum(jnp.where(lane == me, metaf, 0.0), axis=-1, keepdims=True)
    pos = jnp.sum(jnp.where(lane == me, cnt, 0.0), axis=-1, keepdims=True)
    gate = jnp.sum(jnp.where((lane == me + experts) | (lane == me + 2 * experts), metaf, 0.0), axis=-1, keepdims=True)
    want = jnp.where(msk > 0.0, pos, -1.0).astype(jnp.int32)
    pick = (want == lax.broadcasted_iota(jnp.int32, (SB, slots), 1)).astype(bf)
    return pick, gate

def forward_kernel(experts, slots, SB, x_ref, wg_hbm, wu_hbm, wd_hbm, out_ref, rows_ref, ga_ref, ua_ref, wg, wu, wd, wsem):
    bf = jnp.bfloat16
    step = pl.program_id(0)
    nsub = x_ref.shape[0] // SB
    D = out_ref.shape[1]
    me = lax.axis_index(("expert", "shard"))
    loads = [pltpu.make_async_copy(h.at[0], v, wsem.at[i]) for i, (h, v) in enumerate(((wg_hbm, wg), (wu_hbm, wu), (wd_hbm, wd)))]
    @pl.when(step == 0)
    def _():
        for l in loads: l.start()
    picks, gates = [], []
    for i in range(nsub):
        r = pl.ds(i * SB, SB)
        pick, gate = token_picks(x_ref[r, D:], experts, slots, me)
        picks.append(pick); gates.append(gate)
        rows_ref[i * slots:(i + 1) * slots, :] = dot(pick, x_ref[r, :D], 0, 0).astype(bf)
    @pl.when(step == 0)
    def _():
        for l in loads: l.wait()
    ga = dot(rows_ref[...], wg[...], 1, 0)
    ua = dot(rows_ref[...], wu[...], 1, 0)
    ga_ref[...] = ga
    ua_ref[...] = ua
    hid = (ga * (1.0 / (1.0 + jnp.exp(-ga))) * ua).astype(bf)
    eo = dot(hid, wd[...], 1, 0).astype(bf)
    for i in range(nsub):
        r = pl.ds(i * SB, SB)
        tok = dot(picks[i], eo[i * slots:(i + 1) * slots, :], 1, 0)
        out_ref[r, :] = (gates[i] * tok).astype(bf)

def backward_kernel(experts, slots, SB, meta_ref, cot_ref, rows_ref, ga_ref, ua_ref, wg_hbm, wu_hbm, wd_hbm, gr_ref, dwg_hbm, dwu_hbm, dwd_hbm,
                  wg, wu, wd, dwg, dwu, dwd, gp, wsem, osem):
    bf = jnp.bfloat16
    step = pl.program_id(0)
    nsub = cot_ref.shape[0] // SB
    D = cot_ref.shape[1]
    WM = meta_ref.shape[1]
    me = lax.axis_index(("expert", "shard"))
    loads = [pltpu.make_async_copy(h.at[0], v, wsem.at[i]) for i, (h, v) in enumerate(((wg_hbm, wg), (wu_hbm, wu), (wd_hbm, wd)))]
    @pl.when(step == 0)
    def _():
        for l in loads: l.start()
        for a in (dwg, dwu, dwd): a[...] = jnp.zeros_like(a)
    picks = []
    for i in range(nsub):
        r = pl.ds(i * SB, SB)
        pick, gate = token_picks(meta_ref[r, :], experts, slots, me)
        picks.append(pick)
        gcot = (gate * cot_ref[r, :].astype(jnp.float32)).astype(bf)
        gp[i * slots:(i + 1) * slots, :] = dot(pick, gcot, 0, 0).astype(bf)
    @pl.when(step == 0)
    def _():
        for l in loads: l.wait()
    ga = ga_ref[...]
    ua = ua_ref[...]
    sig = 1.0 / (1.0 + jnp.exp(-ga))
    act = ga * sig
    hidf = act * ua
    hid = hidf.astype(bf)
    gh = dot(gp[...], wd[...], 1, 1)
    share = jnp.sum(gh * hid.astype(jnp.float32), axis=-1, keepdims=True)
    dga = (gh * ua * (sig * (1.0 + ga * (1.0 - sig)))).astype(bf)
    dua = (gh * act).astype(bf)
    dwd[...] += dot(hid, gp[...], 0, 0)
    grow = (dot(dga, wg[...], 1, 1) + dot(dua, wu[...], 1, 1)).astype(bf)
    dwg[...] += dot(rows_ref[...], dga, 0, 0)
    dwu[...] += dot(rows_ref[...], dua, 0, 0)
    lane = lax.broadcasted_iota(jnp.int32, (share.shape[0], WM), 1)
    high = share.astype(bf).astype(jnp.float32)
    tail = (jnp.where(lane == me, high, 0.0) + jnp.where(lane == me + experts, share - high, 0.0)).astype(bf)
    for i in range(nsub):
        r = pl.ds(i * SB, SB)
        q = slice(i * slots, (i + 1) * slots)
        gr_ref[r, :D] = dot(picks[i], grow[q, :], 1, 0).astype(bf)
        gr_ref[r, D:] = dot(picks[i], tail[q, :], 1, 0).astype(bf)
    @pl.when(step == pl.num_programs(0) - 1)
    def _():
        outs = [pltpu.make_async_copy(v, h.at[0], osem.at[i]) for i, (v, h) in enumerate(((dwg, dwg_hbm), (dwu, dwu_hbm), (dwd, dwd_hbm)))]
        for o in outs: o.start()
        for o in outs: o.wait()

def experts_forward(x_all, w_gate, w_up, w_down, experts, block, capacity, TB=512, SB=256):
    T, C = x_all.shape; D, F = w_gate.shape[1:]
    slots = max(SB // block, 1) * capacity
    total = TB // SB * slots
    S = T // SB * slots
    any_ = pl.BlockSpec(memory_space=pl.ANY)
    V = pltpu.VMEM; bf = jnp.bfloat16; f32 = jnp.float32
    blk = lambda r, c: pl.BlockSpec((r, c), lambda i: (i, 0))
    return pl.pallas_call(
        functools.partial(forward_kernel, experts, slots, SB),
        grid=(T // TB,),
        out_shape=[jax.ShapeDtypeStruct((T, D), bf), jax.ShapeDtypeStruct((S, D), bf), jax.ShapeDtypeStruct((S, F), f32), jax.ShapeDtypeStruct((S, F), f32)],
        in_specs=[blk(TB, C), any_, any_, any_],
        out_specs=[blk(TB, D), blk(total, D), blk(total, F), blk(total, F)],
        scratch_shapes=[V((D, F), bf), V((D, F), bf), V((F, D), bf), pltpu.SemaphoreType.DMA((3,))],
        compiler_params=pltpu.CompilerParams(dimension_semantics=("arbitrary",), vmem_limit_bytes=65000 * 1024),
        cost_estimate=pl.CostEstimate(flops=48_000_000_000, bytes_accessed=130_000_000, transcendentals=0),
        name="experts_forward",
    )(x_all, w_gate, w_up, w_down)

def experts_backward(x_all, cot_all, rows, ga, ua, w_gate, w_up, w_down, experts, block, capacity, TB=512, SB=256):
    T, C = x_all.shape; D, F = w_gate.shape[1:]
    slots = max(SB // block, 1) * capacity
    total = TB // SB * slots
    WM = C - D
    any_ = pl.BlockSpec(memory_space=pl.ANY)
    V = pltpu.VMEM; bf = jnp.bfloat16; f32 = jnp.float32
    blk = lambda r, c: pl.BlockSpec((r, c), lambda i: (i, 0))
    meta = pl.BlockSpec((TB, WM), lambda i: (i, D // WM)) if D % WM == 0 else blk(TB, WM)
    meta_in = x_all if D % WM == 0 else x_all[:, D:]
    return pl.pallas_call(
        functools.partial(backward_kernel, experts, slots, SB),
        grid=(T // TB,),
        out_shape=[jax.ShapeDtypeStruct((T, C), bf), jax.ShapeDtypeStruct(w_gate.shape, f32), jax.ShapeDtypeStruct(w_up.shape, f32), jax.ShapeDtypeStruct(w_down.shape, f32)],
        in_specs=[meta, blk(TB, D), blk(total, D), blk(total, F), blk(total, F), any_, any_, any_],
        out_specs=[blk(TB, C), any_, any_, any_],
        scratch_shapes=[V((D, F), bf), V((D, F), bf), V((F, D), bf), V((D, F), f32), V((D, F), f32), V((F, D), f32), V((total, D), bf), pltpu.SemaphoreType.DMA((3,)), pltpu.SemaphoreType.DMA((3,))],
        compiler_params=pltpu.CompilerParams(dimension_semantics=("arbitrary",), vmem_limit_bytes=65000 * 1024),
        cost_estimate=pl.CostEstimate(flops=85_000_000_000, bytes_accessed=150_000_000, transcendentals=0),
        name="experts_backward",
    )(meta_in, cot_all, rows, ga, ua, w_gate, w_up, w_down)


def rope_tables(seq_len):
    half = HD // 2
    frequency = theta_base ** (-2.0 * jnp.arange(half, dtype=jnp.float32) / HD)
    angles = jnp.arange(seq_len, dtype=jnp.float32)[:, None] * frequency[None, :]
    return jnp.concatenate([jnp.cos(angles)] * 2, axis=-1), jnp.concatenate([-jnp.sin(angles), jnp.sin(angles)], axis=-1)

def turn(u, cos, sin):
    return u * cos + pltpu.roll(u, HD // 2, 1) * sin

def scale_of(u):
    return lax.rsqrt(jnp.mean(u * u, axis=-1, keepdims=True) + epsilon)

def attention_forward_kernel(group, q_ref, k_ref, v_ref, gq_ref, gk_ref, cos_ref, sin_ref, ql_ref, kl_ref, vl_ref, mix_ref):
    bf, f32 = jnp.bfloat16, jnp.float32
    rows, seq = q_ref.shape[0], k_ref.shape[0]
    first = lax.axis_index("shard") * rows
    k = k_ref[...]
    kl_ref[...] = turn(k * scale_of(k) * gk_ref[...], cos_ref[...], sin_ref[...]).astype(bf)
    vl_ref[...] = v_ref[...].astype(bf)
    cos, sin = cos_ref[pl.ds(first, rows), :], sin_ref[pl.ds(first, rows), :]
    allowed = lax.broadcasted_iota(jnp.int32, (rows, seq), 1) <= first + lax.broadcasted_iota(jnp.int32, (rows, seq), 0)
    for j in range(group):
        cols = slice(j * HD, (j + 1) * HD)
        u = q_ref[:, cols]
        ql = (turn(u * scale_of(u) * gq_ref[...], cos, sin) * HD ** (-0.5)).astype(bf)
        ql_ref[:, cols] = ql
        scores = dot(ql, kl_ref[...], 1, 1)
        raised = jnp.where(allowed, jnp.exp(scores), 0.0)
        probs = (raised * (1.0 / jnp.sum(raised, axis=-1, keepdims=True))).astype(bf)
        mix_ref[:, cols] = dot(probs, vl_ref[...], 1, 0).astype(bf)

def attention_forward(q_proj, kv_proj, gq, gk, cos, sin):
    rows, seq = q_proj.shape[0], kv_proj.shape[0]
    group = HQ // HK
    bf = jnp.bfloat16
    whole = lambda a: pl.BlockSpec(a.shape, lambda i: (0, 0))
    gq, gk = gq[None, :], gk[None, :]
    return pl.pallas_call(
        functools.partial(attention_forward_kernel, group),
        grid=(HK,),
        out_shape=[jax.ShapeDtypeStruct(q_proj.shape, bf), jax.ShapeDtypeStruct((seq, HK * HD), bf), jax.ShapeDtypeStruct((seq, HK * HD), bf), jax.ShapeDtypeStruct(q_proj.shape, bf)],
        in_specs=[pl.BlockSpec((rows, group * HD), lambda i: (0, i)), pl.BlockSpec((seq, HD), lambda i: (0, i)), pl.BlockSpec((seq, HD), lambda i: (0, HK + i)), whole(gq), whole(gk), whole(cos), whole(sin)],
        out_specs=[pl.BlockSpec((rows, group * HD), lambda i: (0, i)), pl.BlockSpec((seq, HD), lambda i: (0, i)), pl.BlockSpec((seq, HD), lambda i: (0, i)), pl.BlockSpec((rows, group * HD), lambda i: (0, i))],
        compiler_params=pltpu.CompilerParams(dimension_semantics=("arbitrary",), vmem_limit_bytes=48 << 20),
        cost_estimate=pl.CostEstimate(flops=4_300_000_000, bytes_accessed=20_000_000, transcendentals=8_400_000),
        name="attention_forward",
    )(q_proj, kv_proj, kv_proj, gq, gk, cos, sin)

def attention_backward_kernel(group, u_ref, ql_ref, kl_ref, vl_ref, gm_ref, gq_ref, cos_ref, sin_ref, gu_ref, gk_ref, gv_ref, gg_ref, gk_acc, gv_acc):
    bf, f32 = jnp.bfloat16, jnp.float32
    rows, seq = ql_ref.shape[0], kl_ref.shape[0]
    first = lax.axis_index("shard") * rows
    cos, sin = cos_ref[pl.ds(first, rows), :], sin_ref[pl.ds(first, rows), :]
    allowed = lax.broadcasted_iota(jnp.int32, (rows, seq), 1) <= first + lax.broadcasted_iota(jnp.int32, (rows, seq), 0)
    gain_grad = jnp.zeros((1, HD), f32)
    for j in range(group):
        cols = slice(j * HD, (j + 1) * HD)
        ql, gm = ql_ref[:, cols], gm_ref[:, cols]
        raised = jnp.where(allowed, jnp.exp(dot(ql, kl_ref[...], 1, 1)), 0.0)
        probs = raised * (1.0 / jnp.sum(raised, axis=-1, keepdims=True))
        gp = dot(gm, vl_ref[...], 1, 1)
        gs = (probs * (gp - jnp.sum(probs * gp, axis=-1, keepdims=True))).astype(bf)
        gv = dot(probs.astype(bf), gm, 0, 0)
        gk = dot(gs, ql, 0, 0)
        if j == 0:
            gv_acc[...] = gv
            gk_acc[...] = gk
        else:
            gv_acc[...] += gv
            gk_acc[...] += gk
        m = dot(gs, kl_ref[...], 1, 0) * HD ** (-0.5)
        m = m * cos + pltpu.roll(m * sin, HD // 2, 1)
        u = u_ref[:, cols]
        r = scale_of(u)
        gain_grad = gain_grad + jnp.sum(m * u * r, axis=0, keepdims=True)
        mg = m * gq_ref[...]
        gu_ref[:, cols] = (r * mg - u * (r * r * r) * jnp.mean(mg * u, axis=-1, keepdims=True)).astype(bf)
    gk_ref[...] = gk_acc[...].astype(bf)
    gv_ref[...] = gv_acc[...].astype(bf)
    gg_ref[0] = jnp.broadcast_to(gain_grad, (8, HD))

def attention_backward(q_proj, q_low, k_low, v_low, grad_mix, gq, cos, sin):
    rows, seq = q_low.shape[0], k_low.shape[0]
    group = HQ // HK
    bf, f32 = jnp.bfloat16, jnp.float32
    gq = gq[None, :]
    whole = lambda a: pl.BlockSpec(a.shape, lambda i: (0, 0))
    qb = pl.BlockSpec((rows, group * HD), lambda i: (0, i)); kb = pl.BlockSpec((seq, HD), lambda i: (0, i))
    grad_q, grad_k, grad_v, gain = pl.pallas_call(
        functools.partial(attention_backward_kernel, group),
        grid=(HK,),
        out_shape=[jax.ShapeDtypeStruct(q_low.shape, bf), jax.ShapeDtypeStruct(k_low.shape, bf), jax.ShapeDtypeStruct(k_low.shape, bf), jax.ShapeDtypeStruct((HK, 8, HD), f32)],
        in_specs=[qb, qb, kb, kb, qb, whole(gq), whole(cos), whole(sin)],
        out_specs=[qb, kb, kb, pl.BlockSpec((1, 8, HD), lambda i: (i, 0, 0))],
        scratch_shapes=[pltpu.VMEM((seq, HD), f32), pltpu.VMEM((seq, HD), f32)],
        compiler_params=pltpu.CompilerParams(dimension_semantics=("arbitrary",), vmem_limit_bytes=48 << 20),
        cost_estimate=pl.CostEstimate(flops=10_700_000_000, bytes_accessed=20_000_000, transcendentals=8_400_000),
        name="attention_backward",
    )(q_proj, q_low, k_low, v_low, grad_mix, gq, cos, sin)
    return grad_q, jnp.concatenate([grad_k, grad_v], axis=1), jnp.sum(gain[:, 0], axis=0)

HQ = 32
HK = 4
HD = 128
epsilon = 1e-06
theta_base = 1000000.0
BOTH = ("expert", "shard")


def matmul(left, right):
    return jnp.dot(left, right, preferred_element_type=jnp.float32)


def matmul_tn(left, right):
    return lax.dot_general(
        left, right, (((0,), (0,)), ((), ())), preferred_element_type=jnp.float32
    )


def matmul_nt(left, right):
    return lax.dot_general(
        left, right, (((1,), (1,)), ((), ())), preferred_element_type=jnp.float32
    )


def norm_rows(values, gain_vec):
    return (
        values * lax.rsqrt(jnp.mean(values * values, axis=-1, keepdims=True) + epsilon) * gain_vec
    )


def norm_back(values, gain_vec, upstream):
    scaling = lax.rsqrt(jnp.mean(values * values, axis=-1, keepdims=True) + epsilon)
    gain_grad = jnp.sum(upstream * values * scaling, axis=0)
    weighted = upstream * gain_vec
    inner_sum = jnp.mean(weighted * values, axis=-1, keepdims=True)
    return (scaling * weighted - values * (scaling * scaling * scaling) * inner_sum, gain_grad)


def rotary(values, positions):
    head_width = values.shape[-1]
    half_width = head_width // 2
    frequency = theta_base ** (-2.0 * jnp.arange(half_width, dtype=jnp.float32) / head_width)
    angles = positions.astype(jnp.float32)[:, None] * frequency[None, :]
    cosine = jnp.concatenate([jnp.cos(angles), jnp.cos(angles)], axis=-1)[:, None, :]
    sine_part = jnp.concatenate([jnp.sin(angles), jnp.sin(angles)], axis=-1)[:, None, :]
    turned = jnp.concatenate([-values[..., half_width:], values[..., :half_width]], axis=-1)
    return values * cosine + turned * sine_part


def head_prep(projected, gain_vec, positions, head_count, factor):
    shaped = projected.reshape(projected.shape[0], head_count, projected.shape[1] // head_count)
    return rotary(norm_rows(shaped, gain_vec), positions) * factor


def gather_all(arrays, cid, line=()):
    if placed():
        return [o.reshape(-1, o.shape[-1]) for o in ag32(arrays, cid, line)]
    return [lax.all_gather(a, BOTH, axis=0, tiled=True) for a in arrays] + [
        lax.all_gather(a, "shard", axis=0, tiled=True) for a in line
    ]


def scatter_all(arrays, cid, out_dtype=jnp.float32):
    if placed():
        return rs32([a.reshape(32, -1, a.shape[-1]) for a in arrays], cid, out_dtype)
    return [lax.psum_scatter(a, BOTH, scatter_dimension=0, tiled=True).astype(out_dtype) for a in arrays]


def per_device(
    hidden_in,
    g_attn,
    w_query,
    w_key,
    w_value,
    g_query,
    g_key,
    w_out,
    g_ffn,
    w_router,
    w_gate,
    w_up,
    w_down,
    routes,
    cotangent,
):
    bf, f32 = jnp.bfloat16, jnp.float32
    tok_rows, model_width = hidden_in.shape
    top_count = routes.shape[1]
    devices = lax.axis_size(BOTH)
    expert_count = devices * w_gate.shape[0]
    capacity = 2 * tok_rows * top_count // expert_count
    shard_count = lax.axis_size("shard")
    shard_pos = lax.axis_index("shard")
    seq_len = tok_rows * shard_count
    q_cols, kv_cols = HQ * HD, HK * HD

    pieces = [w_router.reshape(-1), g_attn, g_ffn, g_query, g_key]
    sizes = [p.shape[0] for p in pieces]
    used = sum(sizes)
    small_rows = -(-used // (64 * 128)) * 64
    small = jnp.concatenate(pieces + [jnp.zeros((small_rows * 128 - used,), bf)]).reshape(small_rows, 128)
    wqkv = jnp.concatenate([w_query, w_key, w_value], axis=1)
    wqkv_full, small_all, wo_full, hidden_seq = gather_all([wqkv, small, w_out], 1, [hidden_in])
    small_all = small_all.reshape(devices, small_rows * 128)
    starts = [sum(sizes[:i]) for i in range(5)]
    wr_full, attn_gain, ffn_gain, query_gain, key_gain = [small_all[:, o : o + n].reshape(-1) for o, n in zip(starts, sizes)]
    wr_full = wr_full.reshape(model_width, expert_count)
    attn_gain, ffn_gain, query_gain, key_gain = [g.astype(f32) for g in (attn_gain, ffn_gain, query_gain, key_gain)]
    cotangent, wo_full = lax.optimization_barrier((cotangent, wo_full))
    cot_all = lax.all_gather(cotangent, BOTH, axis=0, tiled=True)

    inputs_f = hidden_in.astype(f32)
    normed_low = norm_rows(inputs_f, attn_gain).astype(bf)
    normed_seq = norm_rows(hidden_seq.astype(f32), attn_gain).astype(bf)
    kv_proj = matmul(normed_seq, wqkv_full[:, q_cols:])
    q_proj = matmul(normed_low, wqkv_full[:, :q_cols])
    cosine, sine = rope_tables(seq_len)
    q_low, k_low, v_low, mix_low = attention_forward(q_proj, kv_proj, query_gain, key_gain, cosine, sine)
    residual = inputs_f + matmul(mix_low, wo_full)
    ffn_low = norm_rows(residual, ffn_gain).astype(bf)

    logits = matmul(ffn_low, wr_full)
    expert_ids = jnp.arange(expert_count, dtype=jnp.int32)
    chosen = jnp.any(routes[:, :, None] == expert_ids[None, None, :], axis=1)
    raised_gate = jnp.where(chosen, jnp.exp(logits), 0.0)
    gates = raised_gate / jnp.sum(raised_gate, axis=-1, keepdims=True)
    gate_high = lax.reduce_precision(gates, 8, 7)
    gate_low = gates - gate_high
    extra = -(-3 * expert_count // 128) * 128
    payload = jnp.concatenate(
        [
            ffn_low,
            chosen.astype(bf),
            gate_high.astype(bf),
            gate_low.astype(bf),
            jnp.zeros((tok_rows, extra - 3 * expert_count), bf),
        ],
        axis=1,
    )
    (payload_all,) = gather_all([payload], 3)
    out_part, rows, gate_act, up_act = experts_forward(
        payload_all, w_gate, w_up, w_down, expert_count, tok_rows, capacity
    )
    moe_out = lax.psum_scatter(out_part, "expert", scatter_dimension=0, tiled=True)
    grad_part, grad_wgate, grad_wup, grad_wdown = experts_backward(
        payload_all, cot_all, rows, gate_act, up_act, w_gate, w_up, w_down, expert_count, tok_rows, capacity
    )
    (grad_sum,) = scatter_all([grad_part], 4)
    upstream = cotangent.astype(f32)
    grad_ffn = grad_sum[:, :model_width]
    grad_shares = (
        grad_sum[:, model_width : model_width + expert_count]
        + grad_sum[:, model_width + expert_count : model_width + 2 * expert_count]
    )
    grad_logits = (grad_shares - gates * jnp.sum(grad_shares, axis=-1, keepdims=True)).astype(bf)
    grad_wrouter = matmul_tn(ffn_low, grad_logits)
    grad_ffn = grad_ffn + matmul_nt(grad_logits, wr_full)
    grad_second, grad_ffn_gain = norm_back(residual, ffn_gain, grad_ffn)
    grad_residual = upstream + grad_second
    grad_attn_low = grad_residual.astype(bf)
    grad_wout = matmul_tn(mix_low, grad_attn_low).astype(bf)
    grad_mix = matmul_nt(grad_attn_low, wo_full).astype(bf)
    grad_mix, grad_wout = lax.optimization_barrier((grad_mix, grad_wout))
    out_grad = lax.psum_scatter(grad_wout, "expert", scatter_dimension=0, tiled=True)
    out_grad = lax.psum_scatter(out_grad, "shard", scatter_dimension=0, tiled=True).astype(f32)

    grad_q_low, grad_kv, grad_query_gain = attention_backward(
        q_proj, q_low, k_low, v_low, grad_mix, query_gain, cosine, sine
    )
    grad_kv = line_scatter(grad_kv, 6)
    grad_kv, moe_out = lax.optimization_barrier((grad_kv, moe_out))
    moe_out = lax.psum_scatter(moe_out, "shard", scatter_dimension=0, tiled=True).astype(f32)
    block_out = (residual + moe_out).astype(bf)
    own_rows = shard_pos * tok_rows
    k_proj = lax.dynamic_slice(kv_proj, (own_rows, 0), (tok_rows, kv_cols))
    positions = own_rows + jnp.arange(tok_rows, dtype=jnp.int32)
    _, k_pull = jax.vjp(
        lambda projected, gain_vec: head_prep(projected, gain_vec, positions, HK, 1.0), k_proj, key_gain
    )
    grad_k_proj, grad_key_gain = k_pull(grad_kv[:, :kv_cols].reshape(tok_rows, HK, HD))
    grad_qkv_low = jnp.concatenate(
        [grad_q_low, grad_k_proj.astype(bf), grad_kv[:, kv_cols:].astype(bf)], axis=1
    )
    grad_wqkv = matmul_tn(normed_low, grad_qkv_low).astype(bf)
    grad_normed = matmul_nt(grad_qkv_low, wqkv_full)
    grad_front, grad_attn_gain = norm_back(inputs_f, attn_gain, grad_normed)
    grad_input = (grad_residual + grad_front).astype(bf)

    grads = [grad_wrouter, grad_attn_gain, grad_ffn_gain, grad_query_gain, grad_key_gain]
    packed = jnp.concatenate(
        [g.astype(bf).reshape(devices, -1) for g in grads] + [jnp.zeros((devices, small_rows * 128 - used), bf)], axis=1
    ).reshape(devices * small_rows, 128)
    qkv_grad, small_grad = scatter_all([grad_wqkv, packed], 8)
    small_grad = small_grad.reshape(-1)
    router_g, attn_g, ffn_g, query_g, key_g = [small_grad[o : o + n] for o, n in zip(starts, sizes)]
    return (
        block_out,
        grad_input,
        attn_g,
        qkv_grad[:, :q_cols],
        qkv_grad[:, q_cols : q_cols + kv_cols],
        qkv_grad[:, q_cols + kv_cols :],
        query_g,
        key_g,
        out_grad,
        ffn_g,
        router_g.reshape(w_router.shape),
        grad_wgate,
        grad_wup,
        grad_wdown,
    )


def solution(mesh):
    row = P(BOTH, None)
    vec = P(BOTH)
    cube = P(BOTH, None, None)
    in_specs = (row, vec, row, row, row, vec, vec, row, vec, row, cube, cube, cube, row, row)
    out_specs = (row, row, vec, row, row, row, vec, vec, row, vec, row, cube, cube, cube)
    return jax.shard_map(
        per_device, mesh=mesh, in_specs=in_specs, out_specs=out_specs, check_vma=False
    )
```

```python
import functools

import jax
import jax.numpy as jnp
from jax import lax
from jax.experimental import pallas as pl
from jax.experimental.pallas import tpu as pltpu
from jax.sharding import PartitionSpec as P

MESH = pl.DeviceIdType.MESH
NZ = 4

def placed():
    return lax.axis_size("expert") == 8 and lax.axis_size("shard") == NZ

def place():
    e = lax.axis_index("expert"); s = lax.axis_index("shard")
    return e // 4, lax.rem(e // 2, 2), lax.rem(e, 2), s

def dev(y, x, c, s):
    return (y * 4 + x * 2 + c, s)

def barrier_all(y, x, c, s):
    bar = pltpu.get_barrier_semaphore()
    def sig(d): pl.semaphore_signal(bar, inc=1, device_id=d, device_id_type=MESH)
    sig(dev(1 - y, x, c, s)); sig(dev(y, 1 - x, c, s)); sig(dev(y, x, 1 - c, s))
    @pl.when(s > 0)
    def _(): sig(dev(y, x, c, s - 1))
    @pl.when(s < NZ - 1)
    def _(): sig(dev(y, x, c, s + 1))
    pl.semaphore_wait(bar, 3 + jnp.where(s > 0, 1, 0) + jnp.where(s < NZ - 1, 1, 0))

def ag_kernel(n_arr, n_line, *refs):
    n_all = n_arr + n_line
    for run in ag_steps(n_arr, n_line, refs[:n_all], refs[n_all:2 * n_all], refs[2 * n_all:]): run()

AG_STEPS = 10

def ag_steps(n_arr, n_line, ins, outs, sems):
    n_all = n_arr + n_line
    loc_sem, zs, zr, ps, pr, cs, cr = sems
    y, x, c, s = place()
    def rc(src, dst, ss, rs, d):
        return pltpu.make_async_remote_copy(src_ref=src, dst_ref=dst, send_sem=ss, recv_sem=rs, device_id=d, device_id_type=MESH)
    X = dev(y, 1 - x, c, s); Y = dev(1 - y, x, c, s); C = dev(y, x, 1 - c, s)
    A = range(n_arr)
    every = range(n_all)
    def home(a, zz):
        return outs[a].at[y, x, c, zz] if a < n_arr else outs[a].at[zz]
    steps = [(0, 0)] + [(d, g) for d in range(1, NZ) for g in (1, -1)]
    def valid(d, g):
        return (s >= d) if g == 1 else (s + d <= NZ - 1)
    def zof(d, g): return s - d * g
    def src_own(a, h, zz, k):
        return ins[a].at[h] if k == 0 else home(a, zz).at[h]
    def zcopy(a, h, zz, k, g):
        kk = 1 + 2 * (k_dist(k)) + (0 if g == 1 else 1)
        return rc(src_own(a, h, zz, k), home(a, zz).at[h], zs.at[a, h, kk], zr.at[a, h, kk], dev(y, x, c, s + g))
    def k_dist(k): return steps[k][0]
    def plane(a, h, zz, k, which):
        return rc(src_own(a, h, zz, k), outs[a].at[y, x, c, zz, h], ps.at[a, k, h, which], pr.at[a, k, h, which], X if which == 0 else Y)
    def plane_recv(a, h, zz, k, which):
        d = outs[a].at[y, 1 - x, c, zz, h] if which == 0 else outs[a].at[1 - y, x, c, zz, h]
        return rc(d, d, ps.at[a, k, h, which], pr.at[a, k, h, which], X if which == 0 else Y)
    def diag(a, h, zz, k):
        d = outs[a].at[y, 1 - x, c, zz, h] if h == 0 else outs[a].at[1 - y, x, c, zz, h]
        return rc(d, d, ps.at[a, k, h, 2], pr.at[a, k, h, 2], Y if h == 0 else X)
    def diag_recv(a, h, zz, k):
        d = outs[a].at[1 - y, 1 - x, c, zz, h]
        return rc(d, d, ps.at[a, k, h, 2], pr.at[a, k, h, 2], Y if h == 0 else X)
    def core(a, zz, k, part):
        d = outs[a].at[:, :, c, zz]
        return rc(d, d, cs.at[a, k], cr.at[a, k], C)
    def core_recv(a, zz, k):
        d = outs[a].at[:, :, 1 - c, zz]
        return rc(d, d, cs.at[a, k], cr.at[a, k], C)
    def loc(a):
        return pltpu.make_async_copy(ins[a], home(a, s), loc_sem.at[a])

    def when(k, f):
        d, g = steps[k]
        if k == 0: f()
        else: pl.when(valid(d, g))(f)

    def stage_a(k):
        d, g = steps[k]
        def go():
            zz = zof(d, g)
            for a in every:
                for h in range(2):
                    if k:
                        kk = k
                        dref = home(a, zz).at[h]
                        rc(dref, dref, zs.at[a, h, kk], zr.at[a, h, kk], X).wait_recv()
                    for gg in ((1, -1) if k == 0 else (g,)):
                        okc = (s < NZ - 1) if gg == 1 else (s > 0)
                        if d + 1 < NZ:
                            @pl.when(okc)
                            def _(): zcopy(a, h, zz, k, gg).start()
                    if a < n_arr:
                        plane(a, h, zz, k, 0).start()
                        plane(a, h, zz, k, 1).start()
        when(k, go)
    def stage_b(k):
        d, g = steps[k]
        def go():
            zz = zof(d, g)
            for a in A:
                plane_recv(a, 0, zz, k, 0).wait_recv()
                diag(a, 0, zz, k).start()
                plane_recv(a, 1, zz, k, 1).wait_recv()
                diag(a, 1, zz, k).start()
        when(k, go)
    def stage_c(k):
        d, g = steps[k]
        def go():
            zz = zof(d, g)
            for a in A:
                if k == 0: loc(a).wait()
                plane_recv(a, 1, zz, k, 0).wait_recv()
                plane_recv(a, 0, zz, k, 1).wait_recv()
                diag_recv(a, 0, zz, k).wait_recv()
                diag_recv(a, 1, zz, k).wait_recv()
                core(a, zz, k, 0).start()
        when(k, go)
    n = len(steps)
    def advance(i):
        if i == 0:
            barrier_all(y, x, c, s)
            for a in every: loc(a).start()
        if i < n: stage_a(i)
        if 0 <= i - 1 < n: stage_b(i - 1)
        if 0 <= i - 2 < n: stage_c(i - 2)
    def finish():
        for k in range(n):
            d, g = steps[k]
            def go():
                zz = zof(d, g)
                for a in every:
                    if a < n_arr:
                        core_recv(a, zz, k).wait_recv()
                        core(a, zz, k, 0).wait_send()
                    elif k == 0: loc(a).wait()
                    for h in range(2):
                        for gg in ((1, -1) if k == 0 else (g,)):
                            okc = (s < NZ - 1) if gg == 1 else (s > 0)
                            if d + 1 < NZ:
                                @pl.when(okc)
                                def _(): zcopy(a, h, zz, k, gg).wait_send()
                        if a < n_arr:
                            plane(a, h, zz, k, 0).wait_send()
                            plane(a, h, zz, k, 1).wait_send()
                            diag(a, h, zz, k).wait_send()
            when(k, go)
    return [functools.partial(advance, i) for i in range(n + 2)] + [finish]

def ag_sems(n, m=0):
    D = pltpu.SemaphoreType.DMA
    return [D((n + m,)), D((n + m, 2, 9)), D((n + m, 2, 9)), D((n, 7, 2, 3)), D((n, 7, 2, 3)), D((n, 7)), D((n, 7))]

def ag32(arrs, cid, line=()):
    ins = [a.reshape(2, a.shape[0] // 2, a.shape[1]) for a in list(arrs) + list(line)]
    n, m = len(arrs), len(line)
    outs = pl.pallas_call(
        functools.partial(ag_kernel, n, m),
        out_shape=[jax.ShapeDtypeStruct(((2, 2, 2, NZ) if i < n else (NZ,)) + a.shape, a.dtype) for i, a in enumerate(ins)],
        in_specs=[pl.BlockSpec(memory_space=pltpu.VMEM)] * (n + m),
        out_specs=[pl.BlockSpec(memory_space=pl.ANY)] * (n + m),
        scratch_shapes=ag_sems(n, m),
        compiler_params=pltpu.CompilerParams(collective_id=cid, has_side_effects=True, vmem_limit_bytes=64000 * 1024),
        name="gather_all",
    )(*ins)
    return [o.reshape(-1, a.shape[1] * 2, a.shape[2]) for o, a in zip(outs, ins)]

ZORDER = (0, 3, 1, 2)
LAGS = (1, 1, 1, 1)

def rs_kernel(n_arr, n_line, parts, *refs):
    n_all = n_arr + n_line
    ins = refs[:n_all]; outs = refs[n_all:2 * n_all]
    sc = list(refs[2 * n_all:])
    own_b = [sc.pop(0) for _ in range(n_all)]; zu_b = [sc.pop(0) for _ in range(n_all)]; zd_b = [sc.pop(0) for _ in range(n_all)]
    r0_b, ra_b, rb_b = [[sc.pop(0) for _ in range(n_arr)] for _ in range(3)]
    lsem, s0s, s0r, sas, sar, sbs, sbr, zus, zur, zds, zdr = sc
    y, x, c, s = place()
    barrier_all(y, x, c, s)
    X = dev(y, 1 - x, c, s); Y = dev(1 - y, x, c, s); C = dev(y, x, 1 - c, s)
    UP = dev(y, x, c, s + 1); DN = dev(y, x, c, s - 1)
    def rc(src, dst, ss, rs, d):
        return pltpu.make_async_remote_copy(src_ref=src, dst_ref=dst, send_sem=ss, recv_sem=rs, device_id=d, device_id_type=MESH)
    units = [(a, zz, h) for zz in ZORDER for h in range(parts) for a in range(n_arr)]
    lines = [(a, zz, h) for zz in ZORDER for h in range(parts) for a in range(n_arr, n_all)]
    def jj(zz, h): return ZORDER.index(zz) * parts + h
    def load(a, zz, h):
        j = jj(zz, h)
        src = ins[a].at[:, :, c, zz, h] if a < n_arr else ins[a].at[zz, h]
        return pltpu.make_async_copy(src, own_b[a].at[j], lsem.at[a, j])
    def mine(a, j):
        return own_b[a].at[j, y, x] if a < n_arr else own_b[a].at[j]
    def c0(a, zz, h):
        j = jj(zz, h)
        return rc(ins[a].at[:, :, 1 - c, zz, h], r0_b[a].at[j], s0s.at[a, j], s0r.at[a, j], C)
    def ca(a, zz, h):
        j = jj(zz, h)
        if h % 2 == 0: return rc(own_b[a].at[j, :, 1 - x], ra_b[a].at[j], sas.at[a, j], sar.at[a, j], X)
        return rc(own_b[a].at[j, 1 - y], ra_b[a].at[j], sas.at[a, j], sar.at[a, j], Y)
    def cb(a, zz, h):
        j = jj(zz, h)
        if h % 2 == 0: return rc(own_b[a].at[j, 1 - y, x], rb_b[a].at[j], sbs.at[a, j], sbr.at[a, j], Y)
        return rc(own_b[a].at[j, y, 1 - x], rb_b[a].at[j], sbs.at[a, j], sbr.at[a, j], X)
    def cu(a, zz, h):
        j = jj(zz, h)
        return rc(mine(a, j), zu_b[a].at[j], zus.at[a, j], zur.at[a, j], UP)
    def cd(a, zz, h):
        j = jj(zz, h)
        return rc(mine(a, j), zd_b[a].at[j], zds.at[a, j], zdr.at[a, j], DN)
    def add_into(dst, other):
        rows = dst.shape[0]
        st = 16 if rows % 16 == 0 else rows
        @pl.loop(0, rows // st)
        def _(i):
            r = pl.ds(i * st, st)
            dst[r, :] = (dst[r, :].astype(jnp.float32) + other[r, :].astype(jnp.float32)).astype(dst.dtype)
    def stage0(u):
        a, zz, h = u; j = jj(zz, h)
        load(a, zz, h).wait()
        c0(a, zz, h).wait_recv()
        for yy in range(2):
            for xx in range(2):
                add_into(own_b[a].at[j, yy, xx], r0_b[a].at[j, yy, xx])
        ca(a, zz, h).start()
    def stage1(u):
        a, zz, h = u; j = jj(zz, h)
        ca(a, zz, h).wait_recv()
        for q in range(2):
            if h % 2 == 0: add_into(own_b[a].at[j, q, x], ra_b[a].at[j, q])
            else: add_into(own_b[a].at[j, y, q], ra_b[a].at[j, q])
        cb(a, zz, h).start()
    def stage2(u):
        a, zz, h = u; j = jj(zz, h)
        cb(a, zz, h).wait_recv()
        add_into(own_b[a].at[j, y, x], rb_b[a].at[j])
    def hop(u, k):
        a, zz, h = u; j = jj(zz, h)
        if k < zz:
            @pl.when(s == k)
            def _():
                if k > 0:
                    cu(a, zz, h).wait_recv()
                    add_into(mine(a, j), zu_b[a].at[j])
                cu(a, zz, h).start()
        t = NZ - 1 - k
        if t > zz:
            @pl.when(s == t)
            def _():
                if k > 0:
                    cd(a, zz, h).wait_recv()
                    add_into(mine(a, j), zd_b[a].at[j])
                cd(a, zz, h).start()
    def last(u):
        a, zz, h = u; j = jj(zz, h)
        @pl.when(s == zz)
        def _():
            if zz > 0: cu(a, zz, h).wait_recv()
            if zz < NZ - 1: cd(a, zz, h).wait_recv()
            t = mine(a, j)[...].astype(jnp.float32)
            if zz > 0: t = t + zu_b[a][j].astype(jnp.float32)
            if zz < NZ - 1: t = t + zd_b[a][j].astype(jnp.float32)
            outs[a][h] = t.astype(outs[a].dtype)
    for u in lines: load(*u).start()
    for u in units:
        c0(*u).start(); load(*u).start()
    n = len(units); nl = len(lines)
    L1 = LAGS[0] * n_arr; L2 = L1 + LAGS[1] * n_arr; L3 = L2 + LAGS[2] * n_arr; dl = LAGS[3] * n_arr
    for i in range(n + L3 + (NZ - 1) * dl):
        if i < n: stage0(units[i])
        if 0 <= i - L1 < n: stage1(units[i - L1])
        if 0 <= i - L2 < n: stage2(units[i - L2])
        for k in range(NZ - 1):
            for q in (2 * (i - k), 2 * (i - k) + 1):
                if 0 <= q < nl:
                    if k == 0: load(*lines[q]).wait()
                    hop(lines[q], k)
        for k in range(NZ - 1):
            if 0 <= i - L3 - k * dl < n: hop(units[i - L3 - k * dl], k)
    for u in lines + units: last(u)
    for u in lines + units:
        a, zz, h = u
        if a < n_arr:
            c0(*u).wait_send(); ca(*u).wait_send(); cb(*u).wait_send()
        if zz > 0:
            @pl.when(s < zz)
            def _(): cu(*u).wait_send()
        if zz < NZ - 1:
            @pl.when(s > zz)
            def _(): cd(*u).wait_send()

def rs32(arrs, cid, out_dtype=jnp.float32, parts=4, line=()):
    n, nl = len(arrs), len(line)
    both = list(arrs) + list(line)
    if any(a.shape[1] % (parts * 16) for a in both): parts = 2
    ins = [a.reshape(((2, 2, 2) if i < n else ()) + (NZ, parts, a.shape[1] // parts, a.shape[2])) for i, a in enumerate(both)]
    hs = [i.shape[-2:] for i in ins]
    V = pltpu.VMEM; bt = jnp.bfloat16; m = NZ * parts
    sems = [pltpu.SemaphoreType.DMA((n + nl, m))] * 11
    outs = pl.pallas_call(
        functools.partial(rs_kernel, n, nl, parts),
        out_shape=[jax.ShapeDtypeStruct((parts,) + h, out_dtype) for h in hs],
        in_specs=[pl.BlockSpec(memory_space=pl.ANY)] * (n + nl),
        out_specs=[pl.BlockSpec(memory_space=pltpu.VMEM)] * (n + nl),
        scratch_shapes=[V((m,) + ((2, 2) if i < n else ()) + h, bt) for i, h in enumerate(hs)] + [V((m,) + h, bt) for h in hs] + [V((m,) + h, bt) for h in hs]
            + [V((m, 2, 2) + h, bt) for h in hs[:n]] + [V((m, 2) + h, bt) for h in hs[:n]] + [V((m,) + h, bt) for h in hs[:n]] + sems,
        compiler_params=pltpu.CompilerParams(collective_id=cid, has_side_effects=True, vmem_limit_bytes=64000 * 1024),
        name="scatter_all",
    )(*ins)
    return [o.reshape(a.shape[1], a.shape[2]) for o, a in zip(outs, both)]

def line_barrier(y, x, c, s):
    bar = pltpu.get_barrier_semaphore()
    @pl.when(s > 0)
    def _(): pl.semaphore_signal(bar, inc=1, device_id=dev(y, x, c, s - 1), device_id_type=MESH)
    @pl.when(s < NZ - 1)
    def _(): pl.semaphore_signal(bar, inc=1, device_id=dev(y, x, c, s + 1), device_id_type=MESH)
    pl.semaphore_wait(bar, jnp.where(s > 0, 1, 0) + jnp.where(s < NZ - 1, 1, 0))

def line_gather_kernel(parts, x_ref, o_ref, ss, rs):
    y, x, c, s = place()
    line_barrier(y, x, c, s)
    def cp(d, g, h):
        src = x_ref.at[h] if d == 0 else o_ref.at[s - d * g, h]
        k = 0 if g == 1 else 1
        return pltpu.make_async_remote_copy(src_ref=src, dst_ref=o_ref.at[s - d * g, h], send_sem=ss.at[k, d, h], recv_sem=rs.at[k, d, h],
            device_id=dev(y, x, c, s + g), device_id_type=MESH)
    def arrived(d, g, h):
        k = 0 if g == 1 else 1
        ref = o_ref.at[s - (d + 1) * g, h]
        return pltpu.make_async_remote_copy(src_ref=ref, dst_ref=ref, send_sem=ss.at[k, d, h], recv_sem=rs.at[k, d, h],
            device_id=dev(y, x, c, s + g), device_id_type=MESH)
    def sends(d, g): return (s >= d) & (s < NZ - 1) if g == 1 else (s + d <= NZ - 1) & (s > 0)
    def gets(d, g): return s >= d + 1 if g == 1 else s + d + 1 <= NZ - 1
    for d in range(NZ):
        for h in range(parts):
            for g in (1, -1):
                if d:
                    @pl.when(gets(d - 1, g))
                    def _(): arrived(d - 1, g, h).wait_recv()
                if d < NZ - 1:
                    @pl.when(sends(d, g))
                    def _(): cp(d, g, h).start()
        if d == 0: o_ref[s] = x_ref[...]
    for d in range(NZ - 1):
        for h in range(parts):
            for g in (1, -1):
                @pl.when(sends(d, g))
                def _(): cp(d, g, h).wait_send()

def line_gather(x, cid, parts=4):
    if not placed():
        return lax.all_gather(x, "shard", axis=0, tiled=True)
    R, C = x.shape
    sem = pltpu.SemaphoreType.DMA((2, NZ, parts))
    o = pl.pallas_call(functools.partial(line_gather_kernel, parts), out_shape=jax.ShapeDtypeStruct((NZ, parts, R // parts, C), x.dtype),
        in_specs=[pl.BlockSpec(memory_space=pltpu.VMEM)], out_specs=pl.BlockSpec(memory_space=pltpu.VMEM),
        scratch_shapes=[sem, sem], compiler_params=pltpu.CompilerParams(collective_id=cid, has_side_effects=True, vmem_limit_bytes=16 << 20),
        name="line_gather")(x.reshape(parts, R // parts, C))
    return o.reshape(NZ * R, C)

def line_scatter_kernel(parts, p_ref, o_ref, acc, zu, zd, ss_u, rs_u, ss_d, rs_d):
    y, x, c, s = place()
    line_barrier(y, x, c, s)
    def rc(src, dst, a, b, d):
        return pltpu.make_async_remote_copy(src_ref=src, dst_ref=dst, send_sem=a, recv_sem=b, device_id=d, device_id_type=MESH)
    def cu(zz, h, k):
        src = p_ref.at[zz, h] if k == 0 else acc.at[zz, h]
        return rc(src, zu.at[zz, h], ss_u.at[zz, h], rs_u.at[zz, h], dev(y, x, c, s + 1))
    def cd(zz, h, k):
        src = p_ref.at[zz, h] if k == 0 else acc.at[zz, h]
        return rc(src, zd.at[zz, h], ss_d.at[zz, h], rs_d.at[zz, h], dev(y, x, c, s - 1))
    st = 32
    def total(dst, refs):
        @pl.loop(0, dst.shape[0] // st)
        def _(i):
            r = pl.ds(i * st, st)
            t = refs[0][r, :].astype(jnp.float32)
            for f in refs[1:]: t = t + f[r, :].astype(jnp.float32)
            dst[r, :] = t.astype(dst.dtype)
    ups = [(zz, h) for zz in (3, 2, 1) for h in range(parts)]
    dns = [(zz, h) for zz in (0, 1, 2) for h in range(parts)]
    n = len(ups)
    for i in range(n + NZ):
        for k in range(NZ - 1):
            if 0 <= i - k < n:
                zz, h = ups[i - k]
                if k < zz:
                    @pl.when(s == k)
                    def _():
                        if k:
                            cu(zz, h, k).wait_recv()
                            total(acc.at[zz, h], [p_ref.at[zz, h], zu.at[zz, h]])
                        cu(zz, h, k).start()
                zz, h = dns[i - k]
                if NZ - 1 - k > zz:
                    @pl.when(s == NZ - 1 - k)
                    def _():
                        if k:
                            cd(zz, h, k).wait_recv()
                            total(acc.at[zz, h], [p_ref.at[zz, h], zd.at[zz, h]])
                        cd(zz, h, k).start()
    for zz in range(NZ):
        @pl.when(s == zz)
        def _():
            for h in range(parts):
                refs = [p_ref.at[zz, h]]
                if zz > 0:
                    cu(zz, h, 1).wait_recv()
                    refs.append(zu.at[zz, h])
                if zz < NZ - 1:
                    cd(zz, h, 1).wait_recv()
                    refs.append(zd.at[zz, h])
                total(o_ref.at[h], refs)
    for zz, h in ups:
        @pl.when(s < zz)
        def _(): cu(zz, h, 1).wait_send()
    for zz, h in dns:
        @pl.when(s > zz)
        def _(): cd(zz, h, 1).wait_send()

def line_scatter(p, cid, parts=4):
    if not placed():
        return lax.psum_scatter(p, "shard", scatter_dimension=0, tiled=True).astype(jnp.float32)
    R, C = p.shape[0] // NZ, p.shape[1]
    sem = pltpu.SemaphoreType.DMA((NZ, parts))
    shape = (NZ, parts, R // parts, C)
    buf = pltpu.VMEM(shape, p.dtype)
    o = pl.pallas_call(functools.partial(line_scatter_kernel, parts), out_shape=jax.ShapeDtypeStruct(shape[1:], jnp.float32),
        in_specs=[pl.BlockSpec(memory_space=pltpu.VMEM)], out_specs=pl.BlockSpec(memory_space=pltpu.VMEM),
        scratch_shapes=[buf, buf, buf, sem, sem, sem, sem], compiler_params=pltpu.CompilerParams(collective_id=cid, has_side_effects=True, vmem_limit_bytes=24 << 20),
        name="line_scatter")(p.reshape(shape))
    return o.reshape(R, C)


def dot(a, b, ca, cb):
    return lax.dot_general(a, b, (((ca,), (cb,)), ((), ())), preferred_element_type=jnp.float32)

def token_picks(meta, experts, slots, me):
    SB, WM = meta.shape
    bf, f32 = jnp.bfloat16, jnp.float32
    tri = (lax.broadcasted_iota(jnp.int32, (SB, SB), 1) < lax.broadcasted_iota(jnp.int32, (SB, SB), 0)).astype(bf)
    lane = lax.broadcasted_iota(jnp.int32, (SB, WM), 1)
    cnt = dot(tri, meta, 1, 0)
    metaf = meta.astype(f32)
    msk = jnp.sum(jnp.where(lane == me, metaf, 0.0), axis=-1, keepdims=True)
    pos = jnp.sum(jnp.where(lane == me, cnt, 0.0), axis=-1, keepdims=True)
    gate = jnp.sum(jnp.where((lane == me + experts) | (lane == me + 2 * experts), metaf, 0.0), axis=-1, keepdims=True)
    want = jnp.where(msk > 0.0, pos, -1.0).astype(jnp.int32)
    pick = (want == lax.broadcasted_iota(jnp.int32, (SB, slots), 1)).astype(bf)
    return pick, gate

def forward_kernel(experts, slots, SB, guest, *refs):
    if guest:
        cot_ref, x_ref, wg_hbm, wu_hbm, wd_hbm, cot_all, out_ref, rows_ref, ga_ref, ua_ref, wg, wu, wd, wsem = refs[:14]
    else:
        x_ref, wg_hbm, wu_hbm, wd_hbm, out_ref, rows_ref, ga_ref, ua_ref, wg, wu, wd, wsem = refs
    bf = jnp.bfloat16
    step = pl.program_id(0)
    if guest:
        runs = ag_steps(1, 0, [cot_ref], [cot_all], refs[14:])
        for i, run in enumerate(runs[:-1]):
            pl.when(step == GUEST_AT[i])(run)
    nsub = x_ref.shape[0] // SB
    D = out_ref.shape[1]
    me = lax.axis_index(("expert", "shard"))
    loads = [pltpu.make_async_copy(h.at[0], v, wsem.at[i]) for i, (h, v) in enumerate(((wg_hbm, wg), (wu_hbm, wu), (wd_hbm, wd)))]
    @pl.when(step == 0)
    def _():
        for l in loads: l.start()
    picks, gates = [], []
    for i in range(nsub):
        r = pl.ds(i * SB, SB)
        pick, gate = token_picks(x_ref[r, D:], experts, slots, me)
        picks.append(pick); gates.append(gate)
        rows_ref[i * slots:(i + 1) * slots, :] = dot(pick, x_ref[r, :D], 0, 0).astype(bf)
    @pl.when(step == 0)
    def _():
        for l in loads: l.wait()
    ga = dot(rows_ref[...], wg[...], 1, 0)
    ua = dot(rows_ref[...], wu[...], 1, 0)
    ga_ref[...] = ga
    ua_ref[...] = ua
    hid = (ga * (1.0 / (1.0 + jnp.exp(-ga))) * ua).astype(bf)
    eo = dot(hid, wd[...], 1, 0).astype(bf)
    for i in range(nsub):
        r = pl.ds(i * SB, SB)
        tok = dot(picks[i], eo[i * slots:(i + 1) * slots, :], 1, 0)
        out_ref[r, :] = (gates[i] * tok).astype(bf)
    if guest: pl.when(step == pl.num_programs(0) - 1)(runs[-1])

GUEST_AT = (0, 1, 3, 4, 6, 7, 9, 11, 13)

def backward_kernel(experts, slots, SB, block, meta_ref, cota_ref, cotb_ref, rows_ref, ga_ref, ua_ref, wg_hbm, wu_hbm, wd_hbm, gr_ref, dwg_hbm, dwu_hbm, dwd_hbm,
                  wg, wu, wd, dwg, dwu, dwd, gp, wsem, osem):
    bf = jnp.bfloat16
    step = pl.program_id(0)
    nsub = meta_ref.shape[0] // SB
    D = cota_ref.shape[1]
    WM = meta_ref.shape[1]
    half = block // 2
    me = lax.axis_index(("expert", "shard"))
    loads = [pltpu.make_async_copy(h.at[0], v, wsem.at[i]) for i, (h, v) in enumerate(((wg_hbm, wg), (wu_hbm, wu), (wd_hbm, wd)))]
    @pl.when(step == 0)
    def _():
        for l in loads: l.start()
        for a in (dwg, dwu, dwd): a[...] = jnp.zeros_like(a)
    picks = []
    for i in range(nsub):
        r = pl.ds(i * SB, SB)
        pick, gate = token_picks(meta_ref[r, :], experts, slots, me)
        picks.append(pick)
        cot = []
        for b in range(i * SB // block, (i + 1) * SB // block):
            cot += [cota_ref[b * half:(b + 1) * half, :], cotb_ref[b * half:(b + 1) * half, :]]
        gcot = (gate * jnp.concatenate(cot, axis=0).astype(jnp.float32)).astype(bf)
        gp[i * slots:(i + 1) * slots, :] = dot(pick, gcot, 0, 0).astype(bf)
    @pl.when(step == 0)
    def _():
        for l in loads: l.wait()
    ga = ga_ref[...]
    ua = ua_ref[...]
    sig = 1.0 / (1.0 + jnp.exp(-ga))
    act = ga * sig
    hidf = act * ua
    hid = hidf.astype(bf)
    gh = dot(gp[...], wd[...], 1, 1)
    share = jnp.sum(gh * hid.astype(jnp.float32), axis=-1, keepdims=True)
    dga = (gh * ua * (sig * (1.0 + ga * (1.0 - sig)))).astype(bf)
    dua = (gh * act).astype(bf)
    dwd[...] += dot(hid, gp[...], 0, 0)
    grow = (dot(dga, wg[...], 1, 1) + dot(dua, wu[...], 1, 1)).astype(bf)
    dwg[...] += dot(rows_ref[...], dga, 0, 0)
    dwu[...] += dot(rows_ref[...], dua, 0, 0)
    lane = lax.broadcasted_iota(jnp.int32, (share.shape[0], WM), 1)
    high = share.astype(bf).astype(jnp.float32)
    tail = (jnp.where(lane == me, high, 0.0) + jnp.where(lane == me + experts, share - high, 0.0)).astype(bf)
    for i in range(nsub):
        r = pl.ds(i * SB, SB)
        q = slice(i * slots, (i + 1) * slots)
        gr_ref[r, :D] = dot(picks[i], grow[q, :], 1, 0).astype(bf)
        gr_ref[r, D:] = dot(picks[i], tail[q, :], 1, 0).astype(bf)
    @pl.when(step == pl.num_programs(0) - 1)
    def _():
        outs = [pltpu.make_async_copy(v, h.at[0], osem.at[i]) for i, (v, h) in enumerate(((dwg, dwg_hbm), (dwu, dwu_hbm), (dwd, dwd_hbm)))]
        for o in outs: o.start()
        for o in outs: o.wait()

def experts_forward(x_all, w_gate, w_up, w_down, experts, block, capacity, guest, cid, TB=512, SB=256):
    hosted = placed()
    T, C = x_all.shape; D, F = w_gate.shape[1:]
    slots = max(SB // block, 1) * capacity
    total = TB // SB * slots
    S = T // SB * slots
    any_ = pl.BlockSpec(memory_space=pl.ANY)
    V = pltpu.VMEM; bf = jnp.bfloat16; f32 = jnp.float32
    blk = lambda r, c: pl.BlockSpec((r, c), lambda i: (i, 0))
    g = guest.reshape(2, guest.shape[0] // 2, guest.shape[1])
    res = pl.pallas_call(
        functools.partial(forward_kernel, experts, slots, SB, hosted),
        grid=(T // TB,),
        out_shape=([jax.ShapeDtypeStruct((2, 2, 2, NZ) + g.shape, g.dtype)] if hosted else []) + [jax.ShapeDtypeStruct((T, D), bf), jax.ShapeDtypeStruct((S, D), bf), jax.ShapeDtypeStruct((S, F), f32), jax.ShapeDtypeStruct((S, F), f32)],
        in_specs=([pl.BlockSpec(memory_space=pltpu.VMEM)] if hosted else []) + [blk(TB, C), any_, any_, any_],
        out_specs=([any_] if hosted else []) + [blk(TB, D), blk(total, D), blk(total, F), blk(total, F)],
        scratch_shapes=[V((D, F), bf), V((D, F), bf), V((F, D), bf), pltpu.SemaphoreType.DMA((3,))] + (ag_sems(1) if hosted else []),
        compiler_params=pltpu.CompilerParams(dimension_semantics=("arbitrary",), vmem_limit_bytes=65000 * 1024,
            **(dict(collective_id=cid, has_side_effects=True) if hosted else {})),
        cost_estimate=pl.CostEstimate(flops=48_000_000_000, bytes_accessed=130_000_000, transcendentals=0),
        name="experts_forward",
    )(*([g] if hosted else []), x_all, w_gate, w_up, w_down)
    if hosted: return res[1:], res[0].reshape(-1, guest.shape[1])
    return res, lax.all_gather(guest, BOTH, axis=0, tiled=True)

def experts_backward(x_all, cot_a, cot_b, rows, ga, ua, w_gate, w_up, w_down, experts, block, capacity, TB=512, SB=256):
    T, C = x_all.shape; D, F = w_gate.shape[1:]
    slots = max(SB // block, 1) * capacity
    total = TB // SB * slots
    WM = C - D
    any_ = pl.BlockSpec(memory_space=pl.ANY)
    V = pltpu.VMEM; bf = jnp.bfloat16; f32 = jnp.float32
    blk = lambda r, c: pl.BlockSpec((r, c), lambda i: (i, 0))
    meta = pl.BlockSpec((TB, WM), lambda i: (i, D // WM)) if D % WM == 0 else blk(TB, WM)
    meta_in = x_all if D % WM == 0 else x_all[:, D:]
    return pl.pallas_call(
        functools.partial(backward_kernel, experts, slots, SB, block),
        grid=(T // TB,),
        out_shape=[jax.ShapeDtypeStruct((T, C), bf), jax.ShapeDtypeStruct(w_gate.shape, f32), jax.ShapeDtypeStruct(w_up.shape, f32), jax.ShapeDtypeStruct(w_down.shape, f32)],
        in_specs=[meta, blk(TB // 2, D), blk(TB // 2, D), blk(total, D), blk(total, F), blk(total, F), any_, any_, any_],
        out_specs=[blk(TB, C), any_, any_, any_],
        scratch_shapes=[V((D, F), bf), V((D, F), bf), V((F, D), bf), V((D, F), f32), V((D, F), f32), V((F, D), f32), V((total, D), bf), pltpu.SemaphoreType.DMA((3,)), pltpu.SemaphoreType.DMA((3,))],
        compiler_params=pltpu.CompilerParams(dimension_semantics=("arbitrary",), vmem_limit_bytes=65000 * 1024),
        cost_estimate=pl.CostEstimate(flops=85_000_000_000, bytes_accessed=150_000_000, transcendentals=0),
        name="experts_backward",
    )(meta_in, cot_a, cot_b, rows, ga, ua, w_gate, w_up, w_down)


def rope_tables(seq_len):
    half = HD // 2
    frequency = theta_base ** (-2.0 * jnp.arange(half, dtype=jnp.float32) / HD)
    angles = jnp.arange(seq_len, dtype=jnp.float32)[:, None] * frequency[None, :]
    return jnp.concatenate([jnp.cos(angles)] * 2, axis=-1), jnp.concatenate([-jnp.sin(angles), jnp.sin(angles)], axis=-1)

def turn(u, cos, sin):
    return u * cos + pltpu.roll(u, HD // 2, 1) * sin

def scale_of(u):
    return lax.rsqrt(jnp.mean(u * u, axis=-1, keepdims=True) + epsilon)

def attention_forward_kernel(group, q_ref, k_ref, v_ref, gq_ref, gk_ref, cos_ref, sin_ref, ql_ref, kl_ref, vl_ref, mix_ref):
    bf, f32 = jnp.bfloat16, jnp.float32
    rows, seq = q_ref.shape[0], k_ref.shape[0]
    first = lax.axis_index("shard") * rows
    k = k_ref[...]
    kl_ref[...] = turn(k * scale_of(k) * gk_ref[...], cos_ref[...], sin_ref[...]).astype(bf)
    vl_ref[...] = v_ref[...].astype(bf)
    cos, sin = cos_ref[pl.ds(first, rows), :], sin_ref[pl.ds(first, rows), :]
    allowed = lax.broadcasted_iota(jnp.int32, (rows, seq), 1) <= first + lax.broadcasted_iota(jnp.int32, (rows, seq), 0)
    for j in range(group):
        cols = slice(j * HD, (j + 1) * HD)
        u = q_ref[:, cols]
        ql = (turn(u * scale_of(u) * gq_ref[...], cos, sin) * HD ** (-0.5)).astype(bf)
        ql_ref[:, cols] = ql
        scores = dot(ql, kl_ref[...], 1, 1)
        raised = jnp.where(allowed, jnp.exp(scores), 0.0)
        probs = (raised * (1.0 / jnp.sum(raised, axis=-1, keepdims=True))).astype(bf)
        mix_ref[:, cols] = dot(probs, vl_ref[...], 1, 0).astype(bf)

def attention_forward(q_proj, kv_proj, gq, gk, cos, sin):
    rows, seq = q_proj.shape[0], kv_proj.shape[0]
    group = HQ // HK
    bf = jnp.bfloat16
    whole = lambda a: pl.BlockSpec(a.shape, lambda i: (0, 0))
    gq, gk = gq[None, :], gk[None, :]
    return pl.pallas_call(
        functools.partial(attention_forward_kernel, group),
        grid=(HK,),
        out_shape=[jax.ShapeDtypeStruct(q_proj.shape, bf), jax.ShapeDtypeStruct((seq, HK * HD), bf), jax.ShapeDtypeStruct((seq, HK * HD), bf), jax.ShapeDtypeStruct(q_proj.shape, bf)],
        in_specs=[pl.BlockSpec((rows, group * HD), lambda i: (0, i)), pl.BlockSpec((seq, HD), lambda i: (0, i)), pl.BlockSpec((seq, HD), lambda i: (0, HK + i)), whole(gq), whole(gk), whole(cos), whole(sin)],
        out_specs=[pl.BlockSpec((rows, group * HD), lambda i: (0, i)), pl.BlockSpec((seq, HD), lambda i: (0, i)), pl.BlockSpec((seq, HD), lambda i: (0, i)), pl.BlockSpec((rows, group * HD), lambda i: (0, i))],
        compiler_params=pltpu.CompilerParams(dimension_semantics=("arbitrary",), vmem_limit_bytes=48 << 20),
        cost_estimate=pl.CostEstimate(flops=4_300_000_000, bytes_accessed=20_000_000, transcendentals=8_400_000),
        name="attention_forward",
    )(q_proj, kv_proj, kv_proj, gq, gk, cos, sin)

def attention_backward_kernel(group, u_ref, ql_ref, kl_ref, vl_ref, gm_ref, gq_ref, cos_ref, sin_ref, gu_ref, gk_ref, gv_ref, gg_ref, gk_acc, gv_acc):
    bf, f32 = jnp.bfloat16, jnp.float32
    rows, seq = ql_ref.shape[0], kl_ref.shape[0]
    first = lax.axis_index("shard") * rows
    cos, sin = cos_ref[pl.ds(first, rows), :], sin_ref[pl.ds(first, rows), :]
    allowed = lax.broadcasted_iota(jnp.int32, (rows, seq), 1) <= first + lax.broadcasted_iota(jnp.int32, (rows, seq), 0)
    gain_grad = jnp.zeros((1, HD), f32)
    for j in range(group):
        cols = slice(j * HD, (j + 1) * HD)
        ql, gm = ql_ref[:, cols], gm_ref[:, cols]
        raised = jnp.where(allowed, jnp.exp(dot(ql, kl_ref[...], 1, 1)), 0.0)
        probs = raised * (1.0 / jnp.sum(raised, axis=-1, keepdims=True))
        gp = dot(gm, vl_ref[...], 1, 1)
        gs = (probs * (gp - jnp.sum(probs * gp, axis=-1, keepdims=True))).astype(bf)
        gv = dot(probs.astype(bf), gm, 0, 0)
        gk = dot(gs, ql, 0, 0)
        if j == 0:
            gv_acc[...] = gv
            gk_acc[...] = gk
        else:
            gv_acc[...] += gv
            gk_acc[...] += gk
        m = dot(gs, kl_ref[...], 1, 0) * HD ** (-0.5)
        m = m * cos + pltpu.roll(m * sin, HD // 2, 1)
        u = u_ref[:, cols]
        r = scale_of(u)
        gain_grad = gain_grad + jnp.sum(m * u * r, axis=0, keepdims=True)
        mg = m * gq_ref[...]
        gu_ref[:, cols] = (r * mg - u * (r * r * r) * jnp.mean(mg * u, axis=-1, keepdims=True)).astype(bf)
    gk_ref[...] = gk_acc[...].astype(bf)
    gv_ref[...] = gv_acc[...].astype(bf)
    gg_ref[0] = jnp.broadcast_to(gain_grad, (8, HD))

def attention_backward(q_proj, q_low, k_low, v_low, grad_mix, gq, cos, sin):
    rows, seq = q_low.shape[0], k_low.shape[0]
    group = HQ // HK
    bf, f32 = jnp.bfloat16, jnp.float32
    gq = gq[None, :]
    whole = lambda a: pl.BlockSpec(a.shape, lambda i: (0, 0))
    qb = pl.BlockSpec((rows, group * HD), lambda i: (0, i)); kb = pl.BlockSpec((seq, HD), lambda i: (0, i))
    grad_q, grad_k, grad_v, gain = pl.pallas_call(
        functools.partial(attention_backward_kernel, group),
        grid=(HK,),
        out_shape=[jax.ShapeDtypeStruct(q_low.shape, bf), jax.ShapeDtypeStruct(k_low.shape, bf), jax.ShapeDtypeStruct(k_low.shape, bf), jax.ShapeDtypeStruct((HK, 8, HD), f32)],
        in_specs=[qb, qb, kb, kb, qb, whole(gq), whole(cos), whole(sin)],
        out_specs=[qb, kb, kb, pl.BlockSpec((1, 8, HD), lambda i: (i, 0, 0))],
        scratch_shapes=[pltpu.VMEM((seq, HD), f32), pltpu.VMEM((seq, HD), f32)],
        compiler_params=pltpu.CompilerParams(dimension_semantics=("arbitrary",), vmem_limit_bytes=48 << 20),
        cost_estimate=pl.CostEstimate(flops=10_700_000_000, bytes_accessed=20_000_000, transcendentals=8_400_000),
        name="attention_backward",
    )(q_proj, q_low, k_low, v_low, grad_mix, gq, cos, sin)
    return grad_q, jnp.concatenate([grad_k, grad_v], axis=1), jnp.sum(gain[:, 0], axis=0)

HQ = 32
HK = 4
HD = 128
epsilon = 1e-06
theta_base = 1000000.0
BOTH = ("expert", "shard")


def matmul(left, right):
    return jnp.dot(left, right, preferred_element_type=jnp.float32)


def matmul_tn(left, right):
    return lax.dot_general(
        left, right, (((0,), (0,)), ((), ())), preferred_element_type=jnp.float32
    )


def matmul_nt(left, right):
    return lax.dot_general(
        left, right, (((1,), (1,)), ((), ())), preferred_element_type=jnp.float32
    )


def norm_rows(values, gain_vec):
    return (
        values * lax.rsqrt(jnp.mean(values * values, axis=-1, keepdims=True) + epsilon) * gain_vec
    )


def norm_back(values, gain_vec, upstream):
    scaling = lax.rsqrt(jnp.mean(values * values, axis=-1, keepdims=True) + epsilon)
    gain_grad = jnp.sum(upstream * values * scaling, axis=0)
    weighted = upstream * gain_vec
    inner_sum = jnp.mean(weighted * values, axis=-1, keepdims=True)
    return (scaling * weighted - values * (scaling * scaling * scaling) * inner_sum, gain_grad)


def rotary(values, positions):
    head_width = values.shape[-1]
    half_width = head_width // 2
    frequency = theta_base ** (-2.0 * jnp.arange(half_width, dtype=jnp.float32) / head_width)
    angles = positions.astype(jnp.float32)[:, None] * frequency[None, :]
    cosine = jnp.concatenate([jnp.cos(angles), jnp.cos(angles)], axis=-1)[:, None, :]
    sine_part = jnp.concatenate([jnp.sin(angles), jnp.sin(angles)], axis=-1)[:, None, :]
    turned = jnp.concatenate([-values[..., half_width:], values[..., :half_width]], axis=-1)
    return values * cosine + turned * sine_part


def head_prep(projected, gain_vec, positions, head_count, factor):
    shaped = projected.reshape(projected.shape[0], head_count, projected.shape[1] // head_count)
    return rotary(norm_rows(shaped, gain_vec), positions) * factor


def gather_all(arrays, cid, line=()):
    if placed():
        return [o.reshape(-1, o.shape[-1]) for o in ag32(arrays, cid, line)]
    return [lax.all_gather(a, BOTH, axis=0, tiled=True) for a in arrays] + [
        lax.all_gather(a, "shard", axis=0, tiled=True) for a in line
    ]


def scatter_all(arrays, cid, out_dtype=jnp.float32, line=()):
    if placed():
        return rs32(
            [a.reshape(32, -1, a.shape[-1]) for a in arrays], cid, out_dtype, line=[a.reshape(NZ, -1, a.shape[-1]) for a in line]
        )
    return [lax.psum_scatter(a, BOTH, scatter_dimension=0, tiled=True).astype(out_dtype) for a in arrays] + [
        lax.psum_scatter(a, "shard", scatter_dimension=0, tiled=True).astype(out_dtype) for a in line
    ]


def per_device(
    hidden_in,
    g_attn,
    w_query,
    w_key,
    w_value,
    g_query,
    g_key,
    w_out,
    g_ffn,
    w_router,
    w_gate,
    w_up,
    w_down,
    routes,
    cotangent,
):
    bf, f32 = jnp.bfloat16, jnp.float32
    tok_rows, model_width = hidden_in.shape
    top_count = routes.shape[1]
    devices = lax.axis_size(BOTH)
    expert_count = devices * w_gate.shape[0]
    capacity = 2 * tok_rows * top_count // expert_count
    shard_count = lax.axis_size("shard")
    shard_pos = lax.axis_index("shard")
    seq_len = tok_rows * shard_count
    q_cols, kv_cols = HQ * HD, HK * HD

    pieces = [w_router.reshape(-1), g_attn, g_ffn, g_query, g_key]
    sizes = [p.shape[0] for p in pieces]
    used = sum(sizes)
    small_rows = -(-used // (64 * 128)) * 64
    small = jnp.concatenate(pieces + [jnp.zeros((small_rows * 128 - used,), bf)]).reshape(small_rows, 128)
    wqkv = jnp.concatenate([w_query, w_key, w_value], axis=1)
    wqkv_full, small_all, wo_full, hidden_seq = gather_all([wqkv, small, w_out], 1, [hidden_in])
    small_all = small_all.reshape(devices, small_rows * 128)
    starts = [sum(sizes[:i]) for i in range(5)]
    wr_full, attn_gain, ffn_gain, query_gain, key_gain = [small_all[:, o : o + n].reshape(-1) for o, n in zip(starts, sizes)]
    wr_full = wr_full.reshape(model_width, expert_count)
    attn_gain, ffn_gain, query_gain, key_gain = [g.astype(f32) for g in (attn_gain, ffn_gain, query_gain, key_gain)]
    half = tok_rows // 2
    cot_first, wo_full = lax.optimization_barrier((cotangent[:half], wo_full))
    cot_a = lax.all_gather(cot_first, BOTH, axis=0, tiled=True)

    inputs_f = hidden_in.astype(f32)
    normed_low = norm_rows(inputs_f, attn_gain).astype(bf)
    normed_seq = norm_rows(hidden_seq.astype(f32), attn_gain).astype(bf)
    kv_proj = matmul(normed_seq, wqkv_full[:, q_cols:])
    q_proj = matmul(normed_low, wqkv_full[:, :q_cols])
    cosine, sine = rope_tables(seq_len)
    q_low, k_low, v_low, mix_low = attention_forward(q_proj, kv_proj, query_gain, key_gain, cosine, sine)
    residual = inputs_f + matmul(mix_low, wo_full)
    ffn_low = norm_rows(residual, ffn_gain).astype(bf)

    logits = matmul(ffn_low, wr_full)
    expert_ids = jnp.arange(expert_count, dtype=jnp.int32)
    chosen = jnp.any(routes[:, :, None] == expert_ids[None, None, :], axis=1)
    raised_gate = jnp.where(chosen, jnp.exp(logits), 0.0)
    gates = raised_gate / jnp.sum(raised_gate, axis=-1, keepdims=True)
    gate_high = lax.reduce_precision(gates, 8, 7)
    gate_low = gates - gate_high
    extra = -(-3 * expert_count // 128) * 128
    payload = jnp.concatenate(
        [
            ffn_low,
            chosen.astype(bf),
            gate_high.astype(bf),
            gate_low.astype(bf),
            jnp.zeros((tok_rows, extra - 3 * expert_count), bf),
        ],
        axis=1,
    )
    (payload_all,) = gather_all([payload], 3)
    (out_part, rows, gate_act, up_act), cot_b = experts_forward(
        payload_all, w_gate, w_up, w_down, expert_count, tok_rows, capacity, cotangent[half:], 2
    )
    moe_out = lax.psum_scatter(out_part, "expert", scatter_dimension=0, tiled=True)
    grad_part, grad_wgate, grad_wup, grad_wdown = experts_backward(
        payload_all, cot_a, cot_b, rows, gate_act, up_act, w_gate, w_up, w_down, expert_count, tok_rows, capacity
    )
    (grad_sum,) = scatter_all([grad_part], 4)
    grad_sum, moe_out = lax.optimization_barrier((grad_sum, moe_out))
    upstream = cotangent.astype(f32)
    grad_ffn = grad_sum[:, :model_width]
    grad_shares = (
        grad_sum[:, model_width : model_width + expert_count]
        + grad_sum[:, model_width + expert_count : model_width + 2 * expert_count]
    )
    grad_logits = (grad_shares - gates * jnp.sum(grad_shares, axis=-1, keepdims=True)).astype(bf)
    grad_wrouter = matmul_tn(ffn_low, grad_logits)
    grad_ffn = grad_ffn + matmul_nt(grad_logits, wr_full)
    grad_second, grad_ffn_gain = norm_back(residual, ffn_gain, grad_ffn)
    grad_residual = upstream + grad_second
    grad_attn_low = grad_residual.astype(bf)
    grad_wout = matmul_tn(mix_low, grad_attn_low).astype(bf)
    grad_mix = matmul_nt(grad_attn_low, wo_full).astype(bf)
    grad_mix, grad_wout = lax.optimization_barrier((grad_mix, grad_wout))
    out_grad = lax.psum_scatter(grad_wout, "expert", scatter_dimension=0, tiled=True)

    grad_q_low, grad_kv, grad_query_gain = attention_backward(
        q_proj, q_low, k_low, v_low, grad_mix, query_gain, cosine, sine
    )
    grad_kv = line_scatter(grad_kv, 6)
    own_rows = shard_pos * tok_rows
    k_proj = lax.dynamic_slice(kv_proj, (own_rows, 0), (tok_rows, kv_cols))
    positions = own_rows + jnp.arange(tok_rows, dtype=jnp.int32)
    _, k_pull = jax.vjp(
        lambda projected, gain_vec: head_prep(projected, gain_vec, positions, HK, 1.0), k_proj, key_gain
    )
    grad_k_proj, grad_key_gain = k_pull(grad_kv[:, :kv_cols].reshape(tok_rows, HK, HD))
    grad_qkv_low = jnp.concatenate(
        [grad_q_low, grad_k_proj.astype(bf), grad_kv[:, kv_cols:].astype(bf)], axis=1
    )
    grad_wqkv = matmul_tn(normed_low, grad_qkv_low).astype(bf)
    grad_normed = matmul_nt(grad_qkv_low, wqkv_full)
    grad_front, grad_attn_gain = norm_back(inputs_f, attn_gain, grad_normed)
    grad_input = (grad_residual + grad_front).astype(bf)

    grads = [grad_wrouter, grad_attn_gain, grad_ffn_gain, grad_query_gain, grad_key_gain]
    packed = jnp.concatenate(
        [g.astype(bf).reshape(devices, -1) for g in grads] + [jnp.zeros((devices, small_rows * 128 - used), bf)], axis=1
    ).reshape(devices * small_rows, 128)
    grad_wqkv, out_grad = lax.optimization_barrier((grad_wqkv, out_grad))
    out_grad = lax.psum_scatter(out_grad, "shard", scatter_dimension=0, tiled=True).astype(f32)
    qkv_grad, small_grad, moe_out = scatter_all([grad_wqkv, packed], 8, line=[moe_out])
    block_out = (residual + moe_out).astype(bf)
    small_grad = small_grad.reshape(-1)
    router_g, attn_g, ffn_g, query_g, key_g = [small_grad[o : o + n] for o, n in zip(starts, sizes)]
    return (
        block_out,
        grad_input,
        attn_g,
        qkv_grad[:, :q_cols],
        qkv_grad[:, q_cols : q_cols + kv_cols],
        qkv_grad[:, q_cols + kv_cols :],
        query_g,
        key_g,
        out_grad,
        ffn_g,
        router_g.reshape(w_router.shape),
        grad_wgate,
        grad_wup,
        grad_wdown,
    )


def solution(mesh):
    row = P(BOTH, None)
    vec = P(BOTH)
    cube = P(BOTH, None, None)
    in_specs = (row, vec, row, row, row, vec, vec, row, vec, row, cube, cube, cube, row, row)
    out_specs = (row, row, vec, row, row, row, vec, vec, row, vec, row, cube, cube, cube)
    return jax.shard_map(
        per_device, mesh=mesh, in_specs=in_specs, out_specs=out_specs, check_vma=False
    )
```

```python
import functools

import jax
import jax.numpy as jnp
from jax import lax
from jax.experimental import pallas as pl
from jax.experimental.pallas import tpu as pltpu
from jax.sharding import PartitionSpec as P

MESH = pl.DeviceIdType.MESH
NZ = 4

def placed():
    return lax.axis_size("expert") == 8 and lax.axis_size("shard") == NZ

def place():
    e = lax.axis_index("expert"); s = lax.axis_index("shard")
    return e // 4, lax.rem(e // 2, 2), lax.rem(e, 2), s

def dev(y, x, c, s):
    return (y * 4 + x * 2 + c, s)

def barrier_all(y, x, c, s):
    bar = pltpu.get_barrier_semaphore()
    def sig(d): pl.semaphore_signal(bar, inc=1, device_id=d, device_id_type=MESH)
    sig(dev(1 - y, x, c, s)); sig(dev(y, 1 - x, c, s)); sig(dev(y, x, 1 - c, s))
    @pl.when(s > 0)
    def _(): sig(dev(y, x, c, s - 1))
    @pl.when(s < NZ - 1)
    def _(): sig(dev(y, x, c, s + 1))
    pl.semaphore_wait(bar, 3 + jnp.where(s > 0, 1, 0) + jnp.where(s < NZ - 1, 1, 0))

def ag_kernel(n_arr, n_line, *refs):
    n_all = n_arr + n_line
    for run in ag_steps(n_arr, n_line, refs[:n_all], refs[n_all:2 * n_all], refs[2 * n_all:]): run()

AG_STEPS = 10

def ag_steps(n_arr, n_line, ins, outs, sems):
    n_all = n_arr + n_line
    loc_sem, zs, zr, ps, pr, cs, cr = sems
    y, x, c, s = place()
    def rc(src, dst, ss, rs, d):
        return pltpu.make_async_remote_copy(src_ref=src, dst_ref=dst, send_sem=ss, recv_sem=rs, device_id=d, device_id_type=MESH)
    X = dev(y, 1 - x, c, s); Y = dev(1 - y, x, c, s); C = dev(y, x, 1 - c, s)
    A = range(n_arr)
    every = range(n_all)
    def home(a, zz):
        return outs[a].at[y, x, c, zz] if a < n_arr else outs[a].at[zz]
    steps = [(0, 0)] + [(d, g) for d in range(1, NZ) for g in (1, -1)]
    def valid(d, g):
        return (s >= d) if g == 1 else (s + d <= NZ - 1)
    def zof(d, g): return s - d * g
    def src_own(a, h, zz, k):
        return ins[a].at[h] if k == 0 else home(a, zz).at[h]
    def zcopy(a, h, zz, k, g):
        kk = 1 + 2 * (k_dist(k)) + (0 if g == 1 else 1)
        return rc(src_own(a, h, zz, k), home(a, zz).at[h], zs.at[a, h, kk], zr.at[a, h, kk], dev(y, x, c, s + g))
    def k_dist(k): return steps[k][0]
    def plane(a, h, zz, k, which):
        return rc(src_own(a, h, zz, k), outs[a].at[y, x, c, zz, h], ps.at[a, k, h, which], pr.at[a, k, h, which], X if which == 0 else Y)
    def plane_recv(a, h, zz, k, which):
        d = outs[a].at[y, 1 - x, c, zz, h] if which == 0 else outs[a].at[1 - y, x, c, zz, h]
        return rc(d, d, ps.at[a, k, h, which], pr.at[a, k, h, which], X if which == 0 else Y)
    def diag(a, h, zz, k):
        d = outs[a].at[y, 1 - x, c, zz, h] if h == 0 else outs[a].at[1 - y, x, c, zz, h]
        return rc(d, d, ps.at[a, k, h, 2], pr.at[a, k, h, 2], Y if h == 0 else X)
    def diag_recv(a, h, zz, k):
        d = outs[a].at[1 - y, 1 - x, c, zz, h]
        return rc(d, d, ps.at[a, k, h, 2], pr.at[a, k, h, 2], Y if h == 0 else X)
    def core(a, zz, k, part):
        d = outs[a].at[:, :, c, zz]
        return rc(d, d, cs.at[a, k], cr.at[a, k], C)
    def core_recv(a, zz, k):
        d = outs[a].at[:, :, 1 - c, zz]
        return rc(d, d, cs.at[a, k], cr.at[a, k], C)
    def loc(a):
        return pltpu.make_async_copy(ins[a], home(a, s), loc_sem.at[a])

    def when(k, f):
        d, g = steps[k]
        if k == 0: f()
        else: pl.when(valid(d, g))(f)

    def stage_a(k):
        d, g = steps[k]
        def go():
            zz = zof(d, g)
            for a in every:
                for h in range(2):
                    if k:
                        kk = k
                        dref = home(a, zz).at[h]
                        rc(dref, dref, zs.at[a, h, kk], zr.at[a, h, kk], X).wait_recv()
                    for gg in ((1, -1) if k == 0 else (g,)):
                        okc = (s < NZ - 1) if gg == 1 else (s > 0)
                        if d + 1 < NZ:
                            @pl.when(okc)
                            def _(): zcopy(a, h, zz, k, gg).start()
                    if a < n_arr:
                        plane(a, h, zz, k, 0).start()
                        plane(a, h, zz, k, 1).start()
        when(k, go)
    def stage_b(k):
        d, g = steps[k]
        def go():
            zz = zof(d, g)
            for a in A:
                plane_recv(a, 0, zz, k, 0).wait_recv()
                diag(a, 0, zz, k).start()
                plane_recv(a, 1, zz, k, 1).wait_recv()
                diag(a, 1, zz, k).start()
        when(k, go)
    def stage_c(k):
        d, g = steps[k]
        def go():
            zz = zof(d, g)
            for a in A:
                if k == 0: loc(a).wait()
                plane_recv(a, 1, zz, k, 0).wait_recv()
                plane_recv(a, 0, zz, k, 1).wait_recv()
                diag_recv(a, 0, zz, k).wait_recv()
                diag_recv(a, 1, zz, k).wait_recv()
                core(a, zz, k, 0).start()
        when(k, go)
    n = len(steps)
    def advance(i):
        if i == 0:
            barrier_all(y, x, c, s)
            for a in every: loc(a).start()
        if i < n: stage_a(i)
        if 0 <= i - 1 < n: stage_b(i - 1)
        if 0 <= i - 2 < n: stage_c(i - 2)
    def finish():
        for k in range(n):
            d, g = steps[k]
            def go():
                zz = zof(d, g)
                for a in every:
                    if a < n_arr:
                        core_recv(a, zz, k).wait_recv()
                        core(a, zz, k, 0).wait_send()
                    elif k == 0: loc(a).wait()
                    for h in range(2):
                        for gg in ((1, -1) if k == 0 else (g,)):
                            okc = (s < NZ - 1) if gg == 1 else (s > 0)
                            if d + 1 < NZ:
                                @pl.when(okc)
                                def _(): zcopy(a, h, zz, k, gg).wait_send()
                        if a < n_arr:
                            plane(a, h, zz, k, 0).wait_send()
                            plane(a, h, zz, k, 1).wait_send()
                            diag(a, h, zz, k).wait_send()
            when(k, go)
    return [functools.partial(advance, i) for i in range(n + 2)] + [finish]

def ag_sems(n, m=0):
    D = pltpu.SemaphoreType.DMA
    return [D((n + m,)), D((n + m, 2, 9)), D((n + m, 2, 9)), D((n, 7, 2, 3)), D((n, 7, 2, 3)), D((n, 7)), D((n, 7))]

def ag32(arrs, cid, line=()):
    ins = [a.reshape(2, a.shape[0] // 2, a.shape[1]) for a in list(arrs) + list(line)]
    n, m = len(arrs), len(line)
    outs = pl.pallas_call(
        functools.partial(ag_kernel, n, m),
        out_shape=[jax.ShapeDtypeStruct(((2, 2, 2, NZ) if i < n else (NZ,)) + a.shape, a.dtype) for i, a in enumerate(ins)],
        in_specs=[pl.BlockSpec(memory_space=pltpu.VMEM)] * (n + m),
        out_specs=[pl.BlockSpec(memory_space=pl.ANY)] * (n + m),
        scratch_shapes=ag_sems(n, m),
        compiler_params=pltpu.CompilerParams(collective_id=cid, has_side_effects=True, vmem_limit_bytes=64000 * 1024),
        name="gather_all",
    )(*ins)
    return [o.reshape(-1, a.shape[1] * 2, a.shape[2]) for o, a in zip(outs, ins)]

ZORDER = (0, 3, 1, 2)
LAGS = (1, 1, 1, 1)

def rs_kernel(n_arr, n_line, parts, *refs):
    n_all = n_arr + n_line
    ins = refs[:n_all]; outs = refs[n_all:2 * n_all]
    sc = list(refs[2 * n_all:])
    own_b = [sc.pop(0) for _ in range(n_all)]; zu_b = [sc.pop(0) for _ in range(n_all)]; zd_b = [sc.pop(0) for _ in range(n_all)]
    r0_b, ra_b, rb_b = [[sc.pop(0) for _ in range(n_arr)] for _ in range(3)]
    lsem, s0s, s0r, sas, sar, sbs, sbr, zus, zur, zds, zdr = sc
    y, x, c, s = place()
    barrier_all(y, x, c, s)
    X = dev(y, 1 - x, c, s); Y = dev(1 - y, x, c, s); C = dev(y, x, 1 - c, s)
    UP = dev(y, x, c, s + 1); DN = dev(y, x, c, s - 1)
    def rc(src, dst, ss, rs, d):
        return pltpu.make_async_remote_copy(src_ref=src, dst_ref=dst, send_sem=ss, recv_sem=rs, device_id=d, device_id_type=MESH)
    units = [(a, zz, h) for zz in ZORDER for h in range(parts) for a in range(n_arr)]
    lines = [(a, zz, h) for zz in ZORDER for h in range(parts) for a in range(n_arr, n_all)]
    def jj(zz, h): return ZORDER.index(zz) * parts + h
    def load(a, zz, h):
        j = jj(zz, h)
        src = ins[a].at[:, :, c, zz, h] if a < n_arr else ins[a].at[zz, h]
        return pltpu.make_async_copy(src, own_b[a].at[j], lsem.at[a, j])
    def mine(a, j):
        return own_b[a].at[j, y, x] if a < n_arr else own_b[a].at[j]
    def c0(a, zz, h):
        j = jj(zz, h)
        return rc(ins[a].at[:, :, 1 - c, zz, h], r0_b[a].at[j], s0s.at[a, j], s0r.at[a, j], C)
    def ca(a, zz, h):
        j = jj(zz, h)
        if h % 2 == 0: return rc(own_b[a].at[j, :, 1 - x], ra_b[a].at[j], sas.at[a, j], sar.at[a, j], X)
        return rc(own_b[a].at[j, 1 - y], ra_b[a].at[j], sas.at[a, j], sar.at[a, j], Y)
    def cb(a, zz, h):
        j = jj(zz, h)
        if h % 2 == 0: return rc(own_b[a].at[j, 1 - y, x], rb_b[a].at[j], sbs.at[a, j], sbr.at[a, j], Y)
        return rc(own_b[a].at[j, y, 1 - x], rb_b[a].at[j], sbs.at[a, j], sbr.at[a, j], X)
    def cu(a, zz, h):
        j = jj(zz, h)
        return rc(mine(a, j), zu_b[a].at[j], zus.at[a, j], zur.at[a, j], UP)
    def cd(a, zz, h):
        j = jj(zz, h)
        return rc(mine(a, j), zd_b[a].at[j], zds.at[a, j], zdr.at[a, j], DN)
    def add_into(dst, other):
        rows = dst.shape[0]
        st = 16 if rows % 16 == 0 else rows
        @pl.loop(0, rows // st)
        def _(i):
            r = pl.ds(i * st, st)
            dst[r, :] = (dst[r, :].astype(jnp.float32) + other[r, :].astype(jnp.float32)).astype(dst.dtype)
    def stage0(u):
        a, zz, h = u; j = jj(zz, h)
        load(a, zz, h).wait()
        c0(a, zz, h).wait_recv()
        for yy in range(2):
            for xx in range(2):
                add_into(own_b[a].at[j, yy, xx], r0_b[a].at[j, yy, xx])
        ca(a, zz, h).start()
    def stage1(u):
        a, zz, h = u; j = jj(zz, h)
        ca(a, zz, h).wait_recv()
        for q in range(2):
            if h % 2 == 0: add_into(own_b[a].at[j, q, x], ra_b[a].at[j, q])
            else: add_into(own_b[a].at[j, y, q], ra_b[a].at[j, q])
        cb(a, zz, h).start()
    def stage2(u):
        a, zz, h = u; j = jj(zz, h)
        cb(a, zz, h).wait_recv()
        add_into(own_b[a].at[j, y, x], rb_b[a].at[j])
    def hop(u, k):
        a, zz, h = u; j = jj(zz, h)
        if k < zz:
            @pl.when(s == k)
            def _():
                if k > 0:
                    cu(a, zz, h).wait_recv()
                    add_into(mine(a, j), zu_b[a].at[j])
                cu(a, zz, h).start()
        t = NZ - 1 - k
        if t > zz:
            @pl.when(s == t)
            def _():
                if k > 0:
                    cd(a, zz, h).wait_recv()
                    add_into(mine(a, j), zd_b[a].at[j])
                cd(a, zz, h).start()
    def last(u):
        a, zz, h = u; j = jj(zz, h)
        @pl.when(s == zz)
        def _():
            if zz > 0: cu(a, zz, h).wait_recv()
            if zz < NZ - 1: cd(a, zz, h).wait_recv()
            t = mine(a, j)[...].astype(jnp.float32)
            if zz > 0: t = t + zu_b[a][j].astype(jnp.float32)
            if zz < NZ - 1: t = t + zd_b[a][j].astype(jnp.float32)
            outs[a][h] = t.astype(outs[a].dtype)
    for u in lines: load(*u).start()
    for u in units:
        c0(*u).start(); load(*u).start()
    n = len(units); nl = len(lines)
    L1 = LAGS[0] * n_arr; L2 = L1 + LAGS[1] * n_arr; L3 = L2 + LAGS[2] * n_arr; dl = LAGS[3] * n_arr
    for i in range(n + L3 + (NZ - 1) * dl):
        if i < n: stage0(units[i])
        if 0 <= i - L1 < n: stage1(units[i - L1])
        if 0 <= i - L2 < n: stage2(units[i - L2])
        for k in range(NZ - 1):
            for q in (2 * (i - k), 2 * (i - k) + 1):
                if 0 <= q < nl:
                    if k == 0: load(*lines[q]).wait()
                    hop(lines[q], k)
        for k in range(NZ - 1):
            if 0 <= i - L3 - k * dl < n: hop(units[i - L3 - k * dl], k)
    for u in lines + units: last(u)
    for u in lines + units:
        a, zz, h = u
        if a < n_arr:
            c0(*u).wait_send(); ca(*u).wait_send(); cb(*u).wait_send()
        if zz > 0:
            @pl.when(s < zz)
            def _(): cu(*u).wait_send()
        if zz < NZ - 1:
            @pl.when(s > zz)
            def _(): cd(*u).wait_send()

def rs32(arrs, cid, out_dtype=jnp.float32, parts=4, line=()):
    n, nl = len(arrs), len(line)
    both = list(arrs) + list(line)
    if any(a.shape[1] % (parts * 16) for a in both): parts = 2
    ins = [a.reshape(((2, 2, 2) if i < n else ()) + (NZ, parts, a.shape[1] // parts, a.shape[2])) for i, a in enumerate(both)]
    hs = [i.shape[-2:] for i in ins]
    V = pltpu.VMEM; bt = jnp.bfloat16; m = NZ * parts
    sems = [pltpu.SemaphoreType.DMA((n + nl, m))] * 11
    outs = pl.pallas_call(
        functools.partial(rs_kernel, n, nl, parts),
        out_shape=[jax.ShapeDtypeStruct((parts,) + h, out_dtype) for h in hs],
        in_specs=[pl.BlockSpec(memory_space=pl.ANY)] * (n + nl),
        out_specs=[pl.BlockSpec(memory_space=pltpu.VMEM)] * (n + nl),
        scratch_shapes=[V((m,) + ((2, 2) if i < n else ()) + h, bt) for i, h in enumerate(hs)] + [V((m,) + h, bt) for h in hs] + [V((m,) + h, bt) for h in hs]
            + [V((m, 2, 2) + h, bt) for h in hs[:n]] + [V((m, 2) + h, bt) for h in hs[:n]] + [V((m,) + h, bt) for h in hs[:n]] + sems,
        compiler_params=pltpu.CompilerParams(collective_id=cid, has_side_effects=True, vmem_limit_bytes=64000 * 1024),
        name="scatter_all",
    )(*ins)
    return [o.reshape(a.shape[1], a.shape[2]) for o, a in zip(outs, both)]

def line_barrier(y, x, c, s):
    bar = pltpu.get_barrier_semaphore()
    @pl.when(s > 0)
    def _(): pl.semaphore_signal(bar, inc=1, device_id=dev(y, x, c, s - 1), device_id_type=MESH)
    @pl.when(s < NZ - 1)
    def _(): pl.semaphore_signal(bar, inc=1, device_id=dev(y, x, c, s + 1), device_id_type=MESH)
    pl.semaphore_wait(bar, jnp.where(s > 0, 1, 0) + jnp.where(s < NZ - 1, 1, 0))

def line_gather_kernel(parts, x_ref, o_ref, ss, rs):
    y, x, c, s = place()
    line_barrier(y, x, c, s)
    def cp(d, g, h):
        src = x_ref.at[h] if d == 0 else o_ref.at[s - d * g, h]
        k = 0 if g == 1 else 1
        return pltpu.make_async_remote_copy(src_ref=src, dst_ref=o_ref.at[s - d * g, h], send_sem=ss.at[k, d, h], recv_sem=rs.at[k, d, h],
            device_id=dev(y, x, c, s + g), device_id_type=MESH)
    def arrived(d, g, h):
        k = 0 if g == 1 else 1
        ref = o_ref.at[s - (d + 1) * g, h]
        return pltpu.make_async_remote_copy(src_ref=ref, dst_ref=ref, send_sem=ss.at[k, d, h], recv_sem=rs.at[k, d, h],
            device_id=dev(y, x, c, s + g), device_id_type=MESH)
    def sends(d, g): return (s >= d) & (s < NZ - 1) if g == 1 else (s + d <= NZ - 1) & (s > 0)
    def gets(d, g): return s >= d + 1 if g == 1 else s + d + 1 <= NZ - 1
    for d in range(NZ):
        for h in range(parts):
            for g in (1, -1):
                if d:
                    @pl.when(gets(d - 1, g))
                    def _(): arrived(d - 1, g, h).wait_recv()
                if d < NZ - 1:
                    @pl.when(sends(d, g))
                    def _(): cp(d, g, h).start()
        if d == 0: o_ref[s] = x_ref[...]
    for d in range(NZ - 1):
        for h in range(parts):
            for g in (1, -1):
                @pl.when(sends(d, g))
                def _(): cp(d, g, h).wait_send()

def line_gather(x, cid, parts=4):
    if not placed():
        return lax.all_gather(x, "shard", axis=0, tiled=True)
    R, C = x.shape
    sem = pltpu.SemaphoreType.DMA((2, NZ, parts))
    o = pl.pallas_call(functools.partial(line_gather_kernel, parts), out_shape=jax.ShapeDtypeStruct((NZ, parts, R // parts, C), x.dtype),
        in_specs=[pl.BlockSpec(memory_space=pltpu.VMEM)], out_specs=pl.BlockSpec(memory_space=pltpu.VMEM),
        scratch_shapes=[sem, sem], compiler_params=pltpu.CompilerParams(collective_id=cid, has_side_effects=True, vmem_limit_bytes=16 << 20),
        name="line_gather")(x.reshape(parts, R // parts, C))
    return o.reshape(NZ * R, C)

def line_scatter_kernel(parts, p_ref, o_ref, *scratch):
    for run in line_scatter_steps(parts, p_ref, o_ref, scratch): run()

LINE_PARTS = 4
LINE_STEPS = 3 * LINE_PARTS + NZ + 1

def line_scatter_steps(parts, p_ref, o_ref, scratch):
    acc, zu, zd, ss_u, rs_u, ss_d, rs_d = scratch
    y, x, c, s = place()
    def rc(src, dst, a, b, d):
        return pltpu.make_async_remote_copy(src_ref=src, dst_ref=dst, send_sem=a, recv_sem=b, device_id=d, device_id_type=MESH)
    def cu(zz, h, k):
        src = p_ref.at[zz, h] if k == 0 else acc.at[zz, h]
        return rc(src, zu.at[zz, h], ss_u.at[zz, h], rs_u.at[zz, h], dev(y, x, c, s + 1))
    def cd(zz, h, k):
        src = p_ref.at[zz, h] if k == 0 else acc.at[zz, h]
        return rc(src, zd.at[zz, h], ss_d.at[zz, h], rs_d.at[zz, h], dev(y, x, c, s - 1))
    st = 32
    def total(dst, refs):
        @pl.loop(0, dst.shape[0] // st)
        def _(i):
            r = pl.ds(i * st, st)
            t = refs[0][r, :].astype(jnp.float32)
            for f in refs[1:]: t = t + f[r, :].astype(jnp.float32)
            dst[r, :] = t.astype(dst.dtype)
    ups = [(zz, h) for zz in (3, 2, 1) for h in range(parts)]
    dns = [(zz, h) for zz in (0, 1, 2) for h in range(parts)]
    n = len(ups)
    def advance(i):
        if i == 0: line_barrier(y, x, c, s)
        for k in range(NZ - 1):
            if 0 <= i - k < n:
                zz, h = ups[i - k]
                if k < zz:
                    @pl.when(s == k)
                    def _():
                        if k:
                            cu(zz, h, k).wait_recv()
                            total(acc.at[zz, h], [p_ref.at[zz, h], zu.at[zz, h]])
                        cu(zz, h, k).start()
                zz, h = dns[i - k]
                if NZ - 1 - k > zz:
                    @pl.when(s == NZ - 1 - k)
                    def _():
                        if k:
                            cd(zz, h, k).wait_recv()
                            total(acc.at[zz, h], [p_ref.at[zz, h], zd.at[zz, h]])
                        cd(zz, h, k).start()
    def finish():
        for zz in range(NZ):
            @pl.when(s == zz)
            def _():
                for h in range(parts):
                    refs = [p_ref.at[zz, h]]
                    if zz > 0:
                        cu(zz, h, 1).wait_recv()
                        refs.append(zu.at[zz, h])
                    if zz < NZ - 1:
                        cd(zz, h, 1).wait_recv()
                        refs.append(zd.at[zz, h])
                    total(o_ref.at[h], refs)
        for zz, h in ups:
            @pl.when(s < zz)
            def _(): cu(zz, h, 1).wait_send()
        for zz, h in dns:
            @pl.when(s > zz)
            def _(): cd(zz, h, 1).wait_send()
    return [functools.partial(advance, i) for i in range(n + NZ)] + [finish]

def line_scatter_scratch(parts, rows, cols, dtype):
    sem = pltpu.SemaphoreType.DMA((NZ, parts))
    buf = pltpu.VMEM((NZ, parts, rows // parts, cols), dtype)
    return [buf, buf, buf, sem, sem, sem, sem]

def line_scatter(p, cid, parts=LINE_PARTS):
    if not placed():
        return lax.psum_scatter(p, "shard", scatter_dimension=0, tiled=True).astype(jnp.float32)
    R, C = p.shape[0] // NZ, p.shape[1]
    shape = (NZ, parts, R // parts, C)
    o = pl.pallas_call(functools.partial(line_scatter_kernel, parts), out_shape=jax.ShapeDtypeStruct(shape[1:], jnp.float32),
        in_specs=[pl.BlockSpec(memory_space=pltpu.VMEM)], out_specs=pl.BlockSpec(memory_space=pltpu.VMEM),
        scratch_shapes=line_scatter_scratch(parts, R, C, p.dtype), compiler_params=pltpu.CompilerParams(collective_id=cid, has_side_effects=True, vmem_limit_bytes=24 << 20),
        name="line_scatter")(p.reshape(shape))
    return o.reshape(R, C)


def dot(a, b, ca, cb):
    return lax.dot_general(a, b, (((ca,), (cb,)), ((), ())), preferred_element_type=jnp.float32)

def token_picks(meta, experts, slots, me):
    SB, WM = meta.shape
    bf, f32 = jnp.bfloat16, jnp.float32
    tri = (lax.broadcasted_iota(jnp.int32, (SB, SB), 1) < lax.broadcasted_iota(jnp.int32, (SB, SB), 0)).astype(bf)
    lane = lax.broadcasted_iota(jnp.int32, (SB, WM), 1)
    cnt = dot(tri, meta, 1, 0)
    metaf = meta.astype(f32)
    msk = jnp.sum(jnp.where(lane == me, metaf, 0.0), axis=-1, keepdims=True)
    pos = jnp.sum(jnp.where(lane == me, cnt, 0.0), axis=-1, keepdims=True)
    gate = jnp.sum(jnp.where((lane == me + experts) | (lane == me + 2 * experts), metaf, 0.0), axis=-1, keepdims=True)
    want = jnp.where(msk > 0.0, pos, -1.0).astype(jnp.int32)
    pick = (want == lax.broadcasted_iota(jnp.int32, (SB, slots), 1)).astype(bf)
    return pick, gate

def forward_kernel(experts, slots, SB, guest, *refs):
    if guest:
        cot_ref, x_ref, wg_hbm, wu_hbm, wd_hbm, cot_all, out_ref, rows_ref, ga_ref, ua_ref, wg, wu, wd, wsem = refs[:14]
    else:
        x_ref, wg_hbm, wu_hbm, wd_hbm, out_ref, rows_ref, ga_ref, ua_ref, wg, wu, wd, wsem = refs
    bf = jnp.bfloat16
    step = pl.program_id(0)
    if guest:
        runs = ag_steps(1, 0, [cot_ref], [cot_all], refs[14:])
        for i, run in enumerate(runs[:-1]):
            pl.when(step == GUEST_AT[i])(run)
    nsub = x_ref.shape[0] // SB
    D = out_ref.shape[1]
    me = lax.axis_index(("expert", "shard"))
    loads = [pltpu.make_async_copy(h.at[0], v, wsem.at[i]) for i, (h, v) in enumerate(((wg_hbm, wg), (wu_hbm, wu), (wd_hbm, wd)))]
    @pl.when(step == 0)
    def _():
        for l in loads: l.start()
    picks, gates = [], []
    for i in range(nsub):
        r = pl.ds(i * SB, SB)
        pick, gate = token_picks(x_ref[r, D:], experts, slots, me)
        picks.append(pick); gates.append(gate)
        rows_ref[i * slots:(i + 1) * slots, :] = dot(pick, x_ref[r, :D], 0, 0).astype(bf)
    @pl.when(step == 0)
    def _():
        for l in loads: l.wait()
    ga = dot(rows_ref[...], wg[...], 1, 0)
    ua = dot(rows_ref[...], wu[...], 1, 0)
    ga_ref[...] = ga
    ua_ref[...] = ua
    hid = (ga * (1.0 / (1.0 + jnp.exp(-ga))) * ua).astype(bf)
    eo = dot(hid, wd[...], 1, 0).astype(bf)
    for i in range(nsub):
        r = pl.ds(i * SB, SB)
        tok = dot(picks[i], eo[i * slots:(i + 1) * slots, :], 1, 0)
        out_ref[r, :] = (gates[i] * tok).astype(bf)
    if guest: pl.when(step == pl.num_programs(0) - 1)(runs[-1])

GUEST_AT = (0, 1, 3, 4, 6, 7, 9, 11, 13)

def backward_kernel(experts, slots, SB, block, meta_ref, cota_ref, cotb_ref, rows_ref, ga_ref, ua_ref, wg_hbm, wu_hbm, wd_hbm, gr_ref, dwg_hbm, dwu_hbm, dwd_hbm,
                  wg, wu, wd, dwg, dwu, dwd, gp, wsem, osem):
    bf = jnp.bfloat16
    step = pl.program_id(0)
    nsub = meta_ref.shape[0] // SB
    D = cota_ref.shape[1]
    WM = meta_ref.shape[1]
    na, nb = [r.shape[0] * block // meta_ref.shape[0] for r in (cota_ref, cotb_ref)]
    me = lax.axis_index(("expert", "shard"))
    loads = [pltpu.make_async_copy(h.at[0], v, wsem.at[i]) for i, (h, v) in enumerate(((wg_hbm, wg), (wu_hbm, wu), (wd_hbm, wd)))]
    @pl.when(step == 0)
    def _():
        for l in loads: l.start()
        for a in (dwg, dwu, dwd): a[...] = jnp.zeros_like(a)
    picks = []
    for i in range(nsub):
        r = pl.ds(i * SB, SB)
        pick, gate = token_picks(meta_ref[r, :], experts, slots, me)
        picks.append(pick)
        cot = []
        for b in range(i * SB // block, (i + 1) * SB // block):
            cot += [cota_ref[b * na:(b + 1) * na, :], cotb_ref[b * nb:(b + 1) * nb, :]]
        gcot = (gate * jnp.concatenate(cot, axis=0).astype(jnp.float32)).astype(bf)
        gp[i * slots:(i + 1) * slots, :] = dot(pick, gcot, 0, 0).astype(bf)
    @pl.when(step == 0)
    def _():
        for l in loads: l.wait()
    ga = ga_ref[...]
    ua = ua_ref[...]
    sig = 1.0 / (1.0 + jnp.exp(-ga))
    act = ga * sig
    hidf = act * ua
    hid = hidf.astype(bf)
    gh = dot(gp[...], wd[...], 1, 1)
    share = jnp.sum(gh * hid.astype(jnp.float32), axis=-1, keepdims=True)
    dga = (gh * ua * (sig * (1.0 + ga * (1.0 - sig)))).astype(bf)
    dua = (gh * act).astype(bf)
    dwd[...] += dot(hid, gp[...], 0, 0)
    grow = (dot(dga, wg[...], 1, 1) + dot(dua, wu[...], 1, 1)).astype(bf)
    dwg[...] += dot(rows_ref[...], dga, 0, 0)
    dwu[...] += dot(rows_ref[...], dua, 0, 0)
    lane = lax.broadcasted_iota(jnp.int32, (share.shape[0], WM), 1)
    high = share.astype(bf).astype(jnp.float32)
    tail = (jnp.where(lane == me, high, 0.0) + jnp.where(lane == me + experts, share - high, 0.0)).astype(bf)
    for i in range(nsub):
        r = pl.ds(i * SB, SB)
        q = slice(i * slots, (i + 1) * slots)
        gr_ref[r, :D] = dot(picks[i], grow[q, :], 1, 0).astype(bf)
        gr_ref[r, D:] = dot(picks[i], tail[q, :], 1, 0).astype(bf)
    @pl.when(step == pl.num_programs(0) - 1)
    def _():
        outs = [pltpu.make_async_copy(v, h.at[0], osem.at[i]) for i, (v, h) in enumerate(((dwg, dwg_hbm), (dwu, dwu_hbm), (dwd, dwd_hbm)))]
        for o in outs: o.start()
        for o in outs: o.wait()

def experts_forward(x_all, w_gate, w_up, w_down, experts, block, capacity, guest, cid, TB=512, SB=256):
    hosted = placed()
    T, C = x_all.shape; D, F = w_gate.shape[1:]
    slots = max(SB // block, 1) * capacity
    total = TB // SB * slots
    S = T // SB * slots
    any_ = pl.BlockSpec(memory_space=pl.ANY)
    V = pltpu.VMEM; bf = jnp.bfloat16; f32 = jnp.float32
    blk = lambda r, c: pl.BlockSpec((r, c), lambda i: (i, 0))
    g = guest.reshape(2, guest.shape[0] // 2, guest.shape[1])
    res = pl.pallas_call(
        functools.partial(forward_kernel, experts, slots, SB, hosted),
        grid=(T // TB,),
        out_shape=([jax.ShapeDtypeStruct((2, 2, 2, NZ) + g.shape, g.dtype)] if hosted else []) + [jax.ShapeDtypeStruct((T, D), bf), jax.ShapeDtypeStruct((S, D), bf), jax.ShapeDtypeStruct((S, F), f32), jax.ShapeDtypeStruct((S, F), f32)],
        in_specs=([pl.BlockSpec(memory_space=pltpu.VMEM)] if hosted else []) + [blk(TB, C), any_, any_, any_],
        out_specs=([any_] if hosted else []) + [blk(TB, D), blk(total, D), blk(total, F), blk(total, F)],
        scratch_shapes=[V((D, F), bf), V((D, F), bf), V((F, D), bf), pltpu.SemaphoreType.DMA((3,))] + (ag_sems(1) if hosted else []),
        compiler_params=pltpu.CompilerParams(dimension_semantics=("arbitrary",), vmem_limit_bytes=65000 * 1024,
            **(dict(collective_id=cid, has_side_effects=True) if hosted else {})),
        cost_estimate=pl.CostEstimate(flops=48_000_000_000, bytes_accessed=130_000_000, transcendentals=0),
        name="experts_forward",
    )(*([g] if hosted else []), x_all, w_gate, w_up, w_down)
    if hosted: return res[1:], res[0].reshape(-1, guest.shape[1])
    return res, lax.all_gather(guest, BOTH, axis=0, tiled=True)

def experts_backward(x_all, cot_a, cot_b, rows, ga, ua, w_gate, w_up, w_down, experts, block, capacity, TB=512, SB=256):
    T, C = x_all.shape; D, F = w_gate.shape[1:]
    slots = max(SB // block, 1) * capacity
    total = TB // SB * slots
    WM = C - D
    any_ = pl.BlockSpec(memory_space=pl.ANY)
    V = pltpu.VMEM; bf = jnp.bfloat16; f32 = jnp.float32
    blk = lambda r, c: pl.BlockSpec((r, c), lambda i: (i, 0))
    meta = pl.BlockSpec((TB, WM), lambda i: (i, D // WM)) if D % WM == 0 else blk(TB, WM)
    meta_in = x_all if D % WM == 0 else x_all[:, D:]
    return pl.pallas_call(
        functools.partial(backward_kernel, experts, slots, SB, block),
        grid=(T // TB,),
        out_shape=[jax.ShapeDtypeStruct((T, C), bf), jax.ShapeDtypeStruct(w_gate.shape, f32), jax.ShapeDtypeStruct(w_up.shape, f32), jax.ShapeDtypeStruct(w_down.shape, f32)],
        in_specs=[meta, blk(cot_a.shape[0] * TB // T, D), blk(cot_b.shape[0] * TB // T, D), blk(total, D), blk(total, F), blk(total, F), any_, any_, any_],
        out_specs=[blk(TB, C), any_, any_, any_],
        scratch_shapes=[V((D, F), bf), V((D, F), bf), V((F, D), bf), V((D, F), f32), V((D, F), f32), V((F, D), f32), V((total, D), bf), pltpu.SemaphoreType.DMA((3,)), pltpu.SemaphoreType.DMA((3,))],
        compiler_params=pltpu.CompilerParams(dimension_semantics=("arbitrary",), vmem_limit_bytes=65000 * 1024),
        cost_estimate=pl.CostEstimate(flops=85_000_000_000, bytes_accessed=150_000_000, transcendentals=0),
        name="experts_backward",
    )(meta_in, cot_a, cot_b, rows, ga, ua, w_gate, w_up, w_down)


def rope_tables(seq_len):
    half = HD // 2
    frequency = theta_base ** (-2.0 * jnp.arange(half, dtype=jnp.float32) / HD)
    angles = jnp.arange(seq_len, dtype=jnp.float32)[:, None] * frequency[None, :]
    return jnp.concatenate([jnp.cos(angles)] * 2, axis=-1), jnp.concatenate([-jnp.sin(angles), jnp.sin(angles)], axis=-1)

def turn(u, cos, sin):
    return u * cos + pltpu.roll(u, HD // 2, 1) * sin

def scale_of(u):
    return lax.rsqrt(jnp.mean(u * u, axis=-1, keepdims=True) + epsilon)

def attention_forward_kernel(group, q_ref, k_ref, v_ref, gq_ref, gk_ref, cos_ref, sin_ref, ql_ref, kl_ref, vl_ref, mix_ref):
    bf, f32 = jnp.bfloat16, jnp.float32
    rows, seq = q_ref.shape[0], k_ref.shape[0]
    first = lax.axis_index("shard") * rows
    k = k_ref[...]
    kl_ref[...] = turn(k * scale_of(k) * gk_ref[...], cos_ref[...], sin_ref[...]).astype(bf)
    vl_ref[...] = v_ref[...].astype(bf)
    cos, sin = cos_ref[pl.ds(first, rows), :], sin_ref[pl.ds(first, rows), :]
    allowed = lax.broadcasted_iota(jnp.int32, (rows, seq), 1) <= first + lax.broadcasted_iota(jnp.int32, (rows, seq), 0)
    for j in range(group):
        cols = slice(j * HD, (j + 1) * HD)
        u = q_ref[:, cols]
        ql = (turn(u * scale_of(u) * gq_ref[...], cos, sin) * HD ** (-0.5)).astype(bf)
        ql_ref[:, cols] = ql
        scores = dot(ql, kl_ref[...], 1, 1)
        raised = jnp.where(allowed, jnp.exp(scores), 0.0)
        probs = (raised * (1.0 / jnp.sum(raised, axis=-1, keepdims=True))).astype(bf)
        mix_ref[:, cols] = dot(probs, vl_ref[...], 1, 0).astype(bf)

def attention_forward(q_proj, kv_proj, gq, gk, cos, sin):
    rows, seq = q_proj.shape[0], kv_proj.shape[0]
    group = HQ // HK
    bf = jnp.bfloat16
    whole = lambda a: pl.BlockSpec(a.shape, lambda i: (0, 0))
    gq, gk = gq[None, :], gk[None, :]
    return pl.pallas_call(
        functools.partial(attention_forward_kernel, group),
        grid=(HK,),
        out_shape=[jax.ShapeDtypeStruct(q_proj.shape, bf), jax.ShapeDtypeStruct((seq, HK * HD), bf), jax.ShapeDtypeStruct((seq, HK * HD), bf), jax.ShapeDtypeStruct(q_proj.shape, bf)],
        in_specs=[pl.BlockSpec((rows, group * HD), lambda i: (0, i)), pl.BlockSpec((seq, HD), lambda i: (0, i)), pl.BlockSpec((seq, HD), lambda i: (0, HK + i)), whole(gq), whole(gk), whole(cos), whole(sin)],
        out_specs=[pl.BlockSpec((rows, group * HD), lambda i: (0, i)), pl.BlockSpec((seq, HD), lambda i: (0, i)), pl.BlockSpec((seq, HD), lambda i: (0, i)), pl.BlockSpec((rows, group * HD), lambda i: (0, i))],
        compiler_params=pltpu.CompilerParams(dimension_semantics=("arbitrary",), vmem_limit_bytes=48 << 20),
        cost_estimate=pl.CostEstimate(flops=4_300_000_000, bytes_accessed=20_000_000, transcendentals=8_400_000),
        name="attention_forward",
    )(q_proj, kv_proj, kv_proj, gq, gk, cos, sin)

def attention_backward_kernel(group, guest, *refs):
    if guest:
        p_ref, u_ref, ql_ref, kl_ref, vl_ref, ga_ref, wo_ref, gq_ref, cos_ref, sin_ref, po_ref, gu_ref, gk_ref, gv_ref, gg_ref, gk_acc, gv_acc = refs[:17]
        runs = line_scatter_steps(LINE_PARTS, p_ref, po_ref, refs[17:])
        slots = HK * group
        at = {i * slots // (LINE_STEPS - 1): run for i, run in enumerate(runs[:-1])}
    else:
        u_ref, ql_ref, kl_ref, vl_ref, ga_ref, wo_ref, gq_ref, cos_ref, sin_ref, gu_ref, gk_ref, gv_ref, gg_ref, gk_acc, gv_acc = refs
        at = {}
    step = pl.program_id(0)
    bf, f32 = jnp.bfloat16, jnp.float32
    gm_all = dot(ga_ref[...], wo_ref[...], 1, 1).astype(bf)
    rows, seq = ql_ref.shape[0], kl_ref.shape[0]
    first = lax.axis_index("shard") * rows
    cos, sin = cos_ref[pl.ds(first, rows), :], sin_ref[pl.ds(first, rows), :]
    allowed = lax.broadcasted_iota(jnp.int32, (rows, seq), 1) <= first + lax.broadcasted_iota(jnp.int32, (rows, seq), 0)
    gain_grad = jnp.zeros((1, HD), f32)
    for j in range(group):
        for i in range(HK):
            if i * group + j in at: pl.when(step == i)(at[i * group + j])
        cols = slice(j * HD, (j + 1) * HD)
        ql, gm = ql_ref[:, cols], gm_all[:, cols]
        raised = jnp.where(allowed, jnp.exp(dot(ql, kl_ref[...], 1, 1)), 0.0)
        probs = raised * (1.0 / jnp.sum(raised, axis=-1, keepdims=True))
        gp = dot(gm, vl_ref[...], 1, 1)
        gs = (probs * (gp - jnp.sum(probs * gp, axis=-1, keepdims=True))).astype(bf)
        gv = dot(probs.astype(bf), gm, 0, 0)
        gk = dot(gs, ql, 0, 0)
        if j == 0:
            gv_acc[...] = gv
            gk_acc[...] = gk
        else:
            gv_acc[...] += gv
            gk_acc[...] += gk
        m = dot(gs, kl_ref[...], 1, 0) * HD ** (-0.5)
        m = m * cos + pltpu.roll(m * sin, HD // 2, 1)
        u = u_ref[:, cols]
        r = scale_of(u)
        gain_grad = gain_grad + jnp.sum(m * u * r, axis=0, keepdims=True)
        mg = m * gq_ref[...]
        gu_ref[:, cols] = (r * mg - u * (r * r * r) * jnp.mean(mg * u, axis=-1, keepdims=True)).astype(bf)
    gk_ref[...] = gk_acc[...].astype(bf)
    gv_ref[...] = gv_acc[...].astype(bf)
    gg_ref[0] = jnp.broadcast_to(gain_grad, (8, HD))
    if guest: pl.when(step == HK - 1)(runs[-1])

def attention_backward(q_proj, q_low, k_low, v_low, grad_attn, w_out, gq, cos, sin, guest, cid):
    rows, seq = q_low.shape[0], k_low.shape[0]
    group = HQ // HK
    bf, f32 = jnp.bfloat16, jnp.float32
    gq = gq[None, :]
    whole = lambda a: pl.BlockSpec(a.shape, lambda i: (0, 0))
    qb = pl.BlockSpec((rows, group * HD), lambda i: (0, i)); kb = pl.BlockSpec((seq, HD), lambda i: (0, i))
    hosted = placed()
    R, C = guest.shape[0] // lax.axis_size("shard"), guest.shape[1]
    shape = (NZ, LINE_PARTS, R // LINE_PARTS, C)
    vm = pl.BlockSpec(memory_space=pltpu.VMEM)
    *summed, grad_q, grad_k, grad_v, gain = pl.pallas_call(
        functools.partial(attention_backward_kernel, group, hosted),
        grid=(HK,),
        out_shape=([jax.ShapeDtypeStruct(shape[1:], f32)] if hosted else []) + [jax.ShapeDtypeStruct(q_low.shape, bf), jax.ShapeDtypeStruct(k_low.shape, bf), jax.ShapeDtypeStruct(k_low.shape, bf), jax.ShapeDtypeStruct((HK, 8, HD), f32)],
        in_specs=([vm] if hosted else []) + [qb, qb, kb, kb, whole(grad_attn), pl.BlockSpec((group * HD, w_out.shape[1]), lambda i: (i, 0)), whole(gq), whole(cos), whole(sin)],
        out_specs=([vm] if hosted else []) + [qb, kb, kb, pl.BlockSpec((1, 8, HD), lambda i: (i, 0, 0))],
        scratch_shapes=[pltpu.VMEM((seq, HD), f32), pltpu.VMEM((seq, HD), f32)] + (line_scatter_scratch(LINE_PARTS, R, C, bf) if hosted else []),
        compiler_params=pltpu.CompilerParams(dimension_semantics=("arbitrary",), vmem_limit_bytes=60 << 20,
            **(dict(collective_id=cid, has_side_effects=True) if hosted else {})),
        cost_estimate=pl.CostEstimate(flops=15_000_000_000, bytes_accessed=20_000_000, transcendentals=8_400_000),
        name="attention_backward",
    )(*([guest.reshape(shape)] if hosted else []), q_proj, q_low, k_low, v_low, grad_attn, w_out, gq, cos, sin)
    if hosted: total = summed[0].reshape(R, C)
    else: total = lax.psum_scatter(guest, "shard", scatter_dimension=0, tiled=True).astype(f32)
    return total, grad_q, jnp.concatenate([grad_k, grad_v], axis=1), jnp.sum(gain[:, 0], axis=0)

HQ = 32
HK = 4
HD = 128
epsilon = 1e-06
theta_base = 1000000.0
BOTH = ("expert", "shard")


def matmul(left, right):
    return jnp.dot(left, right, preferred_element_type=jnp.float32)


def matmul_tn(left, right):
    return lax.dot_general(
        left, right, (((0,), (0,)), ((), ())), preferred_element_type=jnp.float32
    )


def matmul_nt(left, right):
    return lax.dot_general(
        left, right, (((1,), (1,)), ((), ())), preferred_element_type=jnp.float32
    )


def norm_rows(values, gain_vec):
    return (
        values * lax.rsqrt(jnp.mean(values * values, axis=-1, keepdims=True) + epsilon) * gain_vec
    )


def norm_back(values, gain_vec, upstream):
    scaling = lax.rsqrt(jnp.mean(values * values, axis=-1, keepdims=True) + epsilon)
    gain_grad = jnp.sum(upstream * values * scaling, axis=0)
    weighted = upstream * gain_vec
    inner_sum = jnp.mean(weighted * values, axis=-1, keepdims=True)
    return (scaling * weighted - values * (scaling * scaling * scaling) * inner_sum, gain_grad)


def rotary(values, positions):
    head_width = values.shape[-1]
    half_width = head_width // 2
    frequency = theta_base ** (-2.0 * jnp.arange(half_width, dtype=jnp.float32) / head_width)
    angles = positions.astype(jnp.float32)[:, None] * frequency[None, :]
    cosine = jnp.concatenate([jnp.cos(angles), jnp.cos(angles)], axis=-1)[:, None, :]
    sine_part = jnp.concatenate([jnp.sin(angles), jnp.sin(angles)], axis=-1)[:, None, :]
    turned = jnp.concatenate([-values[..., half_width:], values[..., :half_width]], axis=-1)
    return values * cosine + turned * sine_part


def head_prep(projected, gain_vec, positions, head_count, factor):
    shaped = projected.reshape(projected.shape[0], head_count, projected.shape[1] // head_count)
    return rotary(norm_rows(shaped, gain_vec), positions) * factor


def gather_all(arrays, cid, line=()):
    if placed():
        return [o.reshape(-1, o.shape[-1]) for o in ag32(arrays, cid, line)]
    return [lax.all_gather(a, BOTH, axis=0, tiled=True) for a in arrays] + [
        lax.all_gather(a, "shard", axis=0, tiled=True) for a in line
    ]


def scatter_all(arrays, cid, out_dtype=jnp.float32, line=()):
    if placed():
        return rs32(
            [a.reshape(32, -1, a.shape[-1]) for a in arrays], cid, out_dtype, line=[a.reshape(NZ, -1, a.shape[-1]) for a in line]
        )
    return [lax.psum_scatter(a, BOTH, scatter_dimension=0, tiled=True).astype(out_dtype) for a in arrays] + [
        lax.psum_scatter(a, "shard", scatter_dimension=0, tiled=True).astype(out_dtype) for a in line
    ]


def per_device(
    hidden_in,
    g_attn,
    w_query,
    w_key,
    w_value,
    g_query,
    g_key,
    w_out,
    g_ffn,
    w_router,
    w_gate,
    w_up,
    w_down,
    routes,
    cotangent,
):
    bf, f32 = jnp.bfloat16, jnp.float32
    tok_rows, model_width = hidden_in.shape
    top_count = routes.shape[1]
    devices = lax.axis_size(BOTH)
    expert_count = devices * w_gate.shape[0]
    capacity = 2 * tok_rows * top_count // expert_count
    shard_count = lax.axis_size("shard")
    shard_pos = lax.axis_index("shard")
    seq_len = tok_rows * shard_count
    q_cols, kv_cols = HQ * HD, HK * HD

    pieces = [w_router.reshape(-1), g_attn, g_ffn, g_query, g_key]
    sizes = [p.shape[0] for p in pieces]
    used = sum(sizes)
    small_rows = -(-used // (64 * 128)) * 64
    small = jnp.concatenate(pieces + [jnp.zeros((small_rows * 128 - used,), bf)]).reshape(small_rows, 128)
    wqkv = jnp.concatenate([w_query, w_key, w_value], axis=1)
    wqkv_full, small_all, wo_full, hidden_seq = gather_all([wqkv, small, w_out], 1, [hidden_in])
    small_all = small_all.reshape(devices, small_rows * 128)
    starts = [sum(sizes[:i]) for i in range(5)]
    wr_full, attn_gain, ffn_gain, query_gain, key_gain = [small_all[:, o : o + n].reshape(-1) for o, n in zip(starts, sizes)]
    wr_full = wr_full.reshape(model_width, expert_count)
    attn_gain, ffn_gain, query_gain, key_gain = [g.astype(f32) for g in (attn_gain, ffn_gain, query_gain, key_gain)]
    first = 3 * tok_rows // 8
    cot_first, wo_full = lax.optimization_barrier((cotangent[:first], wo_full))
    cot_a = lax.all_gather(cot_first, BOTH, axis=0, tiled=True)

    inputs_f = hidden_in.astype(f32)
    normed_low = norm_rows(inputs_f, attn_gain).astype(bf)
    normed_seq = norm_rows(hidden_seq.astype(f32), attn_gain).astype(bf)
    kv_proj = matmul(normed_seq, wqkv_full[:, q_cols:])
    q_proj = matmul(normed_low, wqkv_full[:, :q_cols])
    cosine, sine = rope_tables(seq_len)
    q_low, k_low, v_low, mix_low = attention_forward(q_proj, kv_proj, query_gain, key_gain, cosine, sine)
    residual = inputs_f + matmul(mix_low, wo_full)
    ffn_low = norm_rows(residual, ffn_gain).astype(bf)

    logits = matmul(ffn_low, wr_full)
    expert_ids = jnp.arange(expert_count, dtype=jnp.int32)
    chosen = jnp.any(routes[:, :, None] == expert_ids[None, None, :], axis=1)
    raised_gate = jnp.where(chosen, jnp.exp(logits), 0.0)
    gates = raised_gate / jnp.sum(raised_gate, axis=-1, keepdims=True)
    gate_high = lax.reduce_precision(gates, 8, 7)
    gate_low = gates - gate_high
    extra = -(-3 * expert_count // 128) * 128
    payload = jnp.concatenate(
        [
            ffn_low,
            chosen.astype(bf),
            gate_high.astype(bf),
            gate_low.astype(bf),
            jnp.zeros((tok_rows, extra - 3 * expert_count), bf),
        ],
        axis=1,
    )
    (payload_all,) = gather_all([payload], 3)
    (out_part, rows, gate_act, up_act), cot_b = experts_forward(
        payload_all, w_gate, w_up, w_down, expert_count, tok_rows, capacity, cotangent[first:], 2
    )
    moe_out = lax.psum_scatter(out_part, "expert", scatter_dimension=0, tiled=True)
    grad_part, grad_wgate, grad_wup, grad_wdown = experts_backward(
        payload_all, cot_a, cot_b, rows, gate_act, up_act, w_gate, w_up, w_down, expert_count, tok_rows, capacity
    )
    (grad_sum,) = scatter_all([grad_part], 4)
    grad_sum, moe_out = lax.optimization_barrier((grad_sum, moe_out))
    upstream = cotangent.astype(f32)
    grad_ffn = grad_sum[:, :model_width]
    grad_shares = (
        grad_sum[:, model_width : model_width + expert_count]
        + grad_sum[:, model_width + expert_count : model_width + 2 * expert_count]
    )
    grad_logits = (grad_shares - gates * jnp.sum(grad_shares, axis=-1, keepdims=True)).astype(bf)
    grad_wrouter = matmul_tn(ffn_low, grad_logits)
    grad_ffn = grad_ffn + matmul_nt(grad_logits, wr_full)
    grad_second, grad_ffn_gain = norm_back(residual, ffn_gain, grad_ffn)
    grad_residual = upstream + grad_second
    grad_attn_low = grad_residual.astype(bf)
    grad_wout = matmul_tn(mix_low, grad_attn_low).astype(bf)
    grad_attn_low, grad_wout = lax.optimization_barrier((grad_attn_low, grad_wout))
    out_grad = lax.psum_scatter(grad_wout, "expert", scatter_dimension=0, tiled=True)

    moe_parts = moe_out.reshape(shard_count, 2, tok_rows // 2, model_width)
    moe_a, moe_b = [moe_parts[:, i].reshape(-1, model_width) for i in range(2)]
    moe_a, grad_q_low, grad_kv, grad_query_gain = attention_backward(
        q_proj, q_low, k_low, v_low, grad_attn_low, wo_full, query_gain, cosine, sine, moe_a, 5
    )
    grad_kv = line_scatter(grad_kv, 6)
    own_rows = shard_pos * tok_rows
    k_proj = lax.dynamic_slice(kv_proj, (own_rows, 0), (tok_rows, kv_cols))
    positions = own_rows + jnp.arange(tok_rows, dtype=jnp.int32)
    _, k_pull = jax.vjp(
        lambda projected, gain_vec: head_prep(projected, gain_vec, positions, HK, 1.0), k_proj, key_gain
    )
    grad_k_proj, grad_key_gain = k_pull(grad_kv[:, :kv_cols].reshape(tok_rows, HK, HD))
    grad_qkv_low = jnp.concatenate(
        [grad_q_low, grad_k_proj.astype(bf), grad_kv[:, kv_cols:].astype(bf)], axis=1
    )
    grad_wqkv = matmul_tn(normed_low, grad_qkv_low).astype(bf)
    grad_normed = matmul_nt(grad_qkv_low, wqkv_full)
    grad_front, grad_attn_gain = norm_back(inputs_f, attn_gain, grad_normed)
    grad_input = (grad_residual + grad_front).astype(bf)

    grads = [grad_wrouter, grad_attn_gain, grad_ffn_gain, grad_query_gain, grad_key_gain]
    packed = jnp.concatenate(
        [g.astype(bf).reshape(devices, -1) for g in grads] + [jnp.zeros((devices, small_rows * 128 - used), bf)], axis=1
    ).reshape(devices * small_rows, 128)
    grad_wqkv, out_grad = lax.optimization_barrier((grad_wqkv, out_grad))
    out_grad = lax.psum_scatter(out_grad, "shard", scatter_dimension=0, tiled=True).astype(f32)
    qkv_grad, small_grad, moe_b = scatter_all([grad_wqkv, packed], 8, line=[moe_b])
    block_out = (residual + jnp.concatenate([moe_a, moe_b], axis=0)).astype(bf)
    small_grad = small_grad.reshape(-1)
    router_g, attn_g, ffn_g, query_g, key_g = [small_grad[o : o + n] for o, n in zip(starts, sizes)]
    return (
        block_out,
        grad_input,
        attn_g,
        qkv_grad[:, :q_cols],
        qkv_grad[:, q_cols : q_cols + kv_cols],
        qkv_grad[:, q_cols + kv_cols :],
        query_g,
        key_g,
        out_grad,
        ffn_g,
        router_g.reshape(w_router.shape),
        grad_wgate,
        grad_wup,
        grad_wdown,
    )


def solution(mesh):
    row = P(BOTH, None)
    vec = P(BOTH)
    cube = P(BOTH, None, None)
    in_specs = (row, vec, row, row, row, vec, vec, row, vec, row, cube, cube, cube, row, row)
    out_specs = (row, row, vec, row, row, row, vec, vec, row, vec, row, cube, cube, cube)
    return jax.shard_map(
        per_device, mesh=mesh, in_specs=in_specs, out_specs=out_specs, check_vma=False
    )
```

```python
import functools

import jax
import jax.numpy as jnp
from jax import lax
from jax.experimental import pallas as pl
from jax.experimental.pallas import tpu as pltpu
from jax.sharding import PartitionSpec as P

MESH = pl.DeviceIdType.MESH
NZ = 4

def placed():
    return lax.axis_size("expert") == 8 and lax.axis_size("shard") == NZ

def place():
    e = lax.axis_index("expert"); s = lax.axis_index("shard")
    return e // 4, lax.rem(e // 2, 2), lax.rem(e, 2), s

def dev(y, x, c, s):
    return (y * 4 + x * 2 + c, s)

def barrier_all(y, x, c, s):
    bar = pltpu.get_barrier_semaphore()
    def sig(d): pl.semaphore_signal(bar, inc=1, device_id=d, device_id_type=MESH)
    sig(dev(1 - y, x, c, s)); sig(dev(y, 1 - x, c, s)); sig(dev(y, x, 1 - c, s))
    @pl.when(s > 0)
    def _(): sig(dev(y, x, c, s - 1))
    @pl.when(s < NZ - 1)
    def _(): sig(dev(y, x, c, s + 1))
    pl.semaphore_wait(bar, 3 + jnp.where(s > 0, 1, 0) + jnp.where(s < NZ - 1, 1, 0))

def ag_kernel(n_arr, n_line, *refs):
    n_all = n_arr + n_line
    for run in ag_steps(n_arr, n_line, refs[:n_all], refs[n_all:2 * n_all], refs[2 * n_all:]): run()

def ag_steps(n_arr, n_line, ins, outs, sems, stages=False):
    n_all = n_arr + n_line
    loc_sem, zs, zr, ps, pr, cs, cr = sems
    y, x, c, s = place()
    def rc(src, dst, ss, rs, d):
        return pltpu.make_async_remote_copy(src_ref=src, dst_ref=dst, send_sem=ss, recv_sem=rs, device_id=d, device_id_type=MESH)
    X = dev(y, 1 - x, c, s); Y = dev(1 - y, x, c, s); C = dev(y, x, 1 - c, s)
    A = range(n_arr)
    every = range(n_all)
    def home(a, zz):
        return outs[a].at[y, x, c, zz] if a < n_arr else outs[a].at[zz]
    steps = [(0, 0)] + [(d, g) for d in range(1, NZ) for g in (1, -1)]
    def valid(d, g):
        return (s >= d) if g == 1 else (s + d <= NZ - 1)
    def zof(d, g): return s - d * g
    def src_own(a, h, zz, k):
        return ins[a].at[h] if k == 0 else home(a, zz).at[h]
    def zcopy(a, h, zz, k, g):
        kk = 1 + 2 * (k_dist(k)) + (0 if g == 1 else 1)
        return rc(src_own(a, h, zz, k), home(a, zz).at[h], zs.at[a, h, kk], zr.at[a, h, kk], dev(y, x, c, s + g))
    def k_dist(k): return steps[k][0]
    def plane(a, h, zz, k, which):
        return rc(src_own(a, h, zz, k), outs[a].at[y, x, c, zz, h], ps.at[a, k, h, which], pr.at[a, k, h, which], X if which == 0 else Y)
    def plane_recv(a, h, zz, k, which):
        d = outs[a].at[y, 1 - x, c, zz, h] if which == 0 else outs[a].at[1 - y, x, c, zz, h]
        return rc(d, d, ps.at[a, k, h, which], pr.at[a, k, h, which], X if which == 0 else Y)
    def diag(a, h, zz, k):
        d = outs[a].at[y, 1 - x, c, zz, h] if h == 0 else outs[a].at[1 - y, x, c, zz, h]
        return rc(d, d, ps.at[a, k, h, 2], pr.at[a, k, h, 2], Y if h == 0 else X)
    def diag_recv(a, h, zz, k):
        d = outs[a].at[1 - y, 1 - x, c, zz, h]
        return rc(d, d, ps.at[a, k, h, 2], pr.at[a, k, h, 2], Y if h == 0 else X)
    def core(a, zz, k, part):
        d = outs[a].at[:, :, c, zz]
        return rc(d, d, cs.at[a, k], cr.at[a, k], C)
    def core_recv(a, zz, k):
        d = outs[a].at[:, :, 1 - c, zz]
        return rc(d, d, cs.at[a, k], cr.at[a, k], C)
    def loc(a):
        return pltpu.make_async_copy(ins[a], home(a, s), loc_sem.at[a])

    def when(k, f):
        d, g = steps[k]
        if k == 0: f()
        else: pl.when(valid(d, g))(f)

    def stage_a(k):
        d, g = steps[k]
        def go():
            zz = zof(d, g)
            for a in every:
                for h in range(2):
                    if k:
                        kk = k
                        dref = home(a, zz).at[h]
                        rc(dref, dref, zs.at[a, h, kk], zr.at[a, h, kk], X).wait_recv()
                    for gg in ((1, -1) if k == 0 else (g,)):
                        okc = (s < NZ - 1) if gg == 1 else (s > 0)
                        if d + 1 < NZ:
                            @pl.when(okc)
                            def _(): zcopy(a, h, zz, k, gg).start()
                    if a < n_arr:
                        plane(a, h, zz, k, 0).start()
                        plane(a, h, zz, k, 1).start()
        when(k, go)
    def stage_b(k):
        d, g = steps[k]
        def go():
            zz = zof(d, g)
            for a in A:
                plane_recv(a, 0, zz, k, 0).wait_recv()
                diag(a, 0, zz, k).start()
                plane_recv(a, 1, zz, k, 1).wait_recv()
                diag(a, 1, zz, k).start()
        when(k, go)
    def stage_c(k):
        d, g = steps[k]
        def go():
            zz = zof(d, g)
            for a in A:
                if k == 0: loc(a).wait()
                plane_recv(a, 1, zz, k, 0).wait_recv()
                plane_recv(a, 0, zz, k, 1).wait_recv()
                diag_recv(a, 0, zz, k).wait_recv()
                diag_recv(a, 1, zz, k).wait_recv()
                core(a, zz, k, 0).start()
        when(k, go)
    n = len(steps)
    def start():
        barrier_all(y, x, c, s)
        for a in every: loc(a).start()
        stage_a(0)
    def advance(i):
        if 0 < i < n: stage_a(i)
        if 0 <= i - 1 < n: stage_b(i - 1)
        if 0 <= i - 2 < n: stage_c(i - 2)
    def finish():
        for k in range(n):
            d, g = steps[k]
            def go():
                zz = zof(d, g)
                for a in every:
                    if a < n_arr:
                        core_recv(a, zz, k).wait_recv()
                        core(a, zz, k, 0).wait_send()
                    elif k == 0: loc(a).wait()
                    for h in range(2):
                        for gg in ((1, -1) if k == 0 else (g,)):
                            okc = (s < NZ - 1) if gg == 1 else (s > 0)
                            if d + 1 < NZ:
                                @pl.when(okc)
                                def _(): zcopy(a, h, zz, k, gg).wait_send()
                        if a < n_arr:
                            plane(a, h, zz, k, 0).wait_send()
                            plane(a, h, zz, k, 1).wait_send()
                            diag(a, h, zz, k).wait_send()
            when(k, go)
    if stages: return start, stage_a, stage_b, stage_c, finish
    return [start] + [functools.partial(advance, i) for i in range(1, n + 2)] + [finish]

def ag_sems(n, m=0):
    D = pltpu.SemaphoreType.DMA
    return [D((n + m,)), D((n + m, 2, 9)), D((n + m, 2, 9)), D((n, 7, 2, 3)), D((n, 7, 2, 3)), D((n, 7)), D((n, 7))]

def ag32(arrs, cid, line=()):
    ins = [a.reshape(2, a.shape[0] // 2, a.shape[1]) for a in list(arrs) + list(line)]
    n, m = len(arrs), len(line)
    outs = pl.pallas_call(
        functools.partial(ag_kernel, n, m),
        out_shape=[jax.ShapeDtypeStruct(((2, 2, 2, NZ) if i < n else (NZ,)) + a.shape, a.dtype) for i, a in enumerate(ins)],
        in_specs=[pl.BlockSpec(memory_space=pltpu.VMEM)] * (n + m),
        out_specs=[pl.BlockSpec(memory_space=pl.ANY)] * (n + m),
        scratch_shapes=ag_sems(n, m),
        compiler_params=pltpu.CompilerParams(collective_id=cid, has_side_effects=True, vmem_limit_bytes=64000 * 1024),
        name="gather_all",
    )(*ins)
    return [o.reshape(-1, a.shape[1] * 2, a.shape[2]) for o, a in zip(outs, ins)]

ZORDER = (0, 3, 1, 2)
LAGS = (1, 1, 1, 1)

def rs_kernel(n_arr, n_line, parts, *refs):
    n_all = n_arr + n_line
    ins = refs[:n_all]; outs = refs[n_all:2 * n_all]
    sc = list(refs[2 * n_all:])
    own_b = [sc.pop(0) for _ in range(n_all)]; zu_b = [sc.pop(0) for _ in range(n_all)]; zd_b = [sc.pop(0) for _ in range(n_all)]
    r0_b, ra_b, rb_b = [[sc.pop(0) for _ in range(n_arr)] for _ in range(3)]
    lsem, s0s, s0r, sas, sar, sbs, sbr, zus, zur, zds, zdr = sc
    y, x, c, s = place()
    barrier_all(y, x, c, s)
    X = dev(y, 1 - x, c, s); Y = dev(1 - y, x, c, s); C = dev(y, x, 1 - c, s)
    UP = dev(y, x, c, s + 1); DN = dev(y, x, c, s - 1)
    def rc(src, dst, ss, rs, d):
        return pltpu.make_async_remote_copy(src_ref=src, dst_ref=dst, send_sem=ss, recv_sem=rs, device_id=d, device_id_type=MESH)
    units = [(a, zz, h) for zz in ZORDER for h in range(parts) for a in range(n_arr)]
    lines = [(a, zz, h) for zz in ZORDER for h in range(parts) for a in range(n_arr, n_all)]
    def jj(zz, h): return ZORDER.index(zz) * parts + h
    def load(a, zz, h):
        j = jj(zz, h)
        src = ins[a].at[:, :, c, zz, h] if a < n_arr else ins[a].at[zz, h]
        return pltpu.make_async_copy(src, own_b[a].at[j], lsem.at[a, j])
    def mine(a, j):
        return own_b[a].at[j, y, x] if a < n_arr else own_b[a].at[j]
    def c0(a, zz, h):
        j = jj(zz, h)
        return rc(ins[a].at[:, :, 1 - c, zz, h], r0_b[a].at[j], s0s.at[a, j], s0r.at[a, j], C)
    def ca(a, zz, h):
        j = jj(zz, h)
        if h % 2 == 0: return rc(own_b[a].at[j, :, 1 - x], ra_b[a].at[j], sas.at[a, j], sar.at[a, j], X)
        return rc(own_b[a].at[j, 1 - y], ra_b[a].at[j], sas.at[a, j], sar.at[a, j], Y)
    def cb(a, zz, h):
        j = jj(zz, h)
        if h % 2 == 0: return rc(own_b[a].at[j, 1 - y, x], rb_b[a].at[j], sbs.at[a, j], sbr.at[a, j], Y)
        return rc(own_b[a].at[j, y, 1 - x], rb_b[a].at[j], sbs.at[a, j], sbr.at[a, j], X)
    def cu(a, zz, h):
        j = jj(zz, h)
        return rc(mine(a, j), zu_b[a].at[j], zus.at[a, j], zur.at[a, j], UP)
    def cd(a, zz, h):
        j = jj(zz, h)
        return rc(mine(a, j), zd_b[a].at[j], zds.at[a, j], zdr.at[a, j], DN)
    def add_into(dst, other):
        rows = dst.shape[0]
        st = 16 if rows % 16 == 0 else rows
        @pl.loop(0, rows // st)
        def _(i):
            r = pl.ds(i * st, st)
            dst[r, :] = (dst[r, :].astype(jnp.float32) + other[r, :].astype(jnp.float32)).astype(dst.dtype)
    def stage0(u):
        a, zz, h = u; j = jj(zz, h)
        load(a, zz, h).wait()
        c0(a, zz, h).wait_recv()
        for yy in range(2):
            for xx in range(2):
                add_into(own_b[a].at[j, yy, xx], r0_b[a].at[j, yy, xx])
        ca(a, zz, h).start()
    def stage1(u):
        a, zz, h = u; j = jj(zz, h)
        ca(a, zz, h).wait_recv()
        for q in range(2):
            if h % 2 == 0: add_into(own_b[a].at[j, q, x], ra_b[a].at[j, q])
            else: add_into(own_b[a].at[j, y, q], ra_b[a].at[j, q])
        cb(a, zz, h).start()
    def stage2(u):
        a, zz, h = u; j = jj(zz, h)
        cb(a, zz, h).wait_recv()
        add_into(own_b[a].at[j, y, x], rb_b[a].at[j])
    def hop(u, k):
        a, zz, h = u; j = jj(zz, h)
        if k < zz:
            @pl.when(s == k)
            def _():
                if k > 0:
                    cu(a, zz, h).wait_recv()
                    add_into(mine(a, j), zu_b[a].at[j])
                cu(a, zz, h).start()
        t = NZ - 1 - k
        if t > zz:
            @pl.when(s == t)
            def _():
                if k > 0:
                    cd(a, zz, h).wait_recv()
                    add_into(mine(a, j), zd_b[a].at[j])
                cd(a, zz, h).start()
    def last(u):
        a, zz, h = u; j = jj(zz, h)
        @pl.when(s == zz)
        def _():
            if zz > 0: cu(a, zz, h).wait_recv()
            if zz < NZ - 1: cd(a, zz, h).wait_recv()
            t = mine(a, j)[...].astype(jnp.float32)
            if zz > 0: t = t + zu_b[a][j].astype(jnp.float32)
            if zz < NZ - 1: t = t + zd_b[a][j].astype(jnp.float32)
            outs[a][h] = t.astype(outs[a].dtype)
    for u in lines: load(*u).start()
    for u in units:
        c0(*u).start(); load(*u).start()
    n = len(units); nl = len(lines)
    L1 = LAGS[0] * n_arr; L2 = L1 + LAGS[1] * n_arr; L3 = L2 + LAGS[2] * n_arr; dl = LAGS[3] * n_arr
    for i in range(n + L3 + (NZ - 1) * dl):
        if i < n: stage0(units[i])
        if 0 <= i - L1 < n: stage1(units[i - L1])
        if 0 <= i - L2 < n: stage2(units[i - L2])
        for k in range(NZ - 1):
            for q in (2 * (i - k), 2 * (i - k) + 1):
                if 0 <= q < nl:
                    if k == 0: load(*lines[q]).wait()
                    hop(lines[q], k)
        for k in range(NZ - 1):
            if 0 <= i - L3 - k * dl < n: hop(units[i - L3 - k * dl], k)
    for u in lines + units: last(u)
    for u in lines + units:
        a, zz, h = u
        if a < n_arr:
            c0(*u).wait_send(); ca(*u).wait_send(); cb(*u).wait_send()
        if zz > 0:
            @pl.when(s < zz)
            def _(): cu(*u).wait_send()
        if zz < NZ - 1:
            @pl.when(s > zz)
            def _(): cd(*u).wait_send()

def rs32(arrs, cid, out_dtype=jnp.float32, parts=4, line=()):
    n, nl = len(arrs), len(line)
    both = list(arrs) + list(line)
    if any(a.shape[1] % (parts * 16) for a in both): parts = 2
    ins = [a.reshape(((2, 2, 2) if i < n else ()) + (NZ, parts, a.shape[1] // parts, a.shape[2])) for i, a in enumerate(both)]
    hs = [i.shape[-2:] for i in ins]
    V = pltpu.VMEM; bt = jnp.bfloat16; m = NZ * parts
    sems = [pltpu.SemaphoreType.DMA((n + nl, m))] * 11
    outs = pl.pallas_call(
        functools.partial(rs_kernel, n, nl, parts),
        out_shape=[jax.ShapeDtypeStruct((parts,) + h, out_dtype) for h in hs],
        in_specs=[pl.BlockSpec(memory_space=pl.ANY)] * (n + nl),
        out_specs=[pl.BlockSpec(memory_space=pltpu.VMEM)] * (n + nl),
        scratch_shapes=[V((m,) + ((2, 2) if i < n else ()) + h, bt) for i, h in enumerate(hs)] + [V((m,) + h, bt) for h in hs] + [V((m,) + h, bt) for h in hs]
            + [V((m, 2, 2) + h, bt) for h in hs[:n]] + [V((m, 2) + h, bt) for h in hs[:n]] + [V((m,) + h, bt) for h in hs[:n]] + sems,
        compiler_params=pltpu.CompilerParams(collective_id=cid, has_side_effects=True, vmem_limit_bytes=64000 * 1024),
        name="scatter_all",
    )(*ins)
    return [o.reshape(a.shape[1], a.shape[2]) for o, a in zip(outs, both)]

def line_barrier(y, x, c, s):
    bar = pltpu.get_barrier_semaphore()
    @pl.when(s > 0)
    def _(): pl.semaphore_signal(bar, inc=1, device_id=dev(y, x, c, s - 1), device_id_type=MESH)
    @pl.when(s < NZ - 1)
    def _(): pl.semaphore_signal(bar, inc=1, device_id=dev(y, x, c, s + 1), device_id_type=MESH)
    pl.semaphore_wait(bar, jnp.where(s > 0, 1, 0) + jnp.where(s < NZ - 1, 1, 0))

def line_gather_kernel(parts, x_ref, o_ref, ss, rs):
    y, x, c, s = place()
    line_barrier(y, x, c, s)
    def cp(d, g, h):
        src = x_ref.at[h] if d == 0 else o_ref.at[s - d * g, h]
        k = 0 if g == 1 else 1
        return pltpu.make_async_remote_copy(src_ref=src, dst_ref=o_ref.at[s - d * g, h], send_sem=ss.at[k, d, h], recv_sem=rs.at[k, d, h],
            device_id=dev(y, x, c, s + g), device_id_type=MESH)
    def arrived(d, g, h):
        k = 0 if g == 1 else 1
        ref = o_ref.at[s - (d + 1) * g, h]
        return pltpu.make_async_remote_copy(src_ref=ref, dst_ref=ref, send_sem=ss.at[k, d, h], recv_sem=rs.at[k, d, h],
            device_id=dev(y, x, c, s + g), device_id_type=MESH)
    def sends(d, g): return (s >= d) & (s < NZ - 1) if g == 1 else (s + d <= NZ - 1) & (s > 0)
    def gets(d, g): return s >= d + 1 if g == 1 else s + d + 1 <= NZ - 1
    for d in range(NZ):
        for h in range(parts):
            for g in (1, -1):
                if d:
                    @pl.when(gets(d - 1, g))
                    def _(): arrived(d - 1, g, h).wait_recv()
                if d < NZ - 1:
                    @pl.when(sends(d, g))
                    def _(): cp(d, g, h).start()
        if d == 0: o_ref[s] = x_ref[...]
    for d in range(NZ - 1):
        for h in range(parts):
            for g in (1, -1):
                @pl.when(sends(d, g))
                def _(): cp(d, g, h).wait_send()

def line_gather(x, cid, parts=4):
    if not placed():
        return lax.all_gather(x, "shard", axis=0, tiled=True)
    R, C = x.shape
    sem = pltpu.SemaphoreType.DMA((2, NZ, parts))
    o = pl.pallas_call(functools.partial(line_gather_kernel, parts), out_shape=jax.ShapeDtypeStruct((NZ, parts, R // parts, C), x.dtype),
        in_specs=[pl.BlockSpec(memory_space=pltpu.VMEM)], out_specs=pl.BlockSpec(memory_space=pltpu.VMEM),
        scratch_shapes=[sem, sem], compiler_params=pltpu.CompilerParams(collective_id=cid, has_side_effects=True, vmem_limit_bytes=16 << 20),
        name="line_gather")(x.reshape(parts, R // parts, C))
    return o.reshape(NZ * R, C)

def line_scatter_kernel(parts, p_ref, o_ref, *scratch):
    for run in line_scatter_steps(parts, p_ref, o_ref, scratch): run()

LINE_PARTS = 4
LINE_STEPS = 3 * LINE_PARTS + NZ + 1

def line_scatter_steps(parts, p_ref, o_ref, scratch):
    acc, zu, zd, ss_u, rs_u, ss_d, rs_d = scratch
    y, x, c, s = place()
    def rc(src, dst, a, b, d):
        return pltpu.make_async_remote_copy(src_ref=src, dst_ref=dst, send_sem=a, recv_sem=b, device_id=d, device_id_type=MESH)
    def cu(zz, h, k):
        src = p_ref.at[zz, h] if k == 0 else acc.at[zz, h]
        return rc(src, zu.at[zz, h], ss_u.at[zz, h], rs_u.at[zz, h], dev(y, x, c, s + 1))
    def cd(zz, h, k):
        src = p_ref.at[zz, h] if k == 0 else acc.at[zz, h]
        return rc(src, zd.at[zz, h], ss_d.at[zz, h], rs_d.at[zz, h], dev(y, x, c, s - 1))
    st = 32
    def total(dst, refs):
        @pl.loop(0, dst.shape[0] // st)
        def _(i):
            r = pl.ds(i * st, st)
            t = refs[0][r, :].astype(jnp.float32)
            for f in refs[1:]: t = t + f[r, :].astype(jnp.float32)
            dst[r, :] = t.astype(dst.dtype)
    ups = [(zz, h) for zz in (3, 2, 1) for h in range(parts)]
    dns = [(zz, h) for zz in (0, 1, 2) for h in range(parts)]
    n = len(ups)
    def advance(i):
        if i == 0: line_barrier(y, x, c, s)
        for k in range(NZ - 1):
            if 0 <= i - k < n:
                zz, h = ups[i - k]
                if k < zz:
                    @pl.when(s == k)
                    def _():
                        if k:
                            cu(zz, h, k).wait_recv()
                            total(acc.at[zz, h], [p_ref.at[zz, h], zu.at[zz, h]])
                        cu(zz, h, k).start()
                zz, h = dns[i - k]
                if NZ - 1 - k > zz:
                    @pl.when(s == NZ - 1 - k)
                    def _():
                        if k:
                            cd(zz, h, k).wait_recv()
                            total(acc.at[zz, h], [p_ref.at[zz, h], zd.at[zz, h]])
                        cd(zz, h, k).start()
    def finish():
        for zz in range(NZ):
            @pl.when(s == zz)
            def _():
                for h in range(parts):
                    refs = [p_ref.at[zz, h]]
                    if zz > 0:
                        cu(zz, h, 1).wait_recv()
                        refs.append(zu.at[zz, h])
                    if zz < NZ - 1:
                        cd(zz, h, 1).wait_recv()
                        refs.append(zd.at[zz, h])
                    total(o_ref.at[h], refs)
        for zz, h in ups:
            @pl.when(s < zz)
            def _(): cu(zz, h, 1).wait_send()
        for zz, h in dns:
            @pl.when(s > zz)
            def _(): cd(zz, h, 1).wait_send()
    return [functools.partial(advance, i) for i in range(n + NZ)] + [finish]

def line_scatter_scratch(parts, rows, cols, dtype):
    sem = pltpu.SemaphoreType.DMA((NZ, parts))
    buf = pltpu.VMEM((NZ, parts, rows // parts, cols), dtype)
    return [buf, buf, buf, sem, sem, sem, sem]

def line_scatter(p, cid, parts=LINE_PARTS):
    if not placed():
        return lax.psum_scatter(p, "shard", scatter_dimension=0, tiled=True).astype(jnp.float32)
    R, C = p.shape[0] // NZ, p.shape[1]
    shape = (NZ, parts, R // parts, C)
    o = pl.pallas_call(functools.partial(line_scatter_kernel, parts), out_shape=jax.ShapeDtypeStruct(shape[1:], jnp.float32),
        in_specs=[pl.BlockSpec(memory_space=pltpu.VMEM)], out_specs=pl.BlockSpec(memory_space=pltpu.VMEM),
        scratch_shapes=line_scatter_scratch(parts, R, C, p.dtype), compiler_params=pltpu.CompilerParams(collective_id=cid, has_side_effects=True, vmem_limit_bytes=24 << 20),
        name="line_scatter")(p.reshape(shape))
    return o.reshape(R, C)


def dot(a, b, ca, cb):
    return lax.dot_general(a, b, (((ca,), (cb,)), ((), ())), preferred_element_type=jnp.float32)

def token_picks(meta, experts, slots, me):
    SB, WM = meta.shape
    bf, f32 = jnp.bfloat16, jnp.float32
    tri = (lax.broadcasted_iota(jnp.int32, (SB, SB), 1) < lax.broadcasted_iota(jnp.int32, (SB, SB), 0)).astype(bf)
    lane = lax.broadcasted_iota(jnp.int32, (SB, WM), 1)
    cnt = dot(tri, meta, 1, 0)
    metaf = meta.astype(f32)
    msk = jnp.sum(jnp.where(lane == me, metaf, 0.0), axis=-1, keepdims=True)
    pos = jnp.sum(jnp.where(lane == me, cnt, 0.0), axis=-1, keepdims=True)
    gate = jnp.sum(jnp.where((lane == me + experts) | (lane == me + 2 * experts), metaf, 0.0), axis=-1, keepdims=True)
    want = jnp.where(msk > 0.0, pos, -1.0).astype(jnp.int32)
    pick = (want == lax.broadcasted_iota(jnp.int32, (SB, slots), 1)).astype(bf)
    return pick, gate

def forward_kernel(experts, slots, SB, guest, *refs):
    if guest:
        cot_ref, x_ref, wg_hbm, wu_hbm, wd_hbm, cot_all, out_ref, rows_ref, ga_ref, ua_ref, wg, wu, wd, wsem = refs[:14]
    else:
        x_ref, wg_hbm, wu_hbm, wd_hbm, out_ref, rows_ref, ga_ref, ua_ref, wg, wu, wd, wsem = refs
    bf = jnp.bfloat16
    step = pl.program_id(0)
    if guest:
        start, stage_a, stage_b, stage_c, finish = ag_steps(1, 0, [cot_ref], [cot_all], refs[14:], True)
        pl.when(step == 0)(start)
        for at, stage, k in GUEST_AT: pl.when(step == at)(functools.partial(stage_a if stage == 0 else stage_b if stage == 1 else stage_c, k))
    nsub = x_ref.shape[0] // SB
    D = out_ref.shape[1]
    me = lax.axis_index(("expert", "shard"))
    loads = [pltpu.make_async_copy(h.at[0], v, wsem.at[i]) for i, (h, v) in enumerate(((wg_hbm, wg), (wu_hbm, wu), (wd_hbm, wd)))]
    @pl.when(step == 0)
    def _():
        for l in loads: l.start()
    picks, gates = [], []
    for i in range(nsub):
        r = pl.ds(i * SB, SB)
        pick, gate = token_picks(x_ref[r, D:], experts, slots, me)
        picks.append(pick); gates.append(gate)
        rows_ref[i * slots:(i + 1) * slots, :] = dot(pick, x_ref[r, :D], 0, 0).astype(bf)
    @pl.when(step == 0)
    def _():
        for l in loads: l.wait()
    ga = dot(rows_ref[...], wg[...], 1, 0)
    ua = dot(rows_ref[...], wu[...], 1, 0)
    ga_ref[...] = ga
    ua_ref[...] = ua
    hid = (ga * (1.0 / (1.0 + jnp.exp(-ga))) * ua).astype(bf)
    eo = dot(hid, wd[...], 1, 0).astype(bf)
    for i in range(nsub):
        r = pl.ds(i * SB, SB)
        tok = dot(picks[i], eo[i * slots:(i + 1) * slots, :], 1, 0)
        out_ref[r, :] = (gates[i] * tok).astype(bf)
    if guest: pl.when(step == pl.num_programs(0) - 1)(finish)

GUEST_AT = (
    (3, 0, 1), (3, 0, 2), (3, 1, 0), (5, 0, 3), (5, 0, 4), (5, 2, 0), (7, 1, 1), (7, 0, 5), (7, 0, 6), (8, 1, 2),
    (9, 2, 1), (10, 2, 2), (11, 1, 3), (11, 1, 4), (13, 2, 3), (13, 2, 4), (14, 1, 5), (14, 1, 6), (15, 2, 5), (15, 2, 6),
)

def backward_kernel(experts, slots, SB, block, meta_ref, cota_ref, cotb_ref, rows_ref, ga_ref, ua_ref, wg_hbm, wu_hbm, wd_hbm, gr_ref, dwg_hbm, dwu_hbm, dwd_hbm,
                  wg, wu, wd, dwg, dwu, dwd, gp, wsem, osem):
    bf = jnp.bfloat16
    step = pl.program_id(0)
    nsub = meta_ref.shape[0] // SB
    D = cota_ref.shape[1]
    WM = meta_ref.shape[1]
    na, nb = [r.shape[0] * block // meta_ref.shape[0] for r in (cota_ref, cotb_ref)]
    me = lax.axis_index(("expert", "shard"))
    loads = [pltpu.make_async_copy(h.at[0], v, wsem.at[i]) for i, (h, v) in enumerate(((wg_hbm, wg), (wu_hbm, wu), (wd_hbm, wd)))]
    @pl.when(step == 0)
    def _():
        for l in loads: l.start()
        for a in (dwg, dwu, dwd): a[...] = jnp.zeros_like(a)
    picks = []
    for i in range(nsub):
        r = pl.ds(i * SB, SB)
        pick, gate = token_picks(meta_ref[r, :], experts, slots, me)
        picks.append(pick)
        cot = []
        for b in range(i * SB // block, (i + 1) * SB // block):
            cot += [cota_ref[b * na:(b + 1) * na, :], cotb_ref[b * nb:(b + 1) * nb, :]]
        gcot = (gate * jnp.concatenate(cot, axis=0).astype(jnp.float32)).astype(bf)
        gp[i * slots:(i + 1) * slots, :] = dot(pick, gcot, 0, 0).astype(bf)
    @pl.when(step == 0)
    def _():
        for l in loads: l.wait()
    ga = ga_ref[...]
    ua = ua_ref[...]
    sig = 1.0 / (1.0 + jnp.exp(-ga))
    act = ga * sig
    hidf = act * ua
    hid = hidf.astype(bf)
    gh = dot(gp[...], wd[...], 1, 1)
    share = jnp.sum(gh * hid.astype(jnp.float32), axis=-1, keepdims=True)
    dga = (gh * ua * (sig * (1.0 + ga * (1.0 - sig)))).astype(bf)
    dua = (gh * act).astype(bf)
    dwd[...] += dot(hid, gp[...], 0, 0)
    grow = (dot(dga, wg[...], 1, 1) + dot(dua, wu[...], 1, 1)).astype(bf)
    dwg[...] += dot(rows_ref[...], dga, 0, 0)
    dwu[...] += dot(rows_ref[...], dua, 0, 0)
    lane = lax.broadcasted_iota(jnp.int32, (share.shape[0], WM), 1)
    high = share.astype(bf).astype(jnp.float32)
    tail = (jnp.where(lane == me, high, 0.0) + jnp.where(lane == me + experts, share - high, 0.0)).astype(bf)
    for i in range(nsub):
        r = pl.ds(i * SB, SB)
        q = slice(i * slots, (i + 1) * slots)
        gr_ref[r, :D] = dot(picks[i], grow[q, :], 1, 0).astype(bf)
        gr_ref[r, D:] = dot(picks[i], tail[q, :], 1, 0).astype(bf)
    @pl.when(step == pl.num_programs(0) - 1)
    def _():
        outs = [pltpu.make_async_copy(v, h.at[0], osem.at[i]) for i, (v, h) in enumerate(((dwg, dwg_hbm), (dwu, dwu_hbm), (dwd, dwd_hbm)))]
        for o in outs: o.start()
        for o in outs: o.wait()

def experts_forward(x_all, w_gate, w_up, w_down, experts, block, capacity, guest, cid, TB=512, SB=256):
    hosted = placed()
    T, C = x_all.shape; D, F = w_gate.shape[1:]
    slots = max(SB // block, 1) * capacity
    total = TB // SB * slots
    S = T // SB * slots
    any_ = pl.BlockSpec(memory_space=pl.ANY)
    V = pltpu.VMEM; bf = jnp.bfloat16; f32 = jnp.float32
    blk = lambda r, c: pl.BlockSpec((r, c), lambda i: (i, 0))
    g = guest.reshape(2, guest.shape[0] // 2, guest.shape[1])
    res = pl.pallas_call(
        functools.partial(forward_kernel, experts, slots, SB, hosted),
        grid=(T // TB,),
        out_shape=([jax.ShapeDtypeStruct((2, 2, 2, NZ) + g.shape, g.dtype)] if hosted else []) + [jax.ShapeDtypeStruct((T, D), bf), jax.ShapeDtypeStruct((S, D), bf), jax.ShapeDtypeStruct((S, F), f32), jax.ShapeDtypeStruct((S, F), f32)],
        in_specs=([pl.BlockSpec(memory_space=pltpu.VMEM)] if hosted else []) + [blk(TB, C), any_, any_, any_],
        out_specs=([any_] if hosted else []) + [blk(TB, D), blk(total, D), blk(total, F), blk(total, F)],
        scratch_shapes=[V((D, F), bf), V((D, F), bf), V((F, D), bf), pltpu.SemaphoreType.DMA((3,))] + (ag_sems(1) if hosted else []),
        compiler_params=pltpu.CompilerParams(dimension_semantics=("arbitrary",), vmem_limit_bytes=65000 * 1024,
            **(dict(collective_id=cid, has_side_effects=True) if hosted else {})),
        cost_estimate=pl.CostEstimate(flops=48_000_000_000, bytes_accessed=130_000_000, transcendentals=0),
        name="experts_forward",
    )(*([g] if hosted else []), x_all, w_gate, w_up, w_down)
    if hosted: return res[1:], res[0].reshape(-1, guest.shape[1])
    return res, lax.all_gather(guest, BOTH, axis=0, tiled=True)

def experts_backward(x_all, cot_a, cot_b, rows, ga, ua, w_gate, w_up, w_down, experts, block, capacity, TB=512, SB=256):
    T, C = x_all.shape; D, F = w_gate.shape[1:]
    slots = max(SB // block, 1) * capacity
    total = TB // SB * slots
    WM = C - D
    any_ = pl.BlockSpec(memory_space=pl.ANY)
    V = pltpu.VMEM; bf = jnp.bfloat16; f32 = jnp.float32
    blk = lambda r, c: pl.BlockSpec((r, c), lambda i: (i, 0))
    meta = pl.BlockSpec((TB, WM), lambda i: (i, D // WM)) if D % WM == 0 else blk(TB, WM)
    meta_in = x_all if D % WM == 0 else x_all[:, D:]
    return pl.pallas_call(
        functools.partial(backward_kernel, experts, slots, SB, block),
        grid=(T // TB,),
        out_shape=[jax.ShapeDtypeStruct((T, C), bf), jax.ShapeDtypeStruct(w_gate.shape, f32), jax.ShapeDtypeStruct(w_up.shape, f32), jax.ShapeDtypeStruct(w_down.shape, f32)],
        in_specs=[meta, blk(cot_a.shape[0] * TB // T, D), blk(cot_b.shape[0] * TB // T, D), blk(total, D), blk(total, F), blk(total, F), any_, any_, any_],
        out_specs=[blk(TB, C), any_, any_, any_],
        scratch_shapes=[V((D, F), bf), V((D, F), bf), V((F, D), bf), V((D, F), f32), V((D, F), f32), V((F, D), f32), V((total, D), bf), pltpu.SemaphoreType.DMA((3,)), pltpu.SemaphoreType.DMA((3,))],
        compiler_params=pltpu.CompilerParams(dimension_semantics=("arbitrary",), vmem_limit_bytes=65000 * 1024),
        cost_estimate=pl.CostEstimate(flops=85_000_000_000, bytes_accessed=150_000_000, transcendentals=0),
        name="experts_backward",
    )(meta_in, cot_a, cot_b, rows, ga, ua, w_gate, w_up, w_down)


def rope_tables(seq_len):
    half = HD // 2
    frequency = theta_base ** (-2.0 * jnp.arange(half, dtype=jnp.float32) / HD)
    angles = jnp.arange(seq_len, dtype=jnp.float32)[:, None] * frequency[None, :]
    return jnp.concatenate([jnp.cos(angles)] * 2, axis=-1), jnp.concatenate([-jnp.sin(angles), jnp.sin(angles)], axis=-1)

def turn(u, cos, sin):
    return u * cos + pltpu.roll(u, HD // 2, 1) * sin

def scale_of(u):
    return lax.rsqrt(jnp.mean(u * u, axis=-1, keepdims=True) + epsilon)

def attention_forward_kernel(group, n_ref, wq_ref, wk_ref, wv_ref, gq_ref, gk_ref, cos_ref, sin_ref, u_ref, ku_ref, ql_ref, kl_ref, vl_ref, mix_ref, k_all):
    bf, f32 = jnp.bfloat16, jnp.float32
    rows, seq = ql_ref.shape[0], kl_ref.shape[0]
    first = lax.axis_index("shard") * rows
    own = pl.ds(first, rows)
    k_all[...] = dot(n_ref[...], wk_ref[...], 1, 0)
    ku_ref[...] = k_all[own, :]
    k = k_all[...]
    kl_ref[...] = turn(k * scale_of(k) * gk_ref[...], cos_ref[...], sin_ref[...]).astype(bf)
    vl_ref[...] = dot(n_ref[...], wv_ref[...], 1, 0).astype(bf)
    u_ref[...] = dot(n_ref[own, :], wq_ref[...], 1, 0)
    cos, sin = cos_ref[own, :], sin_ref[own, :]
    allowed = lax.broadcasted_iota(jnp.int32, (rows, seq), 1) <= first + lax.broadcasted_iota(jnp.int32, (rows, seq), 0)
    for j in range(group):
        cols = slice(j * HD, (j + 1) * HD)
        u = u_ref[:, cols]
        ql = (turn(u * scale_of(u) * gq_ref[...], cos, sin) * HD ** (-0.5)).astype(bf)
        ql_ref[:, cols] = ql
        scores = dot(ql, kl_ref[...], 1, 1)
        raised = jnp.where(allowed, jnp.exp(scores), 0.0)
        probs = (raised * (1.0 / jnp.sum(raised, axis=-1, keepdims=True))).astype(bf)
        mix_ref[:, cols] = dot(probs, vl_ref[...], 1, 0).astype(bf)

def attention_forward(normed_seq, wqkv, rows, gq, gk, cos, sin):
    seq, width = normed_seq.shape
    group = HQ // HK
    bf, f32 = jnp.bfloat16, jnp.float32
    whole = lambda a: pl.BlockSpec(a.shape, lambda i: (0, 0))
    gq, gk = gq[None, :], gk[None, :]
    qb = pl.BlockSpec((rows, group * HD), lambda i: (0, i)); kb = pl.BlockSpec((seq, HD), lambda i: (0, i))
    return pl.pallas_call(
        functools.partial(attention_forward_kernel, group),
        grid=(HK,),
        out_shape=[jax.ShapeDtypeStruct((rows, HQ * HD), f32), jax.ShapeDtypeStruct((rows, HK * HD), f32), jax.ShapeDtypeStruct((rows, HQ * HD), bf),
            jax.ShapeDtypeStruct((seq, HK * HD), bf), jax.ShapeDtypeStruct((seq, HK * HD), bf), jax.ShapeDtypeStruct((rows, HQ * HD), bf)],
        in_specs=[whole(normed_seq), pl.BlockSpec((width, group * HD), lambda i: (0, i)), pl.BlockSpec((width, HD), lambda i: (0, HQ + i)), pl.BlockSpec((width, HD), lambda i: (0, HQ + HK + i)),
            whole(gq), whole(gk), whole(cos), whole(sin)],
        out_specs=[qb, pl.BlockSpec((rows, HD), lambda i: (0, i)), qb, kb, kb, qb],
        scratch_shapes=[pltpu.VMEM((seq, HD), f32)],
        compiler_params=pltpu.CompilerParams(dimension_semantics=("arbitrary",), vmem_limit_bytes=56 << 20),
        cost_estimate=pl.CostEstimate(flops=13_000_000_000, bytes_accessed=45_000_000, transcendentals=8_400_000),
        name="attention_forward",
    )(normed_seq, wqkv, wqkv, wqkv, gq, gk, cos, sin)

def attention_backward_kernel(group, guest, *refs):
    if guest:
        p_ref, u_ref, ql_ref, kl_ref, vl_ref, ga_ref, wo_ref, gq_ref, cos_ref, sin_ref, po_ref, gu_ref, gk_ref, gv_ref, gg_ref, gk_acc, gv_acc = refs[:17]
        runs = line_scatter_steps(LINE_PARTS, p_ref, po_ref, refs[17:])
        slots = HK * group
        at = {i * slots // (LINE_STEPS - 1): run for i, run in enumerate(runs[:-1])}
    else:
        u_ref, ql_ref, kl_ref, vl_ref, ga_ref, wo_ref, gq_ref, cos_ref, sin_ref, gu_ref, gk_ref, gv_ref, gg_ref, gk_acc, gv_acc = refs
        at = {}
    step = pl.program_id(0)
    bf, f32 = jnp.bfloat16, jnp.float32
    gm_all = dot(ga_ref[...], wo_ref[...], 1, 1).astype(bf)
    rows, seq = ql_ref.shape[0], kl_ref.shape[0]
    first = lax.axis_index("shard") * rows
    cos, sin = cos_ref[pl.ds(first, rows), :], sin_ref[pl.ds(first, rows), :]
    allowed = lax.broadcasted_iota(jnp.int32, (rows, seq), 1) <= first + lax.broadcasted_iota(jnp.int32, (rows, seq), 0)
    gain_grad = jnp.zeros((1, HD), f32)
    for j in range(group):
        for i in range(HK):
            if i * group + j in at: pl.when(step == i)(at[i * group + j])
        cols = slice(j * HD, (j + 1) * HD)
        ql, gm = ql_ref[:, cols], gm_all[:, cols]
        raised = jnp.where(allowed, jnp.exp(dot(ql, kl_ref[...], 1, 1)), 0.0)
        probs = raised * (1.0 / jnp.sum(raised, axis=-1, keepdims=True))
        gp = dot(gm, vl_ref[...], 1, 1)
        gs = (probs * (gp - jnp.sum(probs * gp, axis=-1, keepdims=True))).astype(bf)
        gv = dot(probs.astype(bf), gm, 0, 0)
        gk = dot(gs, ql, 0, 0)
        if j == 0:
            gv_acc[...] = gv
            gk_acc[...] = gk
        else:
            gv_acc[...] += gv
            gk_acc[...] += gk
        m = dot(gs, kl_ref[...], 1, 0) * HD ** (-0.5)
        m = m * cos + pltpu.roll(m * sin, HD // 2, 1)
        u = u_ref[:, cols]
        r = scale_of(u)
        gain_grad = gain_grad + jnp.sum(m * u * r, axis=0, keepdims=True)
        mg = m * gq_ref[...]
        gu_ref[:, cols] = (r * mg - u * (r * r * r) * jnp.mean(mg * u, axis=-1, keepdims=True)).astype(bf)
    gk_ref[...] = gk_acc[...].astype(bf)
    gv_ref[...] = gv_acc[...].astype(bf)
    gg_ref[0] = jnp.broadcast_to(gain_grad, (8, HD))
    if guest: pl.when(step == HK - 1)(runs[-1])

def attention_backward(q_proj, q_low, k_low, v_low, grad_attn, w_out, gq, cos, sin, guest, cid):
    rows, seq = q_low.shape[0], k_low.shape[0]
    group = HQ // HK
    bf, f32 = jnp.bfloat16, jnp.float32
    gq = gq[None, :]
    whole = lambda a: pl.BlockSpec(a.shape, lambda i: (0, 0))
    qb = pl.BlockSpec((rows, group * HD), lambda i: (0, i)); kb = pl.BlockSpec((seq, HD), lambda i: (0, i))
    hosted = placed()
    R, C = guest.shape[0] // lax.axis_size("shard"), guest.shape[1]
    shape = (NZ, LINE_PARTS, R // LINE_PARTS, C)
    vm = pl.BlockSpec(memory_space=pltpu.VMEM)
    *summed, grad_q, grad_k, grad_v, gain = pl.pallas_call(
        functools.partial(attention_backward_kernel, group, hosted),
        grid=(HK,),
        out_shape=([jax.ShapeDtypeStruct(shape[1:], f32)] if hosted else []) + [jax.ShapeDtypeStruct(q_low.shape, bf), jax.ShapeDtypeStruct(k_low.shape, bf), jax.ShapeDtypeStruct(k_low.shape, bf), jax.ShapeDtypeStruct((HK, 8, HD), f32)],
        in_specs=([vm] if hosted else []) + [qb, qb, kb, kb, whole(grad_attn), pl.BlockSpec((group * HD, w_out.shape[1]), lambda i: (i, 0)), whole(gq), whole(cos), whole(sin)],
        out_specs=([vm] if hosted else []) + [qb, kb, kb, pl.BlockSpec((1, 8, HD), lambda i: (i, 0, 0))],
        scratch_shapes=[pltpu.VMEM((seq, HD), f32), pltpu.VMEM((seq, HD), f32)] + (line_scatter_scratch(LINE_PARTS, R, C, bf) if hosted else []),
        compiler_params=pltpu.CompilerParams(dimension_semantics=("arbitrary",), vmem_limit_bytes=60 << 20,
            **(dict(collective_id=cid, has_side_effects=True) if hosted else {})),
        cost_estimate=pl.CostEstimate(flops=15_000_000_000, bytes_accessed=20_000_000, transcendentals=8_400_000),
        name="attention_backward",
    )(*([guest.reshape(shape)] if hosted else []), q_proj, q_low, k_low, v_low, grad_attn, w_out, gq, cos, sin)
    if hosted: total = summed[0].reshape(R, C)
    else: total = lax.psum_scatter(guest, "shard", scatter_dimension=0, tiled=True).astype(f32)
    return total, grad_q, jnp.concatenate([grad_k, grad_v], axis=1), jnp.sum(gain[:, 0], axis=0)

HQ = 32
HK = 4
HD = 128
epsilon = 1e-06
theta_base = 1000000.0
BOTH = ("expert", "shard")


def matmul(left, right):
    return jnp.dot(left, right, preferred_element_type=jnp.float32)


def matmul_tn(left, right):
    return lax.dot_general(
        left, right, (((0,), (0,)), ((), ())), preferred_element_type=jnp.float32
    )


def matmul_nt(left, right):
    return lax.dot_general(
        left, right, (((1,), (1,)), ((), ())), preferred_element_type=jnp.float32
    )


def norm_rows(values, gain_vec):
    return (
        values * lax.rsqrt(jnp.mean(values * values, axis=-1, keepdims=True) + epsilon) * gain_vec
    )


def norm_back(values, gain_vec, upstream):
    scaling = lax.rsqrt(jnp.mean(values * values, axis=-1, keepdims=True) + epsilon)
    gain_grad = jnp.sum(upstream * values * scaling, axis=0)
    weighted = upstream * gain_vec
    inner_sum = jnp.mean(weighted * values, axis=-1, keepdims=True)
    return (scaling * weighted - values * (scaling * scaling * scaling) * inner_sum, gain_grad)


def rotary(values, positions):
    head_width = values.shape[-1]
    half_width = head_width // 2
    frequency = theta_base ** (-2.0 * jnp.arange(half_width, dtype=jnp.float32) / head_width)
    angles = positions.astype(jnp.float32)[:, None] * frequency[None, :]
    cosine = jnp.concatenate([jnp.cos(angles), jnp.cos(angles)], axis=-1)[:, None, :]
    sine_part = jnp.concatenate([jnp.sin(angles), jnp.sin(angles)], axis=-1)[:, None, :]
    turned = jnp.concatenate([-values[..., half_width:], values[..., :half_width]], axis=-1)
    return values * cosine + turned * sine_part


def head_prep(projected, gain_vec, positions, head_count, factor):
    shaped = projected.reshape(projected.shape[0], head_count, projected.shape[1] // head_count)
    return rotary(norm_rows(shaped, gain_vec), positions) * factor


def gather_all(arrays, cid, line=()):
    if placed():
        return [o.reshape(-1, o.shape[-1]) for o in ag32(arrays, cid, line)]
    return [lax.all_gather(a, BOTH, axis=0, tiled=True) for a in arrays] + [
        lax.all_gather(a, "shard", axis=0, tiled=True) for a in line
    ]


def scatter_all(arrays, cid, out_dtype=jnp.float32, line=()):
    if placed():
        return rs32(
            [a.reshape(32, -1, a.shape[-1]) for a in arrays], cid, out_dtype, line=[a.reshape(NZ, -1, a.shape[-1]) for a in line]
        )
    return [lax.psum_scatter(a, BOTH, scatter_dimension=0, tiled=True).astype(out_dtype) for a in arrays] + [
        lax.psum_scatter(a, "shard", scatter_dimension=0, tiled=True).astype(out_dtype) for a in line
    ]


def per_device(
    hidden_in,
    g_attn,
    w_query,
    w_key,
    w_value,
    g_query,
    g_key,
    w_out,
    g_ffn,
    w_router,
    w_gate,
    w_up,
    w_down,
    routes,
    cotangent,
):
    bf, f32 = jnp.bfloat16, jnp.float32
    tok_rows, model_width = hidden_in.shape
    top_count = routes.shape[1]
    devices = lax.axis_size(BOTH)
    expert_count = devices * w_gate.shape[0]
    capacity = 2 * tok_rows * top_count // expert_count
    shard_count = lax.axis_size("shard")
    shard_pos = lax.axis_index("shard")
    seq_len = tok_rows * shard_count
    q_cols, kv_cols = HQ * HD, HK * HD

    pieces = [w_router.reshape(-1), g_attn, g_ffn, g_query, g_key]
    sizes = [p.shape[0] for p in pieces]
    used = sum(sizes)
    small_rows = -(-used // (64 * 128)) * 64
    small = jnp.concatenate(pieces + [jnp.zeros((small_rows * 128 - used,), bf)]).reshape(small_rows, 128)
    wqkv = jnp.concatenate([w_query, w_key, w_value], axis=1)
    wqkv_full, small_all, wo_full, hidden_seq = gather_all([wqkv, small, w_out], 1, [hidden_in])
    small_all = small_all.reshape(devices, small_rows * 128)
    starts = [sum(sizes[:i]) for i in range(5)]
    wr_full, attn_gain, ffn_gain, query_gain, key_gain = [small_all[:, o : o + n].reshape(-1) for o, n in zip(starts, sizes)]
    wr_full = wr_full.reshape(model_width, expert_count)
    attn_gain, ffn_gain, query_gain, key_gain = [g.astype(f32) for g in (attn_gain, ffn_gain, query_gain, key_gain)]
    first = tok_rows // 2
    cot_first, wo_full = lax.optimization_barrier((cotangent[:first], wo_full))
    cot_a = lax.all_gather(cot_first, BOTH, axis=0, tiled=True)

    inputs_f = hidden_in.astype(f32)
    normed_low = norm_rows(inputs_f, attn_gain).astype(bf)
    normed_seq = norm_rows(hidden_seq.astype(f32), attn_gain).astype(bf)
    cosine, sine = rope_tables(seq_len)
    q_proj, k_proj, q_low, k_low, v_low, mix_low = attention_forward(
        normed_seq, wqkv_full, tok_rows, query_gain, key_gain, cosine, sine
    )
    residual = inputs_f + matmul(mix_low, wo_full)
    ffn_low = norm_rows(residual, ffn_gain).astype(bf)

    logits = matmul(ffn_low, wr_full)
    expert_ids = jnp.arange(expert_count, dtype=jnp.int32)
    chosen = jnp.any(routes[:, :, None] == expert_ids[None, None, :], axis=1)
    raised_gate = jnp.where(chosen, jnp.exp(logits), 0.0)
    gates = raised_gate / jnp.sum(raised_gate, axis=-1, keepdims=True)
    gate_high = lax.reduce_precision(gates, 8, 7)
    gate_low = gates - gate_high
    extra = -(-3 * expert_count // 128) * 128
    payload = jnp.concatenate(
        [
            ffn_low,
            chosen.astype(bf),
            gate_high.astype(bf),
            gate_low.astype(bf),
            jnp.zeros((tok_rows, extra - 3 * expert_count), bf),
        ],
        axis=1,
    )
    (payload_all,) = gather_all([payload], 3)
    (out_part, rows, gate_act, up_act), cot_b = experts_forward(
        payload_all, w_gate, w_up, w_down, expert_count, tok_rows, capacity, cotangent[first:], 2
    )
    moe_out = lax.psum_scatter(out_part, "expert", scatter_dimension=0, tiled=True)
    grad_part, grad_wgate, grad_wup, grad_wdown = experts_backward(
        payload_all, cot_a, cot_b, rows, gate_act, up_act, w_gate, w_up, w_down, expert_count, tok_rows, capacity
    )
    (grad_sum,) = scatter_all([grad_part], 4)
    grad_sum, moe_out = lax.optimization_barrier((grad_sum, moe_out))
    upstream = cotangent.astype(f32)
    grad_ffn = grad_sum[:, :model_width]
    grad_shares = (
        grad_sum[:, model_width : model_width + expert_count]
        + grad_sum[:, model_width + expert_count : model_width + 2 * expert_count]
    )
    grad_logits = (grad_shares - gates * jnp.sum(grad_shares, axis=-1, keepdims=True)).astype(bf)
    grad_wrouter = matmul_tn(ffn_low, grad_logits)
    grad_ffn = grad_ffn + matmul_nt(grad_logits, wr_full)
    grad_second, grad_ffn_gain = norm_back(residual, ffn_gain, grad_ffn)
    grad_residual = upstream + grad_second
    grad_attn_low = grad_residual.astype(bf)
    grad_wout = matmul_tn(mix_low, grad_attn_low).astype(bf)
    grad_attn_low, grad_wout = lax.optimization_barrier((grad_attn_low, grad_wout))
    out_grad = lax.psum_scatter(grad_wout, "expert", scatter_dimension=0, tiled=True)

    moe_parts = moe_out.reshape(shard_count, 2, tok_rows // 2, model_width)
    moe_a, moe_b = [moe_parts[:, i].reshape(-1, model_width) for i in range(2)]
    moe_a, grad_q_low, grad_kv, grad_query_gain = attention_backward(
        q_proj, q_low, k_low, v_low, grad_attn_low, wo_full, query_gain, cosine, sine, moe_a, 5
    )
    grad_kv = line_scatter(grad_kv, 6)
    own_rows = shard_pos * tok_rows
    positions = own_rows + jnp.arange(tok_rows, dtype=jnp.int32)
    _, k_pull = jax.vjp(
        lambda projected, gain_vec: head_prep(projected, gain_vec, positions, HK, 1.0), k_proj, key_gain
    )
    grad_k_proj, grad_key_gain = k_pull(grad_kv[:, :kv_cols].reshape(tok_rows, HK, HD))
    grad_qkv_low = jnp.concatenate(
        [grad_q_low, grad_k_proj.astype(bf), grad_kv[:, kv_cols:].astype(bf)], axis=1
    )
    grad_wqkv = matmul_tn(normed_low, grad_qkv_low).astype(bf)
    grad_normed = matmul_nt(grad_qkv_low, wqkv_full)
    grad_front, grad_attn_gain = norm_back(inputs_f, attn_gain, grad_normed)
    grad_input = (grad_residual + grad_front).astype(bf)

    grads = [grad_wrouter, grad_attn_gain, grad_ffn_gain, grad_query_gain, grad_key_gain]
    packed = jnp.concatenate(
        [g.astype(bf).reshape(devices, -1) for g in grads] + [jnp.zeros((devices, small_rows * 128 - used), bf)], axis=1
    ).reshape(devices * small_rows, 128)
    grad_wqkv, out_grad = lax.optimization_barrier((grad_wqkv, out_grad))
    qkv_grad, small_grad, moe_b, out_grad = scatter_all([grad_wqkv, packed], 8, line=[moe_b, out_grad])
    block_out = (residual + jnp.concatenate([moe_a, moe_b], axis=0)).astype(bf)
    small_grad = small_grad.reshape(-1)
    router_g, attn_g, ffn_g, query_g, key_g = [small_grad[o : o + n] for o, n in zip(starts, sizes)]
    return (
        block_out,
        grad_input,
        attn_g,
        qkv_grad[:, :q_cols],
        qkv_grad[:, q_cols : q_cols + kv_cols],
        qkv_grad[:, q_cols + kv_cols :],
        query_g,
        key_g,
        out_grad,
        ffn_g,
        router_g.reshape(w_router.shape),
        grad_wgate,
        grad_wup,
        grad_wdown,
    )


def solution(mesh):
    row = P(BOTH, None)
    vec = P(BOTH)
    cube = P(BOTH, None, None)
    in_specs = (row, vec, row, row, row, vec, vec, row, vec, row, cube, cube, cube, row, row)
    out_specs = (row, row, vec, row, row, row, vec, vec, row, vec, row, cube, cube, cube)
    return jax.shard_map(
        per_device, mesh=mesh, in_specs=in_specs, out_specs=out_specs, check_vma=False
    )
```

```python
import functools

import jax
import jax.numpy as jnp
from jax import lax
from jax.experimental import pallas as pl
from jax.experimental.pallas import tpu as pltpu
from jax.sharding import PartitionSpec as P

MESH = pl.DeviceIdType.MESH
NZ = 4

def placed():
    return lax.axis_size("expert") == 8 and lax.axis_size("shard") == NZ

def place():
    e = lax.axis_index("expert"); s = lax.axis_index("shard")
    return e // 4, lax.rem(e // 2, 2), lax.rem(e, 2), s

def dev(y, x, c, s):
    return (y * 4 + x * 2 + c, s)

def barrier_all(y, x, c, s):
    bar = pltpu.get_barrier_semaphore()
    def sig(d): pl.semaphore_signal(bar, inc=1, device_id=d, device_id_type=MESH)
    sig(dev(1 - y, x, c, s)); sig(dev(y, 1 - x, c, s)); sig(dev(y, x, 1 - c, s))
    @pl.when(s > 0)
    def _(): sig(dev(y, x, c, s - 1))
    @pl.when(s < NZ - 1)
    def _(): sig(dev(y, x, c, s + 1))
    pl.semaphore_wait(bar, 3 + jnp.where(s > 0, 1, 0) + jnp.where(s < NZ - 1, 1, 0))

def ag_kernel(n_arr, n_line, *refs):
    n_all = n_arr + n_line
    for run in ag_steps(n_arr, n_line, refs[:n_all], refs[n_all:2 * n_all], refs[2 * n_all:]): run()

def ag_steps(n_arr, n_line, ins, outs, sems, stages=False):
    n_all = n_arr + n_line
    loc_sem, zs, zr, ps, pr, cs, cr = sems
    y, x, c, s = place()
    def rc(src, dst, ss, rs, d):
        return pltpu.make_async_remote_copy(src_ref=src, dst_ref=dst, send_sem=ss, recv_sem=rs, device_id=d, device_id_type=MESH)
    X = dev(y, 1 - x, c, s); Y = dev(1 - y, x, c, s); C = dev(y, x, 1 - c, s)
    A = range(n_arr)
    every = range(n_all)
    def home(a, zz):
        return outs[a].at[y, x, c, zz] if a < n_arr else outs[a].at[zz]
    steps = [(0, 0)] + [(d, g) for d in range(1, NZ) for g in (1, -1)]
    def valid(d, g):
        return (s >= d) if g == 1 else (s + d <= NZ - 1)
    def zof(d, g): return s - d * g
    def src_own(a, h, zz, k):
        return ins[a].at[h] if k == 0 else home(a, zz).at[h]
    def zcopy(a, h, zz, k, g):
        kk = 1 + 2 * (k_dist(k)) + (0 if g == 1 else 1)
        return rc(src_own(a, h, zz, k), home(a, zz).at[h], zs.at[a, h, kk], zr.at[a, h, kk], dev(y, x, c, s + g))
    def k_dist(k): return steps[k][0]
    def plane(a, h, zz, k, which):
        return rc(src_own(a, h, zz, k), outs[a].at[y, x, c, zz, h], ps.at[a, k, h, which], pr.at[a, k, h, which], X if which == 0 else Y)
    def plane_recv(a, h, zz, k, which):
        d = outs[a].at[y, 1 - x, c, zz, h] if which == 0 else outs[a].at[1 - y, x, c, zz, h]
        return rc(d, d, ps.at[a, k, h, which], pr.at[a, k, h, which], X if which == 0 else Y)
    def diag(a, h, zz, k):
        d = outs[a].at[y, 1 - x, c, zz, h] if h == 0 else outs[a].at[1 - y, x, c, zz, h]
        return rc(d, d, ps.at[a, k, h, 2], pr.at[a, k, h, 2], Y if h == 0 else X)
    def diag_recv(a, h, zz, k):
        d = outs[a].at[1 - y, 1 - x, c, zz, h]
        return rc(d, d, ps.at[a, k, h, 2], pr.at[a, k, h, 2], Y if h == 0 else X)
    def core(a, zz, k, part):
        d = outs[a].at[:, :, c, zz]
        return rc(d, d, cs.at[a, k], cr.at[a, k], C)
    def core_recv(a, zz, k):
        d = outs[a].at[:, :, 1 - c, zz]
        return rc(d, d, cs.at[a, k], cr.at[a, k], C)
    def loc(a):
        return pltpu.make_async_copy(ins[a], home(a, s), loc_sem.at[a])

    def when(k, f):
        d, g = steps[k]
        if k == 0: f()
        else: pl.when(valid(d, g))(f)

    def stage_a(k):
        d, g = steps[k]
        def go():
            zz = zof(d, g)
            for a in every:
                for h in range(2):
                    if k:
                        kk = k
                        dref = home(a, zz).at[h]
                        rc(dref, dref, zs.at[a, h, kk], zr.at[a, h, kk], X).wait_recv()
                    for gg in ((1, -1) if k == 0 else (g,)):
                        okc = (s < NZ - 1) if gg == 1 else (s > 0)
                        if d + 1 < NZ:
                            @pl.when(okc)
                            def _(): zcopy(a, h, zz, k, gg).start()
                    if a < n_arr:
                        plane(a, h, zz, k, 0).start()
                        plane(a, h, zz, k, 1).start()
        when(k, go)
    def stage_b(k):
        d, g = steps[k]
        def go():
            zz = zof(d, g)
            for a in A:
                plane_recv(a, 0, zz, k, 0).wait_recv()
                diag(a, 0, zz, k).start()
                plane_recv(a, 1, zz, k, 1).wait_recv()
                diag(a, 1, zz, k).start()
        when(k, go)
    def stage_c(k):
        d, g = steps[k]
        def go():
            zz = zof(d, g)
            for a in A:
                if k == 0: loc(a).wait()
                plane_recv(a, 1, zz, k, 0).wait_recv()
                plane_recv(a, 0, zz, k, 1).wait_recv()
                diag_recv(a, 0, zz, k).wait_recv()
                diag_recv(a, 1, zz, k).wait_recv()
                core(a, zz, k, 0).start()
        when(k, go)
    n = len(steps)
    def start():
        barrier_all(y, x, c, s)
        for a in every: loc(a).start()
        stage_a(0)
    def advance(i):
        if 0 < i < n: stage_a(i)
        if 0 <= i - 1 < n: stage_b(i - 1)
        if 0 <= i - 2 < n: stage_c(i - 2)
    def finish():
        for k in range(n):
            d, g = steps[k]
            def go():
                zz = zof(d, g)
                for a in every:
                    if a < n_arr:
                        core_recv(a, zz, k).wait_recv()
                        core(a, zz, k, 0).wait_send()
                    elif k == 0: loc(a).wait()
                    for h in range(2):
                        for gg in ((1, -1) if k == 0 else (g,)):
                            okc = (s < NZ - 1) if gg == 1 else (s > 0)
                            if d + 1 < NZ:
                                @pl.when(okc)
                                def _(): zcopy(a, h, zz, k, gg).wait_send()
                        if a < n_arr:
                            plane(a, h, zz, k, 0).wait_send()
                            plane(a, h, zz, k, 1).wait_send()
                            diag(a, h, zz, k).wait_send()
            when(k, go)
    if stages: return start, stage_a, stage_b, stage_c, finish
    return [start] + [functools.partial(advance, i) for i in range(1, n + 2)] + [finish]

def ag_sems(n, m=0):
    D = pltpu.SemaphoreType.DMA
    return [D((n + m,)), D((n + m, 2, 9)), D((n + m, 2, 9)), D((n, 7, 2, 3)), D((n, 7, 2, 3)), D((n, 7)), D((n, 7))]

def ag32(arrs, cid, line=()):
    ins = [a.reshape(2, a.shape[0] // 2, a.shape[1]) for a in list(arrs) + list(line)]
    n, m = len(arrs), len(line)
    outs = pl.pallas_call(
        functools.partial(ag_kernel, n, m),
        out_shape=[jax.ShapeDtypeStruct(((2, 2, 2, NZ) if i < n else (NZ,)) + a.shape, a.dtype) for i, a in enumerate(ins)],
        in_specs=[pl.BlockSpec(memory_space=pltpu.VMEM)] * (n + m),
        out_specs=[pl.BlockSpec(memory_space=pl.ANY)] * (n + m),
        scratch_shapes=ag_sems(n, m),
        compiler_params=pltpu.CompilerParams(collective_id=cid, has_side_effects=True, vmem_limit_bytes=64000 * 1024),
        name="gather_all",
    )(*ins)
    return [o.reshape(-1, a.shape[1] * 2, a.shape[2]) for o, a in zip(outs, ins)]

ZORDER = (0, 3, 1, 2)
LAGS = (1, 1, 1, 1)

def rs_kernel(n_arr, n_line, parts, *refs):
    n_all = n_arr + n_line
    ins = refs[:n_all]; outs = refs[n_all:2 * n_all]
    sc = list(refs[2 * n_all:])
    own_b = [sc.pop(0) for _ in range(n_all)]; zu_b = [sc.pop(0) for _ in range(n_all)]; zd_b = [sc.pop(0) for _ in range(n_all)]
    r0_b, ra_b, rb_b = [[sc.pop(0) for _ in range(n_arr)] for _ in range(3)]
    lsem, s0s, s0r, sas, sar, sbs, sbr, zus, zur, zds, zdr = sc
    y, x, c, s = place()
    barrier_all(y, x, c, s)
    X = dev(y, 1 - x, c, s); Y = dev(1 - y, x, c, s); C = dev(y, x, 1 - c, s)
    UP = dev(y, x, c, s + 1); DN = dev(y, x, c, s - 1)
    def rc(src, dst, ss, rs, d):
        return pltpu.make_async_remote_copy(src_ref=src, dst_ref=dst, send_sem=ss, recv_sem=rs, device_id=d, device_id_type=MESH)
    units = [(a, zz, h) for zz in ZORDER for h in range(parts) for a in range(n_arr)]
    lines = [(a, zz, h) for zz in ZORDER for h in range(parts) for a in range(n_arr, n_all)]
    def jj(zz, h): return ZORDER.index(zz) * parts + h
    def load(a, zz, h):
        j = jj(zz, h)
        src = ins[a].at[:, :, c, zz, h] if a < n_arr else ins[a].at[zz, h]
        return pltpu.make_async_copy(src, own_b[a].at[j], lsem.at[a, j])
    def mine(a, j):
        return own_b[a].at[j, y, x] if a < n_arr else own_b[a].at[j]
    def c0(a, zz, h):
        j = jj(zz, h)
        return rc(ins[a].at[:, :, 1 - c, zz, h], r0_b[a].at[j], s0s.at[a, j], s0r.at[a, j], C)
    def ca(a, zz, h):
        j = jj(zz, h)
        if h % 2 == 0: return rc(own_b[a].at[j, :, 1 - x], ra_b[a].at[j], sas.at[a, j], sar.at[a, j], X)
        return rc(own_b[a].at[j, 1 - y], ra_b[a].at[j], sas.at[a, j], sar.at[a, j], Y)
    def cb(a, zz, h):
        j = jj(zz, h)
        if h % 2 == 0: return rc(own_b[a].at[j, 1 - y, x], rb_b[a].at[j], sbs.at[a, j], sbr.at[a, j], Y)
        return rc(own_b[a].at[j, y, 1 - x], rb_b[a].at[j], sbs.at[a, j], sbr.at[a, j], X)
    def cu(a, zz, h):
        j = jj(zz, h)
        return rc(mine(a, j), zu_b[a].at[j], zus.at[a, j], zur.at[a, j], UP)
    def cd(a, zz, h):
        j = jj(zz, h)
        return rc(mine(a, j), zd_b[a].at[j], zds.at[a, j], zdr.at[a, j], DN)
    def add_into(dst, other):
        rows = dst.shape[0]
        st = 16 if rows % 16 == 0 else rows
        @pl.loop(0, rows // st)
        def _(i):
            r = pl.ds(i * st, st)
            dst[r, :] = (dst[r, :].astype(jnp.float32) + other[r, :].astype(jnp.float32)).astype(dst.dtype)
    def stage0(u):
        a, zz, h = u; j = jj(zz, h)
        load(a, zz, h).wait()
        c0(a, zz, h).wait_recv()
        for yy in range(2):
            for xx in range(2):
                add_into(own_b[a].at[j, yy, xx], r0_b[a].at[j, yy, xx])
        ca(a, zz, h).start()
    def stage1(u):
        a, zz, h = u; j = jj(zz, h)
        ca(a, zz, h).wait_recv()
        for q in range(2):
            if h % 2 == 0: add_into(own_b[a].at[j, q, x], ra_b[a].at[j, q])
            else: add_into(own_b[a].at[j, y, q], ra_b[a].at[j, q])
        cb(a, zz, h).start()
    def stage2(u):
        a, zz, h = u; j = jj(zz, h)
        cb(a, zz, h).wait_recv()
        add_into(own_b[a].at[j, y, x], rb_b[a].at[j])
    def hop(u, k):
        a, zz, h = u; j = jj(zz, h)
        if k < zz:
            @pl.when(s == k)
            def _():
                if k > 0:
                    cu(a, zz, h).wait_recv()
                    add_into(mine(a, j), zu_b[a].at[j])
                cu(a, zz, h).start()
        t = NZ - 1 - k
        if t > zz:
            @pl.when(s == t)
            def _():
                if k > 0:
                    cd(a, zz, h).wait_recv()
                    add_into(mine(a, j), zd_b[a].at[j])
                cd(a, zz, h).start()
    def last(u):
        a, zz, h = u; j = jj(zz, h)
        @pl.when(s == zz)
        def _():
            if zz > 0: cu(a, zz, h).wait_recv()
            if zz < NZ - 1: cd(a, zz, h).wait_recv()
            t = mine(a, j)[...].astype(jnp.float32)
            if zz > 0: t = t + zu_b[a][j].astype(jnp.float32)
            if zz < NZ - 1: t = t + zd_b[a][j].astype(jnp.float32)
            outs[a][h] = t.astype(outs[a].dtype)
    for u in lines: load(*u).start()
    for u in units:
        c0(*u).start(); load(*u).start()
    n = len(units); nl = len(lines)
    per = max(1, -(-nl // n))
    L1 = LAGS[0] * n_arr; L2 = L1 + LAGS[1] * n_arr; L3 = L2 + LAGS[2] * n_arr; dl = LAGS[3] * n_arr
    for i in range(n + L3 + (NZ - 1) * dl):
        if i < n: stage0(units[i])
        if 0 <= i - L1 < n: stage1(units[i - L1])
        if 0 <= i - L2 < n: stage2(units[i - L2])
        for k in range(NZ - 1):
            for q in range(per * (i - k), per * (i - k) + per):
                if 0 <= q < nl:
                    if k == 0: load(*lines[q]).wait()
                    hop(lines[q], k)
        for k in range(NZ - 1):
            if 0 <= i - L3 - k * dl < n: hop(units[i - L3 - k * dl], k)
    for u in lines + units: last(u)
    for u in lines + units:
        a, zz, h = u
        if a < n_arr:
            c0(*u).wait_send(); ca(*u).wait_send(); cb(*u).wait_send()
        if zz > 0:
            @pl.when(s < zz)
            def _(): cu(*u).wait_send()
        if zz < NZ - 1:
            @pl.when(s > zz)
            def _(): cd(*u).wait_send()

def rs32(arrs, cid, out_dtype=jnp.float32, parts=4, line=()):
    n, nl = len(arrs), len(line)
    both = list(arrs) + list(line)
    if any(a.shape[1] % (parts * 16) for a in both): parts = 2
    ins = [a.reshape(((2, 2, 2) if i < n else ()) + (NZ, parts, a.shape[1] // parts, a.shape[2])) for i, a in enumerate(both)]
    hs = [i.shape[-2:] for i in ins]
    V = pltpu.VMEM; bt = jnp.bfloat16; m = NZ * parts
    sems = [pltpu.SemaphoreType.DMA((n + nl, m))] * 11
    outs = pl.pallas_call(
        functools.partial(rs_kernel, n, nl, parts),
        out_shape=[jax.ShapeDtypeStruct((parts,) + h, out_dtype) for h in hs],
        in_specs=[pl.BlockSpec(memory_space=pl.ANY)] * (n + nl),
        out_specs=[pl.BlockSpec(memory_space=pltpu.VMEM)] * (n + nl),
        scratch_shapes=[V((m,) + ((2, 2) if i < n else ()) + h, bt) for i, h in enumerate(hs)] + [V((m,) + h, bt) for h in hs] + [V((m,) + h, bt) for h in hs]
            + [V((m, 2, 2) + h, bt) for h in hs[:n]] + [V((m, 2) + h, bt) for h in hs[:n]] + [V((m,) + h, bt) for h in hs[:n]] + sems,
        compiler_params=pltpu.CompilerParams(collective_id=cid, has_side_effects=True, vmem_limit_bytes=64000 * 1024),
        name="scatter_all",
    )(*ins)
    return [o.reshape(a.shape[1], a.shape[2]) for o, a in zip(outs, both)]

def line_barrier(y, x, c, s):
    bar = pltpu.get_barrier_semaphore()
    @pl.when(s > 0)
    def _(): pl.semaphore_signal(bar, inc=1, device_id=dev(y, x, c, s - 1), device_id_type=MESH)
    @pl.when(s < NZ - 1)
    def _(): pl.semaphore_signal(bar, inc=1, device_id=dev(y, x, c, s + 1), device_id_type=MESH)
    pl.semaphore_wait(bar, jnp.where(s > 0, 1, 0) + jnp.where(s < NZ - 1, 1, 0))

def line_gather_kernel(parts, x_ref, o_ref, ss, rs):
    y, x, c, s = place()
    line_barrier(y, x, c, s)
    def cp(d, g, h):
        src = x_ref.at[h] if d == 0 else o_ref.at[s - d * g, h]
        k = 0 if g == 1 else 1
        return pltpu.make_async_remote_copy(src_ref=src, dst_ref=o_ref.at[s - d * g, h], send_sem=ss.at[k, d, h], recv_sem=rs.at[k, d, h],
            device_id=dev(y, x, c, s + g), device_id_type=MESH)
    def arrived(d, g, h):
        k = 0 if g == 1 else 1
        ref = o_ref.at[s - (d + 1) * g, h]
        return pltpu.make_async_remote_copy(src_ref=ref, dst_ref=ref, send_sem=ss.at[k, d, h], recv_sem=rs.at[k, d, h],
            device_id=dev(y, x, c, s + g), device_id_type=MESH)
    def sends(d, g): return (s >= d) & (s < NZ - 1) if g == 1 else (s + d <= NZ - 1) & (s > 0)
    def gets(d, g): return s >= d + 1 if g == 1 else s + d + 1 <= NZ - 1
    for d in range(NZ):
        for h in range(parts):
            for g in (1, -1):
                if d:
                    @pl.when(gets(d - 1, g))
                    def _(): arrived(d - 1, g, h).wait_recv()
                if d < NZ - 1:
                    @pl.when(sends(d, g))
                    def _(): cp(d, g, h).start()
        if d == 0: o_ref[s] = x_ref[...]
    for d in range(NZ - 1):
        for h in range(parts):
            for g in (1, -1):
                @pl.when(sends(d, g))
                def _(): cp(d, g, h).wait_send()

def line_gather(x, cid, parts=4):
    if not placed():
        return lax.all_gather(x, "shard", axis=0, tiled=True)
    R, C = x.shape
    sem = pltpu.SemaphoreType.DMA((2, NZ, parts))
    o = pl.pallas_call(functools.partial(line_gather_kernel, parts), out_shape=jax.ShapeDtypeStruct((NZ, parts, R // parts, C), x.dtype),
        in_specs=[pl.BlockSpec(memory_space=pltpu.VMEM)], out_specs=pl.BlockSpec(memory_space=pltpu.VMEM),
        scratch_shapes=[sem, sem], compiler_params=pltpu.CompilerParams(collective_id=cid, has_side_effects=True, vmem_limit_bytes=16 << 20),
        name="line_gather")(x.reshape(parts, R // parts, C))
    return o.reshape(NZ * R, C)

def line_scatter_kernel(parts, p_ref, o_ref, *scratch):
    for run in line_scatter_steps(parts, p_ref, o_ref, scratch): run()

LINE_PARTS = 4
LINE_STEPS = 3 * LINE_PARTS + NZ + 1

def line_scatter_steps(parts, p_ref, o_ref, scratch):
    acc, zu, zd, ss_u, rs_u, ss_d, rs_d = scratch
    y, x, c, s = place()
    def rc(src, dst, a, b, d):
        return pltpu.make_async_remote_copy(src_ref=src, dst_ref=dst, send_sem=a, recv_sem=b, device_id=d, device_id_type=MESH)
    def cu(zz, h, k):
        src = p_ref.at[zz, h] if k == 0 else acc.at[zz, h]
        return rc(src, zu.at[zz, h], ss_u.at[zz, h], rs_u.at[zz, h], dev(y, x, c, s + 1))
    def cd(zz, h, k):
        src = p_ref.at[zz, h] if k == 0 else acc.at[zz, h]
        return rc(src, zd.at[zz, h], ss_d.at[zz, h], rs_d.at[zz, h], dev(y, x, c, s - 1))
    st = 32
    def total(dst, refs):
        @pl.loop(0, dst.shape[0] // st)
        def _(i):
            r = pl.ds(i * st, st)
            t = refs[0][r, :].astype(jnp.float32)
            for f in refs[1:]: t = t + f[r, :].astype(jnp.float32)
            dst[r, :] = t.astype(dst.dtype)
    ups = [(zz, h) for zz in (3, 2, 1) for h in range(parts)]
    dns = [(zz, h) for zz in (0, 1, 2) for h in range(parts)]
    n = len(ups)
    def advance(i):
        if i == 0: line_barrier(y, x, c, s)
        for k in range(NZ - 1):
            if 0 <= i - k < n:
                zz, h = ups[i - k]
                if k < zz:
                    @pl.when(s == k)
                    def _():
                        if k:
                            cu(zz, h, k).wait_recv()
                            total(acc.at[zz, h], [p_ref.at[zz, h], zu.at[zz, h]])
                        cu(zz, h, k).start()
                zz, h = dns[i - k]
                if NZ - 1 - k > zz:
                    @pl.when(s == NZ - 1 - k)
                    def _():
                        if k:
                            cd(zz, h, k).wait_recv()
                            total(acc.at[zz, h], [p_ref.at[zz, h], zd.at[zz, h]])
                        cd(zz, h, k).start()
    def finish():
        for zz in range(NZ):
            @pl.when(s == zz)
            def _():
                for h in range(parts):
                    refs = [p_ref.at[zz, h]]
                    if zz > 0:
                        cu(zz, h, 1).wait_recv()
                        refs.append(zu.at[zz, h])
                    if zz < NZ - 1:
                        cd(zz, h, 1).wait_recv()
                        refs.append(zd.at[zz, h])
                    total(o_ref.at[h], refs)
        for zz, h in ups:
            @pl.when(s < zz)
            def _(): cu(zz, h, 1).wait_send()
        for zz, h in dns:
            @pl.when(s > zz)
            def _(): cd(zz, h, 1).wait_send()
    return [functools.partial(advance, i) for i in range(n + NZ)] + [finish]

def line_scatter_scratch(parts, rows, cols, dtype):
    sem = pltpu.SemaphoreType.DMA((NZ, parts))
    buf = pltpu.VMEM((NZ, parts, rows // parts, cols), dtype)
    return [buf, buf, buf, sem, sem, sem, sem]

def line_scatter(p, cid, parts=LINE_PARTS):
    if not placed():
        return lax.psum_scatter(p, "shard", scatter_dimension=0, tiled=True).astype(jnp.float32)
    R, C = p.shape[0] // NZ, p.shape[1]
    shape = (NZ, parts, R // parts, C)
    o = pl.pallas_call(functools.partial(line_scatter_kernel, parts), out_shape=jax.ShapeDtypeStruct(shape[1:], jnp.float32),
        in_specs=[pl.BlockSpec(memory_space=pltpu.VMEM)], out_specs=pl.BlockSpec(memory_space=pltpu.VMEM),
        scratch_shapes=line_scatter_scratch(parts, R, C, p.dtype), compiler_params=pltpu.CompilerParams(collective_id=cid, has_side_effects=True, vmem_limit_bytes=24 << 20),
        name="line_scatter")(p.reshape(shape))
    return o.reshape(R, C)


def dot(a, b, ca, cb):
    return lax.dot_general(a, b, (((ca,), (cb,)), ((), ())), preferred_element_type=jnp.float32)

def token_picks(meta, experts, slots, me):
    SB, WM = meta.shape
    bf, f32 = jnp.bfloat16, jnp.float32
    tri = (lax.broadcasted_iota(jnp.int32, (SB, SB), 1) < lax.broadcasted_iota(jnp.int32, (SB, SB), 0)).astype(bf)
    lane = lax.broadcasted_iota(jnp.int32, (SB, WM), 1)
    cnt = dot(tri, meta, 1, 0)
    metaf = meta.astype(f32)
    msk = jnp.sum(jnp.where(lane == me, metaf, 0.0), axis=-1, keepdims=True)
    pos = jnp.sum(jnp.where(lane == me, cnt, 0.0), axis=-1, keepdims=True)
    gate = jnp.sum(jnp.where((lane == me + experts) | (lane == me + 2 * experts), metaf, 0.0), axis=-1, keepdims=True)
    want = jnp.where(msk > 0.0, pos, -1.0).astype(jnp.int32)
    pick = (want == lax.broadcasted_iota(jnp.int32, (SB, slots), 1)).astype(bf)
    return pick, gate

def forward_kernel(experts, slots, SB, guest, *refs):
    if guest:
        cot_ref, x_ref, wg_hbm, wu_hbm, wd_hbm, cot_all, out_ref, rows_ref, ga_ref, ua_ref, wg, wu, wd, wsem = refs[:14]
    else:
        x_ref, wg_hbm, wu_hbm, wd_hbm, out_ref, rows_ref, ga_ref, ua_ref, wg, wu, wd, wsem = refs
    bf = jnp.bfloat16
    step = pl.program_id(0)
    if guest:
        start, stage_a, stage_b, stage_c, finish = ag_steps(1, 0, [cot_ref], [cot_all], refs[14:], True)
        pl.when(step == 0)(start)
        for at, stage, k in GUEST_AT: pl.when(step == at)(functools.partial(stage_a if stage == 0 else stage_b if stage == 1 else stage_c, k))
    nsub = x_ref.shape[0] // SB
    D = out_ref.shape[1]
    me = lax.axis_index(("expert", "shard"))
    loads = [pltpu.make_async_copy(h.at[0], v, wsem.at[i]) for i, (h, v) in enumerate(((wg_hbm, wg), (wu_hbm, wu), (wd_hbm, wd)))]
    @pl.when(step == 0)
    def _():
        for l in loads: l.start()
    picks, gates = [], []
    for i in range(nsub):
        r = pl.ds(i * SB, SB)
        pick, gate = token_picks(x_ref[r, D:], experts, slots, me)
        picks.append(pick); gates.append(gate)
        rows_ref[i * slots:(i + 1) * slots, :] = dot(pick, x_ref[r, :D], 0, 0).astype(bf)
    @pl.when(step == 0)
    def _():
        for l in loads: l.wait()
    ga = dot(rows_ref[...], wg[...], 1, 0)
    ua = dot(rows_ref[...], wu[...], 1, 0)
    ga_ref[...] = ga
    ua_ref[...] = ua
    hid = (ga * (1.0 / (1.0 + jnp.exp(-ga))) * ua).astype(bf)
    eo = dot(hid, wd[...], 1, 0).astype(bf)
    for i in range(nsub):
        r = pl.ds(i * SB, SB)
        tok = dot(picks[i], eo[i * slots:(i + 1) * slots, :], 1, 0)
        out_ref[r, :] = (gates[i] * tok).astype(bf)
    if guest: pl.when(step == pl.num_programs(0) - 1)(finish)

GUEST_AT = (
    (3, 0, 1), (3, 0, 2), (3, 1, 0), (5, 0, 3), (5, 0, 4), (5, 2, 0), (7, 1, 1), (7, 0, 5), (7, 0, 6), (8, 1, 2),
    (9, 2, 1), (10, 2, 2), (11, 1, 3), (11, 1, 4), (13, 2, 3), (13, 2, 4), (14, 1, 5), (14, 1, 6), (15, 2, 5), (15, 2, 6),
)

def backward_kernel(experts, slots, SB, block, meta_ref, cota_ref, cotb_ref, rows_ref, ga_ref, ua_ref, wg_hbm, wu_hbm, wd_hbm, gr_ref, dwg_hbm, dwu_hbm, dwd_hbm,
                  wg, wu, wd, dwg, dwu, dwd, gp, wsem, osem):
    bf = jnp.bfloat16
    step = pl.program_id(0)
    nsub = meta_ref.shape[0] // SB
    D = cota_ref.shape[1]
    WM = meta_ref.shape[1]
    na, nb = [r.shape[0] * block // meta_ref.shape[0] for r in (cota_ref, cotb_ref)]
    me = lax.axis_index(("expert", "shard"))
    loads = [pltpu.make_async_copy(h.at[0], v, wsem.at[i]) for i, (h, v) in enumerate(((wg_hbm, wg), (wu_hbm, wu), (wd_hbm, wd)))]
    @pl.when(step == 0)
    def _():
        for l in loads: l.start()
        for a in (dwg, dwu, dwd): a[...] = jnp.zeros_like(a)
    picks = []
    for i in range(nsub):
        r = pl.ds(i * SB, SB)
        pick, gate = token_picks(meta_ref[r, :], experts, slots, me)
        picks.append(pick)
        cot = []
        for b in range(i * SB // block, (i + 1) * SB // block):
            cot += [cota_ref[b * na:(b + 1) * na, :], cotb_ref[b * nb:(b + 1) * nb, :]]
        gcot = (gate * jnp.concatenate(cot, axis=0).astype(jnp.float32)).astype(bf)
        gp[i * slots:(i + 1) * slots, :] = dot(pick, gcot, 0, 0).astype(bf)
    @pl.when(step == 0)
    def _():
        for l in loads: l.wait()
    ga = ga_ref[...]
    ua = ua_ref[...]
    sig = 1.0 / (1.0 + jnp.exp(-ga))
    act = ga * sig
    hidf = act * ua
    hid = hidf.astype(bf)
    gh = dot(gp[...], wd[...], 1, 1)
    share = jnp.sum(gh * hid.astype(jnp.float32), axis=-1, keepdims=True)
    dga = (gh * ua * (sig * (1.0 + ga * (1.0 - sig)))).astype(bf)
    dua = (gh * act).astype(bf)
    dwd[...] += dot(hid, gp[...], 0, 0)
    grow = (dot(dga, wg[...], 1, 1) + dot(dua, wu[...], 1, 1)).astype(bf)
    dwg[...] += dot(rows_ref[...], dga, 0, 0)
    dwu[...] += dot(rows_ref[...], dua, 0, 0)
    lane = lax.broadcasted_iota(jnp.int32, (share.shape[0], WM), 1)
    high = share.astype(bf).astype(jnp.float32)
    tail = (jnp.where(lane == me, high, 0.0) + jnp.where(lane == me + experts, share - high, 0.0)).astype(bf)
    for i in range(nsub):
        r = pl.ds(i * SB, SB)
        q = slice(i * slots, (i + 1) * slots)
        gr_ref[r, :D] = dot(picks[i], grow[q, :], 1, 0).astype(bf)
        gr_ref[r, D:] = dot(picks[i], tail[q, :], 1, 0).astype(bf)
    @pl.when(step == pl.num_programs(0) - 1)
    def _():
        outs = [pltpu.make_async_copy(v, h.at[0], osem.at[i]) for i, (v, h) in enumerate(((dwg, dwg_hbm), (dwu, dwu_hbm), (dwd, dwd_hbm)))]
        for o in outs: o.start()
        for o in outs: o.wait()

def experts_forward(x_all, w_gate, w_up, w_down, experts, block, capacity, guest, cid, TB=512, SB=256):
    hosted = placed()
    T, C = x_all.shape; D, F = w_gate.shape[1:]
    slots = max(SB // block, 1) * capacity
    total = TB // SB * slots
    S = T // SB * slots
    any_ = pl.BlockSpec(memory_space=pl.ANY)
    V = pltpu.VMEM; bf = jnp.bfloat16; f32 = jnp.float32
    blk = lambda r, c: pl.BlockSpec((r, c), lambda i: (i, 0))
    g = guest.reshape(2, guest.shape[0] // 2, guest.shape[1])
    res = pl.pallas_call(
        functools.partial(forward_kernel, experts, slots, SB, hosted),
        grid=(T // TB,),
        out_shape=([jax.ShapeDtypeStruct((2, 2, 2, NZ) + g.shape, g.dtype)] if hosted else []) + [jax.ShapeDtypeStruct((T, D), bf), jax.ShapeDtypeStruct((S, D), bf), jax.ShapeDtypeStruct((S, F), f32), jax.ShapeDtypeStruct((S, F), f32)],
        in_specs=([pl.BlockSpec(memory_space=pltpu.VMEM)] if hosted else []) + [blk(TB, C), any_, any_, any_],
        out_specs=([any_] if hosted else []) + [blk(TB, D), blk(total, D), blk(total, F), blk(total, F)],
        scratch_shapes=[V((D, F), bf), V((D, F), bf), V((F, D), bf), pltpu.SemaphoreType.DMA((3,))] + (ag_sems(1) if hosted else []),
        compiler_params=pltpu.CompilerParams(dimension_semantics=("arbitrary",), vmem_limit_bytes=65000 * 1024,
            **(dict(collective_id=cid, has_side_effects=True) if hosted else {})),
        cost_estimate=pl.CostEstimate(flops=48_000_000_000, bytes_accessed=130_000_000, transcendentals=0),
        name="experts_forward",
    )(*([g] if hosted else []), x_all, w_gate, w_up, w_down)
    if hosted: return res[1:], res[0].reshape(-1, guest.shape[1])
    return res, lax.all_gather(guest, BOTH, axis=0, tiled=True)

def experts_backward(x_all, cot_a, cot_b, rows, ga, ua, w_gate, w_up, w_down, experts, block, capacity, TB=512, SB=256):
    T, C = x_all.shape; D, F = w_gate.shape[1:]
    slots = max(SB // block, 1) * capacity
    total = TB // SB * slots
    WM = C - D
    any_ = pl.BlockSpec(memory_space=pl.ANY)
    V = pltpu.VMEM; bf = jnp.bfloat16; f32 = jnp.float32
    blk = lambda r, c: pl.BlockSpec((r, c), lambda i: (i, 0))
    meta = pl.BlockSpec((TB, WM), lambda i: (i, D // WM)) if D % WM == 0 else blk(TB, WM)
    meta_in = x_all if D % WM == 0 else x_all[:, D:]
    return pl.pallas_call(
        functools.partial(backward_kernel, experts, slots, SB, block),
        grid=(T // TB,),
        out_shape=[jax.ShapeDtypeStruct((T, C), bf), jax.ShapeDtypeStruct(w_gate.shape, f32), jax.ShapeDtypeStruct(w_up.shape, f32), jax.ShapeDtypeStruct(w_down.shape, f32)],
        in_specs=[meta, blk(cot_a.shape[0] * TB // T, D), blk(cot_b.shape[0] * TB // T, D), blk(total, D), blk(total, F), blk(total, F), any_, any_, any_],
        out_specs=[blk(TB, C), any_, any_, any_],
        scratch_shapes=[V((D, F), bf), V((D, F), bf), V((F, D), bf), V((D, F), f32), V((D, F), f32), V((F, D), f32), V((total, D), bf), pltpu.SemaphoreType.DMA((3,)), pltpu.SemaphoreType.DMA((3,))],
        compiler_params=pltpu.CompilerParams(dimension_semantics=("arbitrary",), vmem_limit_bytes=65000 * 1024),
        cost_estimate=pl.CostEstimate(flops=85_000_000_000, bytes_accessed=150_000_000, transcendentals=0),
        name="experts_backward",
    )(meta_in, cot_a, cot_b, rows, ga, ua, w_gate, w_up, w_down)


def rope_tables(seq_len):
    half = HD // 2
    frequency = theta_base ** (-2.0 * jnp.arange(half, dtype=jnp.float32) / HD)
    angles = jnp.arange(seq_len, dtype=jnp.float32)[:, None] * frequency[None, :]
    return jnp.concatenate([jnp.cos(angles)] * 2, axis=-1), jnp.concatenate([-jnp.sin(angles), jnp.sin(angles)], axis=-1)

def turn(u, cos, sin):
    return u * cos + pltpu.roll(u, HD // 2, 1) * sin

def scale_of(u):
    return lax.rsqrt(jnp.mean(u * u, axis=-1, keepdims=True) + epsilon)

def attention_forward_kernel(group, n_ref, wq_ref, wk_ref, wv_ref, gq_ref, gk_ref, cos_ref, sin_ref, u_ref, ku_ref, ql_ref, kl_ref, vl_ref, mix_ref, k_all):
    bf, f32 = jnp.bfloat16, jnp.float32
    rows, seq = ql_ref.shape[0], kl_ref.shape[0]
    first = lax.axis_index("shard") * rows
    own = pl.ds(first, rows)
    k_all[...] = dot(n_ref[...], wk_ref[...], 1, 0)
    ku_ref[...] = k_all[own, :]
    k = k_all[...]
    kl_ref[...] = turn(k * scale_of(k) * gk_ref[...], cos_ref[...], sin_ref[...]).astype(bf)
    vl_ref[...] = dot(n_ref[...], wv_ref[...], 1, 0).astype(bf)
    u_ref[...] = dot(n_ref[own, :], wq_ref[...], 1, 0)
    cos, sin = cos_ref[own, :], sin_ref[own, :]
    allowed = lax.broadcasted_iota(jnp.int32, (rows, seq), 1) <= first + lax.broadcasted_iota(jnp.int32, (rows, seq), 0)
    for j in range(group):
        cols = slice(j * HD, (j + 1) * HD)
        u = u_ref[:, cols]
        ql = (turn(u * scale_of(u) * gq_ref[...], cos, sin) * HD ** (-0.5)).astype(bf)
        ql_ref[:, cols] = ql
        scores = dot(ql, kl_ref[...], 1, 1)
        raised = jnp.where(allowed, jnp.exp(scores), 0.0)
        probs = (raised * (1.0 / jnp.sum(raised, axis=-1, keepdims=True))).astype(bf)
        mix_ref[:, cols] = dot(probs, vl_ref[...], 1, 0).astype(bf)

def attention_forward(normed_seq, wqkv, rows, gq, gk, cos, sin):
    seq, width = normed_seq.shape
    group = HQ // HK
    bf, f32 = jnp.bfloat16, jnp.float32
    whole = lambda a: pl.BlockSpec(a.shape, lambda i: (0, 0))
    gq, gk = gq[None, :], gk[None, :]
    qb = pl.BlockSpec((rows, group * HD), lambda i: (0, i)); kb = pl.BlockSpec((seq, HD), lambda i: (0, i))
    return pl.pallas_call(
        functools.partial(attention_forward_kernel, group),
        grid=(HK,),
        out_shape=[jax.ShapeDtypeStruct((rows, HQ * HD), f32), jax.ShapeDtypeStruct((rows, HK * HD), f32), jax.ShapeDtypeStruct((rows, HQ * HD), bf),
            jax.ShapeDtypeStruct((seq, HK * HD), bf), jax.ShapeDtypeStruct((seq, HK * HD), bf), jax.ShapeDtypeStruct((rows, HQ * HD), bf)],
        in_specs=[whole(normed_seq), pl.BlockSpec((width, group * HD), lambda i: (0, i)), pl.BlockSpec((width, HD), lambda i: (0, HQ + i)), pl.BlockSpec((width, HD), lambda i: (0, HQ + HK + i)),
            whole(gq), whole(gk), whole(cos), whole(sin)],
        out_specs=[qb, pl.BlockSpec((rows, HD), lambda i: (0, i)), qb, kb, kb, qb],
        scratch_shapes=[pltpu.VMEM((seq, HD), f32)],
        compiler_params=pltpu.CompilerParams(dimension_semantics=("arbitrary",), vmem_limit_bytes=56 << 20),
        cost_estimate=pl.CostEstimate(flops=13_000_000_000, bytes_accessed=45_000_000, transcendentals=8_400_000),
        name="attention_forward",
    )(normed_seq, wqkv, wqkv, wqkv, gq, gk, cos, sin)

def attention_backward_kernel(group, guest, *refs):
    if guest:
        p_ref, u_ref, ql_ref, kl_ref, vl_ref, ga_ref, wo_ref, gq_ref, cos_ref, sin_ref, po_ref, gu_ref, gk_ref, gv_ref, gg_ref, gk_acc, gv_acc = refs[:17]
        runs = line_scatter_steps(LINE_PARTS, p_ref, po_ref, refs[17:])
        slots = HK * group
        at = {i * slots // (LINE_STEPS - 1): run for i, run in enumerate(runs[:-1])}
    else:
        u_ref, ql_ref, kl_ref, vl_ref, ga_ref, wo_ref, gq_ref, cos_ref, sin_ref, gu_ref, gk_ref, gv_ref, gg_ref, gk_acc, gv_acc = refs
        at = {}
    step = pl.program_id(0)
    bf, f32 = jnp.bfloat16, jnp.float32
    gm_all = dot(ga_ref[...], wo_ref[...], 1, 1).astype(bf)
    rows, seq = ql_ref.shape[0], kl_ref.shape[0]
    first = lax.axis_index("shard") * rows
    cos, sin = cos_ref[pl.ds(first, rows), :], sin_ref[pl.ds(first, rows), :]
    allowed = lax.broadcasted_iota(jnp.int32, (rows, seq), 1) <= first + lax.broadcasted_iota(jnp.int32, (rows, seq), 0)
    gain_grad = jnp.zeros((1, HD), f32)
    for j in range(group):
        for i in range(HK):
            if i * group + j in at: pl.when(step == i)(at[i * group + j])
        cols = slice(j * HD, (j + 1) * HD)
        ql, gm = ql_ref[:, cols], gm_all[:, cols]
        raised = jnp.where(allowed, jnp.exp(dot(ql, kl_ref[...], 1, 1)), 0.0)
        probs = raised * (1.0 / jnp.sum(raised, axis=-1, keepdims=True))
        gp = dot(gm, vl_ref[...], 1, 1)
        gs = (probs * (gp - jnp.sum(probs * gp, axis=-1, keepdims=True))).astype(bf)
        gv = dot(probs.astype(bf), gm, 0, 0)
        gk = dot(gs, ql, 0, 0)
        if j == 0:
            gv_acc[...] = gv
            gk_acc[...] = gk
        else:
            gv_acc[...] += gv
            gk_acc[...] += gk
        m = dot(gs, kl_ref[...], 1, 0) * HD ** (-0.5)
        m = m * cos + pltpu.roll(m * sin, HD // 2, 1)
        u = u_ref[:, cols]
        r = scale_of(u)
        gain_grad = gain_grad + jnp.sum(m * u * r, axis=0, keepdims=True)
        mg = m * gq_ref[...]
        gu_ref[:, cols] = (r * mg - u * (r * r * r) * jnp.mean(mg * u, axis=-1, keepdims=True)).astype(bf)
    gk_ref[...] = gk_acc[...].astype(bf)
    gv_ref[...] = gv_acc[...].astype(bf)
    gg_ref[0] = jnp.broadcast_to(gain_grad, (8, HD))
    if guest: pl.when(step == HK - 1)(runs[-1])

def attention_backward(q_proj, q_low, k_low, v_low, grad_attn, w_out, gq, cos, sin, guest, cid):
    rows, seq = q_low.shape[0], k_low.shape[0]
    group = HQ // HK
    bf, f32 = jnp.bfloat16, jnp.float32
    gq = gq[None, :]
    whole = lambda a: pl.BlockSpec(a.shape, lambda i: (0, 0))
    qb = pl.BlockSpec((rows, group * HD), lambda i: (0, i)); kb = pl.BlockSpec((seq, HD), lambda i: (0, i))
    hosted = placed()
    R, C = guest.shape[0] // lax.axis_size("shard"), guest.shape[1]
    shape = (NZ, LINE_PARTS, R // LINE_PARTS, C)
    vm = pl.BlockSpec(memory_space=pltpu.VMEM)
    *summed, grad_q, grad_k, grad_v, gain = pl.pallas_call(
        functools.partial(attention_backward_kernel, group, hosted),
        grid=(HK,),
        out_shape=([jax.ShapeDtypeStruct(shape[1:], f32)] if hosted else []) + [jax.ShapeDtypeStruct(q_low.shape, bf), jax.ShapeDtypeStruct(k_low.shape, bf), jax.ShapeDtypeStruct(k_low.shape, bf), jax.ShapeDtypeStruct((HK, 8, HD), f32)],
        in_specs=([vm] if hosted else []) + [qb, qb, kb, kb, whole(grad_attn), pl.BlockSpec((group * HD, w_out.shape[1]), lambda i: (i, 0)), whole(gq), whole(cos), whole(sin)],
        out_specs=([vm] if hosted else []) + [qb, kb, kb, pl.BlockSpec((1, 8, HD), lambda i: (i, 0, 0))],
        scratch_shapes=[pltpu.VMEM((seq, HD), f32), pltpu.VMEM((seq, HD), f32)] + (line_scatter_scratch(LINE_PARTS, R, C, bf) if hosted else []),
        compiler_params=pltpu.CompilerParams(dimension_semantics=("arbitrary",), vmem_limit_bytes=60 << 20,
            **(dict(collective_id=cid, has_side_effects=True) if hosted else {})),
        cost_estimate=pl.CostEstimate(flops=15_000_000_000, bytes_accessed=20_000_000, transcendentals=8_400_000),
        name="attention_backward",
    )(*([guest.reshape(shape)] if hosted else []), q_proj, q_low, k_low, v_low, grad_attn, w_out, gq, cos, sin)
    if hosted: total = summed[0].reshape(R, C)
    else: total = lax.psum_scatter(guest, "shard", scatter_dimension=0, tiled=True).astype(f32)
    return total, grad_q, jnp.concatenate([grad_k, grad_v], axis=1), jnp.sum(gain[:, 0], axis=0)

HQ = 32
HK = 4
HD = 128
epsilon = 1e-06
theta_base = 1000000.0
BOTH = ("expert", "shard")


def matmul(left, right):
    return jnp.dot(left, right, preferred_element_type=jnp.float32)


def matmul_tn(left, right):
    return lax.dot_general(
        left, right, (((0,), (0,)), ((), ())), preferred_element_type=jnp.float32
    )


def matmul_nt(left, right):
    return lax.dot_general(
        left, right, (((1,), (1,)), ((), ())), preferred_element_type=jnp.float32
    )


def norm_rows(values, gain_vec):
    return (
        values * lax.rsqrt(jnp.mean(values * values, axis=-1, keepdims=True) + epsilon) * gain_vec
    )


def norm_back(values, gain_vec, upstream):
    scaling = lax.rsqrt(jnp.mean(values * values, axis=-1, keepdims=True) + epsilon)
    gain_grad = jnp.sum(upstream * values * scaling, axis=0)
    weighted = upstream * gain_vec
    inner_sum = jnp.mean(weighted * values, axis=-1, keepdims=True)
    return (scaling * weighted - values * (scaling * scaling * scaling) * inner_sum, gain_grad)


def rotary(values, positions):
    head_width = values.shape[-1]
    half_width = head_width // 2
    frequency = theta_base ** (-2.0 * jnp.arange(half_width, dtype=jnp.float32) / head_width)
    angles = positions.astype(jnp.float32)[:, None] * frequency[None, :]
    cosine = jnp.concatenate([jnp.cos(angles), jnp.cos(angles)], axis=-1)[:, None, :]
    sine_part = jnp.concatenate([jnp.sin(angles), jnp.sin(angles)], axis=-1)[:, None, :]
    turned = jnp.concatenate([-values[..., half_width:], values[..., :half_width]], axis=-1)
    return values * cosine + turned * sine_part


def head_prep(projected, gain_vec, positions, head_count, factor):
    shaped = projected.reshape(projected.shape[0], head_count, projected.shape[1] // head_count)
    return rotary(norm_rows(shaped, gain_vec), positions) * factor


def gather_all(arrays, cid, line=()):
    if placed():
        return [o.reshape(-1, o.shape[-1]) for o in ag32(arrays, cid, line)]
    return [lax.all_gather(a, BOTH, axis=0, tiled=True) for a in arrays] + [
        lax.all_gather(a, "shard", axis=0, tiled=True) for a in line
    ]


def scatter_all(arrays, cid, out_dtype=jnp.float32, line=()):
    if placed():
        return rs32(
            [a.reshape(32, -1, a.shape[-1]) for a in arrays], cid, out_dtype, line=[a.reshape(NZ, -1, a.shape[-1]) for a in line]
        )
    return [lax.psum_scatter(a, BOTH, scatter_dimension=0, tiled=True).astype(out_dtype) for a in arrays] + [
        lax.psum_scatter(a, "shard", scatter_dimension=0, tiled=True).astype(out_dtype) for a in line
    ]


def per_device(
    hidden_in,
    g_attn,
    w_query,
    w_key,
    w_value,
    g_query,
    g_key,
    w_out,
    g_ffn,
    w_router,
    w_gate,
    w_up,
    w_down,
    routes,
    cotangent,
):
    bf, f32 = jnp.bfloat16, jnp.float32
    tok_rows, model_width = hidden_in.shape
    top_count = routes.shape[1]
    devices = lax.axis_size(BOTH)
    expert_count = devices * w_gate.shape[0]
    capacity = 2 * tok_rows * top_count // expert_count
    shard_count = lax.axis_size("shard")
    shard_pos = lax.axis_index("shard")
    seq_len = tok_rows * shard_count
    q_cols, kv_cols = HQ * HD, HK * HD

    pieces = [w_router.reshape(-1), g_attn, g_ffn, g_query, g_key]
    sizes = [p.shape[0] for p in pieces]
    used = sum(sizes)
    small_rows = -(-used // (64 * 128)) * 64
    small = jnp.concatenate(pieces + [jnp.zeros((small_rows * 128 - used,), bf)]).reshape(small_rows, 128)
    wqkv = jnp.concatenate([w_query, w_key, w_value], axis=1)
    wqkv_full, small_all, wo_full, hidden_seq = gather_all([wqkv, small, w_out], 1, [hidden_in])
    small_all = small_all.reshape(devices, small_rows * 128)
    starts = [sum(sizes[:i]) for i in range(5)]
    wr_full, attn_gain, ffn_gain, query_gain, key_gain = [small_all[:, o : o + n].reshape(-1) for o, n in zip(starts, sizes)]
    wr_full = wr_full.reshape(model_width, expert_count)
    attn_gain, ffn_gain, query_gain, key_gain = [g.astype(f32) for g in (attn_gain, ffn_gain, query_gain, key_gain)]
    first = tok_rows // 2
    cot_first, wo_full = lax.optimization_barrier((cotangent[:first], wo_full))
    cot_a = lax.all_gather(cot_first, BOTH, axis=0, tiled=True)

    inputs_f = hidden_in.astype(f32)
    normed_low = norm_rows(inputs_f, attn_gain).astype(bf)
    normed_seq = norm_rows(hidden_seq.astype(f32), attn_gain).astype(bf)
    cosine, sine = rope_tables(seq_len)
    q_proj, k_proj, q_low, k_low, v_low, mix_low = attention_forward(
        normed_seq, wqkv_full, tok_rows, query_gain, key_gain, cosine, sine
    )
    residual = inputs_f + matmul(mix_low, wo_full)
    ffn_low = norm_rows(residual, ffn_gain).astype(bf)

    logits = matmul(ffn_low, wr_full)
    expert_ids = jnp.arange(expert_count, dtype=jnp.int32)
    chosen = jnp.any(routes[:, :, None] == expert_ids[None, None, :], axis=1)
    raised_gate = jnp.where(chosen, jnp.exp(logits), 0.0)
    gates = raised_gate / jnp.sum(raised_gate, axis=-1, keepdims=True)
    gate_high = lax.reduce_precision(gates, 8, 7)
    gate_low = gates - gate_high
    extra = -(-3 * expert_count // 128) * 128
    payload = jnp.concatenate(
        [
            ffn_low,
            chosen.astype(bf),
            gate_high.astype(bf),
            gate_low.astype(bf),
            jnp.zeros((tok_rows, extra - 3 * expert_count), bf),
        ],
        axis=1,
    )
    (payload_all,) = gather_all([payload], 3)
    (out_part, rows, gate_act, up_act), cot_b = experts_forward(
        payload_all, w_gate, w_up, w_down, expert_count, tok_rows, capacity, cotangent[first:], 2
    )
    moe_out = lax.psum_scatter(out_part, "expert", scatter_dimension=0, tiled=True)
    grad_part, grad_wgate, grad_wup, grad_wdown = experts_backward(
        payload_all, cot_a, cot_b, rows, gate_act, up_act, w_gate, w_up, w_down, expert_count, tok_rows, capacity
    )
    (grad_sum,) = scatter_all([grad_part], 4)
    grad_sum, moe_out = lax.optimization_barrier((grad_sum, moe_out))
    upstream = cotangent.astype(f32)
    grad_ffn = grad_sum[:, :model_width]
    grad_shares = (
        grad_sum[:, model_width : model_width + expert_count]
        + grad_sum[:, model_width + expert_count : model_width + 2 * expert_count]
    )
    grad_logits = (grad_shares - gates * jnp.sum(grad_shares, axis=-1, keepdims=True)).astype(bf)
    grad_wrouter = matmul_tn(ffn_low, grad_logits)
    grad_ffn = grad_ffn + matmul_nt(grad_logits, wr_full)
    grad_second, grad_ffn_gain = norm_back(residual, ffn_gain, grad_ffn)
    grad_residual = upstream + grad_second
    grad_attn_low = grad_residual.astype(bf)
    grad_wout = matmul_tn(mix_low, grad_attn_low).astype(bf)
    grad_attn_low, grad_wout = lax.optimization_barrier((grad_attn_low, grad_wout))
    out_grad = lax.psum_scatter(grad_wout, "expert", scatter_dimension=0, tiled=True)

    moe_parts = moe_out.reshape(shard_count, 2, tok_rows // 2, model_width)
    moe_a, moe_b = [moe_parts[:, i].reshape(-1, model_width) for i in range(2)]
    moe_a, grad_q_low, grad_kv, grad_query_gain = attention_backward(
        q_proj, q_low, k_low, v_low, grad_attn_low, wo_full, query_gain, cosine, sine, moe_a, 5
    )
    grad_wq = matmul_tn(normed_low, grad_q_low).astype(bf)
    q_grad, grad_kv = scatter_all([grad_wq], 7, line=[grad_kv])
    q_grad, out_grad = lax.optimization_barrier((q_grad, out_grad))
    out_grad = lax.psum_scatter(out_grad, "shard", scatter_dimension=0, tiled=True).astype(f32)
    own_rows = shard_pos * tok_rows
    positions = own_rows + jnp.arange(tok_rows, dtype=jnp.int32)
    _, k_pull = jax.vjp(
        lambda projected, gain_vec: head_prep(projected, gain_vec, positions, HK, 1.0), k_proj, key_gain
    )
    grad_k_proj, grad_key_gain = k_pull(grad_kv[:, :kv_cols].reshape(tok_rows, HK, HD))
    grad_kv_low = jnp.concatenate([grad_k_proj.astype(bf), grad_kv[:, kv_cols:].astype(bf)], axis=1)
    grad_wkv = matmul_tn(normed_low, grad_kv_low).astype(bf)
    grad_qkv_low = jnp.concatenate([grad_q_low, grad_kv_low], axis=1)
    grad_normed = matmul_nt(grad_qkv_low, wqkv_full)
    grad_front, grad_attn_gain = norm_back(inputs_f, attn_gain, grad_normed)
    grad_input = (grad_residual + grad_front).astype(bf)

    grads = [grad_wrouter, grad_attn_gain, grad_ffn_gain, grad_query_gain, grad_key_gain]
    packed = jnp.concatenate(
        [g.astype(bf).reshape(devices, -1) for g in grads] + [jnp.zeros((devices, small_rows * 128 - used), bf)], axis=1
    ).reshape(devices * small_rows, 128)
    kv_grad, small_grad, moe_b = scatter_all([grad_wkv, packed], 8, line=[moe_b])
    block_out = (residual + jnp.concatenate([moe_a, moe_b], axis=0)).astype(bf)
    small_grad = small_grad.reshape(-1)
    router_g, attn_g, ffn_g, query_g, key_g = [small_grad[o : o + n] for o, n in zip(starts, sizes)]
    return (
        block_out,
        grad_input,
        attn_g,
        q_grad,
        kv_grad[:, :kv_cols],
        kv_grad[:, kv_cols:],
        query_g,
        key_g,
        out_grad,
        ffn_g,
        router_g.reshape(w_router.shape),
        grad_wgate,
        grad_wup,
        grad_wdown,
    )


def solution(mesh):
    row = P(BOTH, None)
    vec = P(BOTH)
    cube = P(BOTH, None, None)
    in_specs = (row, vec, row, row, row, vec, vec, row, vec, row, cube, cube, cube, row, row)
    out_specs = (row, row, vec, row, row, row, vec, vec, row, vec, row, cube, cube, cube)
    return jax.shard_map(
        per_device, mesh=mesh, in_specs=in_specs, out_specs=out_specs, check_vma=False
    )
```

```python
import functools

import jax
import jax.numpy as jnp
from jax import lax
from jax.experimental import pallas as pl
from jax.experimental.pallas import tpu as pltpu
from jax.sharding import PartitionSpec as P

MESH = pl.DeviceIdType.MESH
NZ = 4

def placed():
    return lax.axis_size("expert") == 8 and lax.axis_size("shard") == NZ

def place():
    e = lax.axis_index("expert"); s = lax.axis_index("shard")
    return e // 4, lax.rem(e // 2, 2), lax.rem(e, 2), s

def dev(y, x, c, s):
    return (y * 4 + x * 2 + c, s)

def barrier_all(y, x, c, s):
    bar = pltpu.get_barrier_semaphore()
    def sig(d): pl.semaphore_signal(bar, inc=1, device_id=d, device_id_type=MESH)
    sig(dev(1 - y, x, c, s)); sig(dev(y, 1 - x, c, s)); sig(dev(y, x, 1 - c, s))
    @pl.when(s > 0)
    def _(): sig(dev(y, x, c, s - 1))
    @pl.when(s < NZ - 1)
    def _(): sig(dev(y, x, c, s + 1))
    pl.semaphore_wait(bar, 3 + jnp.where(s > 0, 1, 0) + jnp.where(s < NZ - 1, 1, 0))

def ag_kernel(n_arr, n_line, *refs):
    n_all = n_arr + n_line
    for run in ag_steps(n_arr, n_line, refs[:n_all], refs[n_all:2 * n_all], refs[2 * n_all:]): run()

def ag_steps(n_arr, n_line, ins, outs, sems, stages=False):
    n_all = n_arr + n_line
    loc_sem, zs, zr, ps, pr, cs, cr = sems
    y, x, c, s = place()
    def rc(src, dst, ss, rs, d):
        return pltpu.make_async_remote_copy(src_ref=src, dst_ref=dst, send_sem=ss, recv_sem=rs, device_id=d, device_id_type=MESH)
    X = dev(y, 1 - x, c, s); Y = dev(1 - y, x, c, s); C = dev(y, x, 1 - c, s)
    A = range(n_arr)
    every = range(n_all)
    def home(a, zz):
        return outs[a].at[y, x, c, zz] if a < n_arr else outs[a].at[zz]
    steps = [(0, 0)] + [(d, g) for d in range(1, NZ) for g in (1, -1)]
    def valid(d, g):
        return (s >= d) if g == 1 else (s + d <= NZ - 1)
    def zof(d, g): return s - d * g
    def src_own(a, h, zz, k):
        return ins[a].at[h] if k == 0 else home(a, zz).at[h]
    def zcopy(a, h, zz, k, g):
        kk = 1 + 2 * (k_dist(k)) + (0 if g == 1 else 1)
        return rc(src_own(a, h, zz, k), home(a, zz).at[h], zs.at[a, h, kk], zr.at[a, h, kk], dev(y, x, c, s + g))
    def k_dist(k): return steps[k][0]
    def plane(a, h, zz, k, which):
        return rc(src_own(a, h, zz, k), outs[a].at[y, x, c, zz, h], ps.at[a, k, h, which], pr.at[a, k, h, which], X if which == 0 else Y)
    def plane_recv(a, h, zz, k, which):
        d = outs[a].at[y, 1 - x, c, zz, h] if which == 0 else outs[a].at[1 - y, x, c, zz, h]
        return rc(d, d, ps.at[a, k, h, which], pr.at[a, k, h, which], X if which == 0 else Y)
    def diag(a, h, zz, k):
        d = outs[a].at[y, 1 - x, c, zz, h] if h == 0 else outs[a].at[1 - y, x, c, zz, h]
        return rc(d, d, ps.at[a, k, h, 2], pr.at[a, k, h, 2], Y if h == 0 else X)
    def diag_recv(a, h, zz, k):
        d = outs[a].at[1 - y, 1 - x, c, zz, h]
        return rc(d, d, ps.at[a, k, h, 2], pr.at[a, k, h, 2], Y if h == 0 else X)
    def core(a, zz, k, part):
        d = outs[a].at[:, :, c, zz]
        return rc(d, d, cs.at[a, k], cr.at[a, k], C)
    def core_recv(a, zz, k):
        d = outs[a].at[:, :, 1 - c, zz]
        return rc(d, d, cs.at[a, k], cr.at[a, k], C)
    def loc(a):
        return pltpu.make_async_copy(ins[a], home(a, s), loc_sem.at[a])

    def when(k, f):
        d, g = steps[k]
        if k == 0: f()
        else: pl.when(valid(d, g))(f)

    def stage_a(k):
        d, g = steps[k]
        def go():
            zz = zof(d, g)
            for a in every:
                for h in range(2):
                    if k:
                        kk = k
                        dref = home(a, zz).at[h]
                        rc(dref, dref, zs.at[a, h, kk], zr.at[a, h, kk], X).wait_recv()
                    for gg in ((1, -1) if k == 0 else (g,)):
                        okc = (s < NZ - 1) if gg == 1 else (s > 0)
                        if d + 1 < NZ:
                            @pl.when(okc)
                            def _(): zcopy(a, h, zz, k, gg).start()
                    if a < n_arr:
                        plane(a, h, zz, k, 0).start()
                        plane(a, h, zz, k, 1).start()
        when(k, go)
    def stage_b(k):
        d, g = steps[k]
        def go():
            zz = zof(d, g)
            for a in A:
                plane_recv(a, 0, zz, k, 0).wait_recv()
                diag(a, 0, zz, k).start()
                plane_recv(a, 1, zz, k, 1).wait_recv()
                diag(a, 1, zz, k).start()
        when(k, go)
    def stage_c(k):
        d, g = steps[k]
        def go():
            zz = zof(d, g)
            for a in A:
                if k == 0: loc(a).wait()
                plane_recv(a, 1, zz, k, 0).wait_recv()
                plane_recv(a, 0, zz, k, 1).wait_recv()
                diag_recv(a, 0, zz, k).wait_recv()
                diag_recv(a, 1, zz, k).wait_recv()
                core(a, zz, k, 0).start()
        when(k, go)
    n = len(steps)
    def start():
        barrier_all(y, x, c, s)
        for a in every: loc(a).start()
        stage_a(0)
    def advance(i):
        if 0 < i < n: stage_a(i)
        if 0 <= i - 1 < n: stage_b(i - 1)
        if 0 <= i - 2 < n: stage_c(i - 2)
    def finish():
        for k in range(n):
            d, g = steps[k]
            def go():
                zz = zof(d, g)
                for a in every:
                    if a < n_arr:
                        core_recv(a, zz, k).wait_recv()
                        core(a, zz, k, 0).wait_send()
                    elif k == 0: loc(a).wait()
                    for h in range(2):
                        for gg in ((1, -1) if k == 0 else (g,)):
                            okc = (s < NZ - 1) if gg == 1 else (s > 0)
                            if d + 1 < NZ:
                                @pl.when(okc)
                                def _(): zcopy(a, h, zz, k, gg).wait_send()
                        if a < n_arr:
                            plane(a, h, zz, k, 0).wait_send()
                            plane(a, h, zz, k, 1).wait_send()
                            diag(a, h, zz, k).wait_send()
            when(k, go)
    if stages: return start, stage_a, stage_b, stage_c, finish
    return [start] + [functools.partial(advance, i) for i in range(1, n + 2)] + [finish]

def ag_sems(n, m=0):
    D = pltpu.SemaphoreType.DMA
    return [D((n + m,)), D((n + m, 2, 9)), D((n + m, 2, 9)), D((n, 7, 2, 3)), D((n, 7, 2, 3)), D((n, 7)), D((n, 7))]

def ag32(arrs, cid, line=()):
    ins = [a.reshape(2, a.shape[0] // 2, a.shape[1]) for a in list(arrs) + list(line)]
    n, m = len(arrs), len(line)
    outs = pl.pallas_call(
        functools.partial(ag_kernel, n, m),
        out_shape=[jax.ShapeDtypeStruct(((2, 2, 2, NZ) if i < n else (NZ,)) + a.shape, a.dtype) for i, a in enumerate(ins)],
        in_specs=[pl.BlockSpec(memory_space=pltpu.VMEM)] * (n + m),
        out_specs=[pl.BlockSpec(memory_space=pl.ANY)] * (n + m),
        scratch_shapes=ag_sems(n, m),
        compiler_params=pltpu.CompilerParams(collective_id=cid, has_side_effects=True, vmem_limit_bytes=64000 * 1024),
        name="gather_all",
    )(*ins)
    return [o.reshape(-1, a.shape[1] * 2, a.shape[2]) for o, a in zip(outs, ins)]

ZORDER = (0, 3, 1, 2)
LAGS = (1, 1, 1, 1)

def rs_kernel(n_arr, n_line, parts, *refs):
    n_all = n_arr + n_line
    ins = refs[:n_all]; outs = refs[n_all:2 * n_all]
    sc = list(refs[2 * n_all:])
    own_b = [sc.pop(0) for _ in range(n_all)]; zu_b = [sc.pop(0) for _ in range(n_all)]; zd_b = [sc.pop(0) for _ in range(n_all)]
    r0_b, ra_b, rb_b = [[sc.pop(0) for _ in range(n_arr)] for _ in range(3)]
    lsem, s0s, s0r, sas, sar, sbs, sbr, zus, zur, zds, zdr = sc
    y, x, c, s = place()
    barrier_all(y, x, c, s)
    X = dev(y, 1 - x, c, s); Y = dev(1 - y, x, c, s); C = dev(y, x, 1 - c, s)
    UP = dev(y, x, c, s + 1); DN = dev(y, x, c, s - 1)
    def rc(src, dst, ss, rs, d):
        return pltpu.make_async_remote_copy(src_ref=src, dst_ref=dst, send_sem=ss, recv_sem=rs, device_id=d, device_id_type=MESH)
    units = [(a, zz, h) for zz in ZORDER for h in range(parts) for a in range(n_arr)]
    lines = [(a, zz, h) for zz in ZORDER for h in range(parts) for a in range(n_arr, n_all)]
    def jj(zz, h): return ZORDER.index(zz) * parts + h
    def load(a, zz, h):
        j = jj(zz, h)
        src = ins[a].at[:, :, c, zz, h] if a < n_arr else ins[a].at[zz, h]
        return pltpu.make_async_copy(src, own_b[a].at[j], lsem.at[a, j])
    def mine(a, j):
        return own_b[a].at[j, y, x] if a < n_arr else own_b[a].at[j]
    def c0(a, zz, h):
        j = jj(zz, h)
        return rc(ins[a].at[:, :, 1 - c, zz, h], r0_b[a].at[j], s0s.at[a, j], s0r.at[a, j], C)
    def ca(a, zz, h):
        j = jj(zz, h)
        if h % 2 == 0: return rc(own_b[a].at[j, :, 1 - x], ra_b[a].at[j], sas.at[a, j], sar.at[a, j], X)
        return rc(own_b[a].at[j, 1 - y], ra_b[a].at[j], sas.at[a, j], sar.at[a, j], Y)
    def cb(a, zz, h):
        j = jj(zz, h)
        if h % 2 == 0: return rc(own_b[a].at[j, 1 - y, x], rb_b[a].at[j], sbs.at[a, j], sbr.at[a, j], Y)
        return rc(own_b[a].at[j, y, 1 - x], rb_b[a].at[j], sbs.at[a, j], sbr.at[a, j], X)
    def cu(a, zz, h):
        j = jj(zz, h)
        return rc(mine(a, j), zu_b[a].at[j], zus.at[a, j], zur.at[a, j], UP)
    def cd(a, zz, h):
        j = jj(zz, h)
        return rc(mine(a, j), zd_b[a].at[j], zds.at[a, j], zdr.at[a, j], DN)
    def add_into(dst, other):
        rows = dst.shape[0]
        st = 16 if rows % 16 == 0 else rows
        @pl.loop(0, rows // st)
        def _(i):
            r = pl.ds(i * st, st)
            dst[r, :] = (dst[r, :].astype(jnp.float32) + other[r, :].astype(jnp.float32)).astype(dst.dtype)
    def stage0(u):
        a, zz, h = u; j = jj(zz, h)
        load(a, zz, h).wait()
        c0(a, zz, h).wait_recv()
        for yy in range(2):
            for xx in range(2):
                add_into(own_b[a].at[j, yy, xx], r0_b[a].at[j, yy, xx])
        ca(a, zz, h).start()
    def stage1(u):
        a, zz, h = u; j = jj(zz, h)
        ca(a, zz, h).wait_recv()
        for q in range(2):
            if h % 2 == 0: add_into(own_b[a].at[j, q, x], ra_b[a].at[j, q])
            else: add_into(own_b[a].at[j, y, q], ra_b[a].at[j, q])
        cb(a, zz, h).start()
    def stage2(u):
        a, zz, h = u; j = jj(zz, h)
        cb(a, zz, h).wait_recv()
        add_into(own_b[a].at[j, y, x], rb_b[a].at[j])
    def hop(u, k):
        a, zz, h = u; j = jj(zz, h)
        if k < zz:
            @pl.when(s == k)
            def _():
                if k > 0:
                    cu(a, zz, h).wait_recv()
                    add_into(mine(a, j), zu_b[a].at[j])
                cu(a, zz, h).start()
        t = NZ - 1 - k
        if t > zz:
            @pl.when(s == t)
            def _():
                if k > 0:
                    cd(a, zz, h).wait_recv()
                    add_into(mine(a, j), zd_b[a].at[j])
                cd(a, zz, h).start()
    def last(u):
        a, zz, h = u; j = jj(zz, h)
        @pl.when(s == zz)
        def _():
            if zz > 0: cu(a, zz, h).wait_recv()
            if zz < NZ - 1: cd(a, zz, h).wait_recv()
            t = mine(a, j)[...].astype(jnp.float32)
            if zz > 0: t = t + zu_b[a][j].astype(jnp.float32)
            if zz < NZ - 1: t = t + zd_b[a][j].astype(jnp.float32)
            outs[a][h] = t.astype(outs[a].dtype)
    for u in lines: load(*u).start()
    for u in units:
        c0(*u).start(); load(*u).start()
    n = len(units); nl = len(lines)
    per = max(1, -(-nl // n))
    L1 = LAGS[0] * n_arr; L2 = L1 + LAGS[1] * n_arr; L3 = L2 + LAGS[2] * n_arr; dl = LAGS[3] * n_arr
    for i in range(n + L3 + (NZ - 1) * dl):
        if i < n: stage0(units[i])
        if 0 <= i - L1 < n: stage1(units[i - L1])
        if 0 <= i - L2 < n: stage2(units[i - L2])
        for k in range(NZ - 1):
            for q in range(per * (i - k), per * (i - k) + per):
                if 0 <= q < nl:
                    if k == 0: load(*lines[q]).wait()
                    hop(lines[q], k)
        for k in range(NZ - 1):
            if 0 <= i - L3 - k * dl < n: hop(units[i - L3 - k * dl], k)
    for u in lines + units: last(u)
    for u in lines + units:
        a, zz, h = u
        if a < n_arr:
            c0(*u).wait_send(); ca(*u).wait_send(); cb(*u).wait_send()
        if zz > 0:
            @pl.when(s < zz)
            def _(): cu(*u).wait_send()
        if zz < NZ - 1:
            @pl.when(s > zz)
            def _(): cd(*u).wait_send()

def rs32(arrs, cid, out_dtype=jnp.float32, parts=4, line=()):
    n, nl = len(arrs), len(line)
    both = list(arrs) + list(line)
    if any(a.shape[1] % (parts * 16) for a in both): parts = 2
    ins = [a.reshape(((2, 2, 2) if i < n else ()) + (NZ, parts, a.shape[1] // parts, a.shape[2])) for i, a in enumerate(both)]
    hs = [i.shape[-2:] for i in ins]
    V = pltpu.VMEM; bt = jnp.bfloat16; m = NZ * parts
    sems = [pltpu.SemaphoreType.DMA((n + nl, m))] * 11
    outs = pl.pallas_call(
        functools.partial(rs_kernel, n, nl, parts),
        out_shape=[jax.ShapeDtypeStruct((parts,) + h, out_dtype) for h in hs],
        in_specs=[pl.BlockSpec(memory_space=pl.ANY)] * (n + nl),
        out_specs=[pl.BlockSpec(memory_space=pltpu.VMEM)] * (n + nl),
        scratch_shapes=[V((m,) + ((2, 2) if i < n else ()) + h, bt) for i, h in enumerate(hs)] + [V((m,) + h, bt) for h in hs] + [V((m,) + h, bt) for h in hs]
            + [V((m, 2, 2) + h, bt) for h in hs[:n]] + [V((m, 2) + h, bt) for h in hs[:n]] + [V((m,) + h, bt) for h in hs[:n]] + sems,
        compiler_params=pltpu.CompilerParams(collective_id=cid, has_side_effects=True, vmem_limit_bytes=64000 * 1024),
        name="scatter_all",
    )(*ins)
    return [o.reshape(a.shape[1], a.shape[2]) for o, a in zip(outs, both)]

def line_barrier(y, x, c, s):
    bar = pltpu.get_barrier_semaphore()
    @pl.when(s > 0)
    def _(): pl.semaphore_signal(bar, inc=1, device_id=dev(y, x, c, s - 1), device_id_type=MESH)
    @pl.when(s < NZ - 1)
    def _(): pl.semaphore_signal(bar, inc=1, device_id=dev(y, x, c, s + 1), device_id_type=MESH)
    pl.semaphore_wait(bar, jnp.where(s > 0, 1, 0) + jnp.where(s < NZ - 1, 1, 0))

def line_gather_kernel(parts, x_ref, o_ref, ss, rs):
    y, x, c, s = place()
    line_barrier(y, x, c, s)
    def cp(d, g, h):
        src = x_ref.at[h] if d == 0 else o_ref.at[s - d * g, h]
        k = 0 if g == 1 else 1
        return pltpu.make_async_remote_copy(src_ref=src, dst_ref=o_ref.at[s - d * g, h], send_sem=ss.at[k, d, h], recv_sem=rs.at[k, d, h],
            device_id=dev(y, x, c, s + g), device_id_type=MESH)
    def arrived(d, g, h):
        k = 0 if g == 1 else 1
        ref = o_ref.at[s - (d + 1) * g, h]
        return pltpu.make_async_remote_copy(src_ref=ref, dst_ref=ref, send_sem=ss.at[k, d, h], recv_sem=rs.at[k, d, h],
            device_id=dev(y, x, c, s + g), device_id_type=MESH)
    def sends(d, g): return (s >= d) & (s < NZ - 1) if g == 1 else (s + d <= NZ - 1) & (s > 0)
    def gets(d, g): return s >= d + 1 if g == 1 else s + d + 1 <= NZ - 1
    for d in range(NZ):
        for h in range(parts):
            for g in (1, -1):
                if d:
                    @pl.when(gets(d - 1, g))
                    def _(): arrived(d - 1, g, h).wait_recv()
                if d < NZ - 1:
                    @pl.when(sends(d, g))
                    def _(): cp(d, g, h).start()
        if d == 0: o_ref[s] = x_ref[...]
    for d in range(NZ - 1):
        for h in range(parts):
            for g in (1, -1):
                @pl.when(sends(d, g))
                def _(): cp(d, g, h).wait_send()

def line_gather(x, cid, parts=4):
    if not placed():
        return lax.all_gather(x, "shard", axis=0, tiled=True)
    R, C = x.shape
    sem = pltpu.SemaphoreType.DMA((2, NZ, parts))
    o = pl.pallas_call(functools.partial(line_gather_kernel, parts), out_shape=jax.ShapeDtypeStruct((NZ, parts, R // parts, C), x.dtype),
        in_specs=[pl.BlockSpec(memory_space=pltpu.VMEM)], out_specs=pl.BlockSpec(memory_space=pltpu.VMEM),
        scratch_shapes=[sem, sem], compiler_params=pltpu.CompilerParams(collective_id=cid, has_side_effects=True, vmem_limit_bytes=16 << 20),
        name="line_gather")(x.reshape(parts, R // parts, C))
    return o.reshape(NZ * R, C)

def line_scatter_kernel(parts, p_ref, o_ref, *scratch):
    for run in line_scatter_steps(parts, p_ref, o_ref, scratch): run()

LINE_PARTS = 4
LINE_STEPS = 3 * LINE_PARTS + NZ + 1

def line_scatter_steps(parts, p_ref, o_ref, scratch):
    acc, zu, zd, ss_u, rs_u, ss_d, rs_d = scratch
    y, x, c, s = place()
    def rc(src, dst, a, b, d):
        return pltpu.make_async_remote_copy(src_ref=src, dst_ref=dst, send_sem=a, recv_sem=b, device_id=d, device_id_type=MESH)
    def cu(zz, h, k):
        src = p_ref.at[zz, h] if k == 0 else acc.at[zz, h]
        return rc(src, zu.at[zz, h], ss_u.at[zz, h], rs_u.at[zz, h], dev(y, x, c, s + 1))
    def cd(zz, h, k):
        src = p_ref.at[zz, h] if k == 0 else acc.at[zz, h]
        return rc(src, zd.at[zz, h], ss_d.at[zz, h], rs_d.at[zz, h], dev(y, x, c, s - 1))
    st = 32
    def total(dst, refs):
        @pl.loop(0, dst.shape[0] // st)
        def _(i):
            r = pl.ds(i * st, st)
            t = refs[0][r, :].astype(jnp.float32)
            for f in refs[1:]: t = t + f[r, :].astype(jnp.float32)
            dst[r, :] = t.astype(dst.dtype)
    ups = [(zz, h) for zz in (3, 2, 1) for h in range(parts)]
    dns = [(zz, h) for zz in (0, 1, 2) for h in range(parts)]
    n = len(ups)
    def advance(i):
        if i == 0: line_barrier(y, x, c, s)
        for k in range(NZ - 1):
            if 0 <= i - k < n:
                zz, h = ups[i - k]
                if k < zz:
                    @pl.when(s == k)
                    def _():
                        if k:
                            cu(zz, h, k).wait_recv()
                            total(acc.at[zz, h], [p_ref.at[zz, h], zu.at[zz, h]])
                        cu(zz, h, k).start()
                zz, h = dns[i - k]
                if NZ - 1 - k > zz:
                    @pl.when(s == NZ - 1 - k)
                    def _():
                        if k:
                            cd(zz, h, k).wait_recv()
                            total(acc.at[zz, h], [p_ref.at[zz, h], zd.at[zz, h]])
                        cd(zz, h, k).start()
    def finish():
        for zz in range(NZ):
            @pl.when(s == zz)
            def _():
                for h in range(parts):
                    refs = [p_ref.at[zz, h]]
                    if zz > 0:
                        cu(zz, h, 1).wait_recv()
                        refs.append(zu.at[zz, h])
                    if zz < NZ - 1:
                        cd(zz, h, 1).wait_recv()
                        refs.append(zd.at[zz, h])
                    total(o_ref.at[h], refs)
        for zz, h in ups:
            @pl.when(s < zz)
            def _(): cu(zz, h, 1).wait_send()
        for zz, h in dns:
            @pl.when(s > zz)
            def _(): cd(zz, h, 1).wait_send()
    return [functools.partial(advance, i) for i in range(n + NZ)] + [finish]

def line_scatter_scratch(parts, rows, cols, dtype):
    sem = pltpu.SemaphoreType.DMA((NZ, parts))
    buf = pltpu.VMEM((NZ, parts, rows // parts, cols), dtype)
    return [buf, buf, buf, sem, sem, sem, sem]

def line_scatter(p, cid, parts=LINE_PARTS):
    if not placed():
        return lax.psum_scatter(p, "shard", scatter_dimension=0, tiled=True).astype(jnp.float32)
    R, C = p.shape[0] // NZ, p.shape[1]
    shape = (NZ, parts, R // parts, C)
    o = pl.pallas_call(functools.partial(line_scatter_kernel, parts), out_shape=jax.ShapeDtypeStruct(shape[1:], jnp.float32),
        in_specs=[pl.BlockSpec(memory_space=pltpu.VMEM)], out_specs=pl.BlockSpec(memory_space=pltpu.VMEM),
        scratch_shapes=line_scatter_scratch(parts, R, C, p.dtype), compiler_params=pltpu.CompilerParams(collective_id=cid, has_side_effects=True, vmem_limit_bytes=24 << 20),
        name="line_scatter")(p.reshape(shape))
    return o.reshape(R, C)


def dot(a, b, ca, cb):
    return lax.dot_general(a, b, (((ca,), (cb,)), ((), ())), preferred_element_type=jnp.float32)

def token_picks(meta, experts, slots, me):
    SB, WM = meta.shape
    bf, f32 = jnp.bfloat16, jnp.float32
    tri = (lax.broadcasted_iota(jnp.int32, (SB, SB), 1) < lax.broadcasted_iota(jnp.int32, (SB, SB), 0)).astype(bf)
    lane = lax.broadcasted_iota(jnp.int32, (SB, WM), 1)
    cnt = dot(tri, meta, 1, 0)
    metaf = meta.astype(f32)
    msk = jnp.sum(jnp.where(lane == me, metaf, 0.0), axis=-1, keepdims=True)
    pos = jnp.sum(jnp.where(lane == me, cnt, 0.0), axis=-1, keepdims=True)
    gate = jnp.sum(jnp.where((lane == me + experts) | (lane == me + 2 * experts), metaf, 0.0), axis=-1, keepdims=True)
    want = jnp.where(msk > 0.0, pos, -1.0).astype(jnp.int32)
    pick = (want == lax.broadcasted_iota(jnp.int32, (SB, slots), 1)).astype(bf)
    return pick, gate

def forward_kernel(experts, slots, SB, guest, *refs):
    if guest:
        cot_ref, x_ref, wg_hbm, wu_hbm, wd_hbm, cot_all, out_ref, rows_ref, ga_ref, ua_ref, wg, wu, wd, wsem = refs[:14]
    else:
        x_ref, wg_hbm, wu_hbm, wd_hbm, out_ref, rows_ref, ga_ref, ua_ref, wg, wu, wd, wsem = refs
    bf = jnp.bfloat16
    step = pl.program_id(0)
    if guest:
        start, stage_a, stage_b, stage_c, finish = ag_steps(1, 0, [cot_ref], [cot_all], refs[14:], True)
        pl.when(step == 0)(start)
        shard = lax.axis_index("shard")
        for at in range(1, 16):
            for z in range(NZ):
                now = guest_stages(z, at)
                if now:
                    @pl.when((step == at) & (shard == z))
                    def _():
                        for stage, k in now: (stage_a, stage_b, stage_c)[stage](k)
    nsub = x_ref.shape[0] // SB
    D = out_ref.shape[1]
    me = lax.axis_index(("expert", "shard"))
    loads = [pltpu.make_async_copy(h.at[0], v, wsem.at[i]) for i, (h, v) in enumerate(((wg_hbm, wg), (wu_hbm, wu), (wd_hbm, wd)))]
    @pl.when(step == 0)
    def _():
        for l in loads: l.start()
    picks, gates = [], []
    for i in range(nsub):
        r = pl.ds(i * SB, SB)
        pick, gate = token_picks(x_ref[r, D:], experts, slots, me)
        picks.append(pick); gates.append(gate)
        rows_ref[i * slots:(i + 1) * slots, :] = dot(pick, x_ref[r, :D], 0, 0).astype(bf)
    @pl.when(step == 0)
    def _():
        for l in loads: l.wait()
    ga = dot(rows_ref[...], wg[...], 1, 0)
    ua = dot(rows_ref[...], wu[...], 1, 0)
    ga_ref[...] = ga
    ua_ref[...] = ua
    hid = (ga * (1.0 / (1.0 + jnp.exp(-ga))) * ua).astype(bf)
    eo = dot(hid, wd[...], 1, 0).astype(bf)
    for i in range(nsub):
        r = pl.ds(i * SB, SB)
        tok = dot(picks[i], eo[i * slots:(i + 1) * slots, :], 1, 0)
        out_ref[r, :] = (gates[i] * tok).astype(bf)
    if guest: pl.when(step == pl.num_programs(0) - 1)(finish)

GUEST_HOP = (0, 3, 5, 8)
GUEST_NEAR = (3, 7, 11, 14)
GUEST_FAR = (5, 9, 12, 15)

def guest_stages(z, at):
    order = [(0, 0)] + [(d, 2 * d - 1 + up) for d in range(1, NZ) for up in range(2) if (z - d >= 0, z + d < NZ)[up]]
    return ([(0, k) for d, k in order if k and GUEST_HOP[d] == at]
        + [(1, k) for i, (d, k) in enumerate(order) if GUEST_NEAR[i] == at]
        + [(2, k) for i, (d, k) in enumerate(order) if GUEST_FAR[i] == at])

def backward_kernel(experts, slots, SB, block, meta_ref, cota_ref, cotb_ref, rows_ref, ga_ref, ua_ref, wg_hbm, wu_hbm, wd_hbm, gr_ref, dwg_hbm, dwu_hbm, dwd_hbm,
                  wg, wu, wd, dwg, dwu, dwd, gp, wsem, osem):
    bf = jnp.bfloat16
    step = pl.program_id(0)
    nsub = meta_ref.shape[0] // SB
    D = cota_ref.shape[1]
    WM = meta_ref.shape[1]
    na, nb = [r.shape[0] * block // meta_ref.shape[0] for r in (cota_ref, cotb_ref)]
    me = lax.axis_index(("expert", "shard"))
    loads = [pltpu.make_async_copy(h.at[0], v, wsem.at[i]) for i, (h, v) in enumerate(((wg_hbm, wg), (wu_hbm, wu), (wd_hbm, wd)))]
    @pl.when(step == 0)
    def _():
        for l in loads: l.start()
        for a in (dwg, dwu, dwd): a[...] = jnp.zeros_like(a)
    picks = []
    for i in range(nsub):
        r = pl.ds(i * SB, SB)
        pick, gate = token_picks(meta_ref[r, :], experts, slots, me)
        picks.append(pick)
        cot = []
        for b in range(i * SB // block, (i + 1) * SB // block):
            cot += [cota_ref[b * na:(b + 1) * na, :], cotb_ref[b * nb:(b + 1) * nb, :]]
        gcot = (gate * jnp.concatenate(cot, axis=0).astype(jnp.float32)).astype(bf)
        gp[i * slots:(i + 1) * slots, :] = dot(pick, gcot, 0, 0).astype(bf)
    @pl.when(step == 0)
    def _():
        for l in loads: l.wait()
    ga = ga_ref[...]
    ua = ua_ref[...]
    sig = 1.0 / (1.0 + jnp.exp(-ga))
    act = ga * sig
    hidf = act * ua
    hid = hidf.astype(bf)
    gh = dot(gp[...], wd[...], 1, 1)
    share = jnp.sum(gh * hid.astype(jnp.float32), axis=-1, keepdims=True)
    dga = (gh * ua * (sig * (1.0 + ga * (1.0 - sig)))).astype(bf)
    dua = (gh * act).astype(bf)
    dwd[...] += dot(hid, gp[...], 0, 0)
    grow = (dot(dga, wg[...], 1, 1) + dot(dua, wu[...], 1, 1)).astype(bf)
    dwg[...] += dot(rows_ref[...], dga, 0, 0)
    dwu[...] += dot(rows_ref[...], dua, 0, 0)
    lane = lax.broadcasted_iota(jnp.int32, (share.shape[0], WM), 1)
    high = share.astype(bf).astype(jnp.float32)
    tail = (jnp.where(lane == me, high, 0.0) + jnp.where(lane == me + experts, share - high, 0.0)).astype(bf)
    for i in range(nsub):
        r = pl.ds(i * SB, SB)
        q = slice(i * slots, (i + 1) * slots)
        gr_ref[r, :D] = dot(picks[i], grow[q, :], 1, 0).astype(bf)
        gr_ref[r, D:] = dot(picks[i], tail[q, :], 1, 0).astype(bf)
    @pl.when(step == pl.num_programs(0) - 1)
    def _():
        outs = [pltpu.make_async_copy(v, h.at[0], osem.at[i]) for i, (v, h) in enumerate(((dwg, dwg_hbm), (dwu, dwu_hbm), (dwd, dwd_hbm)))]
        for o in outs: o.start()
        for o in outs: o.wait()

def experts_forward(x_all, w_gate, w_up, w_down, experts, block, capacity, guest, cid, TB=512, SB=256):
    hosted = placed()
    T, C = x_all.shape; D, F = w_gate.shape[1:]
    slots = max(SB // block, 1) * capacity
    total = TB // SB * slots
    S = T // SB * slots
    any_ = pl.BlockSpec(memory_space=pl.ANY)
    V = pltpu.VMEM; bf = jnp.bfloat16; f32 = jnp.float32
    blk = lambda r, c: pl.BlockSpec((r, c), lambda i: (i, 0))
    g = guest.reshape(2, guest.shape[0] // 2, guest.shape[1])
    res = pl.pallas_call(
        functools.partial(forward_kernel, experts, slots, SB, hosted),
        grid=(T // TB,),
        out_shape=([jax.ShapeDtypeStruct((2, 2, 2, NZ) + g.shape, g.dtype)] if hosted else []) + [jax.ShapeDtypeStruct((T, D), bf), jax.ShapeDtypeStruct((S, D), bf), jax.ShapeDtypeStruct((S, F), f32), jax.ShapeDtypeStruct((S, F), f32)],
        in_specs=([pl.BlockSpec(memory_space=pltpu.VMEM)] if hosted else []) + [blk(TB, C), any_, any_, any_],
        out_specs=([any_] if hosted else []) + [blk(TB, D), blk(total, D), blk(total, F), blk(total, F)],
        scratch_shapes=[V((D, F), bf), V((D, F), bf), V((F, D), bf), pltpu.SemaphoreType.DMA((3,))] + (ag_sems(1) if hosted else []),
        compiler_params=pltpu.CompilerParams(dimension_semantics=("arbitrary",), vmem_limit_bytes=65000 * 1024,
            **(dict(collective_id=cid, has_side_effects=True) if hosted else {})),
        cost_estimate=pl.CostEstimate(flops=48_000_000_000, bytes_accessed=130_000_000, transcendentals=0),
        name="experts_forward",
    )(*([g] if hosted else []), x_all, w_gate, w_up, w_down)
    if hosted: return res[1:], res[0].reshape(-1, guest.shape[1])
    return res, lax.all_gather(guest, BOTH, axis=0, tiled=True)

def experts_backward(x_all, cot_a, cot_b, rows, ga, ua, w_gate, w_up, w_down, experts, block, capacity, TB=512, SB=256):
    T, C = x_all.shape; D, F = w_gate.shape[1:]
    slots = max(SB // block, 1) * capacity
    total = TB // SB * slots
    WM = C - D
    any_ = pl.BlockSpec(memory_space=pl.ANY)
    V = pltpu.VMEM; bf = jnp.bfloat16; f32 = jnp.float32
    blk = lambda r, c: pl.BlockSpec((r, c), lambda i: (i, 0))
    meta = pl.BlockSpec((TB, WM), lambda i: (i, D // WM)) if D % WM == 0 else blk(TB, WM)
    meta_in = x_all if D % WM == 0 else x_all[:, D:]
    return pl.pallas_call(
        functools.partial(backward_kernel, experts, slots, SB, block),
        grid=(T // TB,),
        out_shape=[jax.ShapeDtypeStruct((T, C), bf), jax.ShapeDtypeStruct(w_gate.shape, f32), jax.ShapeDtypeStruct(w_up.shape, f32), jax.ShapeDtypeStruct(w_down.shape, f32)],
        in_specs=[meta, blk(cot_a.shape[0] * TB // T, D), blk(cot_b.shape[0] * TB // T, D), blk(total, D), blk(total, F), blk(total, F), any_, any_, any_],
        out_specs=[blk(TB, C), any_, any_, any_],
        scratch_shapes=[V((D, F), bf), V((D, F), bf), V((F, D), bf), V((D, F), f32), V((D, F), f32), V((F, D), f32), V((total, D), bf), pltpu.SemaphoreType.DMA((3,)), pltpu.SemaphoreType.DMA((3,))],
        compiler_params=pltpu.CompilerParams(dimension_semantics=("arbitrary",), vmem_limit_bytes=65000 * 1024),
        cost_estimate=pl.CostEstimate(flops=85_000_000_000, bytes_accessed=150_000_000, transcendentals=0),
        name="experts_backward",
    )(meta_in, cot_a, cot_b, rows, ga, ua, w_gate, w_up, w_down)


def rope_tables(seq_len):
    half = HD // 2
    frequency = theta_base ** (-2.0 * jnp.arange(half, dtype=jnp.float32) / HD)
    angles = jnp.arange(seq_len, dtype=jnp.float32)[:, None] * frequency[None, :]
    return jnp.concatenate([jnp.cos(angles)] * 2, axis=-1), jnp.concatenate([-jnp.sin(angles), jnp.sin(angles)], axis=-1)

def turn(u, cos, sin):
    return u * cos + pltpu.roll(u, HD // 2, 1) * sin

def scale_of(u):
    return lax.rsqrt(jnp.mean(u * u, axis=-1, keepdims=True) + epsilon)

def attention_forward_kernel(group, n_ref, wq_ref, wk_ref, wv_ref, gq_ref, gk_ref, cos_ref, sin_ref, u_ref, ku_ref, ql_ref, kl_ref, vl_ref, mix_ref, k_all):
    bf, f32 = jnp.bfloat16, jnp.float32
    rows, seq = ql_ref.shape[0], kl_ref.shape[0]
    first = lax.axis_index("shard") * rows
    own = pl.ds(first, rows)
    k_all[...] = dot(n_ref[...], wk_ref[...], 1, 0)
    ku_ref[...] = k_all[own, :]
    k = k_all[...]
    kl_ref[...] = turn(k * scale_of(k) * gk_ref[...], cos_ref[...], sin_ref[...]).astype(bf)
    vl_ref[...] = dot(n_ref[...], wv_ref[...], 1, 0).astype(bf)
    u_ref[...] = dot(n_ref[own, :], wq_ref[...], 1, 0)
    cos, sin = cos_ref[own, :], sin_ref[own, :]
    allowed = lax.broadcasted_iota(jnp.int32, (rows, seq), 1) <= first + lax.broadcasted_iota(jnp.int32, (rows, seq), 0)
    for j in range(group):
        cols = slice(j * HD, (j + 1) * HD)
        u = u_ref[:, cols]
        ql = (turn(u * scale_of(u) * gq_ref[...], cos, sin) * HD ** (-0.5)).astype(bf)
        ql_ref[:, cols] = ql
        scores = dot(ql, kl_ref[...], 1, 1)
        raised = jnp.where(allowed, jnp.exp(scores), 0.0)
        probs = (raised * (1.0 / jnp.sum(raised, axis=-1, keepdims=True))).astype(bf)
        mix_ref[:, cols] = dot(probs, vl_ref[...], 1, 0).astype(bf)

def attention_forward(normed_seq, wqkv, rows, gq, gk, cos, sin):
    seq, width = normed_seq.shape
    group = HQ // HK
    bf, f32 = jnp.bfloat16, jnp.float32
    whole = lambda a: pl.BlockSpec(a.shape, lambda i: (0, 0))
    gq, gk = gq[None, :], gk[None, :]
    qb = pl.BlockSpec((rows, group * HD), lambda i: (0, i)); kb = pl.BlockSpec((seq, HD), lambda i: (0, i))
    return pl.pallas_call(
        functools.partial(attention_forward_kernel, group),
        grid=(HK,),
        out_shape=[jax.ShapeDtypeStruct((rows, HQ * HD), f32), jax.ShapeDtypeStruct((rows, HK * HD), f32), jax.ShapeDtypeStruct((rows, HQ * HD), bf),
            jax.ShapeDtypeStruct((seq, HK * HD), bf), jax.ShapeDtypeStruct((seq, HK * HD), bf), jax.ShapeDtypeStruct((rows, HQ * HD), bf)],
        in_specs=[whole(normed_seq), pl.BlockSpec((width, group * HD), lambda i: (0, i)), pl.BlockSpec((width, HD), lambda i: (0, HQ + i)), pl.BlockSpec((width, HD), lambda i: (0, HQ + HK + i)),
            whole(gq), whole(gk), whole(cos), whole(sin)],
        out_specs=[qb, pl.BlockSpec((rows, HD), lambda i: (0, i)), qb, kb, kb, qb],
        scratch_shapes=[pltpu.VMEM((seq, HD), f32)],
        compiler_params=pltpu.CompilerParams(dimension_semantics=("arbitrary",), vmem_limit_bytes=56 << 20),
        cost_estimate=pl.CostEstimate(flops=13_000_000_000, bytes_accessed=45_000_000, transcendentals=8_400_000),
        name="attention_forward",
    )(normed_seq, wqkv, wqkv, wqkv, gq, gk, cos, sin)

def attention_backward_kernel(group, guest, *refs):
    if guest:
        p_ref, u_ref, ql_ref, kl_ref, vl_ref, ga_ref, wo_ref, gq_ref, cos_ref, sin_ref, po_ref, gu_ref, gk_ref, gv_ref, gg_ref, gk_acc, gv_acc = refs[:17]
        runs = line_scatter_steps(LINE_PARTS, p_ref, po_ref, refs[17:])
        slots = HK * group
        at = {i * slots // (LINE_STEPS - 1): run for i, run in enumerate(runs[:-1])}
    else:
        u_ref, ql_ref, kl_ref, vl_ref, ga_ref, wo_ref, gq_ref, cos_ref, sin_ref, gu_ref, gk_ref, gv_ref, gg_ref, gk_acc, gv_acc = refs
        at = {}
    step = pl.program_id(0)
    bf, f32 = jnp.bfloat16, jnp.float32
    gm_all = dot(ga_ref[...], wo_ref[...], 1, 1).astype(bf)
    rows, seq = ql_ref.shape[0], kl_ref.shape[0]
    first = lax.axis_index("shard") * rows
    cos, sin = cos_ref[pl.ds(first, rows), :], sin_ref[pl.ds(first, rows), :]
    allowed = lax.broadcasted_iota(jnp.int32, (rows, seq), 1) <= first + lax.broadcasted_iota(jnp.int32, (rows, seq), 0)
    gain_grad = jnp.zeros((1, HD), f32)
    for j in range(group):
        for i in range(HK):
            if i * group + j in at: pl.when(step == i)(at[i * group + j])
        cols = slice(j * HD, (j + 1) * HD)
        ql, gm = ql_ref[:, cols], gm_all[:, cols]
        raised = jnp.where(allowed, jnp.exp(dot(ql, kl_ref[...], 1, 1)), 0.0)
        probs = raised * (1.0 / jnp.sum(raised, axis=-1, keepdims=True))
        gp = dot(gm, vl_ref[...], 1, 1)
        gs = (probs * (gp - jnp.sum(probs * gp, axis=-1, keepdims=True))).astype(bf)
        gv = dot(probs.astype(bf), gm, 0, 0)
        gk = dot(gs, ql, 0, 0)
        if j == 0:
            gv_acc[...] = gv
            gk_acc[...] = gk
        else:
            gv_acc[...] += gv
            gk_acc[...] += gk
        m = dot(gs, kl_ref[...], 1, 0) * HD ** (-0.5)
        m = m * cos + pltpu.roll(m * sin, HD // 2, 1)
        u = u_ref[:, cols]
        r = scale_of(u)
        gain_grad = gain_grad + jnp.sum(m * u * r, axis=0, keepdims=True)
        mg = m * gq_ref[...]
        gu_ref[:, cols] = (r * mg - u * (r * r * r) * jnp.mean(mg * u, axis=-1, keepdims=True)).astype(bf)
    gk_ref[...] = gk_acc[...].astype(bf)
    gv_ref[...] = gv_acc[...].astype(bf)
    gg_ref[0] = jnp.broadcast_to(gain_grad, (8, HD))
    if guest: pl.when(step == HK - 1)(runs[-1])

def attention_backward(q_proj, q_low, k_low, v_low, grad_attn, w_out, gq, cos, sin, guest, cid):
    rows, seq = q_low.shape[0], k_low.shape[0]
    group = HQ // HK
    bf, f32 = jnp.bfloat16, jnp.float32
    gq = gq[None, :]
    whole = lambda a: pl.BlockSpec(a.shape, lambda i: (0, 0))
    qb = pl.BlockSpec((rows, group * HD), lambda i: (0, i)); kb = pl.BlockSpec((seq, HD), lambda i: (0, i))
    hosted = placed()
    R, C = guest.shape[0] // lax.axis_size("shard"), guest.shape[1]
    shape = (NZ, LINE_PARTS, R // LINE_PARTS, C)
    vm = pl.BlockSpec(memory_space=pltpu.VMEM)
    *summed, grad_q, grad_k, grad_v, gain = pl.pallas_call(
        functools.partial(attention_backward_kernel, group, hosted),
        grid=(HK,),
        out_shape=([jax.ShapeDtypeStruct(shape[1:], f32)] if hosted else []) + [jax.ShapeDtypeStruct(q_low.shape, bf), jax.ShapeDtypeStruct(k_low.shape, bf), jax.ShapeDtypeStruct(k_low.shape, bf), jax.ShapeDtypeStruct((HK, 8, HD), f32)],
        in_specs=([vm] if hosted else []) + [qb, qb, kb, kb, whole(grad_attn), pl.BlockSpec((group * HD, w_out.shape[1]), lambda i: (i, 0)), whole(gq), whole(cos), whole(sin)],
        out_specs=([vm] if hosted else []) + [qb, kb, kb, pl.BlockSpec((1, 8, HD), lambda i: (i, 0, 0))],
        scratch_shapes=[pltpu.VMEM((seq, HD), f32), pltpu.VMEM((seq, HD), f32)] + (line_scatter_scratch(LINE_PARTS, R, C, bf) if hosted else []),
        compiler_params=pltpu.CompilerParams(dimension_semantics=("arbitrary",), vmem_limit_bytes=60 << 20,
            **(dict(collective_id=cid, has_side_effects=True) if hosted else {})),
        cost_estimate=pl.CostEstimate(flops=15_000_000_000, bytes_accessed=20_000_000, transcendentals=8_400_000),
        name="attention_backward",
    )(*([guest.reshape(shape)] if hosted else []), q_proj, q_low, k_low, v_low, grad_attn, w_out, gq, cos, sin)
    if hosted: total = summed[0].reshape(R, C)
    else: total = lax.psum_scatter(guest, "shard", scatter_dimension=0, tiled=True).astype(f32)
    return total, grad_q, jnp.concatenate([grad_k, grad_v], axis=1), jnp.sum(gain[:, 0], axis=0)

HQ = 32
HK = 4
HD = 128
epsilon = 1e-06
theta_base = 1000000.0
BOTH = ("expert", "shard")


def matmul(left, right):
    return jnp.dot(left, right, preferred_element_type=jnp.float32)


def matmul_tn(left, right):
    return lax.dot_general(
        left, right, (((0,), (0,)), ((), ())), preferred_element_type=jnp.float32
    )


def matmul_nt(left, right):
    return lax.dot_general(
        left, right, (((1,), (1,)), ((), ())), preferred_element_type=jnp.float32
    )


def norm_rows(values, gain_vec):
    return (
        values * lax.rsqrt(jnp.mean(values * values, axis=-1, keepdims=True) + epsilon) * gain_vec
    )


def norm_back(values, gain_vec, upstream):
    scaling = lax.rsqrt(jnp.mean(values * values, axis=-1, keepdims=True) + epsilon)
    gain_grad = jnp.sum(upstream * values * scaling, axis=0)
    weighted = upstream * gain_vec
    inner_sum = jnp.mean(weighted * values, axis=-1, keepdims=True)
    return (scaling * weighted - values * (scaling * scaling * scaling) * inner_sum, gain_grad)


def rotary(values, positions):
    head_width = values.shape[-1]
    half_width = head_width // 2
    frequency = theta_base ** (-2.0 * jnp.arange(half_width, dtype=jnp.float32) / head_width)
    angles = positions.astype(jnp.float32)[:, None] * frequency[None, :]
    cosine = jnp.concatenate([jnp.cos(angles), jnp.cos(angles)], axis=-1)[:, None, :]
    sine_part = jnp.concatenate([jnp.sin(angles), jnp.sin(angles)], axis=-1)[:, None, :]
    turned = jnp.concatenate([-values[..., half_width:], values[..., :half_width]], axis=-1)
    return values * cosine + turned * sine_part


def head_prep(projected, gain_vec, positions, head_count, factor):
    shaped = projected.reshape(projected.shape[0], head_count, projected.shape[1] // head_count)
    return rotary(norm_rows(shaped, gain_vec), positions) * factor


def gather_all(arrays, cid, line=()):
    if placed():
        return [o.reshape(-1, o.shape[-1]) for o in ag32(arrays, cid, line)]
    return [lax.all_gather(a, BOTH, axis=0, tiled=True) for a in arrays] + [
        lax.all_gather(a, "shard", axis=0, tiled=True) for a in line
    ]


def scatter_all(arrays, cid, out_dtype=jnp.float32, line=()):
    if placed():
        return rs32(
            [a.reshape(32, -1, a.shape[-1]) for a in arrays], cid, out_dtype, line=[a.reshape(NZ, -1, a.shape[-1]) for a in line]
        )
    return [lax.psum_scatter(a, BOTH, scatter_dimension=0, tiled=True).astype(out_dtype) for a in arrays] + [
        lax.psum_scatter(a, "shard", scatter_dimension=0, tiled=True).astype(out_dtype) for a in line
    ]


def per_device(
    hidden_in,
    g_attn,
    w_query,
    w_key,
    w_value,
    g_query,
    g_key,
    w_out,
    g_ffn,
    w_router,
    w_gate,
    w_up,
    w_down,
    routes,
    cotangent,
):
    bf, f32 = jnp.bfloat16, jnp.float32
    tok_rows, model_width = hidden_in.shape
    top_count = routes.shape[1]
    devices = lax.axis_size(BOTH)
    expert_count = devices * w_gate.shape[0]
    capacity = 2 * tok_rows * top_count // expert_count
    shard_count = lax.axis_size("shard")
    shard_pos = lax.axis_index("shard")
    seq_len = tok_rows * shard_count
    q_cols, kv_cols = HQ * HD, HK * HD

    pieces = [w_router.reshape(-1), g_attn, g_ffn, g_query, g_key]
    sizes = [p.shape[0] for p in pieces]
    used = sum(sizes)
    small_rows = -(-used // (64 * 128)) * 64
    small = jnp.concatenate(pieces + [jnp.zeros((small_rows * 128 - used,), bf)]).reshape(small_rows, 128)
    wqkv = jnp.concatenate([w_query, w_key, w_value], axis=1)
    wqkv_full, small_all, wo_full, hidden_seq = gather_all([wqkv, small, w_out], 1, [hidden_in])
    small_all = small_all.reshape(devices, small_rows * 128)
    starts = [sum(sizes[:i]) for i in range(5)]
    wr_full, attn_gain, ffn_gain, query_gain, key_gain = [small_all[:, o : o + n].reshape(-1) for o, n in zip(starts, sizes)]
    wr_full = wr_full.reshape(model_width, expert_count)
    attn_gain, ffn_gain, query_gain, key_gain = [g.astype(f32) for g in (attn_gain, ffn_gain, query_gain, key_gain)]
    first = tok_rows // 2
    cot_first, wo_full = lax.optimization_barrier((cotangent[:first], wo_full))
    cot_a = lax.all_gather(cot_first, BOTH, axis=0, tiled=True)

    inputs_f = hidden_in.astype(f32)
    normed_low = norm_rows(inputs_f, attn_gain).astype(bf)
    normed_seq = norm_rows(hidden_seq.astype(f32), attn_gain).astype(bf)
    cosine, sine = rope_tables(seq_len)
    q_proj, k_proj, q_low, k_low, v_low, mix_low = attention_forward(
        normed_seq, wqkv_full, tok_rows, query_gain, key_gain, cosine, sine
    )
    residual = inputs_f + matmul(mix_low, wo_full)
    ffn_low = norm_rows(residual, ffn_gain).astype(bf)

    logits = matmul(ffn_low, wr_full)
    expert_ids = jnp.arange(expert_count, dtype=jnp.int32)
    chosen = jnp.any(routes[:, :, None] == expert_ids[None, None, :], axis=1)
    raised_gate = jnp.where(chosen, jnp.exp(logits), 0.0)
    gates = raised_gate / jnp.sum(raised_gate, axis=-1, keepdims=True)
    gate_high = lax.reduce_precision(gates, 8, 7)
    gate_low = gates - gate_high
    extra = -(-3 * expert_count // 128) * 128
    payload = jnp.concatenate(
        [
            ffn_low,
            chosen.astype(bf),
            gate_high.astype(bf),
            gate_low.astype(bf),
            jnp.zeros((tok_rows, extra - 3 * expert_count), bf),
        ],
        axis=1,
    )
    (payload_all,) = gather_all([payload], 3)
    (out_part, rows, gate_act, up_act), cot_b = experts_forward(
        payload_all, w_gate, w_up, w_down, expert_count, tok_rows, capacity, cotangent[first:], 2
    )
    moe_out = lax.psum_scatter(out_part, "expert", scatter_dimension=0, tiled=True)
    grad_part, grad_wgate, grad_wup, grad_wdown = experts_backward(
        payload_all, cot_a, cot_b, rows, gate_act, up_act, w_gate, w_up, w_down, expert_count, tok_rows, capacity
    )
    (grad_sum,) = scatter_all([grad_part], 4)
    grad_sum, moe_out = lax.optimization_barrier((grad_sum, moe_out))
    upstream = cotangent.astype(f32)
    grad_ffn = grad_sum[:, :model_width]
    grad_shares = (
        grad_sum[:, model_width : model_width + expert_count]
        + grad_sum[:, model_width + expert_count : model_width + 2 * expert_count]
    )
    grad_logits = (grad_shares - gates * jnp.sum(grad_shares, axis=-1, keepdims=True)).astype(bf)
    grad_wrouter = matmul_tn(ffn_low, grad_logits)
    grad_ffn = grad_ffn + matmul_nt(grad_logits, wr_full)
    grad_second, grad_ffn_gain = norm_back(residual, ffn_gain, grad_ffn)
    grad_residual = upstream + grad_second
    grad_attn_low = grad_residual.astype(bf)
    grad_wout = matmul_tn(mix_low, grad_attn_low).astype(bf)
    grad_attn_low, grad_wout = lax.optimization_barrier((grad_attn_low, grad_wout))
    out_grad = lax.psum_scatter(grad_wout, "expert", scatter_dimension=0, tiled=True)

    moe_parts = moe_out.reshape(shard_count, 2, tok_rows // 2, model_width)
    moe_a, moe_b = [moe_parts[:, i].reshape(-1, model_width) for i in range(2)]
    moe_a, grad_q_low, grad_kv, grad_query_gain = attention_backward(
        q_proj, q_low, k_low, v_low, grad_attn_low, wo_full, query_gain, cosine, sine, moe_a, 5
    )
    grad_kv = line_scatter(grad_kv, 6)
    own_rows = shard_pos * tok_rows
    positions = own_rows + jnp.arange(tok_rows, dtype=jnp.int32)
    _, k_pull = jax.vjp(
        lambda projected, gain_vec: head_prep(projected, gain_vec, positions, HK, 1.0), k_proj, key_gain
    )
    grad_k_proj, grad_key_gain = k_pull(grad_kv[:, :kv_cols].reshape(tok_rows, HK, HD))
    grad_qkv_low = jnp.concatenate(
        [grad_q_low, grad_k_proj.astype(bf), grad_kv[:, kv_cols:].astype(bf)], axis=1
    )
    grad_wqkv = matmul_tn(normed_low, grad_qkv_low).astype(bf)
    grad_normed = matmul_nt(grad_qkv_low, wqkv_full)
    grad_front, grad_attn_gain = norm_back(inputs_f, attn_gain, grad_normed)
    grad_input = (grad_residual + grad_front).astype(bf)

    grads = [grad_wrouter, grad_attn_gain, grad_ffn_gain, grad_query_gain, grad_key_gain]
    packed = jnp.concatenate(
        [g.astype(bf).reshape(devices, -1) for g in grads] + [jnp.zeros((devices, small_rows * 128 - used), bf)], axis=1
    ).reshape(devices * small_rows, 128)
    grad_wqkv, out_grad = lax.optimization_barrier((grad_wqkv, out_grad))
    out_grad = lax.psum_scatter(out_grad, "shard", scatter_dimension=0, tiled=True).astype(f32)
    qkv_grad, small_grad, moe_b = scatter_all([grad_wqkv, packed], 8, line=[moe_b])
    block_out = (residual + jnp.concatenate([moe_a, moe_b], axis=0)).astype(bf)
    small_grad = small_grad.reshape(-1)
    router_g, attn_g, ffn_g, query_g, key_g = [small_grad[o : o + n] for o, n in zip(starts, sizes)]
    return (
        block_out,
        grad_input,
        attn_g,
        qkv_grad[:, :q_cols],
        qkv_grad[:, q_cols : q_cols + kv_cols],
        qkv_grad[:, q_cols + kv_cols :],
        query_g,
        key_g,
        out_grad,
        ffn_g,
        router_g.reshape(w_router.shape),
        grad_wgate,
        grad_wup,
        grad_wdown,
    )


def solution(mesh):
    row = P(BOTH, None)
    vec = P(BOTH)
    cube = P(BOTH, None, None)
    in_specs = (row, vec, row, row, row, vec, vec, row, vec, row, cube, cube, cube, row, row)
    out_specs = (row, row, vec, row, row, row, vec, vec, row, vec, row, cube, cube, cube)
    return jax.shard_map(
        per_device, mesh=mesh, in_specs=in_specs, out_specs=out_specs, check_vma=False
    )
```

```python
import functools

import jax
import jax.numpy as jnp
from jax import lax
from jax.experimental import pallas as pl
from jax.experimental.pallas import tpu as pltpu
from jax.sharding import PartitionSpec as P

MESH = pl.DeviceIdType.MESH
NZ = 4

def placed():
    return lax.axis_size("expert") == 8 and lax.axis_size("shard") == NZ

def place():
    e = lax.axis_index("expert"); s = lax.axis_index("shard")
    return e // 4, lax.rem(e // 2, 2), lax.rem(e, 2), s

def dev(y, x, c, s):
    return (y * 4 + x * 2 + c, s)

def barrier_all(y, x, c, s):
    bar = pltpu.get_barrier_semaphore()
    def sig(d): pl.semaphore_signal(bar, inc=1, device_id=d, device_id_type=MESH)
    sig(dev(1 - y, x, c, s)); sig(dev(y, 1 - x, c, s)); sig(dev(y, x, 1 - c, s))
    @pl.when(s > 0)
    def _(): sig(dev(y, x, c, s - 1))
    @pl.when(s < NZ - 1)
    def _(): sig(dev(y, x, c, s + 1))
    pl.semaphore_wait(bar, 3 + jnp.where(s > 0, 1, 0) + jnp.where(s < NZ - 1, 1, 0))

def ag_kernel(n_arr, n_line, *refs):
    n_all = n_arr + n_line
    for run in ag_steps(n_arr, n_line, refs[:n_all], refs[n_all:2 * n_all], refs[2 * n_all:]): run()

def ag_steps(n_arr, n_line, ins, outs, sems, stages=False):
    n_all = n_arr + n_line
    loc_sem, zs, zr, ps, pr, cs, cr = sems
    y, x, c, s = place()
    def rc(src, dst, ss, rs, d):
        return pltpu.make_async_remote_copy(src_ref=src, dst_ref=dst, send_sem=ss, recv_sem=rs, device_id=d, device_id_type=MESH)
    X = dev(y, 1 - x, c, s); Y = dev(1 - y, x, c, s); C = dev(y, x, 1 - c, s)
    A = range(n_arr)
    every = range(n_all)
    def home(a, zz):
        return outs[a].at[y, x, c, zz] if a < n_arr else outs[a].at[zz]
    steps = [(0, 0)] + [(d, g) for d in range(1, NZ) for g in (1, -1)]
    def valid(d, g):
        return (s >= d) if g == 1 else (s + d <= NZ - 1)
    def zof(d, g): return s - d * g
    def src_own(a, h, zz, k):
        return ins[a].at[h] if k == 0 else home(a, zz).at[h]
    def zcopy(a, h, zz, k, g):
        kk = 1 + 2 * (k_dist(k)) + (0 if g == 1 else 1)
        return rc(src_own(a, h, zz, k), home(a, zz).at[h], zs.at[a, h, kk], zr.at[a, h, kk], dev(y, x, c, s + g))
    def k_dist(k): return steps[k][0]
    def plane(a, h, zz, k, which):
        return rc(src_own(a, h, zz, k), outs[a].at[y, x, c, zz, h], ps.at[a, k, h, which], pr.at[a, k, h, which], X if which == 0 else Y)
    def plane_recv(a, h, zz, k, which):
        d = outs[a].at[y, 1 - x, c, zz, h] if which == 0 else outs[a].at[1 - y, x, c, zz, h]
        return rc(d, d, ps.at[a, k, h, which], pr.at[a, k, h, which], X if which == 0 else Y)
    def diag(a, h, zz, k):
        d = outs[a].at[y, 1 - x, c, zz, h] if h == 0 else outs[a].at[1 - y, x, c, zz, h]
        return rc(d, d, ps.at[a, k, h, 2], pr.at[a, k, h, 2], Y if h == 0 else X)
    def diag_recv(a, h, zz, k):
        d = outs[a].at[1 - y, 1 - x, c, zz, h]
        return rc(d, d, ps.at[a, k, h, 2], pr.at[a, k, h, 2], Y if h == 0 else X)
    def core(a, zz, k, part):
        d = outs[a].at[:, :, c, zz]
        return rc(d, d, cs.at[a, k], cr.at[a, k], C)
    def core_recv(a, zz, k):
        d = outs[a].at[:, :, 1 - c, zz]
        return rc(d, d, cs.at[a, k], cr.at[a, k], C)
    def loc(a):
        return pltpu.make_async_copy(ins[a], home(a, s), loc_sem.at[a])

    def when(k, f):
        d, g = steps[k]
        if k == 0: f()
        else: pl.when(valid(d, g))(f)

    def stage_a(k):
        d, g = steps[k]
        def go():
            zz = zof(d, g)
            for a in every:
                for h in range(2):
                    if k:
                        kk = k
                        dref = home(a, zz).at[h]
                        rc(dref, dref, zs.at[a, h, kk], zr.at[a, h, kk], X).wait_recv()
                    for gg in ((1, -1) if k == 0 else (g,)):
                        okc = (s < NZ - 1) if gg == 1 else (s > 0)
                        if d + 1 < NZ:
                            @pl.when(okc)
                            def _(): zcopy(a, h, zz, k, gg).start()
                    if a < n_arr:
                        plane(a, h, zz, k, 0).start()
                        plane(a, h, zz, k, 1).start()
        when(k, go)
    def stage_b(k):
        d, g = steps[k]
        def go():
            zz = zof(d, g)
            for a in A:
                plane_recv(a, 0, zz, k, 0).wait_recv()
                diag(a, 0, zz, k).start()
                plane_recv(a, 1, zz, k, 1).wait_recv()
                diag(a, 1, zz, k).start()
        when(k, go)
    def stage_c(k):
        d, g = steps[k]
        def go():
            zz = zof(d, g)
            for a in A:
                if k == 0: loc(a).wait()
                plane_recv(a, 1, zz, k, 0).wait_recv()
                plane_recv(a, 0, zz, k, 1).wait_recv()
                diag_recv(a, 0, zz, k).wait_recv()
                diag_recv(a, 1, zz, k).wait_recv()
                core(a, zz, k, 0).start()
        when(k, go)
    n = len(steps)
    def start():
        barrier_all(y, x, c, s)
        for a in every: loc(a).start()
        stage_a(0)
    def advance(i):
        if 0 < i < n: stage_a(i)
        if 0 <= i - 1 < n: stage_b(i - 1)
        if 0 <= i - 2 < n: stage_c(i - 2)
    def finish():
        for k in range(n):
            d, g = steps[k]
            def go():
                zz = zof(d, g)
                for a in every:
                    if a < n_arr:
                        core_recv(a, zz, k).wait_recv()
                        core(a, zz, k, 0).wait_send()
                    elif k == 0: loc(a).wait()
                    for h in range(2):
                        for gg in ((1, -1) if k == 0 else (g,)):
                            okc = (s < NZ - 1) if gg == 1 else (s > 0)
                            if d + 1 < NZ:
                                @pl.when(okc)
                                def _(): zcopy(a, h, zz, k, gg).wait_send()
                        if a < n_arr:
                            plane(a, h, zz, k, 0).wait_send()
                            plane(a, h, zz, k, 1).wait_send()
                            diag(a, h, zz, k).wait_send()
            when(k, go)
    if stages: return start, stage_a, stage_b, stage_c, finish
    return [start] + [functools.partial(advance, i) for i in range(1, n + 2)] + [finish]

def ag_sems(n, m=0):
    D = pltpu.SemaphoreType.DMA
    return [D((n + m,)), D((n + m, 2, 9)), D((n + m, 2, 9)), D((n, 7, 2, 3)), D((n, 7, 2, 3)), D((n, 7)), D((n, 7))]

def ag32(arrs, cid, line=()):
    ins = [a.reshape(2, a.shape[0] // 2, a.shape[1]) for a in list(arrs) + list(line)]
    n, m = len(arrs), len(line)
    outs = pl.pallas_call(
        functools.partial(ag_kernel, n, m),
        out_shape=[jax.ShapeDtypeStruct(((2, 2, 2, NZ) if i < n else (NZ,)) + a.shape, a.dtype) for i, a in enumerate(ins)],
        in_specs=[pl.BlockSpec(memory_space=pltpu.VMEM)] * (n + m),
        out_specs=[pl.BlockSpec(memory_space=pl.ANY)] * (n + m),
        scratch_shapes=ag_sems(n, m),
        compiler_params=pltpu.CompilerParams(collective_id=cid, has_side_effects=True, vmem_limit_bytes=64000 * 1024),
        name="gather_all",
    )(*ins)
    return [o.reshape(-1, a.shape[1] * 2, a.shape[2]) for o, a in zip(outs, ins)]

ZORDER = (0, 3, 1, 2)
LAGS = (1, 1, 1, 1)
LINE_LAG = 3

def rs_kernel(n_arr, n_line, parts, *refs):
    n_all = n_arr + n_line
    ins = refs[:n_all]; outs = refs[n_all:2 * n_all]
    sc = list(refs[2 * n_all:])
    own_b = [sc.pop(0) for _ in range(n_all)]; zu_b = [sc.pop(0) for _ in range(n_all)]; zd_b = [sc.pop(0) for _ in range(n_all)]
    r0_b, ra_b, rb_b = [[sc.pop(0) for _ in range(n_arr)] for _ in range(3)]
    lsem, s0s, s0r, sas, sar, sbs, sbr, zus, zur, zds, zdr = sc
    y, x, c, s = place()
    barrier_all(y, x, c, s)
    X = dev(y, 1 - x, c, s); Y = dev(1 - y, x, c, s); C = dev(y, x, 1 - c, s)
    UP = dev(y, x, c, s + 1); DN = dev(y, x, c, s - 1)
    def rc(src, dst, ss, rs, d):
        return pltpu.make_async_remote_copy(src_ref=src, dst_ref=dst, send_sem=ss, recv_sem=rs, device_id=d, device_id_type=MESH)
    units = [(a, zz, h) for zz in ZORDER for h in range(parts) for a in range(n_arr)]
    lines = [(a, zz, h) for zz in ZORDER for h in range(parts) for a in range(n_arr, n_all)]
    def jj(zz, h): return ZORDER.index(zz) * parts + h
    def load(a, zz, h):
        j = jj(zz, h)
        src = ins[a].at[:, :, c, zz, h] if a < n_arr else ins[a].at[zz, h]
        return pltpu.make_async_copy(src, own_b[a].at[j], lsem.at[a, j])
    def mine(a, j):
        return own_b[a].at[j, y, x] if a < n_arr else own_b[a].at[j]
    def c0(a, zz, h):
        j = jj(zz, h)
        return rc(ins[a].at[:, :, 1 - c, zz, h], r0_b[a].at[j], s0s.at[a, j], s0r.at[a, j], C)
    def ca(a, zz, h):
        j = jj(zz, h)
        if h % 2 == 0: return rc(own_b[a].at[j, :, 1 - x], ra_b[a].at[j], sas.at[a, j], sar.at[a, j], X)
        return rc(own_b[a].at[j, 1 - y], ra_b[a].at[j], sas.at[a, j], sar.at[a, j], Y)
    def cb(a, zz, h):
        j = jj(zz, h)
        if h % 2 == 0: return rc(own_b[a].at[j, 1 - y, x], rb_b[a].at[j], sbs.at[a, j], sbr.at[a, j], Y)
        return rc(own_b[a].at[j, y, 1 - x], rb_b[a].at[j], sbs.at[a, j], sbr.at[a, j], X)
    def cu(a, zz, h):
        j = jj(zz, h)
        return rc(mine(a, j), zu_b[a].at[j], zus.at[a, j], zur.at[a, j], UP)
    def cd(a, zz, h):
        j = jj(zz, h)
        return rc(mine(a, j), zd_b[a].at[j], zds.at[a, j], zdr.at[a, j], DN)
    def add_into(dst, other):
        rows = dst.shape[0]
        st = 16 if rows % 16 == 0 else rows
        @pl.loop(0, rows // st)
        def _(i):
            r = pl.ds(i * st, st)
            dst[r, :] = (dst[r, :].astype(jnp.float32) + other[r, :].astype(jnp.float32)).astype(dst.dtype)
    def stage0(u):
        a, zz, h = u; j = jj(zz, h)
        load(a, zz, h).wait()
        c0(a, zz, h).wait_recv()
        for yy in range(2):
            for xx in range(2):
                add_into(own_b[a].at[j, yy, xx], r0_b[a].at[j, yy, xx])
        ca(a, zz, h).start()
    def stage1(u):
        a, zz, h = u; j = jj(zz, h)
        ca(a, zz, h).wait_recv()
        for q in range(2):
            if h % 2 == 0: add_into(own_b[a].at[j, q, x], ra_b[a].at[j, q])
            else: add_into(own_b[a].at[j, y, q], ra_b[a].at[j, q])
        cb(a, zz, h).start()
    def stage2(u):
        a, zz, h = u; j = jj(zz, h)
        cb(a, zz, h).wait_recv()
        add_into(own_b[a].at[j, y, x], rb_b[a].at[j])
    def hop(u, k):
        a, zz, h = u; j = jj(zz, h)
        if k < zz:
            @pl.when(s == k)
            def _():
                if k > 0:
                    cu(a, zz, h).wait_recv()
                    add_into(mine(a, j), zu_b[a].at[j])
                cu(a, zz, h).start()
        t = NZ - 1 - k
        if t > zz:
            @pl.when(s == t)
            def _():
                if k > 0:
                    cd(a, zz, h).wait_recv()
                    add_into(mine(a, j), zd_b[a].at[j])
                cd(a, zz, h).start()
    def last(u):
        a, zz, h = u; j = jj(zz, h)
        @pl.when(s == zz)
        def _():
            if zz > 0: cu(a, zz, h).wait_recv()
            if zz < NZ - 1: cd(a, zz, h).wait_recv()
            t = mine(a, j)[...].astype(jnp.float32)
            if zz > 0: t = t + zu_b[a][j].astype(jnp.float32)
            if zz < NZ - 1: t = t + zd_b[a][j].astype(jnp.float32)
            outs[a][h] = t.astype(outs[a].dtype)
    for u in lines: load(*u).start()
    for u in units:
        c0(*u).start(); load(*u).start()
    n = len(units); nl = len(lines)
    per = max(1, -(-nl // n))
    L1 = LAGS[0] * n_arr; L2 = L1 + LAGS[1] * n_arr; L3 = L2 + LAGS[2] * n_arr; dl = LAGS[3] * n_arr
    for i in range(n + L3 + (NZ - 1) * dl):
        if i < n: stage0(units[i])
        if 0 <= i - L1 < n: stage1(units[i - L1])
        if 0 <= i - L2 < n: stage2(units[i - L2])
        for k in range(NZ - 1):
            for q in range(per * (i - LINE_LAG * k), per * (i - LINE_LAG * k) + per):
                if 0 <= q < nl:
                    if k == 0: load(*lines[q]).wait()
                    hop(lines[q], k)
        for k in range(NZ - 1):
            if 0 <= i - L3 - k * dl < n: hop(units[i - L3 - k * dl], k)
    for u in lines + units: last(u)
    for u in lines + units:
        a, zz, h = u
        if a < n_arr:
            c0(*u).wait_send(); ca(*u).wait_send(); cb(*u).wait_send()
        if zz > 0:
            @pl.when(s < zz)
            def _(): cu(*u).wait_send()
        if zz < NZ - 1:
            @pl.when(s > zz)
            def _(): cd(*u).wait_send()

def rs32(arrs, cid, out_dtype=jnp.float32, parts=4, line=()):
    n, nl = len(arrs), len(line)
    both = list(arrs) + list(line)
    if any(a.shape[1] % (parts * 16) for a in both): parts = 2
    ins = [a.reshape(((2, 2, 2) if i < n else ()) + (NZ, parts, a.shape[1] // parts, a.shape[2])) for i, a in enumerate(both)]
    hs = [i.shape[-2:] for i in ins]
    V = pltpu.VMEM; bt = jnp.bfloat16; m = NZ * parts
    sems = [pltpu.SemaphoreType.DMA((n + nl, m))] * 11
    outs = pl.pallas_call(
        functools.partial(rs_kernel, n, nl, parts),
        out_shape=[jax.ShapeDtypeStruct((parts,) + h, out_dtype) for h in hs],
        in_specs=[pl.BlockSpec(memory_space=pl.ANY)] * (n + nl),
        out_specs=[pl.BlockSpec(memory_space=pltpu.VMEM)] * (n + nl),
        scratch_shapes=[V((m,) + ((2, 2) if i < n else ()) + h, bt) for i, h in enumerate(hs)] + [V((m,) + h, bt) for h in hs] + [V((m,) + h, bt) for h in hs]
            + [V((m, 2, 2) + h, bt) for h in hs[:n]] + [V((m, 2) + h, bt) for h in hs[:n]] + [V((m,) + h, bt) for h in hs[:n]] + sems,
        compiler_params=pltpu.CompilerParams(collective_id=cid, has_side_effects=True, vmem_limit_bytes=64000 * 1024),
        name="scatter_all",
    )(*ins)
    return [o.reshape(a.shape[1], a.shape[2]) for o, a in zip(outs, both)]

def line_barrier(y, x, c, s):
    bar = pltpu.get_barrier_semaphore()
    @pl.when(s > 0)
    def _(): pl.semaphore_signal(bar, inc=1, device_id=dev(y, x, c, s - 1), device_id_type=MESH)
    @pl.when(s < NZ - 1)
    def _(): pl.semaphore_signal(bar, inc=1, device_id=dev(y, x, c, s + 1), device_id_type=MESH)
    pl.semaphore_wait(bar, jnp.where(s > 0, 1, 0) + jnp.where(s < NZ - 1, 1, 0))

def line_gather_kernel(parts, x_ref, o_ref, ss, rs):
    y, x, c, s = place()
    line_barrier(y, x, c, s)
    def cp(d, g, h):
        src = x_ref.at[h] if d == 0 else o_ref.at[s - d * g, h]
        k = 0 if g == 1 else 1
        return pltpu.make_async_remote_copy(src_ref=src, dst_ref=o_ref.at[s - d * g, h], send_sem=ss.at[k, d, h], recv_sem=rs.at[k, d, h],
            device_id=dev(y, x, c, s + g), device_id_type=MESH)
    def arrived(d, g, h):
        k = 0 if g == 1 else 1
        ref = o_ref.at[s - (d + 1) * g, h]
        return pltpu.make_async_remote_copy(src_ref=ref, dst_ref=ref, send_sem=ss.at[k, d, h], recv_sem=rs.at[k, d, h],
            device_id=dev(y, x, c, s + g), device_id_type=MESH)
    def sends(d, g): return (s >= d) & (s < NZ - 1) if g == 1 else (s + d <= NZ - 1) & (s > 0)
    def gets(d, g): return s >= d + 1 if g == 1 else s + d + 1 <= NZ - 1
    for d in range(NZ):
        for h in range(parts):
            for g in (1, -1):
                if d:
                    @pl.when(gets(d - 1, g))
                    def _(): arrived(d - 1, g, h).wait_recv()
                if d < NZ - 1:
                    @pl.when(sends(d, g))
                    def _(): cp(d, g, h).start()
        if d == 0: o_ref[s] = x_ref[...]
    for d in range(NZ - 1):
        for h in range(parts):
            for g in (1, -1):
                @pl.when(sends(d, g))
                def _(): cp(d, g, h).wait_send()

def line_gather(x, cid, parts=4):
    if not placed():
        return lax.all_gather(x, "shard", axis=0, tiled=True)
    R, C = x.shape
    sem = pltpu.SemaphoreType.DMA((2, NZ, parts))
    o = pl.pallas_call(functools.partial(line_gather_kernel, parts), out_shape=jax.ShapeDtypeStruct((NZ, parts, R // parts, C), x.dtype),
        in_specs=[pl.BlockSpec(memory_space=pltpu.VMEM)], out_specs=pl.BlockSpec(memory_space=pltpu.VMEM),
        scratch_shapes=[sem, sem], compiler_params=pltpu.CompilerParams(collective_id=cid, has_side_effects=True, vmem_limit_bytes=16 << 20),
        name="line_gather")(x.reshape(parts, R // parts, C))
    return o.reshape(NZ * R, C)

def line_scatter_kernel(parts, p_ref, o_ref, *scratch):
    for run in line_scatter_steps(parts, p_ref, o_ref, scratch): run()

LINE_PARTS = 4
LINE_STEPS = 3 * LINE_PARTS + NZ + 1

def line_scatter_steps(parts, p_ref, o_ref, scratch):
    acc, zu, zd, ss_u, rs_u, ss_d, rs_d = scratch
    y, x, c, s = place()
    def rc(src, dst, a, b, d):
        return pltpu.make_async_remote_copy(src_ref=src, dst_ref=dst, send_sem=a, recv_sem=b, device_id=d, device_id_type=MESH)
    def cu(zz, h, k):
        src = p_ref.at[zz, h] if k == 0 else acc.at[zz, h]
        return rc(src, zu.at[zz, h], ss_u.at[zz, h], rs_u.at[zz, h], dev(y, x, c, s + 1))
    def cd(zz, h, k):
        src = p_ref.at[zz, h] if k == 0 else acc.at[zz, h]
        return rc(src, zd.at[zz, h], ss_d.at[zz, h], rs_d.at[zz, h], dev(y, x, c, s - 1))
    st = 32
    def total(dst, refs):
        @pl.loop(0, dst.shape[0] // st)
        def _(i):
            r = pl.ds(i * st, st)
            t = refs[0][r, :].astype(jnp.float32)
            for f in refs[1:]: t = t + f[r, :].astype(jnp.float32)
            dst[r, :] = t.astype(dst.dtype)
    ups = [(zz, h) for zz in (3, 2, 1) for h in range(parts)]
    dns = [(zz, h) for zz in (0, 1, 2) for h in range(parts)]
    n = len(ups)
    def advance(i):
        if i == 0: line_barrier(y, x, c, s)
        for k in range(NZ - 1):
            if 0 <= i - 2 * k < n:
                zz, h = ups[i - 2 * k]
                if k < zz:
                    @pl.when(s == k)
                    def _():
                        if k:
                            cu(zz, h, k).wait_recv()
                            total(acc.at[zz, h], [p_ref.at[zz, h], zu.at[zz, h]])
                        cu(zz, h, k).start()
                zz, h = dns[i - 2 * k]
                if NZ - 1 - k > zz:
                    @pl.when(s == NZ - 1 - k)
                    def _():
                        if k:
                            cd(zz, h, k).wait_recv()
                            total(acc.at[zz, h], [p_ref.at[zz, h], zd.at[zz, h]])
                        cd(zz, h, k).start()
    def finish():
        for zz in range(NZ):
            @pl.when(s == zz)
            def _():
                for h in range(parts):
                    refs = [p_ref.at[zz, h]]
                    if zz > 0:
                        cu(zz, h, 1).wait_recv()
                        refs.append(zu.at[zz, h])
                    if zz < NZ - 1:
                        cd(zz, h, 1).wait_recv()
                        refs.append(zd.at[zz, h])
                    total(o_ref.at[h], refs)
        for zz, h in ups:
            @pl.when(s < zz)
            def _(): cu(zz, h, 1).wait_send()
        for zz, h in dns:
            @pl.when(s > zz)
            def _(): cd(zz, h, 1).wait_send()
    return [functools.partial(advance, i) for i in range(n + NZ)] + [finish]

def line_scatter_scratch(parts, rows, cols, dtype):
    sem = pltpu.SemaphoreType.DMA((NZ, parts))
    buf = pltpu.VMEM((NZ, parts, rows // parts, cols), dtype)
    return [buf, buf, buf, sem, sem, sem, sem]

def line_scatter(p, cid, parts=LINE_PARTS):
    if not placed():
        return lax.psum_scatter(p, "shard", scatter_dimension=0, tiled=True).astype(jnp.float32)
    R, C = p.shape[0] // NZ, p.shape[1]
    shape = (NZ, parts, R // parts, C)
    o = pl.pallas_call(functools.partial(line_scatter_kernel, parts), out_shape=jax.ShapeDtypeStruct(shape[1:], jnp.float32),
        in_specs=[pl.BlockSpec(memory_space=pltpu.VMEM)], out_specs=pl.BlockSpec(memory_space=pltpu.VMEM),
        scratch_shapes=line_scatter_scratch(parts, R, C, p.dtype), compiler_params=pltpu.CompilerParams(collective_id=cid, has_side_effects=True, vmem_limit_bytes=24 << 20),
        name="line_scatter")(p.reshape(shape))
    return o.reshape(R, C)


def dot(a, b, ca, cb):
    return lax.dot_general(a, b, (((ca,), (cb,)), ((), ())), preferred_element_type=jnp.float32)

def token_picks(meta, experts, slots, me):
    SB, WM = meta.shape
    bf, f32 = jnp.bfloat16, jnp.float32
    tri = (lax.broadcasted_iota(jnp.int32, (SB, SB), 1) < lax.broadcasted_iota(jnp.int32, (SB, SB), 0)).astype(bf)
    lane = lax.broadcasted_iota(jnp.int32, (SB, WM), 1)
    cnt = dot(tri, meta, 1, 0)
    metaf = meta.astype(f32)
    msk = jnp.sum(jnp.where(lane == me, metaf, 0.0), axis=-1, keepdims=True)
    pos = jnp.sum(jnp.where(lane == me, cnt, 0.0), axis=-1, keepdims=True)
    gate = jnp.sum(jnp.where((lane == me + experts) | (lane == me + 2 * experts), metaf, 0.0), axis=-1, keepdims=True)
    want = jnp.where(msk > 0.0, pos, -1.0).astype(jnp.int32)
    pick = (want == lax.broadcasted_iota(jnp.int32, (SB, slots), 1)).astype(bf)
    return pick, gate

def forward_kernel(experts, slots, SB, guest, *refs):
    if guest:
        cot_ref, x_ref, wg_hbm, wu_hbm, wd_hbm, cot_all, out_ref, rows_ref, ga_ref, ua_ref, wg, wu, wd, wsem = refs[:14]
    else:
        x_ref, wg_hbm, wu_hbm, wd_hbm, out_ref, rows_ref, ga_ref, ua_ref, wg, wu, wd, wsem = refs
    bf = jnp.bfloat16
    step = pl.program_id(0)
    if guest:
        start, stage_a, stage_b, stage_c, finish = ag_steps(1, 0, [cot_ref], [cot_all], refs[14:], True)
        pl.when(step == 0)(start)
        for at, stage, k in GUEST_AT: pl.when(step == at)(functools.partial(stage_a if stage == 0 else stage_b if stage == 1 else stage_c, k))
    nsub = x_ref.shape[0] // SB
    D = out_ref.shape[1]
    me = lax.axis_index(("expert", "shard"))
    loads = [pltpu.make_async_copy(h.at[0], v, wsem.at[i]) for i, (h, v) in enumerate(((wg_hbm, wg), (wu_hbm, wu), (wd_hbm, wd)))]
    @pl.when(step == 0)
    def _():
        for l in loads: l.start()
    picks, gates = [], []
    for i in range(nsub):
        r = pl.ds(i * SB, SB)
        pick, gate = token_picks(x_ref[r, D:], experts, slots, me)
        picks.append(pick); gates.append(gate)
        rows_ref[i * slots:(i + 1) * slots, :] = dot(pick, x_ref[r, :D], 0, 0).astype(bf)
    @pl.when(step == 0)
    def _():
        for l in loads: l.wait()
    ga = dot(rows_ref[...], wg[...], 1, 0)
    ua = dot(rows_ref[...], wu[...], 1, 0)
    ga_ref[...] = ga
    ua_ref[...] = ua
    hid = (ga * (1.0 / (1.0 + jnp.exp(-ga))) * ua).astype(bf)
    eo = dot(hid, wd[...], 1, 0).astype(bf)
    for i in range(nsub):
        r = pl.ds(i * SB, SB)
        tok = dot(picks[i], eo[i * slots:(i + 1) * slots, :], 1, 0)
        out_ref[r, :] = (gates[i] * tok).astype(bf)
    if guest: pl.when(step == pl.num_programs(0) - 1)(finish)

GUEST_AT = (
    (3, 0, 1), (3, 0, 2), (3, 1, 0), (5, 0, 3), (5, 0, 4), (5, 2, 0), (7, 1, 1), (7, 0, 5), (7, 0, 6), (8, 1, 2),
    (9, 2, 1), (10, 2, 2), (11, 1, 3), (11, 1, 4), (13, 2, 3), (13, 2, 4), (14, 1, 5), (14, 1, 6), (15, 2, 5), (15, 2, 6),
)

def backward_kernel(experts, slots, SB, block, meta_ref, cota_ref, cotb_ref, rows_ref, ga_ref, ua_ref, wg_hbm, wu_hbm, wd_hbm, gr_ref, dwg_hbm, dwu_hbm, dwd_hbm,
                  wg, wu, wd, dwg, dwu, dwd, gp, wsem, osem):
    bf = jnp.bfloat16
    step = pl.program_id(0)
    nsub = meta_ref.shape[0] // SB
    D = cota_ref.shape[1]
    WM = meta_ref.shape[1]
    na, nb = [r.shape[0] * block // meta_ref.shape[0] for r in (cota_ref, cotb_ref)]
    me = lax.axis_index(("expert", "shard"))
    loads = [pltpu.make_async_copy(h.at[0], v, wsem.at[i]) for i, (h, v) in enumerate(((wg_hbm, wg), (wu_hbm, wu), (wd_hbm, wd)))]
    @pl.when(step == 0)
    def _():
        for l in loads: l.start()
        for a in (dwg, dwu, dwd): a[...] = jnp.zeros_like(a)
    picks = []
    for i in range(nsub):
        r = pl.ds(i * SB, SB)
        pick, gate = token_picks(meta_ref[r, :], experts, slots, me)
        picks.append(pick)
        cot = []
        for b in range(i * SB // block, (i + 1) * SB // block):
            cot += [cota_ref[b * na:(b + 1) * na, :], cotb_ref[b * nb:(b + 1) * nb, :]]
        gcot = (gate * jnp.concatenate(cot, axis=0).astype(jnp.float32)).astype(bf)
        gp[i * slots:(i + 1) * slots, :] = dot(pick, gcot, 0, 0).astype(bf)
    @pl.when(step == 0)
    def _():
        for l in loads: l.wait()
    ga = ga_ref[...]
    ua = ua_ref[...]
    sig = 1.0 / (1.0 + jnp.exp(-ga))
    act = ga * sig
    hidf = act * ua
    hid = hidf.astype(bf)
    gh = dot(gp[...], wd[...], 1, 1)
    share = jnp.sum(gh * hid.astype(jnp.float32), axis=-1, keepdims=True)
    dga = (gh * ua * (sig * (1.0 + ga * (1.0 - sig)))).astype(bf)
    dua = (gh * act).astype(bf)
    dwd[...] += dot(hid, gp[...], 0, 0)
    grow = (dot(dga, wg[...], 1, 1) + dot(dua, wu[...], 1, 1)).astype(bf)
    dwg[...] += dot(rows_ref[...], dga, 0, 0)
    dwu[...] += dot(rows_ref[...], dua, 0, 0)
    lane = lax.broadcasted_iota(jnp.int32, (share.shape[0], WM), 1)
    high = share.astype(bf).astype(jnp.float32)
    tail = (jnp.where(lane == me, high, 0.0) + jnp.where(lane == me + experts, share - high, 0.0)).astype(bf)
    for i in range(nsub):
        r = pl.ds(i * SB, SB)
        q = slice(i * slots, (i + 1) * slots)
        gr_ref[r, :D] = dot(picks[i], grow[q, :], 1, 0).astype(bf)
        gr_ref[r, D:] = dot(picks[i], tail[q, :], 1, 0).astype(bf)
    @pl.when(step == pl.num_programs(0) - 1)
    def _():
        outs = [pltpu.make_async_copy(v, h.at[0], osem.at[i]) for i, (v, h) in enumerate(((dwg, dwg_hbm), (dwu, dwu_hbm), (dwd, dwd_hbm)))]
        for o in outs: o.start()
        for o in outs: o.wait()

def experts_forward(x_all, w_gate, w_up, w_down, experts, block, capacity, guest, cid, TB=512, SB=256):
    hosted = placed()
    T, C = x_all.shape; D, F = w_gate.shape[1:]
    slots = max(SB // block, 1) * capacity
    total = TB // SB * slots
    S = T // SB * slots
    any_ = pl.BlockSpec(memory_space=pl.ANY)
    V = pltpu.VMEM; bf = jnp.bfloat16; f32 = jnp.float32
    blk = lambda r, c: pl.BlockSpec((r, c), lambda i: (i, 0))
    g = guest.reshape(2, guest.shape[0] // 2, guest.shape[1])
    res = pl.pallas_call(
        functools.partial(forward_kernel, experts, slots, SB, hosted),
        grid=(T // TB,),
        out_shape=([jax.ShapeDtypeStruct((2, 2, 2, NZ) + g.shape, g.dtype)] if hosted else []) + [jax.ShapeDtypeStruct((T, D), bf), jax.ShapeDtypeStruct((S, D), bf), jax.ShapeDtypeStruct((S, F), f32), jax.ShapeDtypeStruct((S, F), f32)],
        in_specs=([pl.BlockSpec(memory_space=pltpu.VMEM)] if hosted else []) + [blk(TB, C), any_, any_, any_],
        out_specs=([any_] if hosted else []) + [blk(TB, D), blk(total, D), blk(total, F), blk(total, F)],
        scratch_shapes=[V((D, F), bf), V((D, F), bf), V((F, D), bf), pltpu.SemaphoreType.DMA((3,))] + (ag_sems(1) if hosted else []),
        compiler_params=pltpu.CompilerParams(dimension_semantics=("arbitrary",), vmem_limit_bytes=65000 * 1024,
            **(dict(collective_id=cid, has_side_effects=True) if hosted else {})),
        cost_estimate=pl.CostEstimate(flops=48_000_000_000, bytes_accessed=130_000_000, transcendentals=0),
        name="experts_forward",
    )(*([g] if hosted else []), x_all, w_gate, w_up, w_down)
    if hosted: return res[1:], res[0].reshape(-1, guest.shape[1])
    return res, lax.all_gather(guest, BOTH, axis=0, tiled=True)

def experts_backward(x_all, cot_a, cot_b, rows, ga, ua, w_gate, w_up, w_down, experts, block, capacity, TB=512, SB=256):
    T, C = x_all.shape; D, F = w_gate.shape[1:]
    slots = max(SB // block, 1) * capacity
    total = TB // SB * slots
    WM = C - D
    any_ = pl.BlockSpec(memory_space=pl.ANY)
    V = pltpu.VMEM; bf = jnp.bfloat16; f32 = jnp.float32
    blk = lambda r, c: pl.BlockSpec((r, c), lambda i: (i, 0))
    meta = pl.BlockSpec((TB, WM), lambda i: (i, D // WM)) if D % WM == 0 else blk(TB, WM)
    meta_in = x_all if D % WM == 0 else x_all[:, D:]
    return pl.pallas_call(
        functools.partial(backward_kernel, experts, slots, SB, block),
        grid=(T // TB,),
        out_shape=[jax.ShapeDtypeStruct((T, C), bf), jax.ShapeDtypeStruct(w_gate.shape, f32), jax.ShapeDtypeStruct(w_up.shape, f32), jax.ShapeDtypeStruct(w_down.shape, f32)],
        in_specs=[meta, blk(cot_a.shape[0] * TB // T, D), blk(cot_b.shape[0] * TB // T, D), blk(total, D), blk(total, F), blk(total, F), any_, any_, any_],
        out_specs=[blk(TB, C), any_, any_, any_],
        scratch_shapes=[V((D, F), bf), V((D, F), bf), V((F, D), bf), V((D, F), f32), V((D, F), f32), V((F, D), f32), V((total, D), bf), pltpu.SemaphoreType.DMA((3,)), pltpu.SemaphoreType.DMA((3,))],
        compiler_params=pltpu.CompilerParams(dimension_semantics=("arbitrary",), vmem_limit_bytes=65000 * 1024),
        cost_estimate=pl.CostEstimate(flops=85_000_000_000, bytes_accessed=150_000_000, transcendentals=0),
        name="experts_backward",
    )(meta_in, cot_a, cot_b, rows, ga, ua, w_gate, w_up, w_down)


def rope_tables(seq_len):
    half = HD // 2
    frequency = theta_base ** (-2.0 * jnp.arange(half, dtype=jnp.float32) / HD)
    angles = jnp.arange(seq_len, dtype=jnp.float32)[:, None] * frequency[None, :]
    return jnp.concatenate([jnp.cos(angles)] * 2, axis=-1), jnp.concatenate([-jnp.sin(angles), jnp.sin(angles)], axis=-1)

def turn(u, cos, sin):
    return u * cos + pltpu.roll(u, HD // 2, 1) * sin

def scale_of(u):
    return lax.rsqrt(jnp.mean(u * u, axis=-1, keepdims=True) + epsilon)

def attention_forward_kernel(group, n_ref, wq_ref, wk_ref, wv_ref, gq_ref, gk_ref, cos_ref, sin_ref, u_ref, ku_ref, ql_ref, kl_ref, vl_ref, mix_ref, k_all):
    bf, f32 = jnp.bfloat16, jnp.float32
    rows, seq = ql_ref.shape[0], kl_ref.shape[0]
    first = lax.axis_index("shard") * rows
    own = pl.ds(first, rows)
    k_all[...] = dot(n_ref[...], wk_ref[...], 1, 0)
    ku_ref[...] = k_all[own, :]
    k = k_all[...]
    kl_ref[...] = turn(k * scale_of(k) * gk_ref[...], cos_ref[...], sin_ref[...]).astype(bf)
    vl_ref[...] = dot(n_ref[...], wv_ref[...], 1, 0).astype(bf)
    u_ref[...] = dot(n_ref[own, :], wq_ref[...], 1, 0)
    cos, sin = cos_ref[own, :], sin_ref[own, :]
    allowed = lax.broadcasted_iota(jnp.int32, (rows, seq), 1) <= first + lax.broadcasted_iota(jnp.int32, (rows, seq), 0)
    for j in range(group):
        cols = slice(j * HD, (j + 1) * HD)
        u = u_ref[:, cols]
        ql = (turn(u * scale_of(u) * gq_ref[...], cos, sin) * HD ** (-0.5)).astype(bf)
        ql_ref[:, cols] = ql
        scores = dot(ql, kl_ref[...], 1, 1)
        raised = jnp.where(allowed, jnp.exp(scores), 0.0)
        probs = (raised * (1.0 / jnp.sum(raised, axis=-1, keepdims=True))).astype(bf)
        mix_ref[:, cols] = dot(probs, vl_ref[...], 1, 0).astype(bf)

def attention_forward(normed_seq, wqkv, rows, gq, gk, cos, sin):
    seq, width = normed_seq.shape
    group = HQ // HK
    bf, f32 = jnp.bfloat16, jnp.float32
    whole = lambda a: pl.BlockSpec(a.shape, lambda i: (0, 0))
    gq, gk = gq[None, :], gk[None, :]
    qb = pl.BlockSpec((rows, group * HD), lambda i: (0, i)); kb = pl.BlockSpec((seq, HD), lambda i: (0, i))
    return pl.pallas_call(
        functools.partial(attention_forward_kernel, group),
        grid=(HK,),
        out_shape=[jax.ShapeDtypeStruct((rows, HQ * HD), f32), jax.ShapeDtypeStruct((rows, HK * HD), f32), jax.ShapeDtypeStruct((rows, HQ * HD), bf),
            jax.ShapeDtypeStruct((seq, HK * HD), bf), jax.ShapeDtypeStruct((seq, HK * HD), bf), jax.ShapeDtypeStruct((rows, HQ * HD), bf)],
        in_specs=[whole(normed_seq), pl.BlockSpec((width, group * HD), lambda i: (0, i)), pl.BlockSpec((width, HD), lambda i: (0, HQ + i)), pl.BlockSpec((width, HD), lambda i: (0, HQ + HK + i)),
            whole(gq), whole(gk), whole(cos), whole(sin)],
        out_specs=[qb, pl.BlockSpec((rows, HD), lambda i: (0, i)), qb, kb, kb, qb],
        scratch_shapes=[pltpu.VMEM((seq, HD), f32)],
        compiler_params=pltpu.CompilerParams(dimension_semantics=("arbitrary",), vmem_limit_bytes=56 << 20),
        cost_estimate=pl.CostEstimate(flops=13_000_000_000, bytes_accessed=45_000_000, transcendentals=8_400_000),
        name="attention_forward",
    )(normed_seq, wqkv, wqkv, wqkv, gq, gk, cos, sin)

def attention_backward_kernel(group, guest, *refs):
    if guest:
        p_ref, u_ref, ql_ref, kl_ref, vl_ref, ga_ref, wo_ref, gq_ref, cos_ref, sin_ref, po_ref, gu_ref, gk_ref, gv_ref, gg_ref, gk_acc, gv_acc = refs[:17]
        runs = line_scatter_steps(LINE_PARTS, p_ref, po_ref, refs[17:])
        slots = HK * group
        at = {i * slots // (LINE_STEPS - 1): run for i, run in enumerate(runs[:-1])}
    else:
        u_ref, ql_ref, kl_ref, vl_ref, ga_ref, wo_ref, gq_ref, cos_ref, sin_ref, gu_ref, gk_ref, gv_ref, gg_ref, gk_acc, gv_acc = refs
        at = {}
    step = pl.program_id(0)
    bf, f32 = jnp.bfloat16, jnp.float32
    gm_all = dot(ga_ref[...], wo_ref[...], 1, 1).astype(bf)
    rows, seq = ql_ref.shape[0], kl_ref.shape[0]
    first = lax.axis_index("shard") * rows
    cos, sin = cos_ref[pl.ds(first, rows), :], sin_ref[pl.ds(first, rows), :]
    allowed = lax.broadcasted_iota(jnp.int32, (rows, seq), 1) <= first + lax.broadcasted_iota(jnp.int32, (rows, seq), 0)
    gain_grad = jnp.zeros((1, HD), f32)
    for j in range(group):
        for i in range(HK):
            if i * group + j in at: pl.when(step == i)(at[i * group + j])
        cols = slice(j * HD, (j + 1) * HD)
        ql, gm = ql_ref[:, cols], gm_all[:, cols]
        raised = jnp.where(allowed, jnp.exp(dot(ql, kl_ref[...], 1, 1)), 0.0)
        probs = raised * (1.0 / jnp.sum(raised, axis=-1, keepdims=True))
        gp = dot(gm, vl_ref[...], 1, 1)
        gs = (probs * (gp - jnp.sum(probs * gp, axis=-1, keepdims=True))).astype(bf)
        gv = dot(probs.astype(bf), gm, 0, 0)
        gk = dot(gs, ql, 0, 0)
        if j == 0:
            gv_acc[...] = gv
            gk_acc[...] = gk
        else:
            gv_acc[...] += gv
            gk_acc[...] += gk
        m = dot(gs, kl_ref[...], 1, 0) * HD ** (-0.5)
        m = m * cos + pltpu.roll(m * sin, HD // 2, 1)
        u = u_ref[:, cols]
        r = scale_of(u)
        gain_grad = gain_grad + jnp.sum(m * u * r, axis=0, keepdims=True)
        mg = m * gq_ref[...]
        gu_ref[:, cols] = (r * mg - u * (r * r * r) * jnp.mean(mg * u, axis=-1, keepdims=True)).astype(bf)
    gk_ref[...] = gk_acc[...].astype(bf)
    gv_ref[...] = gv_acc[...].astype(bf)
    gg_ref[0] = jnp.broadcast_to(gain_grad, (8, HD))
    if guest: pl.when(step == HK - 1)(runs[-1])

def attention_backward(q_proj, q_low, k_low, v_low, grad_attn, w_out, gq, cos, sin, guest, cid):
    rows, seq = q_low.shape[0], k_low.shape[0]
    group = HQ // HK
    bf, f32 = jnp.bfloat16, jnp.float32
    gq = gq[None, :]
    whole = lambda a: pl.BlockSpec(a.shape, lambda i: (0, 0))
    qb = pl.BlockSpec((rows, group * HD), lambda i: (0, i)); kb = pl.BlockSpec((seq, HD), lambda i: (0, i))
    hosted = placed()
    R, C = guest.shape[0] // lax.axis_size("shard"), guest.shape[1]
    shape = (NZ, LINE_PARTS, R // LINE_PARTS, C)
    vm = pl.BlockSpec(memory_space=pltpu.VMEM)
    *summed, grad_q, grad_k, grad_v, gain = pl.pallas_call(
        functools.partial(attention_backward_kernel, group, hosted),
        grid=(HK,),
        out_shape=([jax.ShapeDtypeStruct(shape[1:], f32)] if hosted else []) + [jax.ShapeDtypeStruct(q_low.shape, bf), jax.ShapeDtypeStruct(k_low.shape, bf), jax.ShapeDtypeStruct(k_low.shape, bf), jax.ShapeDtypeStruct((HK, 8, HD), f32)],
        in_specs=([vm] if hosted else []) + [qb, qb, kb, kb, whole(grad_attn), pl.BlockSpec((group * HD, w_out.shape[1]), lambda i: (i, 0)), whole(gq), whole(cos), whole(sin)],
        out_specs=([vm] if hosted else []) + [qb, kb, kb, pl.BlockSpec((1, 8, HD), lambda i: (i, 0, 0))],
        scratch_shapes=[pltpu.VMEM((seq, HD), f32), pltpu.VMEM((seq, HD), f32)] + (line_scatter_scratch(LINE_PARTS, R, C, bf) if hosted else []),
        compiler_params=pltpu.CompilerParams(dimension_semantics=("arbitrary",), vmem_limit_bytes=60 << 20,
            **(dict(collective_id=cid, has_side_effects=True) if hosted else {})),
        cost_estimate=pl.CostEstimate(flops=15_000_000_000, bytes_accessed=20_000_000, transcendentals=8_400_000),
        name="attention_backward",
    )(*([guest.reshape(shape)] if hosted else []), q_proj, q_low, k_low, v_low, grad_attn, w_out, gq, cos, sin)
    if hosted: total = summed[0].reshape(R, C)
    else: total = lax.psum_scatter(guest, "shard", scatter_dimension=0, tiled=True).astype(f32)
    return total, grad_q, jnp.concatenate([grad_k, grad_v], axis=1), jnp.sum(gain[:, 0], axis=0)

HQ = 32
HK = 4
HD = 128
epsilon = 1e-06
theta_base = 1000000.0
BOTH = ("expert", "shard")


def matmul(left, right):
    return jnp.dot(left, right, preferred_element_type=jnp.float32)


def matmul_tn(left, right):
    return lax.dot_general(
        left, right, (((0,), (0,)), ((), ())), preferred_element_type=jnp.float32
    )


def matmul_nt(left, right):
    return lax.dot_general(
        left, right, (((1,), (1,)), ((), ())), preferred_element_type=jnp.float32
    )


def norm_rows(values, gain_vec):
    return (
        values * lax.rsqrt(jnp.mean(values * values, axis=-1, keepdims=True) + epsilon) * gain_vec
    )


def norm_back(values, gain_vec, upstream):
    scaling = lax.rsqrt(jnp.mean(values * values, axis=-1, keepdims=True) + epsilon)
    gain_grad = jnp.sum(upstream * values * scaling, axis=0)
    weighted = upstream * gain_vec
    inner_sum = jnp.mean(weighted * values, axis=-1, keepdims=True)
    return (scaling * weighted - values * (scaling * scaling * scaling) * inner_sum, gain_grad)


def rotary(values, positions):
    head_width = values.shape[-1]
    half_width = head_width // 2
    frequency = theta_base ** (-2.0 * jnp.arange(half_width, dtype=jnp.float32) / head_width)
    angles = positions.astype(jnp.float32)[:, None] * frequency[None, :]
    cosine = jnp.concatenate([jnp.cos(angles), jnp.cos(angles)], axis=-1)[:, None, :]
    sine_part = jnp.concatenate([jnp.sin(angles), jnp.sin(angles)], axis=-1)[:, None, :]
    turned = jnp.concatenate([-values[..., half_width:], values[..., :half_width]], axis=-1)
    return values * cosine + turned * sine_part


def head_prep(projected, gain_vec, positions, head_count, factor):
    shaped = projected.reshape(projected.shape[0], head_count, projected.shape[1] // head_count)
    return rotary(norm_rows(shaped, gain_vec), positions) * factor


def gather_all(arrays, cid, line=()):
    if placed():
        return [o.reshape(-1, o.shape[-1]) for o in ag32(arrays, cid, line)]
    return [lax.all_gather(a, BOTH, axis=0, tiled=True) for a in arrays] + [
        lax.all_gather(a, "shard", axis=0, tiled=True) for a in line
    ]


def scatter_all(arrays, cid, out_dtype=jnp.float32, line=()):
    if placed():
        return rs32(
            [a.reshape(32, -1, a.shape[-1]) for a in arrays], cid, out_dtype, line=[a.reshape(NZ, -1, a.shape[-1]) for a in line]
        )
    return [lax.psum_scatter(a, BOTH, scatter_dimension=0, tiled=True).astype(out_dtype) for a in arrays] + [
        lax.psum_scatter(a, "shard", scatter_dimension=0, tiled=True).astype(out_dtype) for a in line
    ]


def per_device(
    hidden_in,
    g_attn,
    w_query,
    w_key,
    w_value,
    g_query,
    g_key,
    w_out,
    g_ffn,
    w_router,
    w_gate,
    w_up,
    w_down,
    routes,
    cotangent,
):
    bf, f32 = jnp.bfloat16, jnp.float32
    tok_rows, model_width = hidden_in.shape
    top_count = routes.shape[1]
    devices = lax.axis_size(BOTH)
    expert_count = devices * w_gate.shape[0]
    capacity = 2 * tok_rows * top_count // expert_count
    shard_count = lax.axis_size("shard")
    shard_pos = lax.axis_index("shard")
    seq_len = tok_rows * shard_count
    q_cols, kv_cols = HQ * HD, HK * HD

    pieces = [w_router.reshape(-1), g_attn, g_ffn, g_query, g_key]
    sizes = [p.shape[0] for p in pieces]
    used = sum(sizes)
    small_rows = -(-used // (64 * 128)) * 64
    small = jnp.concatenate(pieces + [jnp.zeros((small_rows * 128 - used,), bf)]).reshape(small_rows, 128)
    wqkv = jnp.concatenate([w_query, w_key, w_value], axis=1)
    wqkv_full, small_all, wo_full, hidden_seq = gather_all([wqkv, small, w_out], 1, [hidden_in])
    small_all = small_all.reshape(devices, small_rows * 128)
    starts = [sum(sizes[:i]) for i in range(5)]
    wr_full, attn_gain, ffn_gain, query_gain, key_gain = [small_all[:, o : o + n].reshape(-1) for o, n in zip(starts, sizes)]
    wr_full = wr_full.reshape(model_width, expert_count)
    attn_gain, ffn_gain, query_gain, key_gain = [g.astype(f32) for g in (attn_gain, ffn_gain, query_gain, key_gain)]
    first = tok_rows // 2
    cot_first, wo_full = lax.optimization_barrier((cotangent[:first], wo_full))
    cot_a = lax.all_gather(cot_first, BOTH, axis=0, tiled=True)

    inputs_f = hidden_in.astype(f32)
    normed_low = norm_rows(inputs_f, attn_gain).astype(bf)
    normed_seq = norm_rows(hidden_seq.astype(f32), attn_gain).astype(bf)
    cosine, sine = rope_tables(seq_len)
    q_proj, k_proj, q_low, k_low, v_low, mix_low = attention_forward(
        normed_seq, wqkv_full, tok_rows, query_gain, key_gain, cosine, sine
    )
    residual = inputs_f + matmul(mix_low, wo_full)
    ffn_low = norm_rows(residual, ffn_gain).astype(bf)

    logits = matmul(ffn_low, wr_full)
    expert_ids = jnp.arange(expert_count, dtype=jnp.int32)
    chosen = jnp.any(routes[:, :, None] == expert_ids[None, None, :], axis=1)
    raised_gate = jnp.where(chosen, jnp.exp(logits), 0.0)
    gates = raised_gate / jnp.sum(raised_gate, axis=-1, keepdims=True)
    gate_high = lax.reduce_precision(gates, 8, 7)
    gate_low = gates - gate_high
    extra = -(-3 * expert_count // 128) * 128
    payload = jnp.concatenate(
        [
            ffn_low,
            chosen.astype(bf),
            gate_high.astype(bf),
            gate_low.astype(bf),
            jnp.zeros((tok_rows, extra - 3 * expert_count), bf),
        ],
        axis=1,
    )
    (payload_all,) = gather_all([payload], 3)
    (out_part, rows, gate_act, up_act), cot_b = experts_forward(
        payload_all, w_gate, w_up, w_down, expert_count, tok_rows, capacity, cotangent[first:], 2
    )
    moe_out = lax.psum_scatter(out_part, "expert", scatter_dimension=0, tiled=True)
    grad_part, grad_wgate, grad_wup, grad_wdown = experts_backward(
        payload_all, cot_a, cot_b, rows, gate_act, up_act, w_gate, w_up, w_down, expert_count, tok_rows, capacity
    )
    (grad_sum,) = scatter_all([grad_part], 4)
    grad_sum, moe_out = lax.optimization_barrier((grad_sum, moe_out))
    upstream = cotangent.astype(f32)
    grad_ffn = grad_sum[:, :model_width]
    grad_shares = (
        grad_sum[:, model_width : model_width + expert_count]
        + grad_sum[:, model_width + expert_count : model_width + 2 * expert_count]
    )
    grad_logits = (grad_shares - gates * jnp.sum(grad_shares, axis=-1, keepdims=True)).astype(bf)
    grad_wrouter = matmul_tn(ffn_low, grad_logits)
    grad_ffn = grad_ffn + matmul_nt(grad_logits, wr_full)
    grad_second, grad_ffn_gain = norm_back(residual, ffn_gain, grad_ffn)
    grad_residual = upstream + grad_second
    grad_attn_low = grad_residual.astype(bf)
    grad_wout = matmul_tn(mix_low, grad_attn_low).astype(bf)
    grad_attn_low, grad_wout = lax.optimization_barrier((grad_attn_low, grad_wout))
    out_grad = lax.psum_scatter(grad_wout, "expert", scatter_dimension=0, tiled=True)

    moe_parts = moe_out.reshape(shard_count, 2, tok_rows // 2, model_width)
    moe_a, moe_b = [moe_parts[:, i].reshape(-1, model_width) for i in range(2)]
    moe_a, grad_q_low, grad_kv, grad_query_gain = attention_backward(
        q_proj, q_low, k_low, v_low, grad_attn_low, wo_full, query_gain, cosine, sine, moe_a, 5
    )
    grad_kv = line_scatter(grad_kv, 6)
    own_rows = shard_pos * tok_rows
    positions = own_rows + jnp.arange(tok_rows, dtype=jnp.int32)
    _, k_pull = jax.vjp(
        lambda projected, gain_vec: head_prep(projected, gain_vec, positions, HK, 1.0), k_proj, key_gain
    )
    grad_k_proj, grad_key_gain = k_pull(grad_kv[:, :kv_cols].reshape(tok_rows, HK, HD))
    grad_qkv_low = jnp.concatenate(
        [grad_q_low, grad_k_proj.astype(bf), grad_kv[:, kv_cols:].astype(bf)], axis=1
    )
    grad_wqkv = matmul_tn(normed_low, grad_qkv_low).astype(bf)
    grad_normed = matmul_nt(grad_qkv_low, wqkv_full)
    grad_front, grad_attn_gain = norm_back(inputs_f, attn_gain, grad_normed)
    grad_input = (grad_residual + grad_front).astype(bf)

    grads = [grad_wrouter, grad_attn_gain, grad_ffn_gain, grad_query_gain, grad_key_gain]
    packed = jnp.concatenate(
        [g.astype(bf).reshape(devices, -1) for g in grads] + [jnp.zeros((devices, small_rows * 128 - used), bf)], axis=1
    ).reshape(devices * small_rows, 128)
    grad_wqkv, out_grad = lax.optimization_barrier((grad_wqkv, out_grad))
    out_grad = lax.psum_scatter(out_grad, "shard", scatter_dimension=0, tiled=True).astype(f32)
    qkv_grad, small_grad, moe_b = scatter_all([grad_wqkv, packed], 8, line=[moe_b])
    block_out = (residual + jnp.concatenate([moe_a, moe_b], axis=0)).astype(bf)
    small_grad = small_grad.reshape(-1)
    router_g, attn_g, ffn_g, query_g, key_g = [small_grad[o : o + n] for o, n in zip(starts, sizes)]
    return (
        block_out,
        grad_input,
        attn_g,
        qkv_grad[:, :q_cols],
        qkv_grad[:, q_cols : q_cols + kv_cols],
        qkv_grad[:, q_cols + kv_cols :],
        query_g,
        key_g,
        out_grad,
        ffn_g,
        router_g.reshape(w_router.shape),
        grad_wgate,
        grad_wup,
        grad_wdown,
    )


def solution(mesh):
    row = P(BOTH, None)
    vec = P(BOTH)
    cube = P(BOTH, None, None)
    in_specs = (row, vec, row, row, row, vec, vec, row, vec, row, cube, cube, cube, row, row)
    out_specs = (row, row, vec, row, row, row, vec, vec, row, vec, row, cube, cube, cube)
    return jax.shard_map(
        per_device, mesh=mesh, in_specs=in_specs, out_specs=out_specs, check_vma=False
    )
```
